16 devices in a mesh: dp: 2 (over y, z), sp: 8 (over x, core).
Axes of the slice: x: 4, y: 2, z: 1, core: 2. Of those that a mesh axis runs over, the one named last changes fastest.
The devices are a block of a 4x4x8 slice.
Arguments:
- hidden: bfloat16 [256, 1280], P(('dp', 'sp')), parts along dimension 0
- seg_ids: int32 [256], P(('dp', 'sp')), parts along dimension 0
- positions: int32 [256], P(('dp', 'sp')), parts along dimension 0
- prefix_lat: bfloat16 [8192, 576], P(('dp', 'sp')), parts along dimension 0
- prefix_seg: int32 [8192], P(('dp', 'sp')), parts along dimension 0
- w_dq: bfloat16 [1280, 384], replicated
- gain_q: bfloat16 [384], replicated
- w_uq: bfloat16 [384, 6144], replicated
- w_dkv: bfloat16 [1280, 576], replicated
- gain_kv: bfloat16 [512], replicated
- w_ukv: bfloat16 [512, 8192], replicated
- w_o: bfloat16 [4096, 1280], replicated
Outputs:
- output: bfloat16 [256, 1280], P(('dp', 'sp')), parts along dimension 0
There are 2 independent parts. The reference program is written for one: setup_inputs(seed, part) draws one part's arguments, and reference() takes and returns one part's arrays. A program takes and returns all parts, laid end to end along the dimension named above; an argument that names none is the same for every part.
All inputs are finite; a program needn't handle non-finite values.
Results may differ from the reference program's by a relative error of at most 0.00489144.
Values are sent between devices in bfloat16 or wider.
A program may use at most 768 MiB of HBM per device.

```python
import jax
import jax.numpy as jnp
from jax import lax

D = 1280
HEADS = 32
QLAT = 384
TOKENS = 128
PREFIX = 4096
PROMPTS = 2
KV_LAT = 512
ROPE_DIM = 64
NOPE_DIM = 128
V_DIM = 128
QK_DIM = NOPE_DIM + ROPE_DIM
KV_HEAD = NOPE_DIM + V_DIM
LAT_DIM = KV_LAT + ROPE_DIM
QBLK = min(TOKENS, max(1, 2048 // HEADS))
OUT_GAIN = 0.6 * ((2 * PREFIX + TOKENS) // (2 * PROMPTS)) ** 0.5
EPS = 1e-6
ROPE_BASE = 10000.0
NEG_BIG = -1e30


def packed_layout(key, total):
    cuts = jnp.sort(jax.random.permutation(key, total - 1)[: PROMPTS - 1] + 1).astype(jnp.int32)
    row_idx = jnp.arange(total, dtype=jnp.int32)
    prompt_ids = jnp.sum((row_idx[:, None] >= cuts[None, :]).astype(jnp.int32), axis=1)
    starts = jnp.concatenate([jnp.zeros((1,), jnp.int32), cuts])
    ends = jnp.concatenate([cuts, jnp.full((1,), total, jnp.int32)])
    offsets = row_idx - starts[prompt_ids]
    return prompt_ids, offsets, ends - starts


def setup_inputs(seed: int = 0, part: int = 0) -> dict:
    part_key = jax.random.fold_in(jax.random.key(seed), part)
    key_hid, key_new, key_pre, key_lat = jax.random.split(part_key, 4)
    weight_keys = jax.random.split(jax.random.key(seed + 1), 7)
    new_layout = packed_layout(key_new, TOKENS)
    pre_layout = packed_layout(key_pre, PREFIX)
    seg_ids = new_layout[0]
    positions = pre_layout[2][seg_ids] + new_layout[1]
    hidden = jax.random.normal(key_hid, (TOKENS, D), jnp.float32)
    prefix_lat = jax.random.normal(key_lat, (PREFIX, LAT_DIM), jnp.float32)
    w_dq = jax.random.normal(weight_keys[0], (D, QLAT), jnp.float32) * D ** -0.5
    gain_q = 1.0 + 0.3 * jax.random.normal(weight_keys[1], (QLAT,), jnp.float32)
    w_uq = jax.random.normal(weight_keys[2], (QLAT, HEADS * QK_DIM), jnp.float32) * QLAT ** -0.5
    w_dkv = jax.random.normal(weight_keys[3], (D, LAT_DIM), jnp.float32) * D ** -0.5
    gain_kv = 1.0 + 0.3 * jax.random.normal(weight_keys[4], (KV_LAT,), jnp.float32)
    w_ukv = jax.random.normal(weight_keys[5], (KV_LAT, HEADS * KV_HEAD), jnp.float32) * KV_LAT ** -0.5
    w_o = jax.random.normal(weight_keys[6], (HEADS * V_DIM, D), jnp.float32) * (HEADS * V_DIM) ** -0.5 * OUT_GAIN
    return {
        "hidden": hidden.astype(jnp.bfloat16),
        "seg_ids": seg_ids,
        "positions": positions,
        "prefix_lat": prefix_lat.astype(jnp.bfloat16),
        "prefix_seg": pre_layout[0],
        "w_dq": w_dq.astype(jnp.bfloat16),
        "gain_q": gain_q.astype(jnp.bfloat16),
        "w_uq": w_uq.astype(jnp.bfloat16),
        "w_dkv": w_dkv.astype(jnp.bfloat16),
        "gain_kv": gain_kv.astype(jnp.bfloat16),
        "w_ukv": w_ukv.astype(jnp.bfloat16),
        "w_o": w_o.astype(jnp.bfloat16),
    }


def rms_norm(values, gain):
    inv_rms = lax.rsqrt(jnp.mean(values * values, axis=-1, keepdims=True) + EPS)
    return values * inv_rms * gain.astype(jnp.float32)


def rope_tables(positions):
    half_dim = ROPE_DIM // 2
    inv_freq = ROPE_BASE ** (-jnp.arange(half_dim, dtype=jnp.float32) / half_dim)
    angles = positions.astype(jnp.float32)[:, None] * inv_freq[None, :]
    return jnp.cos(angles), jnp.sin(angles)


def rope_apply(values, cos_t, sin_t):
    half_dim = ROPE_DIM // 2
    lower_half = values[..., :half_dim]
    upper_half = values[..., half_dim:]
    return jnp.concatenate([lower_half * cos_t - upper_half * sin_t, upper_half * cos_t + lower_half * sin_t], axis=-1)


def reference(hidden, seg_ids, positions, prefix_lat, prefix_seg, w_dq, gain_q, w_uq, w_dkv, gain_kv, w_ukv, w_o):
    q_lat = rms_norm(jnp.dot(hidden, w_dq, preferred_element_type=jnp.float32), gain_q).astype(jnp.bfloat16)
    kv_down = jnp.dot(hidden, w_dkv, preferred_element_type=jnp.float32)
    cos_t, sin_t = rope_tables(positions)
    kv_lat = rms_norm(kv_down[:, :KV_LAT], gain_kv).astype(jnp.bfloat16)
    key_rope_new = rope_apply(kv_down[:, KV_LAT:], cos_t, sin_t).astype(jnp.bfloat16)
    key_lat = jnp.concatenate([prefix_lat, jnp.concatenate([kv_lat, key_rope_new], axis=1)], axis=0)
    key_seg = jnp.concatenate([prefix_seg, seg_ids])
    key_pos = jnp.concatenate([jnp.full((PREFIX,), -1, jnp.int32), positions])
    q_full = jnp.dot(q_lat, w_uq, preferred_element_type=jnp.float32).reshape(TOKENS, HEADS, QK_DIM)
    q_nope = q_full[..., :NOPE_DIM].astype(jnp.bfloat16)
    q_rope = rope_apply(q_full[..., NOPE_DIM:], cos_t[:, None, :], sin_t[:, None, :]).astype(jnp.bfloat16)
    kv_up = jnp.dot(key_lat[:, :KV_LAT], w_ukv, preferred_element_type=jnp.float32).astype(jnp.bfloat16)
    kv_up = kv_up.reshape(PREFIX + TOKENS, HEADS, KV_HEAD)
    k_nope = kv_up[..., :NOPE_DIM].astype(jnp.float32)
    v_heads = kv_up[..., NOPE_DIM:].astype(jnp.float32)
    k_rope = key_lat[:, KV_LAT:].astype(jnp.float32)
    n_blocks = TOKENS // QBLK

    def attend(block):
        qn_blk, qr_blk, seg_blk, pos_blk = block
        scores = jnp.einsum("qhd,khd->hqk", qn_blk.astype(jnp.float32), k_nope)
        scores = scores + jnp.einsum("qhd,kd->hqk", qr_blk.astype(jnp.float32), k_rope)
        allowed = (seg_blk[:, None] == key_seg[None, :]) & (key_pos[None, :] <= pos_blk[:, None])
        scores = jnp.where(allowed[None], scores * QK_DIM ** -0.5, NEG_BIG)
        probs = jax.nn.softmax(scores, axis=-1).astype(jnp.bfloat16).astype(jnp.float32)
        return jnp.einsum("hqk,khd->qhd", probs, v_heads).astype(jnp.bfloat16)

    heads_out = lax.map(attend, (q_nope.reshape(n_blocks, QBLK, HEADS, NOPE_DIM), q_rope.reshape(n_blocks, QBLK, HEADS, ROPE_DIM), seg_ids.reshape(n_blocks, QBLK), positions.reshape(n_blocks, QBLK)))
    return jnp.dot(heads_out.reshape(TOKENS, HEADS * V_DIM), w_o, preferred_element_type=jnp.float32).astype(jnp.bfloat16)
```

```python
import functools
import math

import jax
import jax.numpy as jnp
import numpy as np
from jax import lax
from jax.experimental import pallas as pl
from jax.experimental.pallas import tpu as pltpu
from jax.sharding import PartitionSpec as P

ROPE_DIM = 64
HALF = ROPE_DIM // 2
NOPE_DIM = 128
V_DIM = 128
QK_DIM = NOPE_DIM + ROPE_DIM
KV_HEAD = NOPE_DIM + V_DIM
CORES = 2
EPS = 1e-6
ROPE_BASE = 10000.0
NEG_BIG = -1e30
EXP_SCALE = QK_DIM ** -0.5 * math.log2(math.e)
LANES = 128
N_CHUNK = 256
KV_LOADS = 4

F32 = jnp.float32
BF16 = jnp.bfloat16


def dot(a, b):
    return jnp.dot(a, b, preferred_element_type=F32)


def dot_nt(a, b):
    return lax.dot_general(a, b, (((1,), (1,)), ((), ())), preferred_element_type=F32)


def dot_tn(a, b):
    return lax.dot_general(a, b, (((0,), (0,)), ((), ())), preferred_element_type=F32)


def rms_norm(values, gain):
    inv_rms = lax.rsqrt(jnp.mean(values * values, axis=-1, keepdims=True) + EPS)
    return values * inv_rms * gain.astype(F32)


def row_to_column(row):
    size = row.shape[1]
    here = lax.broadcasted_iota(jnp.int32, (size, size), 0) == lax.broadcasted_iota(jnp.int32, (size, size), 1)
    return jnp.sum(jnp.where(here, jnp.broadcast_to(row, (size, size)), 0.0), axis=1, keepdims=True)


def seg_lanes(seg_column):
    lane = lax.broadcasted_iota(jnp.int32, (seg_column.shape[0], ROPE_DIM), 1).astype(F32)
    return seg_column == lane


def kernel(
    n,
    freq_ref, seg_ref, pos_ref, pseg_ref, gain_q_ref, gain_kv_ref,
    hid_hbm, pre_hbm, wdq_hbm, wuq_hbm, wdkv_hbm, wukv_hbm, wo_hbm,
    out_ref,
    hid_v, wdq_v, wdkv_v, wuq_v, wukv_v, wo_v,
    lat, pseg_mate, qlat_all, meta_all, key_tail, keys, queries, probs,
    stats, stats_rx, acc, split, bias, y_mine, y_out, y_rx, z, z_rx,
    load_sem, ukv_sem, mate_send, mate_recv, gat_send, gat_recv, met_send, met_recv,
    st_send, st_recv, pair_send, pair_recv, red_send, red_recv,
):
    me = lax.axis_index("sp")
    core = lax.rem(me, CORES)
    chip = lax.div(me, CORES)
    chips = n // CORES
    mate = chip * CORES + (CORES - 1 - core)
    toks = hid_v.shape[0]
    pre = pre_hbm.shape[0]
    kv_lat = wukv_v.shape[0]
    heads = keys.shape[0]
    rows = lat.shape[0]
    old = CORES * pre

    def load(src, dst, i):
        copy = pltpu.make_async_copy(src, dst, load_sem.at[i])
        copy.start()
        return copy

    load_hid = load(hid_hbm, hid_v, 0)
    load_dq = load(wdq_hbm, wdq_v, 1)
    load_dkv = load(wdkv_hbm, wdkv_v, 2)
    load_pre = load(pre_hbm, lat.at[pl.ds(0, pre)], 3)
    kv_cols = heads * KV_HEAD
    part = kv_cols // KV_LOADS
    load_ukv = []
    for i in range(KV_LOADS):
        copy = pltpu.make_async_copy(
            wukv_hbm.at[:, pl.ds(pl.multiple_of(core * kv_cols + i * part, LANES), part)],
            wukv_v.at[:, pl.ds(i * part, part)],
            ukv_sem.at[i],
        )
        copy.start()
        load_ukv.append(copy)

    barrier = pltpu.get_barrier_semaphore()
    for j in range(1, n):
        pl.semaphore_signal(barrier, inc=1, device_id={"sp": lax.rem(me + j, n)}, device_id_type=pl.DeviceIdType.MESH)
    pl.semaphore_wait(barrier, n - 1)

    def send(src, dst, send_sem, recv_sem, target):
        copy = pltpu.make_async_remote_copy(
            src_ref=src, dst_ref=dst, send_sem=send_sem, recv_sem=recv_sem,
            device_id={"sp": target}, device_id_type=pl.DeviceIdType.MESH,
        )
        copy.start()
        return copy

    send_pre = send(pre_hbm, lat.at[pl.ds(pre, pre)], mate_send.at[0], mate_recv.at[0], mate)
    send_pseg = send(pseg_ref, pseg_mate, mate_send.at[1], mate_recv.at[1], mate)

    pos_col = row_to_column(pos_ref[...].astype(F32))
    seg_col = row_to_column(seg_ref[...].astype(F32))
    angles = pos_col * freq_ref[...]
    lane = lax.broadcasted_iota(jnp.int32, (toks, LANES), 1)
    cos_t = jnp.cos(angles)
    sin_t = jnp.sin(angles)
    meta = jnp.where(lane < HALF, cos_t, jnp.where(lane < 2 * HALF, sin_t, jnp.where(lane == 2 * HALF, seg_col, pos_col)))
    my_rows = pl.ds(pl.multiple_of(me * toks, toks), toks)
    meta_all[my_rows, :] = meta

    load_hid.wait()
    load_dq.wait()
    qlat_all[my_rows, :] = rms_norm(dot(hid_v[...], wdq_v[...]), gain_q_ref[...]).astype(BF16)
    gathers = []
    for j in range(1, n):
        target = lax.rem(me + j, n)
        gathers.append(send(qlat_all.at[my_rows], qlat_all.at[my_rows], gat_send.at[j - 1], gat_recv.at[j - 1], target))
        gathers.append(send(meta_all.at[my_rows], meta_all.at[my_rows], met_send.at[j - 1], met_recv.at[j - 1], target))

    load_dkv.wait()
    down = dot(hid_v[...], wdkv_v[...])
    c_kv = rms_norm(down[:, :kv_lat], gain_kv_ref[...])
    low, high = down[:, kv_lat:kv_lat + HALF], down[:, kv_lat + HALF:]
    cos_m, sin_m = cos_t[:, :HALF], sin_t[:, :HALF]
    k_new = jnp.concatenate([low * cos_m - high * sin_m, high * cos_m + low * sin_m], axis=1)
    lat[pl.ds(old, toks), :] = jnp.concatenate([c_kv, k_new], axis=1).astype(BF16)
    send_new = send(lat.at[pl.ds(old, toks)], lat.at[pl.ds(old + toks, toks)], mate_send.at[2], mate_recv.at[2], mate)

    load_uq = load(wuq_hbm.at[:, pl.ds(pl.multiple_of(core * heads * QK_DIM, LANES), heads * QK_DIM)], wuq_v, 4)
    load_o = load(wo_hbm.at[pl.ds(pl.multiple_of(core * heads * V_DIM, LANES), heads * V_DIM)], wo_v, 5)

    def pair_weights(pair, offset):
        first = pl.multiple_of(pair * (2 * KV_HEAD) + offset, LANES)
        second = pl.multiple_of(pair * (2 * KV_HEAD) + KV_HEAD + offset, LANES)
        return jnp.concatenate([wukv_v[:, pl.ds(first, LANES)], wukv_v[:, pl.ds(second, LANES)]], axis=1)

    def raise_keys(start, size):
        def step(pair, carry):
            up = dot(lat[pl.ds(start, size), :kv_lat], pair_weights(pair, 0)).astype(BF16)
            keys[2 * pair, pl.ds(start, size), :] = up[:, :NOPE_DIM]
            keys[2 * pair + 1, pl.ds(start, size), :] = up[:, NOPE_DIM:]
            return carry
        return step

    load_pre.wait()
    pairs_per_load = heads // 2 // KV_LOADS
    for i in range(KV_LOADS):
        load_ukv[i].wait()
        lax.fori_loop(i * pairs_per_load, (i + 1) * pairs_per_load, raise_keys(0, pre), 0)
    send_pre.wait_recv()
    send_pseg.wait_recv()
    send_new.wait_recv()
    lax.fori_loop(0, heads // 2, raise_keys(pre, rows - pre), 0)

    def prefix_column(ref):
        wide = jnp.broadcast_to(ref[...].astype(F32), (8, pre))
        return jnp.transpose(wide)[:, :1]

    def put_tail(start, size, seg_column):
        rope = lat[pl.ds(start, size), kv_lat:].astype(F32)
        tail = jnp.concatenate([rope, jnp.where(seg_lanes(seg_column), 1.0, 0.0)], axis=1)
        key_tail[pl.ds(start, size), :] = tail.astype(BF16)

    put_tail(0, pre, prefix_column(pseg_ref))
    put_tail(pre, pre, prefix_column(pseg_mate))

    for copy in gathers:
        copy.wait_recv()
    mate_rows = pl.ds(pl.multiple_of(mate * toks, toks), toks)
    new_meta = jnp.concatenate([meta_all[my_rows, :], meta_all[mate_rows, :]], axis=0)
    put_tail(old, CORES * toks, new_meta[:, 2 * HALF:2 * HALF + 1])
    every = meta_all[...]
    q_pos = jnp.transpose(every)[2 * HALF + 1:2 * HALF + 2, :]
    bias[...] = jnp.where(new_meta[:, 2 * HALF + 1:2 * HALF + 2] <= q_pos, 0.0, NEG_BIG)

    load_uq.wait()
    q_mask = jnp.where(seg_lanes(every[:, 2 * HALF:2 * HALF + 1]), 0.0, NEG_BIG)
    cos_a, sin_a = every[:, :HALF], every[:, HALF:2 * HALF]
    cos_q = jnp.concatenate([cos_a, cos_a], axis=1)
    sin_q = jnp.concatenate([-sin_a, sin_a], axis=1)

    def put_query(head, nope, u):
        turned = jnp.concatenate([u[:, HALF:], u[:, :HALF]], axis=1)
        tail = jnp.concatenate([u * cos_q + turned * sin_q, q_mask], axis=1)
        queries[head] = jnp.concatenate([nope.astype(BF16), tail.astype(BF16)], axis=1)

    def raise_queries(pair, carry):
        cols = pl.ds(pl.multiple_of(pair * (2 * QK_DIM), LANES), 2 * QK_DIM)
        q = dot(qlat_all[...], wuq_v[:, cols])
        put_query(2 * pair, q[:, :NOPE_DIM], q[:, NOPE_DIM:QK_DIM])
        put_query(2 * pair + 1, q[:, QK_DIM:QK_DIM + NOPE_DIM], q[:, QK_DIM + NOPE_DIM:])
        return carry

    lax.fori_loop(0, heads // 2, raise_queries, 0)

    def score(head, carry):
        k_full = jnp.concatenate([keys[head], key_tail[...]], axis=1)
        s = dot_nt(k_full, queries[head])
        s_old, s_new = s[:old], s[old:] + bias[...]
        top = jnp.maximum(jnp.max(s_old, axis=0, keepdims=True), jnp.max(s_new, axis=0, keepdims=True))
        p_old = jnp.exp2((s_old - top) * EXP_SCALE)
        p_new = jnp.exp2((s_new - top) * EXP_SCALE)
        probs[head, :old, :] = p_old.astype(BF16)
        probs[head, old:, :] = p_new.astype(BF16)
        stats[pl.ds(head, 1), :] = top
        stats[pl.ds(heads + head, 1), :] = jnp.sum(p_old, axis=0, keepdims=True) + jnp.sum(p_new, axis=0, keepdims=True)
        return carry

    lax.fori_loop(0, heads, score, 0)

    def peer(j):
        return lax.rem(chip + j, chips)

    send_stats = [
        send(stats, stats_rx.at[j - 1], st_send.at[j - 1], st_recv.at[j - 1], peer(j) * CORES + core)
        for j in range(1, chips)
    ]

    def attend(pair, carry):
        v = dot(lat[:, :kv_lat], pair_weights(pair, NOPE_DIM)).astype(BF16)
        for i in range(2):
            cols = pl.ds(pl.multiple_of((2 * pair + i) * V_DIM, LANES), V_DIM)
            acc[:, cols] = dot_tn(probs[2 * pair + i], v[:, i * V_DIM:(i + 1) * V_DIM])
        return carry

    lax.fori_loop(0, heads // 2, attend, 0)

    for copy in send_stats:
        copy.wait_recv()
    tops = [stats[:heads, :]] + [stats_rx[j, :heads, :] for j in range(chips - 1)]
    sums = [stats[heads:, :]] + [stats_rx[j, heads:, :] for j in range(chips - 1)]
    top = functools.reduce(jnp.maximum, tops)
    shares = [jnp.exp2((t - top) * EXP_SCALE) for t in tops]
    total = functools.reduce(jnp.add, [s * w for s, w in zip(sums, shares)])
    scale = jnp.transpose(shares[0] / total)
    all_toks = n * toks
    for head in range(heads):
        cols = pl.ds(head * V_DIM, V_DIM)
        o = acc[:, cols] * scale[:, head:head + 1]
        o_hi = o.astype(BF16)
        split[:all_toks, cols] = o_hi
        split[all_toks:, cols] = (o - o_hi.astype(F32)).astype(BF16)

    load_o.wait()
    n_chunks = wo_v.shape[1] // N_CHUNK
    block = chips * toks
    pair_copies, red_copies = [], []

    def reduce_chunk(i):
        pair_copies[i].wait_recv()
        z[i] = y_mine[i] + y_rx[i]
        for j in range(1, chips):
            rows_j = pl.ds(pl.multiple_of(peer(j) * toks, toks), toks)
            red_copies.append(send(
                z.at[i, rows_j], z_rx.at[j - 1, i], red_send.at[j - 1, i], red_recv.at[j - 1, i], peer(j) * CORES + core
            ))

    for i in range(n_chunks):
        y = dot(split[...], wo_v[:, i * N_CHUNK:(i + 1) * N_CHUNK])
        y = (y[:all_toks] + y[all_toks:]).reshape(chips, CORES, toks, N_CHUNK)
        first, second = y[:, 0].reshape(block, N_CHUNK), y[:, 1].reshape(block, N_CHUNK)
        y_mine[i] = jnp.where(core == 0, first, second)
        y_out[i] = jnp.where(core == 0, second, first)
        pair_copies.append(send(y_out.at[i], y_rx.at[i], pair_send.at[i], pair_recv.at[i], mate))
        if i:
            reduce_chunk(i - 1)
    reduce_chunk(n_chunks - 1)
    own = pl.ds(pl.multiple_of(chip * toks, toks), toks)
    for i in range(n_chunks):
        y = z[i, own, :]
        for j in range(1, chips):
            red_copies[i * (chips - 1) + j - 1].wait_recv()
            y = y + z_rx[j - 1, i]
        out_ref[:, i * N_CHUNK:(i + 1) * N_CHUNK] = y.astype(BF16)

    for copy in [send_pre, send_pseg, send_new] + gathers + send_stats + pair_copies + red_copies:
        copy.wait_send()


def solution(mesh):
    n = mesh.shape["sp"]
    chips = n // CORES
    tok_spec = P(("dp", "sp"), None)
    vec_spec = P(("dp", "sp"))
    mat_spec = P(None, None)
    gain_spec = P(None)

    def device_step(hidden, seg_ids, positions, prefix_lat, prefix_seg, w_dq, gain_q, w_uq, w_dkv, gain_kv, w_ukv, w_o):
        toks, width = hidden.shape
        pre, lat_dim = prefix_lat.shape
        q_lat = w_dq.shape[1]
        kv_lat = w_ukv.shape[0]
        heads = w_o.shape[0] // V_DIM // CORES
        rows = CORES * (pre + toks)
        all_toks = n * toks
        n_chunks = width // N_CHUNK
        inv_freq = (ROPE_BASE ** (-np.arange(HALF, dtype=np.float64) / HALF)).astype(np.float32)
        freq = jnp.asarray(np.concatenate([inv_freq] * (LANES // HALF)).reshape(1, LANES))
        vmem = pl.BlockSpec(memory_space=pltpu.VMEM)
        hbm = pl.BlockSpec(memory_space=pl.ANY)
        dma = pltpu.SemaphoreType.DMA
        return pl.pallas_call(
            functools.partial(kernel, n),
            out_shape=jax.ShapeDtypeStruct((toks, width), BF16),
            in_specs=[vmem] * 6 + [hbm] * 7,
            out_specs=vmem,
            scratch_shapes=[
                pltpu.VMEM((toks, width), BF16),
                pltpu.VMEM((width, q_lat), BF16),
                pltpu.VMEM((width, lat_dim), BF16),
                pltpu.VMEM((q_lat, heads * QK_DIM), BF16),
                pltpu.VMEM((kv_lat, heads * KV_HEAD), BF16),
                pltpu.VMEM((heads * V_DIM, width), BF16),
                pltpu.VMEM((rows, lat_dim), BF16),
                pltpu.VMEM((1, pre), jnp.int32),
                pltpu.VMEM((all_toks, q_lat), BF16),
                pltpu.VMEM((all_toks, LANES), F32),
                pltpu.VMEM((rows, LANES), BF16),
                pltpu.VMEM((heads, rows, NOPE_DIM), BF16),
                pltpu.VMEM((heads, all_toks, 2 * LANES), BF16),
                pltpu.VMEM((heads, rows, all_toks), BF16),
                pltpu.VMEM((2 * heads, all_toks), F32),
                pltpu.VMEM((chips - 1, 2 * heads, all_toks), F32),
                pltpu.VMEM((all_toks, heads * V_DIM), F32),
                pltpu.VMEM((2 * all_toks, heads * V_DIM), BF16),
                pltpu.VMEM((CORES * toks, all_toks), F32),
                pltpu.VMEM((n_chunks, chips * toks, N_CHUNK), F32),
                pltpu.VMEM((n_chunks, chips * toks, N_CHUNK), F32),
                pltpu.VMEM((n_chunks, chips * toks, N_CHUNK), F32),
                pltpu.VMEM((n_chunks, chips * toks, N_CHUNK), F32),
                pltpu.VMEM((chips - 1, n_chunks, toks, N_CHUNK), F32),
                dma((6,)),
                dma((KV_LOADS,)),
                dma((3,)), dma((3,)),
                dma((n - 1,)), dma((n - 1,)),
                dma((n - 1,)), dma((n - 1,)),
                dma((chips - 1,)), dma((chips - 1,)),
                dma((n_chunks,)), dma((n_chunks,)),
                dma((chips - 1, n_chunks)), dma((chips - 1, n_chunks)),
            ],
            compiler_params=pltpu.CompilerParams(
                collective_id=0, has_side_effects=True, vmem_limit_bytes=60 * 1024 * 1024
            ),
        )(
            freq, seg_ids.reshape(1, toks), positions.reshape(1, toks), prefix_seg.reshape(1, pre),
            gain_q.reshape(1, q_lat), gain_kv.reshape(1, kv_lat),
            hidden, prefix_lat, w_dq, w_uq, w_dkv, w_ukv, w_o,
        )

    return jax.shard_map(
        device_step,
        mesh=mesh,
        in_specs=(tok_spec, vec_spec, vec_spec, tok_spec, vec_spec, mat_spec, gain_spec, mat_spec, mat_spec, gain_spec, mat_spec, mat_spec),
        out_specs=tok_spec,
        check_vma=False,
    )
```

```python
import functools
import math

import jax
import jax.numpy as jnp
import numpy as np
from jax import lax
from jax.experimental import pallas as pl
from jax.experimental.pallas import tpu as pltpu
from jax.sharding import PartitionSpec as P

ROPE_DIM = 64
HALF = ROPE_DIM // 2
NOPE_DIM = 128
V_DIM = 128
QK_DIM = NOPE_DIM + ROPE_DIM
KV_HEAD = NOPE_DIM + V_DIM
CORES = 2
EPS = 1e-6
ROPE_BASE = 10000.0
NEG_BIG = -1e30
EXP_SCALE = QK_DIM ** -0.5 * math.log2(math.e)
LANES = 128
N_CHUNK = 256
KV_LOADS = 4
UNROLL_KV = 4
UNROLL_SCORE = 4
UNROLL_PV = 4

F32 = jnp.float32
BF16 = jnp.bfloat16


def dot(a, b):
    return jnp.dot(a, b, preferred_element_type=F32)


def dot_nt(a, b):
    return lax.dot_general(a, b, (((1,), (1,)), ((), ())), preferred_element_type=F32)


def dot_tn(a, b):
    return lax.dot_general(a, b, (((0,), (0,)), ((), ())), preferred_element_type=F32)


def rms_norm(values, gain):
    inv_rms = lax.rsqrt(jnp.mean(values * values, axis=-1, keepdims=True) + EPS)
    return values * inv_rms * gain.astype(F32).reshape(1, gain.shape[0])


def row_to_column(row):
    size = row.shape[1]
    here = lax.broadcasted_iota(jnp.int32, (size, size), 0) == lax.broadcasted_iota(jnp.int32, (size, size), 1)
    return jnp.sum(jnp.where(here, jnp.broadcast_to(row, (size, size)), 0.0), axis=1, keepdims=True)


def lane_of(shape):
    return lax.broadcasted_iota(jnp.int32, shape, len(shape) - 1)


def turn(x, amount):
    return pltpu.roll(x, amount, 1)


def unrolled(count, step, body):
    def run(i, carry):
        for j in range(step):
            body(i * step + j)
        return carry

    lax.fori_loop(0, count // step, run, 0)


class Phases:
    def __init__(self):
        self.now = None

    def __call__(self, name):
        if self.now is not None:
            self.now.__exit__(None, None, None)
        self.now = None
        if name:
            self.now = jax.named_scope(name)
            self.now.__enter__()


def kernel(
    n,
    freq_ref, seg_ref, pos_ref, pseg_ref, gain_q_ref, gain_kv_ref,
    hid_hbm, pre_hbm, wdq_hbm, wuq_hbm, wdkv_hbm, wukv_hbm, wo_hbm,
    out_ref,
    hid_v, wdq_v, wdkv_v, wuq_v, wukv_v, wo_v,
    lat_t, lat, new_lat, pseg_mate, qlat_all, meta_all, cos_all, sin_all, mask_a, tail_t,
    keys_t, values, queries, probs, tops_all, sums_all,
    stats, stats_rx, acc, split, bias, y_mine, y_out, y_rx, z, z_rx,
    load_sem, ukv_sem, mate_send, mate_recv, gat_send, gat_recv, met_send, met_recv,
    st_send, st_recv, pair_send, pair_recv, red_send, red_recv,
):
    phase = Phases()
    me = lax.axis_index("sp")
    core = lax.rem(me, CORES)
    chip = lax.div(me, CORES)
    chips = n // CORES
    mate = chip * CORES + (CORES - 1 - core)
    toks = hid_v.shape[0]
    pre = pre_hbm.shape[1]
    kv_lat = wukv_v.shape[0]
    heads = keys_t.shape[0]
    old = CORES * pre
    new = CORES * toks
    wide = lat_t.shape[1]
    all_toks = n * toks

    phase("loads")

    def load(src, dst, sem):
        copy = pltpu.make_async_copy(src, dst, sem)
        copy.start()
        return copy

    barrier = pltpu.get_barrier_semaphore()
    for j in range(1, n):
        pl.semaphore_signal(barrier, inc=1, device_id={"sp": lax.rem(me + j, n)}, device_id_type=pl.DeviceIdType.MESH)
    load_hid = load(hid_hbm, hid_v, load_sem.at[0])
    load_dq = load(wdq_hbm, wdq_v, load_sem.at[1])
    load_dkv = load(wdkv_hbm, wdkv_v, load_sem.at[2])
    load_pre = load(pre_hbm, lat_t.at[:, pl.ds(0, pre)], load_sem.at[3])
    kv_cols = heads * KV_HEAD
    part = kv_cols // KV_LOADS
    load_ukv = [
        load(
            wukv_hbm.at[:, pl.ds(pl.multiple_of(core * kv_cols + i * part, LANES), part)],
            wukv_v.at[:, pl.ds(i * part, part)],
            ukv_sem.at[i],
        )
        for i in range(KV_LOADS)
    ]

    phase("meta")
    pos_col = row_to_column(pos_ref[...].astype(F32))
    seg_col = row_to_column(seg_ref[...].astype(F32))
    angles = pos_col * freq_ref[...]
    lane = lane_of((toks, LANES))
    cos_t = jnp.cos(angles)
    sin_t = jnp.sin(angles)
    my_rows = pl.ds(pl.multiple_of(me * toks, toks), toks)
    meta_all[my_rows, :] = jnp.where(
        lane < HALF, cos_t, jnp.where(lane < 2 * HALF, sin_t, jnp.where(lane == 2 * HALF, seg_col, pos_col))
    )

    phase("barrier")
    pl.semaphore_wait(barrier, n - 1)

    def send(src, dst, send_sem, recv_sem, target):
        copy = pltpu.make_async_remote_copy(
            src_ref=src, dst_ref=dst, send_sem=send_sem, recv_sem=recv_sem,
            device_id={"sp": target}, device_id_type=pl.DeviceIdType.MESH,
        )
        copy.start()
        return copy

    send_pre = send(pre_hbm, lat_t.at[:, pl.ds(pre, pre)], mate_send.at[0], mate_recv.at[0], mate)
    send_pseg = send(pseg_ref, pseg_mate, mate_send.at[1], mate_recv.at[1], mate)
    send_meta = [
        send(meta_all.at[my_rows], meta_all.at[my_rows], met_send.at[j - 1], met_recv.at[j - 1], lax.rem(me + j, n))
        for j in range(1, n)
    ]

    phase("wait_dq")
    load_hid.wait()
    load_dq.wait()
    phase("qlat")
    qlat_all[my_rows, :] = rms_norm(dot(hid_v[...], wdq_v[...]), gain_q_ref[...]).astype(BF16)
    send_q = [
        send(qlat_all.at[my_rows], qlat_all.at[my_rows], gat_send.at[j - 1], gat_recv.at[j - 1], lax.rem(me + j, n))
        for j in range(1, n)
    ]

    load_dkv.wait()
    phase("kvlat")
    down = dot_nt(hid_v[...], wdkv_v[...])
    c_kv = rms_norm(down[:, :kv_lat], gain_kv_ref[...])
    low, high = down[:, kv_lat:kv_lat + HALF], down[:, kv_lat + HALF:]
    cos_m, sin_m = cos_t[:, :HALF], sin_t[:, :HALF]
    k_new = jnp.concatenate([low * cos_m - high * sin_m, high * cos_m + low * sin_m], axis=1)
    new_lat[pl.ds(0, toks), :] = jnp.concatenate([c_kv, k_new], axis=1).astype(BF16)
    send_new = send(new_lat.at[pl.ds(0, toks)], new_lat.at[pl.ds(toks, toks)], mate_send.at[2], mate_recv.at[2], mate)

    load_uq = load(
        wuq_hbm.at[:, pl.ds(pl.multiple_of(core * heads * QK_DIM, LANES), heads * QK_DIM)], wuq_v, load_sem.at[4]
    )
    load_o = load(
        wo_hbm.at[pl.ds(pl.multiple_of(core * heads * V_DIM, LANES), heads * V_DIM)], wo_v, load_sem.at[5]
    )

    def pair_weights(pair, offset):
        first = pl.multiple_of(pair * (2 * KV_HEAD) + offset, LANES)
        second = pl.multiple_of(pair * (2 * KV_HEAD) + KV_HEAD + offset, LANES)
        return jnp.concatenate([wukv_v[:, pl.ds(first, LANES)], wukv_v[:, pl.ds(second, LANES)]], axis=1)

    def raise_keys(start, size):
        def step(pair):
            up = dot_tn(pair_weights(pair, 0), lat_t[:kv_lat, pl.ds(start, size)]).astype(BF16)
            keys_t[2 * pair, :, pl.ds(start, size)] = up[:NOPE_DIM]
            keys_t[2 * pair + 1, :, pl.ds(start, size)] = up[NOPE_DIM:]
        return step

    def raise_values(start, size):
        def step(pair):
            values[pair, pl.ds(start, size), :] = dot(lat[pl.ds(start, size), :], pair_weights(pair, NOPE_DIM)).astype(BF16)
        return step

    def put_tail(start, size, seg_row):
        hot = seg_row == lax.broadcasted_iota(jnp.int32, (ROPE_DIM, size), 0)
        hot = jnp.where(hot, 1.0, 0.0).astype(BF16)
        rope = lat_t[kv_lat:, pl.ds(start, size)]
        tail_t[0, :, pl.ds(start, size)] = jnp.concatenate([rope, hot], axis=0)
        tail_t[1, :, pl.ds(start, size)] = jnp.concatenate([hot, rope], axis=0)

    phase("wait_pre")
    load_pre.wait()
    for copy in load_ukv:
        copy.wait()
    phase("keys_own")
    lat[pl.ds(0, pre), :] = jnp.transpose(lat_t[:kv_lat, pl.ds(0, pre)])
    put_tail(0, pre, pseg_ref[...])
    values[:, pl.ds(old + new, wide - old - new), :] = jnp.zeros((heads // 2, wide - old - new, 2 * V_DIM), BF16)
    unrolled(heads // 2, UNROLL_KV, raise_keys(0, pre))
    phase("values_own")
    unrolled(heads // 2, UNROLL_KV, raise_values(0, pre))

    phase("wait_meta")
    for copy in send_meta:
        copy.wait_recv()
    phase("tables")
    every = meta_all[...]
    lanes = lane_of((all_toks, LANES))
    q_seg = every[:, 2 * HALF:2 * HALF + 1]
    q_pos = every[:, 2 * HALF + 1:2 * HALF + 2]
    cos_q = jnp.where(lanes < HALF, every, 0.0)
    cos_q = cos_q + turn(cos_q, HALF)
    cos_all[...] = cos_q + turn(cos_q, 2 * HALF)
    sin_q = jnp.where((lanes >= HALF) & (lanes < 2 * HALF), every, 0.0)
    sin_q = sin_q - turn(sin_q, LANES - HALF)
    sin_all[...] = sin_q + turn(sin_q, 2 * HALF)
    q_mask = jnp.where(q_seg == jnp.where(lanes < ROPE_DIM, lanes, lanes - ROPE_DIM).astype(F32), 0.0, NEG_BIG)
    mask_a[...] = q_mask
    mate_rows = pl.ds(pl.multiple_of(mate * toks, toks), toks)
    new_meta = jnp.concatenate(
        [meta_all[my_rows, :], meta_all[mate_rows, :], jnp.zeros((LANES - new, LANES), F32)], axis=0
    )
    meta_rows = jnp.transpose(new_meta)
    k_seg, k_pos = meta_rows[2 * HALF:2 * HALF + 1], meta_rows[2 * HALF + 1:2 * HALF + 2]
    seen = (q_seg == k_seg) & (k_pos <= q_pos) & (lane_of((all_toks, LANES)) < new)
    bias[...] = jnp.where(seen, 0.0, NEG_BIG)

    phase("wait_mate")
    send_pre.wait_recv()
    send_pseg.wait_recv()
    send_new.wait_recv()
    phase("keys_mate")
    lat[pl.ds(pre, pre), :] = jnp.transpose(lat_t[:kv_lat, pl.ds(pre, pre)])
    lat[pl.ds(old, new), :] = new_lat[:, :kv_lat]
    new_wide = jnp.concatenate([new_lat[...].astype(F32), jnp.zeros((LANES - new, kv_lat + ROPE_DIM), F32)], axis=0)
    lat_t[:, pl.ds(old, LANES)] = jnp.transpose(new_wide).astype(BF16)
    put_tail(pre, pre, pseg_mate[...])
    put_tail(old, LANES, jnp.full((1, LANES), -1, jnp.int32))
    unrolled(heads // 2, UNROLL_KV, raise_keys(pre, wide - pre))

    phase("wait_uq")
    load_uq.wait()
    for copy in send_q:
        copy.wait_recv()
    phase("queries")
    low_half = lane_of((all_toks, LANES)) < ROPE_DIM
    first_half = lax.rem(lane_of((all_toks, LANES)), ROPE_DIM) < HALF

    def raise_queries(pair):
        cols = pl.ds(pl.multiple_of(pair * (2 * QK_DIM), LANES), 2 * QK_DIM)
        q = dot(qlat_all[...], wuq_v[:, cols])
        nope_a, mid, end = q[:, :LANES], q[:, LANES:2 * LANES], q[:, 2 * LANES:]
        nope_b = turn(jnp.where(low_half, end, mid), ROPE_DIM)
        u = jnp.where(low_half, mid, end)
        swapped = jnp.where(first_half, turn(u, LANES - HALF), turn(u, HALF))
        r = u * cos_all[...] + swapped * sin_all[...]
        queries[2 * pair] = jnp.concatenate([nope_a, jnp.where(low_half, r, mask_a[...])], axis=1).astype(BF16)
        queries[2 * pair + 1] = jnp.concatenate([nope_b, jnp.where(low_half, mask_a[...], r)], axis=1).astype(BF16)

    unrolled(heads // 2, UNROLL_KV, raise_queries)

    phase("score")

    def score(head, odd):
        s = dot(queries[head], jnp.concatenate([keys_t[head], tail_t[odd]], axis=0))
        s_old, s_new = s[:, :old], s[:, old:] + bias[...]
        top = jnp.maximum(jnp.max(s_old, axis=1, keepdims=True), jnp.max(s_new, axis=1, keepdims=True))
        p_old = jnp.exp2((s_old - top) * EXP_SCALE)
        p_new = jnp.exp2((s_new - top) * EXP_SCALE)
        probs[head, :, :old] = p_old.astype(BF16)
        probs[head, :, old:] = p_new.astype(BF16)
        total = jnp.sum(p_old, axis=1, keepdims=True) + jnp.sum(p_new, axis=1, keepdims=True)
        tops_all[head] = jnp.broadcast_to(top, (all_toks, LANES))
        sums_all[head] = jnp.broadcast_to(total, (all_toks, LANES))

    def score_group(i, carry):
        for j in range(UNROLL_SCORE):
            score(i * UNROLL_SCORE + j, j % 2)
        return carry

    lax.fori_loop(0, heads // UNROLL_SCORE, score_group, 0)

    phase("stats")

    def peer(j):
        return lax.rem(chip + j, chips)

    packed = jnp.zeros((all_toks, LANES), F32)
    for head in range(heads):
        packed = jnp.where(lanes == head, tops_all[head], packed)
        packed = jnp.where(lanes == heads + head, sums_all[head], packed)
    stats[...] = jnp.transpose(packed)[:2 * heads]
    send_stats = [
        send(stats, stats_rx.at[j - 1], st_send.at[j - 1], st_recv.at[j - 1], peer(j) * CORES + core)
        for j in range(1, chips)
    ]
    phase("values_mate")
    unrolled(heads // 2, UNROLL_KV, raise_values(pre, pre + new))
    phase("attend")

    def attend(pair):
        for i in range(2):
            cols = pl.ds(pl.multiple_of((2 * pair + i) * V_DIM, LANES), V_DIM)
            acc[:, cols] = dot(probs[2 * pair + i], values[pair, :, i * V_DIM:(i + 1) * V_DIM])

    unrolled(heads // 2, UNROLL_PV, attend)

    phase("wait_stats")
    for copy in send_stats:
        copy.wait_recv()
    phase("scale")
    tops = [stats[:heads, :]] + [stats_rx[j, :heads, :] for j in range(chips - 1)]
    sums = [stats[heads:, :]] + [stats_rx[j, heads:, :] for j in range(chips - 1)]
    top = functools.reduce(jnp.maximum, tops)
    shares = [jnp.exp2((t - top) * EXP_SCALE) for t in tops]
    total = functools.reduce(jnp.add, [s * w for s, w in zip(sums, shares)])
    scale = jnp.transpose(shares[0] / total)
    for head in range(heads):
        cols = pl.ds(head * V_DIM, V_DIM)
        o = acc[:, cols] * scale[:, head:head + 1]
        o_hi = o.astype(BF16)
        split[:all_toks, cols] = o_hi
        split[all_toks:, cols] = (o - o_hi.astype(F32)).astype(BF16)

    phase("wait_o")
    load_o.wait()
    phase("outproj")
    n_chunks = wo_v.shape[1] // N_CHUNK
    block = chips * toks
    pair_copies, red_copies = [], []

    def reduce_chunk(i):
        pair_copies[i].wait_recv()
        z[i] = y_mine[i] + y_rx[i]
        for j in range(1, chips):
            rows_j = pl.ds(pl.multiple_of(peer(j) * toks, toks), toks)
            red_copies.append(send(
                z.at[i, rows_j], z_rx.at[j - 1, i], red_send.at[j - 1, i], red_recv.at[j - 1, i], peer(j) * CORES + core
            ))

    for i in range(n_chunks):
        y = dot(split[...], wo_v[:, i * N_CHUNK:(i + 1) * N_CHUNK])
        y = (y[:all_toks] + y[all_toks:]).reshape(chips, CORES, toks, N_CHUNK)
        first, second = y[:, 0].reshape(block, N_CHUNK), y[:, 1].reshape(block, N_CHUNK)
        y_mine[i] = jnp.where(core == 0, first, second)
        y_out[i] = jnp.where(core == 0, second, first)
        pair_copies.append(send(y_out.at[i], y_rx.at[i], pair_send.at[i], pair_recv.at[i], mate))
        if i:
            reduce_chunk(i - 1)
    phase("last_pair")
    reduce_chunk(n_chunks - 1)
    phase("reduce")
    own = pl.ds(pl.multiple_of(chip * toks, toks), toks)
    for i in range(n_chunks):
        y = z[i, own, :]
        for j in range(1, chips):
            red_copies[i * (chips - 1) + j - 1].wait_recv()
            y = y + z_rx[j - 1, i]
        out_ref[:, i * N_CHUNK:(i + 1) * N_CHUNK] = y.astype(BF16)

    phase("drain")
    for copy in [send_pre, send_pseg, send_new] + send_meta + send_q + send_stats + pair_copies + red_copies:
        copy.wait_send()
    phase("")


def solution(mesh):
    n = mesh.shape["sp"]
    chips = n // CORES
    tok_spec = P(("dp", "sp"), None)
    vec_spec = P(("dp", "sp"))
    mat_spec = P(None, None)
    gain_spec = P(None)

    def device_step(hidden, seg_ids, positions, prefix_lat, prefix_seg, w_dq, gain_q, w_uq, w_dkv, gain_kv, w_ukv, w_o):
        toks, width = hidden.shape
        pre, lat_dim = prefix_lat.shape
        q_lat = w_dq.shape[1]
        kv_lat = w_ukv.shape[0]
        heads = w_o.shape[0] // V_DIM // CORES
        rows = CORES * (pre + toks)
        wide = CORES * pre + LANES
        all_toks = n * toks
        n_chunks = width // N_CHUNK
        inv_freq = (ROPE_BASE ** (-np.arange(HALF, dtype=np.float64) / HALF)).astype(np.float32)
        freq = jnp.asarray(np.concatenate([inv_freq] * (LANES // HALF)).reshape(1, LANES))
        vmem = pl.BlockSpec(memory_space=pltpu.VMEM)
        hbm = pl.BlockSpec(memory_space=pl.ANY)
        dma = pltpu.SemaphoreType.DMA
        table = pltpu.VMEM((all_toks, LANES), F32)
        chunks = pltpu.VMEM((n_chunks, chips * toks, N_CHUNK), F32)
        return pl.pallas_call(
            functools.partial(kernel, n),
            out_shape=jax.ShapeDtypeStruct((toks, width), BF16),
            in_specs=[vmem] * 6 + [hbm] * 7,
            out_specs=vmem,
            scratch_shapes=[
                pltpu.VMEM((toks, width), BF16),
                pltpu.VMEM((width, q_lat), BF16),
                pltpu.VMEM((lat_dim, width), BF16),
                pltpu.VMEM((q_lat, heads * QK_DIM), BF16),
                pltpu.VMEM((kv_lat, heads * KV_HEAD), BF16),
                pltpu.VMEM((heads * V_DIM, width), BF16),
                pltpu.VMEM((lat_dim, wide), BF16),
                pltpu.VMEM((rows, kv_lat), BF16),
                pltpu.VMEM((CORES * toks, lat_dim), BF16),
                pltpu.VMEM((1, pre), jnp.int32),
                pltpu.VMEM((all_toks, q_lat), BF16),
                table, table, table, table,
                pltpu.VMEM((2, LANES, wide), BF16),
                pltpu.VMEM((heads, NOPE_DIM, wide), BF16),
                pltpu.VMEM((heads // 2, wide, 2 * V_DIM), BF16),
                pltpu.VMEM((heads, all_toks, 2 * LANES), BF16),
                pltpu.VMEM((heads, all_toks, wide), BF16),
                pltpu.VMEM((heads, all_toks, LANES), F32),
                pltpu.VMEM((heads, all_toks, LANES), F32),
                pltpu.VMEM((2 * heads, all_toks), F32),
                pltpu.VMEM((chips - 1, 2 * heads, all_toks), F32),
                pltpu.VMEM((all_toks, heads * V_DIM), F32),
                pltpu.VMEM((2 * all_toks, heads * V_DIM), BF16),
                table,
                chunks, chunks, chunks, chunks,
                pltpu.VMEM((chips - 1, n_chunks, toks, N_CHUNK), F32),
                dma((6,)),
                dma((KV_LOADS,)),
                dma((3,)), dma((3,)),
                dma((n - 1,)), dma((n - 1,)),
                dma((n - 1,)), dma((n - 1,)),
                dma((chips - 1,)), dma((chips - 1,)),
                dma((n_chunks,)), dma((n_chunks,)),
                dma((chips - 1, n_chunks)), dma((chips - 1, n_chunks)),
            ],
            compiler_params=pltpu.CompilerParams(
                collective_id=0, has_side_effects=True, vmem_limit_bytes=60 * 1024 * 1024
            ),
        )(
            freq, seg_ids.reshape(1, toks), positions.reshape(1, toks), prefix_seg.reshape(1, pre),
            gain_q, gain_kv,
            hidden, prefix_lat.T, w_dq, w_uq, w_dkv.T, w_ukv, w_o,
        )

    return jax.shard_map(
        device_step,
        mesh=mesh,
        in_specs=(tok_spec, vec_spec, vec_spec, tok_spec, vec_spec, mat_spec, gain_spec, mat_spec, mat_spec, gain_spec, mat_spec, mat_spec),
        out_specs=tok_spec,
        check_vma=False,
    )
```

```python
import functools
import math

import jax
import jax.numpy as jnp
import numpy as np
from jax import lax
from jax.experimental import pallas as pl
from jax.experimental.pallas import tpu as pltpu
from jax.sharding import PartitionSpec as P

ROPE_DIM = 64
HALF = ROPE_DIM // 2
NOPE_DIM = 128
V_DIM = 128
QK_DIM = NOPE_DIM + ROPE_DIM
KV_HEAD = NOPE_DIM + V_DIM
CORES = 2
EPS = 1e-6
ROPE_BASE = 10000.0
NEG_BIG = -1e30
EXP_SCALE = QK_DIM ** -0.5 * math.log2(math.e)
LANES = 128
N_CHUNK = 512
LAG = 2
ORDER = ((2, 1), (3, 0))
V_IN_SCORE = 1
KV_LOADS = 4
UNROLL_KV = 8
UNROLL_SCORE = 4
UNROLL_PV = 4

F32 = jnp.float32
BF16 = jnp.bfloat16


def dot(a, b):
    return jnp.dot(a, b, preferred_element_type=F32)


def dot_nt(a, b):
    return lax.dot_general(a, b, (((1,), (1,)), ((), ())), preferred_element_type=F32)


def dot_tn(a, b):
    return lax.dot_general(a, b, (((0,), (0,)), ((), ())), preferred_element_type=F32)


def rms_norm(values, gain):
    inv_rms = lax.rsqrt(jnp.mean(values * values, axis=-1, keepdims=True) + EPS)
    return values * inv_rms * gain.astype(F32).reshape(1, gain.shape[0])


def row_to_column(row):
    size = row.shape[1]
    here = lax.broadcasted_iota(jnp.int32, (size, size), 0) == lax.broadcasted_iota(jnp.int32, (size, size), 1)
    return jnp.sum(jnp.where(here, jnp.broadcast_to(row, (size, size)), 0.0), axis=1, keepdims=True)


def lane_of(shape):
    return lax.broadcasted_iota(jnp.int32, shape, len(shape) - 1)


def turn(x, amount):
    return pltpu.roll(x, amount, 1)


def unrolled(count, step, body):
    if count == step:
        for j in range(step):
            body(j)
        return

    def run(i, carry):
        for j in range(step):
            body(i * step + j)
        return carry

    lax.fori_loop(0, count // step, run, 0)


class Phases:
    def __init__(self):
        self.now = None

    def __call__(self, name):
        if self.now is not None:
            self.now.__exit__(None, None, None)
        self.now = None
        if name:
            self.now = jax.named_scope(name)
            self.now.__enter__()


def kernel(
    n,
    freq_ref, seg_ref, pos_ref, pseg_ref, gain_q_ref, gain_kv_ref,
    hid_hbm, pre_hbm, wdq_hbm, wuq_hbm, wdkv_hbm, wukv_hbm, wo_hbm,
    out_ref,
    hid_v, wdq_v, wdkv_v, wuq_v, wukv_v, wo_v,
    lat_t, lat, new_lat, pseg_mate, qlat_all, meta_all, cos_all, sin_all, mask_a, tail_t,
    keys_t, values, queries, probs, tops_all, sums_all,
    scores, stats, stats_rx, acc, scales, split, bias, y_mine, y_out, y_rx, z, z_rx,
    load_sem, ukv_sem, mate_send, mate_recv, gat_send, gat_recv, met_send, met_recv,
    st_send, st_recv, pair_send, pair_recv, red_send, red_recv,
):
    phase = Phases()
    me = lax.axis_index("sp")
    core = lax.rem(me, CORES)
    chip = lax.div(me, CORES)
    chips = n // CORES
    mate = chip * CORES + (CORES - 1 - core)
    toks = hid_v.shape[0]
    pre = pre_hbm.shape[1]
    kv_lat = wukv_v.shape[0]
    heads = keys_t.shape[0]
    old = CORES * pre
    new = CORES * toks
    wide = lat_t.shape[1]
    all_toks = n * toks

    phase("loads")

    def load(src, dst, sem):
        copy = pltpu.make_async_copy(src, dst, sem)
        copy.start()
        return copy

    barrier = pltpu.get_barrier_semaphore()
    for j in range(1, n):
        pl.semaphore_signal(barrier, inc=1, device_id={"sp": lax.rem(me + j, n)}, device_id_type=pl.DeviceIdType.MESH)
    load_hid = load(hid_hbm, hid_v, load_sem.at[0])
    load_dq = load(wdq_hbm, wdq_v, load_sem.at[1])
    load_dkv = load(wdkv_hbm, wdkv_v, load_sem.at[2])
    load_pre = load(pre_hbm, lat_t.at[:, pl.ds(0, pre)], load_sem.at[3])
    kv_cols = heads * KV_HEAD
    part = kv_cols // KV_LOADS
    load_ukv = [
        load(
            wukv_hbm.at[:, pl.ds(pl.multiple_of(core * kv_cols + i * part, LANES), part)],
            wukv_v.at[:, pl.ds(i * part, part)],
            ukv_sem.at[i],
        )
        for i in range(KV_LOADS)
    ]

    phase("meta")
    pos_col = row_to_column(pos_ref[...].astype(F32))
    seg_col = row_to_column(seg_ref[...].astype(F32))
    angles = pos_col * freq_ref[...]
    lane = lane_of((toks, LANES))
    cos_t = jnp.cos(angles)
    sin_t = jnp.sin(angles)
    my_rows = pl.ds(pl.multiple_of(me * toks, toks), toks)
    meta_all[my_rows, :] = jnp.where(
        lane < HALF, cos_t, jnp.where(lane < 2 * HALF, sin_t, jnp.where(lane == 2 * HALF, seg_col, pos_col))
    )

    def send(src, dst, send_sem, recv_sem, target):
        copy = pltpu.make_async_remote_copy(
            src_ref=src, dst_ref=dst, send_sem=send_sem, recv_sem=recv_sem,
            device_id={"sp": target}, device_id_type=pl.DeviceIdType.MESH,
        )
        copy.start()
        return copy

    phase("wait_dq")
    load_hid.wait()
    load_dq.wait()
    phase("qlat")
    qlat_all[my_rows, :] = rms_norm(dot(hid_v[...], wdq_v[...]), gain_q_ref[...]).astype(BF16)

    load_dkv.wait()
    phase("kvlat")
    down = dot_nt(hid_v[...], wdkv_v[...])
    c_kv = rms_norm(down[:, :kv_lat], gain_kv_ref[...])
    low, high = down[:, kv_lat:kv_lat + HALF], down[:, kv_lat + HALF:]
    cos_m, sin_m = cos_t[:, :HALF], sin_t[:, :HALF]
    k_new = jnp.concatenate([low * cos_m - high * sin_m, high * cos_m + low * sin_m], axis=1)
    new_lat[pl.ds(0, toks), :] = jnp.concatenate([c_kv, k_new], axis=1).astype(BF16)
    phase("barrier")
    pl.semaphore_wait(barrier, n - 1)

    send_pre = send(pre_hbm, lat_t.at[:, pl.ds(pre, pre)], mate_send.at[0], mate_recv.at[0], mate)
    send_pseg = send(pseg_ref, pseg_mate, mate_send.at[1], mate_recv.at[1], mate)
    send_meta = [
        send(meta_all.at[my_rows], meta_all.at[my_rows], met_send.at[j - 1], met_recv.at[j - 1], lax.rem(me + j, n))
        for j in range(1, n)
    ]
    send_q = [
        send(qlat_all.at[my_rows], qlat_all.at[my_rows], gat_send.at[j - 1], gat_recv.at[j - 1], lax.rem(me + j, n))
        for j in range(1, n)
    ]
    send_new = send(new_lat.at[pl.ds(0, toks)], new_lat.at[pl.ds(toks, toks)], mate_send.at[2], mate_recv.at[2], mate)

    load_uq = load(
        wuq_hbm.at[:, pl.ds(pl.multiple_of(core * heads * QK_DIM, LANES), heads * QK_DIM)], wuq_v, load_sem.at[4]
    )
    load_o = load(
        wo_hbm.at[pl.ds(pl.multiple_of(core * heads * V_DIM, LANES), heads * V_DIM)], wo_v, load_sem.at[5]
    )

    def pair_weights(pair, offset):
        first = pl.multiple_of(pair * (2 * KV_HEAD) + offset, LANES)
        second = pl.multiple_of(pair * (2 * KV_HEAD) + KV_HEAD + offset, LANES)
        return jnp.concatenate([wukv_v[:, pl.ds(first, LANES)], wukv_v[:, pl.ds(second, LANES)]], axis=1)

    def raise_keys(start, size):
        def step(pair):
            up = dot_tn(pair_weights(pair, 0), lat_t[:kv_lat, pl.ds(start, size)]).astype(BF16)
            keys_t[2 * pair, :, pl.ds(start, size)] = up[:NOPE_DIM]
            keys_t[2 * pair + 1, :, pl.ds(start, size)] = up[NOPE_DIM:]
        return step

    def raise_values(start, size):
        def step(pair):
            values[pair, pl.ds(start, size), :] = dot(lat[pl.ds(start, size), :], pair_weights(pair, NOPE_DIM)).astype(BF16)
        return step

    def put_tail(start, size, seg_row):
        hot = seg_row == lax.broadcasted_iota(jnp.int32, (ROPE_DIM, size), 0)
        hot = jnp.where(hot, 1.0, 0.0).astype(BF16)
        rope = lat_t[kv_lat:, pl.ds(start, size)]
        tail_t[0, :, pl.ds(start, size)] = jnp.concatenate([rope, hot], axis=0)
        tail_t[1, :, pl.ds(start, size)] = jnp.concatenate([hot, rope], axis=0)

    phase("wait_pre")
    load_pre.wait()
    for copy in load_ukv:
        copy.wait()
    phase("keys_own")
    lat[pl.ds(0, pre), :] = jnp.transpose(lat_t[:kv_lat, pl.ds(0, pre)])
    put_tail(0, pre, pseg_ref[...])
    values[:, pl.ds(old + new, wide - old - new), :] = jnp.zeros((heads // 2, wide - old - new, 2 * V_DIM), BF16)
    unrolled(heads // 2, UNROLL_KV, raise_keys(0, pre))
    unrolled(heads // 2, UNROLL_KV, raise_values(0, pre))

    phase("wait_meta")
    for copy in send_meta:
        copy.wait_recv()
    phase("wait_mate")
    send_pre.wait_recv()
    send_pseg.wait_recv()
    send_new.wait_recv()
    phase("keys_mate")
    every = meta_all[...]
    lanes = lane_of((all_toks, LANES))
    q_seg = every[:, 2 * HALF:2 * HALF + 1]
    q_pos = every[:, 2 * HALF + 1:2 * HALF + 2]
    cos_q = jnp.where(lanes < HALF, every, 0.0)
    cos_q = cos_q + turn(cos_q, HALF)
    cos_all[...] = cos_q + turn(cos_q, 2 * HALF)
    sin_q = jnp.where((lanes >= HALF) & (lanes < 2 * HALF), every, 0.0)
    sin_q = sin_q - turn(sin_q, LANES - HALF)
    sin_all[...] = sin_q + turn(sin_q, 2 * HALF)
    q_mask = jnp.where(q_seg == jnp.where(lanes < ROPE_DIM, lanes, lanes - ROPE_DIM).astype(F32), 0.0, NEG_BIG)
    mask_a[...] = q_mask
    mate_rows = pl.ds(pl.multiple_of(mate * toks, toks), toks)
    new_meta = jnp.concatenate(
        [meta_all[my_rows, :], meta_all[mate_rows, :], jnp.zeros((LANES - new, LANES), F32)], axis=0
    )
    meta_rows = jnp.transpose(new_meta)
    k_seg, k_pos = meta_rows[2 * HALF:2 * HALF + 1], meta_rows[2 * HALF + 1:2 * HALF + 2]
    seen = (q_seg == k_seg) & (k_pos <= q_pos) & (lane_of((all_toks, LANES)) < new)
    bias[...] = jnp.where(seen, 0.0, NEG_BIG)

    lat[pl.ds(pre, pre), :] = jnp.transpose(lat_t[:kv_lat, pl.ds(pre, pre)])
    lat[pl.ds(old, new), :] = new_lat[:, :kv_lat]
    new_wide = jnp.concatenate([new_lat[...].astype(F32), jnp.zeros((LANES - new, kv_lat + ROPE_DIM), F32)], axis=0)
    lat_t[:, pl.ds(old, LANES)] = jnp.transpose(new_wide).astype(BF16)
    put_tail(pre, pre, pseg_mate[...])
    put_tail(old, LANES, jnp.full((1, LANES), -1, jnp.int32))
    unrolled(heads // 2, UNROLL_KV, raise_keys(pre, wide - pre))

    phase("wait_uq")
    load_uq.wait()
    for copy in send_q:
        copy.wait_recv()
    phase("queries")
    low_half = lane_of((all_toks, LANES)) < ROPE_DIM
    first_half = lax.rem(lane_of((all_toks, LANES)), ROPE_DIM) < HALF

    def raise_queries(pair):
        cols = pl.ds(pl.multiple_of(pair * (2 * QK_DIM), LANES), 2 * QK_DIM)
        q = dot(qlat_all[...], wuq_v[:, cols])
        nope_a, mid, end = q[:, :LANES], q[:, LANES:2 * LANES], q[:, 2 * LANES:]
        nope_b = turn(jnp.where(low_half, end, mid), ROPE_DIM)
        u = jnp.where(low_half, mid, end)
        swapped = jnp.where(first_half, turn(u, LANES - HALF), turn(u, HALF))
        r = u * cos_all[...] + swapped * sin_all[...]
        queries[2 * pair] = jnp.concatenate([nope_a, jnp.where(low_half, r, mask_a[...])], axis=1).astype(BF16)
        queries[2 * pair + 1] = jnp.concatenate([nope_b, jnp.where(low_half, mask_a[...], r)], axis=1).astype(BF16)

    unrolled(heads // 2, UNROLL_KV, raise_queries)

    phase("score")

    def score(head, j):
        s = dot(queries[head], jnp.concatenate([keys_t[head], tail_t[j % 2]], axis=0))
        scores[j, :, :old] = s[:, :old]
        scores[j, :, old:] = s[:, old:] + bias[...]
        step = 16
        tops = [jnp.max(scores[j, r:r + step, :], axis=1, keepdims=True) for r in range(0, all_toks, step)]
        for i, top in enumerate(tops):
            rows = pl.ds(i * step, step)
            p = jnp.exp2((scores[j, rows, :] - top) * EXP_SCALE)
            probs[head, rows, :] = p.astype(BF16)
            tops_all[head, rows, :] = jnp.broadcast_to(top, (step, LANES))
            sums_all[head, rows, :] = jnp.broadcast_to(jnp.sum(p, axis=1, keepdims=True), (step, LANES))

    raise_mate = raise_values(pre, pre + new)
    groups = heads // UNROLL_SCORE

    def score_group(i, carry):
        for j in range(UNROLL_SCORE):
            score(i * UNROLL_SCORE + j, j)
            if j % 2 == 0 and j // 2 < V_IN_SCORE:
                raise_mate(i * V_IN_SCORE + j // 2)
        return carry

    lax.fori_loop(0, groups, score_group, 0)

    phase("stats")

    def peer(j):
        return lax.rem(chip + j, chips)

    packed = jnp.zeros((all_toks, LANES), F32)
    for head in range(heads):
        packed = jnp.where(lanes == head, tops_all[head], packed)
        packed = jnp.where(lanes == heads + head, sums_all[head], packed)
    stats[...] = jnp.transpose(packed)[:2 * heads]
    send_stats = [
        send(stats, stats_rx.at[j - 1], st_send.at[j - 1], st_recv.at[j - 1], peer(j) * CORES + core)
        for j in range(1, chips)
    ]
    phase("values_mate")
    for pair in range(groups * V_IN_SCORE, heads // 2):
        raise_mate(pair)

    def attend(pair):
        for i in range(2):
            cols = pl.ds(pl.multiple_of((2 * pair + i) * V_DIM, LANES), V_DIM)
            acc[:, cols] = dot(probs[2 * pair + i], values[pair, :, i * V_DIM:(i + 1) * V_DIM])

    unrolled(heads // 2, UNROLL_PV, attend)

    phase("wait_stats")
    for copy in send_stats:
        copy.wait_recv()
    phase("scale")
    tops = [stats[:heads, :]] + [stats_rx[j, :heads, :] for j in range(chips - 1)]
    sums = [stats[heads:, :]] + [stats_rx[j, heads:, :] for j in range(chips - 1)]
    top = functools.reduce(jnp.maximum, tops)
    shares = [jnp.exp2((t - top) * EXP_SCALE) for t in tops]
    total = functools.reduce(jnp.add, [s * w for s, w in zip(sums, shares)])
    scale = jnp.transpose(shares[0] / total)
    scales[:, :heads] = scale
    load_o.wait()
    phase("outproj")
    width = wo_v.shape[1]
    spans = [(at, min(N_CHUNK, width - at)) for at in range(0, width, N_CHUNK)]
    pair_copies, red_copies = [], {}
    both = CORES * toks
    half = len(ORDER[0]) * both

    def put_split(g):
        for b, j in enumerate(ORDER[g]):
            from_rows = pl.ds(pl.multiple_of(peer(j) * both, both), both)
            factor = scales[from_rows, :]
            for head in range(heads):
                cols = pl.ds(head * V_DIM, V_DIM)
                o = acc[from_rows, cols] * factor[:, head:head + 1]
                o_hi = o.astype(BF16)
                split[g, pl.ds(b * both, both), cols] = o_hi
                split[g, pl.ds(half + b * both, both), cols] = (o - o_hi.astype(F32)).astype(BF16)

    def project(g, i):
        at, size = spans[i]
        cols = pl.ds(at, size)
        y = dot(split[g], wo_v[:, cols])
        y = (y[:half] + y[half:]).reshape(len(ORDER[g]), CORES, toks, size)
        first, second = y[:, 0].reshape(half // CORES, size), y[:, 1].reshape(half // CORES, size)
        y_mine[g, :, cols] = jnp.where(core == 0, first, second)
        y_out[g, :, cols] = jnp.where(core == 0, second, first)
        pair_copies.append(send(
            y_out.at[g, :, cols], y_rx.at[g, :, cols], pair_send.at[g, i], pair_recv.at[g, i], mate
        ))

    def reduce_chunk(g, i):
        at, size = spans[i]
        cols = pl.ds(at, size)
        pair_copies[g * len(spans) + i].wait_recv()
        z[g, :, cols] = y_mine[g, :, cols] + y_rx[g, :, cols]
        for b, j in enumerate(ORDER[g]):
            if j:
                red_copies[j, i] = send(
                    z.at[g, pl.ds(b * toks, toks), cols], z_rx.at[j - 1, :, cols],
                    red_send.at[j - 1, i], red_recv.at[j - 1, i], peer(j) * CORES + core,
                )

    steps = [(g, i) for g in range(len(ORDER)) for i in range(len(spans))]
    put_split(0)
    for at, (g, i) in enumerate(steps):
        project(g, i)
        if at == 0:
            put_split(1)
        if at >= LAG:
            reduce_chunk(*steps[at - LAG])
    phase("last_pair")
    for at in range(len(steps) - LAG, len(steps)):
        reduce_chunk(*steps[at])
    phase("reduce")
    for i, (at, size) in enumerate(spans):
        cols = pl.ds(at, size)
        y = z[1, pl.ds(toks, toks), cols]
        for j in range(1, chips):
            red_copies[j, i].wait_recv()
            y = y + z_rx[j - 1, :, cols]
        out_ref[:, cols] = y.astype(BF16)

    phase("drain")
    for copy in [send_pre, send_pseg, send_new] + send_meta + send_q + send_stats + pair_copies + list(red_copies.values()):
        copy.wait_send()
    phase("")


def solution(mesh):
    n = mesh.shape["sp"]
    chips = n // CORES
    tok_spec = P(("dp", "sp"), None)
    vec_spec = P(("dp", "sp"))
    mat_spec = P(None, None)
    gain_spec = P(None)

    def device_step(hidden, seg_ids, positions, prefix_lat, prefix_seg, w_dq, gain_q, w_uq, w_dkv, gain_kv, w_ukv, w_o):
        toks, width = hidden.shape
        pre, lat_dim = prefix_lat.shape
        q_lat = w_dq.shape[1]
        kv_lat = w_ukv.shape[0]
        heads = w_o.shape[0] // V_DIM // CORES
        rows = CORES * (pre + toks)
        wide = CORES * pre + LANES
        all_toks = n * toks
        n_chunks = -(-width // N_CHUNK)
        inv_freq = (ROPE_BASE ** (-np.arange(HALF, dtype=np.float64) / HALF)).astype(np.float32)
        freq = jnp.asarray(np.concatenate([inv_freq] * (LANES // HALF)).reshape(1, LANES))
        vmem = pl.BlockSpec(memory_space=pltpu.VMEM)
        hbm = pl.BlockSpec(memory_space=pl.ANY)
        dma = pltpu.SemaphoreType.DMA
        table = pltpu.VMEM((all_toks, LANES), F32)
        part = pltpu.VMEM((2, all_toks // 4, width), F32)
        return pl.pallas_call(
            functools.partial(kernel, n),
            out_shape=jax.ShapeDtypeStruct((toks, width), BF16),
            in_specs=[vmem] * 6 + [hbm] * 7,
            out_specs=vmem,
            scratch_shapes=[
                pltpu.VMEM((toks, width), BF16),
                pltpu.VMEM((width, q_lat), BF16),
                pltpu.VMEM((lat_dim, width), BF16),
                pltpu.VMEM((q_lat, heads * QK_DIM), BF16),
                pltpu.VMEM((kv_lat, heads * KV_HEAD), BF16),
                pltpu.VMEM((heads * V_DIM, width), BF16),
                pltpu.VMEM((lat_dim, wide), BF16),
                pltpu.VMEM((rows, kv_lat), BF16),
                pltpu.VMEM((CORES * toks, lat_dim), BF16),
                pltpu.VMEM((1, pre), jnp.int32),
                pltpu.VMEM((all_toks, q_lat), BF16),
                table, table, table, table,
                pltpu.VMEM((2, LANES, wide), BF16),
                pltpu.VMEM((heads, NOPE_DIM, wide), BF16),
                pltpu.VMEM((heads // 2, wide, 2 * V_DIM), BF16),
                pltpu.VMEM((heads, all_toks, 2 * LANES), BF16),
                pltpu.VMEM((heads, all_toks, wide), BF16),
                pltpu.VMEM((heads, all_toks, LANES), F32),
                pltpu.VMEM((heads, all_toks, LANES), F32),
                pltpu.VMEM((UNROLL_SCORE, all_toks, wide), F32),
                pltpu.VMEM((2 * heads, all_toks), F32),
                pltpu.VMEM((chips - 1, 2 * heads, all_toks), F32),
                pltpu.VMEM((all_toks, heads * V_DIM), F32),
                table,
                pltpu.VMEM((2, all_toks, heads * V_DIM), BF16),
                table,
                part, part, part, part,
                pltpu.VMEM((chips - 1, toks, width), F32),
                dma((6,)),
                dma((KV_LOADS,)),
                dma((3,)), dma((3,)),
                dma((n - 1,)), dma((n - 1,)),
                dma((n - 1,)), dma((n - 1,)),
                dma((chips - 1,)), dma((chips - 1,)),
                dma((2, n_chunks)), dma((2, n_chunks)),
                dma((chips - 1, n_chunks)), dma((chips - 1, n_chunks)),
            ],
            compiler_params=pltpu.CompilerParams(
                collective_id=0, has_side_effects=True, vmem_limit_bytes=60 * 1024 * 1024
            ),
        )(
            freq, seg_ids.reshape(1, toks), positions.reshape(1, toks), prefix_seg.reshape(1, pre),
            gain_q, gain_kv,
            hidden, prefix_lat.T, w_dq, w_uq, w_dkv.T, w_ukv, w_o,
        )

    return jax.shard_map(
        device_step,
        mesh=mesh,
        in_specs=(tok_spec, vec_spec, vec_spec, tok_spec, vec_spec, mat_spec, gain_spec, mat_spec, mat_spec, gain_spec, mat_spec, mat_spec),
        out_specs=tok_spec,
        check_vma=False,
    )
```

```python
import functools
import math

import jax
import jax.numpy as jnp
import numpy as np
from jax import lax
from jax.experimental import pallas as pl
from jax.experimental.pallas import tpu as pltpu
from jax.sharding import PartitionSpec as P

ROPE_DIM = 64
HALF = ROPE_DIM // 2
NOPE_DIM = 128
V_DIM = 128
QK_DIM = NOPE_DIM + ROPE_DIM
KV_HEAD = NOPE_DIM + V_DIM
CORES = 2
EPS = 1e-6
ROPE_BASE = 10000.0
NEG_BIG = -1e30
EXP_SCALE = QK_DIM ** -0.5 * math.log2(math.e)
LANES = 128
N_CHUNK = 512
ORDER = ((2, 1), (3, 0))
PARTS = 2
KV_LOADS = 4
UNROLL_KV = 8
SCORE_BUFS = 4

F32 = jnp.float32
BF16 = jnp.bfloat16


def dot(a, b):
    return jnp.dot(a, b, preferred_element_type=F32)


def dot_nt(a, b):
    return lax.dot_general(a, b, (((1,), (1,)), ((), ())), preferred_element_type=F32)


def dot_tn(a, b):
    return lax.dot_general(a, b, (((0,), (0,)), ((), ())), preferred_element_type=F32)


def rms_norm(values, gain):
    inv_rms = lax.rsqrt(jnp.mean(values * values, axis=-1, keepdims=True) + EPS)
    return values * inv_rms * gain.astype(F32).reshape(1, gain.shape[0])


def row_to_column(row):
    size = row.shape[1]
    here = lax.broadcasted_iota(jnp.int32, (size, size), 0) == lax.broadcasted_iota(jnp.int32, (size, size), 1)
    return jnp.sum(jnp.where(here, jnp.broadcast_to(row, (size, size)), 0.0), axis=1, keepdims=True)


def lane_of(shape):
    return lax.broadcasted_iota(jnp.int32, shape, len(shape) - 1)


def turn(x, amount):
    return pltpu.roll(x, amount, 1)


def unrolled(count, step, body):
    if count == step:
        for j in range(step):
            body(j)
        return

    def run(i, carry):
        for j in range(step):
            body(i * step + j)
        return carry

    lax.fori_loop(0, count // step, run, 0)


class Phases:
    def __init__(self):
        self.now = None

    def __call__(self, name):
        if self.now is not None:
            self.now.__exit__(None, None, None)
        self.now = None
        if name:
            self.now = jax.named_scope(name)
            self.now.__enter__()


def kernel(
    n,
    freq_ref, seg_ref, pos_ref, pseg_ref, gain_q_ref, gain_kv_ref,
    hid_hbm, pre_hbm, wdq_hbm, wuq_hbm, wdkv_hbm, wukv_hbm, wo_hbm,
    out_ref,
    hid_v, wdq_v, wdkv_v, wuq_v, wukv_v, wo_v,
    lat_t, lat, new_lat, pseg_mate, qlat_all, meta_all, cos_all, sin_all, mask_a, tail_t,
    keys_t, values, queries, probs, tops_all, sums_all,
    scores, stats, stats_rx, acc, scales, split, bias, y_part, y_mine, y_out, y_rx, z, z_rx,
    load_sem, ukv_sem, mate_send, mate_recv, gat_send, gat_recv, met_send, met_recv,
    st_send, st_recv, pair_send, pair_recv, red_send, red_recv,
):
    phase = Phases()
    me = lax.axis_index("sp")
    core = lax.rem(me, CORES)
    chip = lax.div(me, CORES)
    chips = n // CORES
    mate = chip * CORES + (CORES - 1 - core)
    toks = hid_v.shape[0]
    pre = pre_hbm.shape[1]
    kv_lat = wukv_v.shape[0]
    heads = keys_t.shape[0]
    old = CORES * pre
    new = CORES * toks
    wide = lat_t.shape[1]
    all_toks = n * toks

    phase("loads")

    def load(src, dst, sem):
        copy = pltpu.make_async_copy(src, dst, sem)
        copy.start()
        return copy

    barrier = pltpu.get_barrier_semaphore()
    for j in range(1, n):
        pl.semaphore_signal(barrier, inc=1, device_id={"sp": lax.rem(me + j, n)}, device_id_type=pl.DeviceIdType.MESH)
    load_hid = load(hid_hbm, hid_v, load_sem.at[0])
    load_dq = load(wdq_hbm, wdq_v, load_sem.at[1])
    load_dkv = load(wdkv_hbm, wdkv_v, load_sem.at[2])
    load_pre = load(pre_hbm, lat_t.at[:, pl.ds(0, pre)], load_sem.at[3])
    kv_cols = heads * KV_HEAD
    part = kv_cols // KV_LOADS
    load_ukv = [
        load(
            wukv_hbm.at[:, pl.ds(pl.multiple_of(core * kv_cols + i * part, LANES), part)],
            wukv_v.at[:, pl.ds(i * part, part)],
            ukv_sem.at[i],
        )
        for i in range(KV_LOADS)
    ]

    phase("meta")
    pos_col = row_to_column(pos_ref[...].astype(F32))
    seg_col = row_to_column(seg_ref[...].astype(F32))
    angles = pos_col * freq_ref[...]
    lane = lane_of((toks, LANES))
    cos_t = jnp.cos(angles)
    sin_t = jnp.sin(angles)
    my_rows = pl.ds(pl.multiple_of(me * toks, toks), toks)
    meta_all[my_rows, :] = jnp.where(
        lane < HALF, cos_t, jnp.where(lane < 2 * HALF, sin_t, jnp.where(lane == 2 * HALF, seg_col, pos_col))
    )

    def send(src, dst, send_sem, recv_sem, target):
        copy = pltpu.make_async_remote_copy(
            src_ref=src, dst_ref=dst, send_sem=send_sem, recv_sem=recv_sem,
            device_id={"sp": target}, device_id_type=pl.DeviceIdType.MESH,
        )
        copy.start()
        return copy

    phase("wait_dq")
    load_hid.wait()
    load_dq.wait()
    phase("barrier")
    pl.semaphore_wait(barrier, n - 1)
    send_pre = send(pre_hbm, lat_t.at[:, pl.ds(pre, pre)], mate_send.at[0], mate_recv.at[0], mate)
    send_pseg = send(pseg_ref, pseg_mate, mate_send.at[1], mate_recv.at[1], mate)
    send_meta = [
        send(meta_all.at[my_rows], meta_all.at[my_rows], met_send.at[j - 1], met_recv.at[j - 1], lax.rem(me + j, n))
        for j in range(1, n)
    ]
    phase("qlat")
    qlat_all[my_rows, :] = rms_norm(dot(hid_v[...], wdq_v[...]), gain_q_ref[...]).astype(BF16)

    send_q = [
        send(qlat_all.at[my_rows], qlat_all.at[my_rows], gat_send.at[j - 1], gat_recv.at[j - 1], lax.rem(me + j, n))
        for j in range(1, n)
    ]
    load_dkv.wait()
    phase("kvlat")
    down = dot_nt(hid_v[...], wdkv_v[...])
    c_kv = rms_norm(down[:, :kv_lat], gain_kv_ref[...])
    low, high = down[:, kv_lat:kv_lat + HALF], down[:, kv_lat + HALF:]
    cos_m, sin_m = cos_t[:, :HALF], sin_t[:, :HALF]
    k_new = jnp.concatenate([low * cos_m - high * sin_m, high * cos_m + low * sin_m], axis=1)
    new_lat[pl.ds(0, toks), :] = jnp.concatenate([c_kv, k_new], axis=1).astype(BF16)
    send_new = send(new_lat.at[pl.ds(0, toks)], new_lat.at[pl.ds(toks, toks)], mate_send.at[2], mate_recv.at[2], mate)

    load_uq = load(
        wuq_hbm.at[:, pl.ds(pl.multiple_of(core * heads * QK_DIM, LANES), heads * QK_DIM)], wuq_v, load_sem.at[4]
    )
    load_o = load(
        wo_hbm.at[pl.ds(pl.multiple_of(core * heads * V_DIM, LANES), heads * V_DIM)], wo_v, load_sem.at[5]
    )

    def pair_weights(pair, offset):
        first = pl.multiple_of(pair * (2 * KV_HEAD) + offset, LANES)
        second = pl.multiple_of(pair * (2 * KV_HEAD) + KV_HEAD + offset, LANES)
        return jnp.concatenate([wukv_v[:, pl.ds(first, LANES)], wukv_v[:, pl.ds(second, LANES)]], axis=1)

    def raise_keys(start, size):
        def step(pair):
            up = dot_tn(pair_weights(pair, 0), lat_t[:kv_lat, pl.ds(start, size)]).astype(BF16)
            keys_t[2 * pair, :, pl.ds(start, size)] = up[:NOPE_DIM]
            keys_t[2 * pair + 1, :, pl.ds(start, size)] = up[NOPE_DIM:]
        return step

    def raise_values(start, size):
        def step(pair):
            values[pair, pl.ds(start, size), :] = dot(lat[pl.ds(start, size), :], pair_weights(pair, NOPE_DIM)).astype(BF16)
        return step

    def put_tail(start, size, seg_row):
        hot = seg_row == lax.broadcasted_iota(jnp.int32, (ROPE_DIM, size), 0)
        hot = jnp.where(hot, 1.0, 0.0).astype(BF16)
        rope = lat_t[kv_lat:, pl.ds(start, size)]
        tail_t[0, :, pl.ds(start, size)] = jnp.concatenate([rope, hot], axis=0)
        tail_t[1, :, pl.ds(start, size)] = jnp.concatenate([hot, rope], axis=0)

    phase("wait_pre")
    load_pre.wait()
    for copy in load_ukv:
        copy.wait()
    phase("keys_own")
    lat[pl.ds(0, pre), :] = jnp.transpose(lat_t[:kv_lat, pl.ds(0, pre)])
    put_tail(0, pre, pseg_ref[...])
    values[:, pl.ds(old + new, wide - old - new), :] = jnp.zeros((heads // 2, wide - old - new, 2 * V_DIM), BF16)
    unrolled(heads // 2, UNROLL_KV, raise_keys(0, pre))
    unrolled(heads // 2, UNROLL_KV, raise_values(0, pre))

    phase("wait_meta")
    for copy in send_meta:
        copy.wait_recv()
    phase("wait_mate")
    send_pre.wait_recv()
    send_pseg.wait_recv()
    send_new.wait_recv()
    phase("keys_mate")
    every = meta_all[...]
    lanes = lane_of((all_toks, LANES))
    q_seg = every[:, 2 * HALF:2 * HALF + 1]
    q_pos = every[:, 2 * HALF + 1:2 * HALF + 2]
    cos_q = jnp.where(lanes < HALF, every, 0.0)
    cos_q = cos_q + turn(cos_q, HALF)
    cos_all[...] = cos_q + turn(cos_q, 2 * HALF)
    sin_q = jnp.where((lanes >= HALF) & (lanes < 2 * HALF), every, 0.0)
    sin_q = sin_q - turn(sin_q, LANES - HALF)
    sin_all[...] = sin_q + turn(sin_q, 2 * HALF)
    q_mask = jnp.where(q_seg == jnp.where(lanes < ROPE_DIM, lanes, lanes - ROPE_DIM).astype(F32), 0.0, NEG_BIG)
    mask_a[...] = q_mask
    mate_rows = pl.ds(pl.multiple_of(mate * toks, toks), toks)
    new_meta = jnp.concatenate(
        [meta_all[my_rows, :], meta_all[mate_rows, :], jnp.zeros((LANES - new, LANES), F32)], axis=0
    )
    meta_rows = jnp.transpose(new_meta)
    k_seg, k_pos = meta_rows[2 * HALF:2 * HALF + 1], meta_rows[2 * HALF + 1:2 * HALF + 2]
    seen = (q_seg == k_seg) & (k_pos <= q_pos) & (lane_of((all_toks, LANES)) < new)
    bias[...] = jnp.where(seen, 0.0, NEG_BIG)

    lat[pl.ds(pre, pre), :] = jnp.transpose(lat_t[:kv_lat, pl.ds(pre, pre)])
    lat[pl.ds(old, new), :] = new_lat[:, :kv_lat]
    new_wide = jnp.concatenate([new_lat[...].astype(F32), jnp.zeros((LANES - new, kv_lat + ROPE_DIM), F32)], axis=0)
    lat_t[:, pl.ds(old, LANES)] = jnp.transpose(new_wide).astype(BF16)
    put_tail(pre, pre, pseg_mate[...])
    put_tail(old, LANES, jnp.full((1, LANES), -1, jnp.int32))
    unrolled(heads // 2, UNROLL_KV, raise_keys(pre, wide - pre))

    phase("wait_uq")
    load_uq.wait()
    for copy in send_q:
        copy.wait_recv()
    phase("queries")
    low_half = lane_of((all_toks, LANES)) < ROPE_DIM
    first_half = lax.rem(lane_of((all_toks, LANES)), ROPE_DIM) < HALF

    def raise_queries(pair):
        cols = pl.ds(pl.multiple_of(pair * (2 * QK_DIM), LANES), 2 * QK_DIM)
        q = dot(qlat_all[...], wuq_v[:, cols])
        nope_a, mid, end = q[:, :LANES], q[:, LANES:2 * LANES], q[:, 2 * LANES:]
        nope_b = turn(jnp.where(low_half, end, mid), ROPE_DIM)
        u = jnp.where(low_half, mid, end)
        swapped = jnp.where(first_half, turn(u, LANES - HALF), turn(u, HALF))
        r = u * cos_all[...] + swapped * sin_all[...]
        queries[2 * pair] = jnp.concatenate([nope_a, jnp.where(low_half, r, mask_a[...])], axis=1).astype(BF16)
        queries[2 * pair + 1] = jnp.concatenate([nope_b, jnp.where(low_half, mask_a[...], r)], axis=1).astype(BF16)

    unrolled(heads // 2, UNROLL_KV, raise_queries)

    phase("score")

    def score(head, j):
        s = dot(queries[head], jnp.concatenate([keys_t[head], tail_t[j % 2]], axis=0))
        scores[j, :, :old] = s[:, :old]
        scores[j, :, old:] = s[:, old:] + bias[...]
        step = 16
        tops = [jnp.max(scores[j, r:r + step, :], axis=1, keepdims=True) for r in range(0, all_toks, step)]
        for i, top in enumerate(tops):
            rows = pl.ds(i * step, step)
            p = jnp.exp2((scores[j, rows, :] - top) * EXP_SCALE)
            probs[head, rows, :] = p.astype(BF16)
            tops_all[head, rows, :] = jnp.broadcast_to(top, (step, LANES))
            sums_all[head, rows, :] = jnp.broadcast_to(jnp.sum(p, axis=1, keepdims=True), (step, LANES))

    raise_mate = raise_values(pre, pre + new)
    some = heads // PARTS

    def peer(j):
        return lax.rem(chip + j, chips)

    send_stats = []
    for part in range(PARTS):
        packed = jnp.zeros((all_toks, LANES), F32)
        for head in range(part * some, (part + 1) * some):
            score(head, head % SCORE_BUFS)
            if head % 2 == 0:
                raise_mate(head // 2)
        for i in range(some):
            packed = jnp.where(lanes == i, tops_all[part * some + i], packed)
            packed = jnp.where(lanes == some + i, sums_all[part * some + i], packed)
        stats[part] = jnp.transpose(packed)[:2 * some]
        send_stats.append([
            send(stats.at[part], stats_rx.at[part, j - 1], st_send.at[part, j - 1], st_recv.at[part, j - 1], peer(j) * CORES + core)
            for j in range(1, chips)
        ])
    phase("attend")
    for head in range(heads):
        cols = pl.ds((head % 2) * V_DIM, V_DIM)
        acc[:, pl.ds(head * V_DIM, V_DIM)] = dot(probs[head], values[head // 2, :, cols])

    width = wo_v.shape[1]
    spans = [(at, min(N_CHUNK, width - at)) for at in range(0, width, N_CHUNK)]
    pair_copies, red_copies = {}, {}
    both = CORES * toks
    half = len(ORDER[0]) * both

    def put_scale(part):
        tops = [stats[part, :some, :]] + [stats_rx[part, j, :some, :] for j in range(chips - 1)]
        sums = [stats[part, some:, :]] + [stats_rx[part, j, some:, :] for j in range(chips - 1)]
        top = functools.reduce(jnp.maximum, tops)
        shares = [jnp.exp2((t - top) * EXP_SCALE) for t in tops]
        total = functools.reduce(jnp.add, [s * w for s, w in zip(sums, shares)])
        scales[part, :, :some] = jnp.transpose(shares[0] / total)

    def put_split(part, g):
        for b, j in enumerate(ORDER[g]):
            from_rows = pl.ds(pl.multiple_of(peer(j) * both, both), both)
            factor = scales[part, from_rows, :]
            for i in range(some):
                cols = pl.ds((part * some + i) * V_DIM, V_DIM)
                o = acc[from_rows, cols] * factor[:, i:i + 1]
                o_hi = o.astype(BF16)
                split[g, pl.ds(b * both, both), cols] = o_hi
                split[g, pl.ds(half + b * both, both), cols] = (o - o_hi.astype(F32)).astype(BF16)

    def project(part, g, i):
        at, size = spans[i]
        deep = pl.ds(part * some * V_DIM, some * V_DIM)
        y = dot(split[g, :, deep], wo_v[deep, pl.ds(at, size)])
        return y[:half] + y[half:]

    def finish(g, i):
        at, size = spans[i]
        cols = pl.ds(at, size)
        y = project(PARTS - 1, g, i)
        if PARTS > 1:
            y = y + y_part[g, :, cols]
        y = y.reshape(len(ORDER[g]), CORES, toks, size)
        first, second = y[:, 0].reshape(half // CORES, size), y[:, 1].reshape(half // CORES, size)
        y_mine[g, :, cols] = jnp.where(core == 0, first, second)
        y_out[g, :, cols] = jnp.where(core == 0, second, first)
        pair_copies[g, i] = send(
            y_out.at[g, :, cols], y_rx.at[g, :, cols], pair_send.at[g, i], pair_recv.at[g, i], mate
        )

    def reduce_chunk(g, i):
        at, size = spans[i]
        cols = pl.ds(at, size)
        pair_copies[g, i].wait_recv()
        z[g, :, cols] = y_mine[g, :, cols] + y_rx[g, :, cols]
        for b, j in enumerate(ORDER[g]):
            if j:
                red_copies[j, i] = send(
                    z.at[g, pl.ds(b * toks, toks), cols], z_rx.at[j - 1, :, cols],
                    red_send.at[j - 1, i], red_recv.at[j - 1, i], peer(j) * CORES + core,
                )

    phase("wait_o")
    load_o.wait()
    steps = [(g, i) for g in range(len(ORDER)) for i in range(len(spans))]
    for part in range(PARTS):
        phase(f"wait_stats{part}")
        for copy in send_stats[part]:
            copy.wait_recv()
        phase(f"outproj{part}")
        put_scale(part)
        for g in range(len(ORDER)):
            put_split(part, g)
            for i, (at, size) in enumerate(spans):
                if part < PARTS - 1:
                    y_part[g, :, pl.ds(at, size)] = project(part, g, i)
                else:
                    finish(g, i)
    phase("pairs")
    for step in steps:
        reduce_chunk(*step)
    for j in (1, 3, 2):
        phase(f"wait_red{j}")
        for i in range(len(spans)):
            red_copies[j, i].wait_recv()
    phase("reduce")
    for i, (at, size) in enumerate(spans):
        cols = pl.ds(at, size)
        y = z[1, pl.ds(toks, toks), cols]
        for j in range(1, chips):
            y = y + z_rx[j - 1, :, cols]
        out_ref[:, cols] = y.astype(BF16)

    phase("drain")
    for copy in [send_pre, send_pseg, send_new] + send_meta + send_q + sum(send_stats, []) + list(pair_copies.values()) + list(red_copies.values()):
        copy.wait_send()
    phase("")


def solution(mesh):
    n = mesh.shape["sp"]
    chips = n // CORES
    tok_spec = P(("dp", "sp"), None)
    vec_spec = P(("dp", "sp"))
    mat_spec = P(None, None)
    gain_spec = P(None)

    def device_step(hidden, seg_ids, positions, prefix_lat, prefix_seg, w_dq, gain_q, w_uq, w_dkv, gain_kv, w_ukv, w_o):
        toks, width = hidden.shape
        pre, lat_dim = prefix_lat.shape
        q_lat = w_dq.shape[1]
        kv_lat = w_ukv.shape[0]
        heads = w_o.shape[0] // V_DIM // CORES
        rows = CORES * (pre + toks)
        wide = CORES * pre + LANES
        all_toks = n * toks
        n_chunks = -(-width // N_CHUNK)
        inv_freq = (ROPE_BASE ** (-np.arange(HALF, dtype=np.float64) / HALF)).astype(np.float32)
        freq = jnp.asarray(np.concatenate([inv_freq] * (LANES // HALF)).reshape(1, LANES))
        vmem = pl.BlockSpec(memory_space=pltpu.VMEM)
        hbm = pl.BlockSpec(memory_space=pl.ANY)
        dma = pltpu.SemaphoreType.DMA
        table = pltpu.VMEM((all_toks, LANES), F32)
        part = pltpu.VMEM((2, all_toks // 4, width), F32)
        return pl.pallas_call(
            functools.partial(kernel, n),
            out_shape=jax.ShapeDtypeStruct((toks, width), BF16),
            in_specs=[vmem] * 6 + [hbm] * 7,
            out_specs=vmem,
            scratch_shapes=[
                pltpu.VMEM((toks, width), BF16),
                pltpu.VMEM((width, q_lat), BF16),
                pltpu.VMEM((lat_dim, width), BF16),
                pltpu.VMEM((q_lat, heads * QK_DIM), BF16),
                pltpu.VMEM((kv_lat, heads * KV_HEAD), BF16),
                pltpu.VMEM((heads * V_DIM, width), BF16),
                pltpu.VMEM((lat_dim, wide), BF16),
                pltpu.VMEM((rows, kv_lat), BF16),
                pltpu.VMEM((CORES * toks, lat_dim), BF16),
                pltpu.VMEM((1, pre), jnp.int32),
                pltpu.VMEM((all_toks, q_lat), BF16),
                table, table, table, table,
                pltpu.VMEM((2, LANES, wide), BF16),
                pltpu.VMEM((heads, NOPE_DIM, wide), BF16),
                pltpu.VMEM((heads // 2, wide, 2 * V_DIM), BF16),
                pltpu.VMEM((heads, all_toks, 2 * LANES), BF16),
                pltpu.VMEM((heads, all_toks, wide), BF16),
                pltpu.VMEM((heads, all_toks, LANES), F32),
                pltpu.VMEM((heads, all_toks, LANES), F32),
                pltpu.VMEM((SCORE_BUFS, all_toks, wide), F32),
                pltpu.VMEM((PARTS, 2 * heads // PARTS, all_toks), F32),
                pltpu.VMEM((PARTS, chips - 1, 2 * heads // PARTS, all_toks), F32),
                pltpu.VMEM((all_toks, heads * V_DIM), F32),
                pltpu.VMEM((PARTS, all_toks, LANES), F32),
                pltpu.VMEM((2, all_toks, heads * V_DIM), BF16),
                table,
                pltpu.VMEM((2, all_toks // 2, width), F32),
                part, part, part, part,
                pltpu.VMEM((chips - 1, toks, width), F32),
                dma((6,)),
                dma((KV_LOADS,)),
                dma((3,)), dma((3,)),
                dma((n - 1,)), dma((n - 1,)),
                dma((n - 1,)), dma((n - 1,)),
                dma((PARTS, chips - 1)), dma((PARTS, chips - 1)),
                dma((2, n_chunks)), dma((2, n_chunks)),
                dma((chips - 1, n_chunks)), dma((chips - 1, n_chunks)),
            ],
            compiler_params=pltpu.CompilerParams(
                collective_id=0, has_side_effects=True, vmem_limit_bytes=60 * 1024 * 1024
            ),
        )(
            freq, seg_ids.reshape(1, toks), positions.reshape(1, toks), prefix_seg.reshape(1, pre),
            gain_q, gain_kv,
            hidden, prefix_lat.T, w_dq, w_uq, w_dkv.T, w_ukv, w_o,
        )

    return jax.shard_map(
        device_step,
        mesh=mesh,
        in_specs=(tok_spec, vec_spec, vec_spec, tok_spec, vec_spec, mat_spec, gain_spec, mat_spec, mat_spec, gain_spec, mat_spec, mat_spec),
        out_specs=tok_spec,
        check_vma=False,
    )
```

```python
import functools
import math

import jax
import jax.numpy as jnp
import numpy as np
from jax import lax
from jax.experimental import pallas as pl
from jax.experimental.pallas import tpu as pltpu
from jax.sharding import PartitionSpec as P

ROPE_DIM = 64
HALF = ROPE_DIM // 2
NOPE_DIM = 128
V_DIM = 128
QK_DIM = NOPE_DIM + ROPE_DIM
KV_HEAD = NOPE_DIM + V_DIM
CORES = 2
EPS = 1e-6
ROPE_BASE = 10000.0
NEG_BIG = -1e30
EXP_SCALE = QK_DIM ** -0.5 * math.log2(math.e)
LANES = 128
N_CHUNK = 1280
ORDER = ((2, 1), (3, 0))
PARTS = 2
KV_LOADS = 4
UNROLL_KV = 8
SCORE_BUFS = 4

F32 = jnp.float32
BF16 = jnp.bfloat16


def dot(a, b):
    return jnp.dot(a, b, preferred_element_type=F32)


def dot_nt(a, b):
    return lax.dot_general(a, b, (((1,), (1,)), ((), ())), preferred_element_type=F32)


def dot_tn(a, b):
    return lax.dot_general(a, b, (((0,), (0,)), ((), ())), preferred_element_type=F32)


def rms_norm(values, gain):
    inv_rms = lax.rsqrt(jnp.mean(values * values, axis=-1, keepdims=True) + EPS)
    return values * inv_rms * gain.astype(F32).reshape(1, gain.shape[0])


def row_to_column(row):
    size = row.shape[1]
    here = lax.broadcasted_iota(jnp.int32, (size, size), 0) == lax.broadcasted_iota(jnp.int32, (size, size), 1)
    return jnp.sum(jnp.where(here, jnp.broadcast_to(row, (size, size)), 0.0), axis=1, keepdims=True)


def lane_of(shape):
    return lax.broadcasted_iota(jnp.int32, shape, len(shape) - 1)


def turn(x, amount):
    return pltpu.roll(x, amount, 1)


def unrolled(count, step, body):
    if count == step:
        for j in range(step):
            body(j)
        return

    def run(i, carry):
        for j in range(step):
            body(i * step + j)
        return carry

    lax.fori_loop(0, count // step, run, 0)


class Phases:
    def __init__(self):
        self.now = None

    def __call__(self, name):
        if self.now is not None:
            self.now.__exit__(None, None, None)
        self.now = None
        if name:
            self.now = jax.named_scope(name)
            self.now.__enter__()


def kernel(
    n,
    freq_ref, seg_ref, pos_ref, pseg_ref, gain_q_ref, gain_kv_ref,
    hid_hbm, pre_hbm, wdq_hbm, wuq_hbm, wdkv_hbm, wukv_hbm, wo_hbm,
    out_ref,
    hid_v, wdq_v, wdkv_v, wuq_v, wukv_v, wo_v,
    lat_t, lat, new_lat, pseg_mate, qlat_all, meta_all, cos_all, sin_all, mask_a, tail_t,
    keys_t, values, queries, probs, tops_all, sums_all,
    scores, stats, stats_rx, acc, scales, split, bias, y_part, y_mine, y_out, y_rx, z, z_rx,
    load_sem, ukv_sem, mate_send, mate_recv, gat_send, gat_recv, met_send, met_recv,
    st_send, st_recv, pair_send, pair_recv, red_send, red_recv,
):
    phase = Phases()
    me = lax.axis_index("sp")
    core = lax.rem(me, CORES)
    chip = lax.div(me, CORES)
    chips = n // CORES
    mate = chip * CORES + (CORES - 1 - core)
    toks = hid_v.shape[0]
    pre = pre_hbm.shape[1]
    kv_lat = wukv_v.shape[0]
    heads = keys_t.shape[0]
    old = CORES * pre
    new = CORES * toks
    wide = lat_t.shape[1]
    all_toks = n * toks

    phase("loads")

    def load(src, dst, sem):
        copy = pltpu.make_async_copy(src, dst, sem)
        copy.start()
        return copy

    barrier = pltpu.get_barrier_semaphore()
    for j in range(1, n):
        pl.semaphore_signal(barrier, inc=1, device_id={"sp": lax.rem(me + j, n)}, device_id_type=pl.DeviceIdType.MESH)
    load_hid = load(hid_hbm, hid_v, load_sem.at[0])
    load_dq = load(wdq_hbm, wdq_v, load_sem.at[1])
    load_dkv = load(wdkv_hbm, wdkv_v, load_sem.at[2])
    load_pre = load(pre_hbm, lat_t.at[:, pl.ds(0, pre)], load_sem.at[3])
    kv_cols = heads * KV_HEAD
    part = kv_cols // KV_LOADS
    load_ukv = [
        load(
            wukv_hbm.at[:, pl.ds(pl.multiple_of(core * kv_cols + i * part, LANES), part)],
            wukv_v.at[:, pl.ds(i * part, part)],
            ukv_sem.at[i],
        )
        for i in range(KV_LOADS)
    ]

    phase("meta")
    pos_col = row_to_column(pos_ref[...].astype(F32))
    seg_col = row_to_column(seg_ref[...].astype(F32))
    angles = pos_col * freq_ref[...]
    lane = lane_of((toks, LANES))
    cos_t = jnp.cos(angles)
    sin_t = jnp.sin(angles)
    my_rows = pl.ds(pl.multiple_of(me * toks, toks), toks)
    meta_all[my_rows, :] = jnp.where(
        lane < HALF, cos_t, jnp.where(lane < 2 * HALF, sin_t, jnp.where(lane == 2 * HALF, seg_col, pos_col))
    )

    def send(src, dst, send_sem, recv_sem, target):
        copy = pltpu.make_async_remote_copy(
            src_ref=src, dst_ref=dst, send_sem=send_sem, recv_sem=recv_sem,
            device_id={"sp": target}, device_id_type=pl.DeviceIdType.MESH,
        )
        copy.start()
        return copy

    phase("wait_dq")
    load_hid.wait()
    load_dq.wait()
    phase("barrier")
    pl.semaphore_wait(barrier, n - 1)
    send_pre = send(pre_hbm, lat_t.at[:, pl.ds(pre, pre)], mate_send.at[0], mate_recv.at[0], mate)
    send_pseg = send(pseg_ref, pseg_mate, mate_send.at[1], mate_recv.at[1], mate)
    send_meta = [
        send(meta_all.at[my_rows], meta_all.at[my_rows], met_send.at[j - 1], met_recv.at[j - 1], lax.rem(me + j, n))
        for j in range(1, n)
    ]
    phase("qlat")
    qlat_all[my_rows, :] = rms_norm(dot(hid_v[...], wdq_v[...]), gain_q_ref[...]).astype(BF16)

    send_q = [
        send(qlat_all.at[my_rows], qlat_all.at[my_rows], gat_send.at[j - 1], gat_recv.at[j - 1], lax.rem(me + j, n))
        for j in range(1, n)
    ]
    load_dkv.wait()
    phase("kvlat")
    down = dot_nt(hid_v[...], wdkv_v[...])
    c_kv = rms_norm(down[:, :kv_lat], gain_kv_ref[...])
    low, high = down[:, kv_lat:kv_lat + HALF], down[:, kv_lat + HALF:]
    cos_m, sin_m = cos_t[:, :HALF], sin_t[:, :HALF]
    k_new = jnp.concatenate([low * cos_m - high * sin_m, high * cos_m + low * sin_m], axis=1)
    new_lat[pl.ds(0, toks), :] = jnp.concatenate([c_kv, k_new], axis=1).astype(BF16)
    send_new = send(new_lat.at[pl.ds(0, toks)], new_lat.at[pl.ds(toks, toks)], mate_send.at[2], mate_recv.at[2], mate)

    load_uq = load(
        wuq_hbm.at[:, pl.ds(pl.multiple_of(core * heads * QK_DIM, LANES), heads * QK_DIM)], wuq_v, load_sem.at[4]
    )
    load_o = load(
        wo_hbm.at[pl.ds(pl.multiple_of(core * heads * V_DIM, LANES), heads * V_DIM)], wo_v, load_sem.at[5]
    )

    def pair_weights(pair, offset):
        first = pl.multiple_of(pair * (2 * KV_HEAD) + offset, LANES)
        second = pl.multiple_of(pair * (2 * KV_HEAD) + KV_HEAD + offset, LANES)
        return jnp.concatenate([wukv_v[:, pl.ds(first, LANES)], wukv_v[:, pl.ds(second, LANES)]], axis=1)

    def raise_keys(start, size):
        def step(pair):
            up = dot_tn(pair_weights(pair, 0), lat_t[:kv_lat, pl.ds(start, size)]).astype(BF16)
            keys_t[2 * pair, :, pl.ds(start, size)] = up[:NOPE_DIM]
            keys_t[2 * pair + 1, :, pl.ds(start, size)] = up[NOPE_DIM:]
        return step

    def raise_values(start, size):
        def step(pair):
            values[pair, pl.ds(start, size), :] = dot(lat[pl.ds(start, size), :], pair_weights(pair, NOPE_DIM)).astype(BF16)
        return step

    def put_tail(start, size, seg_row):
        hot = seg_row == lax.broadcasted_iota(jnp.int32, (ROPE_DIM, size), 0)
        hot = jnp.where(hot, 1.0, 0.0).astype(BF16)
        rope = lat_t[kv_lat:, pl.ds(start, size)]
        tail_t[0, :, pl.ds(start, size)] = jnp.concatenate([rope, hot], axis=0)
        tail_t[1, :, pl.ds(start, size)] = jnp.concatenate([hot, rope], axis=0)

    phase("wait_pre")
    load_pre.wait()
    for copy in load_ukv:
        copy.wait()
    phase("keys_own")
    lat[pl.ds(0, pre), :] = jnp.transpose(lat_t[:kv_lat, pl.ds(0, pre)])
    put_tail(0, pre, pseg_ref[...])
    values[:, pl.ds(old + new, wide - old - new), :] = jnp.zeros((heads // 2, wide - old - new, 2 * V_DIM), BF16)
    unrolled(heads // 2, UNROLL_KV, raise_keys(0, pre))
    unrolled(heads // 2, UNROLL_KV, raise_values(0, pre))

    phase("wait_meta")
    for copy in send_meta:
        copy.wait_recv()
    phase("wait_mate")
    send_pre.wait_recv()
    send_pseg.wait_recv()
    send_new.wait_recv()
    phase("keys_mate")
    every = meta_all[...]
    lanes = lane_of((all_toks, LANES))
    q_seg = every[:, 2 * HALF:2 * HALF + 1]
    q_pos = every[:, 2 * HALF + 1:2 * HALF + 2]
    cos_q = jnp.where(lanes < HALF, every, 0.0)
    cos_q = cos_q + turn(cos_q, HALF)
    cos_all[...] = cos_q + turn(cos_q, 2 * HALF)
    sin_q = jnp.where((lanes >= HALF) & (lanes < 2 * HALF), every, 0.0)
    sin_q = sin_q - turn(sin_q, LANES - HALF)
    sin_all[...] = sin_q + turn(sin_q, 2 * HALF)
    q_mask = jnp.where(q_seg == jnp.where(lanes < ROPE_DIM, lanes, lanes - ROPE_DIM).astype(F32), 0.0, NEG_BIG)
    mask_a[...] = q_mask
    mate_rows = pl.ds(pl.multiple_of(mate * toks, toks), toks)
    new_meta = jnp.concatenate(
        [meta_all[my_rows, :], meta_all[mate_rows, :], jnp.zeros((LANES - new, LANES), F32)], axis=0
    )
    meta_rows = jnp.transpose(new_meta)
    k_seg, k_pos = meta_rows[2 * HALF:2 * HALF + 1], meta_rows[2 * HALF + 1:2 * HALF + 2]
    seen = (q_seg == k_seg) & (k_pos <= q_pos) & (lane_of((all_toks, LANES)) < new)
    bias[...] = jnp.where(seen, 0.0, NEG_BIG)

    lat[pl.ds(pre, pre), :] = jnp.transpose(lat_t[:kv_lat, pl.ds(pre, pre)])
    lat[pl.ds(old, new), :] = new_lat[:, :kv_lat]
    new_wide = jnp.concatenate([new_lat[...].astype(F32), jnp.zeros((LANES - new, kv_lat + ROPE_DIM), F32)], axis=0)
    lat_t[:, pl.ds(old, LANES)] = jnp.transpose(new_wide).astype(BF16)
    put_tail(pre, pre, pseg_mate[...])
    put_tail(old, LANES, jnp.full((1, LANES), -1, jnp.int32))
    unrolled(heads // 2, UNROLL_KV, raise_keys(pre, wide - pre))

    phase("wait_uq")
    load_uq.wait()
    for copy in send_q:
        copy.wait_recv()
    phase("queries")
    low_half = lane_of((all_toks, LANES)) < ROPE_DIM
    first_half = lax.rem(lane_of((all_toks, LANES)), ROPE_DIM) < HALF

    def raise_queries(pair):
        cols = pl.ds(pl.multiple_of(pair * (2 * QK_DIM), LANES), 2 * QK_DIM)
        q = dot(qlat_all[...], wuq_v[:, cols])
        nope_a, mid, end = q[:, :LANES], q[:, LANES:2 * LANES], q[:, 2 * LANES:]
        nope_b = turn(jnp.where(low_half, end, mid), ROPE_DIM)
        u = jnp.where(low_half, mid, end)
        swapped = jnp.where(first_half, turn(u, LANES - HALF), turn(u, HALF))
        r = u * cos_all[...] + swapped * sin_all[...]
        queries[2 * pair] = jnp.concatenate([nope_a, jnp.where(low_half, r, mask_a[...])], axis=1).astype(BF16)
        queries[2 * pair + 1] = jnp.concatenate([nope_b, jnp.where(low_half, mask_a[...], r)], axis=1).astype(BF16)

    unrolled(heads // 2, UNROLL_KV, raise_queries)

    phase("score")

    def score(head, j):
        s = dot(queries[head], jnp.concatenate([keys_t[head], tail_t[j % 2]], axis=0))
        scores[j, :, :old] = s[:, :old]
        scores[j, :, old:] = s[:, old:] + bias[...]
        step = 16
        tops = [jnp.max(scores[j, r:r + step, :], axis=1, keepdims=True) for r in range(0, all_toks, step)]
        for i, top in enumerate(tops):
            rows = pl.ds(i * step, step)
            p = jnp.exp2((scores[j, rows, :] - top) * EXP_SCALE)
            probs[head, rows, :] = p.astype(BF16)
            tops_all[head, rows, :] = jnp.broadcast_to(top, (step, LANES))
            sums_all[head, rows, :] = jnp.broadcast_to(jnp.sum(p, axis=1, keepdims=True), (step, LANES))

    raise_mate = raise_values(pre, pre + new)
    some = heads // PARTS

    def peer(j):
        return lax.rem(chip + j, chips)

    send_stats = []
    for part in range(PARTS):
        packed = jnp.zeros((all_toks, LANES), F32)
        for head in range(part * some, (part + 1) * some):
            score(head, head % SCORE_BUFS)
            if head % 2 == 0:
                raise_mate(head // 2)
        for i in range(some):
            packed = jnp.where(lanes == i, tops_all[part * some + i], packed)
            packed = jnp.where(lanes == some + i, sums_all[part * some + i], packed)
        stats[part] = jnp.transpose(packed)[:2 * some]
        send_stats.append([
            send(stats.at[part], stats_rx.at[part, j - 1], st_send.at[part, j - 1], st_recv.at[part, j - 1], peer(j) * CORES + core)
            for j in range(1, chips)
        ])
    phase("attend")
    for head in range(heads):
        cols = pl.ds((head % 2) * V_DIM, V_DIM)
        acc[:, pl.ds(head * V_DIM, V_DIM)] = dot(probs[head], values[head // 2, :, cols])

    width = wo_v.shape[1]
    spans = [(at, min(N_CHUNK, width - at)) for at in range(0, width, N_CHUNK)]
    pair_copies, red_copies = {}, {}
    both = CORES * toks
    half = len(ORDER[0]) * both

    def put_scale(part):
        tops = [stats[part, :some, :]] + [stats_rx[part, j, :some, :] for j in range(chips - 1)]
        sums = [stats[part, some:, :]] + [stats_rx[part, j, some:, :] for j in range(chips - 1)]
        top = functools.reduce(jnp.maximum, tops)
        shares = [jnp.exp2((t - top) * EXP_SCALE) for t in tops]
        total = functools.reduce(jnp.add, [s * w for s, w in zip(sums, shares)])
        scales[part, :, :some] = jnp.transpose(shares[0] / total)

    def put_split(part, g):
        for b, j in enumerate(ORDER[g]):
            from_rows = pl.ds(pl.multiple_of(peer(j) * both, both), both)
            factor = scales[part, from_rows, :]
            for i in range(some):
                cols = pl.ds((part * some + i) * V_DIM, V_DIM)
                o = acc[from_rows, cols] * factor[:, i:i + 1]
                o_hi = o.astype(BF16)
                split[g, pl.ds(b * both, both), cols] = o_hi
                split[g, pl.ds(half + b * both, both), cols] = (o - o_hi.astype(F32)).astype(BF16)

    def project(part, g, i):
        at, size = spans[i]
        deep = pl.ds(part * some * V_DIM, some * V_DIM)
        y = dot(split[g, :, deep], wo_v[deep, pl.ds(at, size)])
        return y[:half] + y[half:]

    def finish(g, i):
        at, size = spans[i]
        cols = pl.ds(at, size)
        y = project(PARTS - 1, g, i)
        if PARTS > 1:
            y = y + y_part[g, :, cols]
        y = y.reshape(len(ORDER[g]), CORES, toks, size)
        first, second = y[:, 0].reshape(half // CORES, size), y[:, 1].reshape(half // CORES, size)
        y_mine[g, :, cols] = jnp.where(core == 0, first, second)
        y_out[g, :, cols] = jnp.where(core == 0, second, first)
        pair_copies[g, i] = send(
            y_out.at[g, :, cols], y_rx.at[g, :, cols], pair_send.at[g, i], pair_recv.at[g, i], mate
        )

    def reduce_chunk(g, i):
        at, size = spans[i]
        cols = pl.ds(at, size)
        pair_copies[g, i].wait_recv()
        z[g, :, cols] = y_mine[g, :, cols] + y_rx[g, :, cols]
        for b, j in enumerate(ORDER[g]):
            if j:
                red_copies[j, i] = send(
                    z.at[g, pl.ds(b * toks, toks), cols], z_rx.at[j - 1, :, cols],
                    red_send.at[j - 1, i], red_recv.at[j - 1, i], peer(j) * CORES + core,
                )

    phase("wait_o")
    load_o.wait()
    steps = [(g, i) for g in range(len(ORDER)) for i in range(len(spans))]
    for part in range(PARTS):
        phase(f"wait_stats{part}")
        for copy in send_stats[part]:
            copy.wait_recv()
        phase(f"outproj{part}")
        put_scale(part)
        for g in range(len(ORDER)):
            put_split(part, g)
            for i, (at, size) in enumerate(spans):
                if part < PARTS - 1:
                    y_part[g, :, pl.ds(at, size)] = project(part, g, i)
                else:
                    finish(g, i)
    phase("pairs")
    for step in steps:
        reduce_chunk(*step)
    for j in (1, 3, 2):
        phase(f"wait_red{j}")
        for i in range(len(spans)):
            red_copies[j, i].wait_recv()
    phase("reduce")
    for i, (at, size) in enumerate(spans):
        cols = pl.ds(at, size)
        y = z[1, pl.ds(toks, toks), cols]
        for j in range(1, chips):
            y = y + z_rx[j - 1, :, cols]
        out_ref[:, cols] = y.astype(BF16)

    phase("drain")
    for copy in [send_pre, send_pseg, send_new] + send_meta + send_q + sum(send_stats, []) + list(pair_copies.values()) + list(red_copies.values()):
        copy.wait_send()
    phase("")


def solution(mesh):
    n = mesh.shape["sp"]
    chips = n // CORES
    tok_spec = P(("dp", "sp"), None)
    vec_spec = P(("dp", "sp"))
    mat_spec = P(None, None)
    gain_spec = P(None)

    def device_step(hidden, seg_ids, positions, prefix_lat, prefix_seg, w_dq, gain_q, w_uq, w_dkv, gain_kv, w_ukv, w_o):
        toks, width = hidden.shape
        pre, lat_dim = prefix_lat.shape
        q_lat = w_dq.shape[1]
        kv_lat = w_ukv.shape[0]
        heads = w_o.shape[0] // V_DIM // CORES
        rows = CORES * (pre + toks)
        wide = CORES * pre + LANES
        all_toks = n * toks
        n_chunks = -(-width // N_CHUNK)
        inv_freq = (ROPE_BASE ** (-np.arange(HALF, dtype=np.float64) / HALF)).astype(np.float32)
        freq = jnp.asarray(np.concatenate([inv_freq] * (LANES // HALF)).reshape(1, LANES))
        vmem = pl.BlockSpec(memory_space=pltpu.VMEM)
        hbm = pl.BlockSpec(memory_space=pl.ANY)
        dma = pltpu.SemaphoreType.DMA
        table = pltpu.VMEM((all_toks, LANES), F32)
        part = pltpu.VMEM((2, all_toks // 4, width), F32)
        return pl.pallas_call(
            functools.partial(kernel, n),
            out_shape=jax.ShapeDtypeStruct((toks, width), BF16),
            in_specs=[vmem] * 6 + [hbm] * 7,
            out_specs=vmem,
            scratch_shapes=[
                pltpu.VMEM((toks, width), BF16),
                pltpu.VMEM((width, q_lat), BF16),
                pltpu.VMEM((lat_dim, width), BF16),
                pltpu.VMEM((q_lat, heads * QK_DIM), BF16),
                pltpu.VMEM((kv_lat, heads * KV_HEAD), BF16),
                pltpu.VMEM((heads * V_DIM, width), BF16),
                pltpu.VMEM((lat_dim, wide), BF16),
                pltpu.VMEM((rows, kv_lat), BF16),
                pltpu.VMEM((CORES * toks, lat_dim), BF16),
                pltpu.VMEM((1, pre), jnp.int32),
                pltpu.VMEM((all_toks, q_lat), BF16),
                table, table, table, table,
                pltpu.VMEM((2, LANES, wide), BF16),
                pltpu.VMEM((heads, NOPE_DIM, wide), BF16),
                pltpu.VMEM((heads // 2, wide, 2 * V_DIM), BF16),
                pltpu.VMEM((heads, all_toks, 2 * LANES), BF16),
                pltpu.VMEM((heads, all_toks, wide), BF16),
                pltpu.VMEM((heads, all_toks, LANES), F32),
                pltpu.VMEM((heads, all_toks, LANES), F32),
                pltpu.VMEM((SCORE_BUFS, all_toks, wide), F32),
                pltpu.VMEM((PARTS, 2 * heads // PARTS, all_toks), F32),
                pltpu.VMEM((PARTS, chips - 1, 2 * heads // PARTS, all_toks), F32),
                pltpu.VMEM((all_toks, heads * V_DIM), F32),
                pltpu.VMEM((PARTS, all_toks, LANES), F32),
                pltpu.VMEM((2, all_toks, heads * V_DIM), BF16),
                table,
                pltpu.VMEM((2, all_toks // 2, width), F32),
                part, part, part, part,
                pltpu.VMEM((chips - 1, toks, width), F32),
                dma((6,)),
                dma((KV_LOADS,)),
                dma((3,)), dma((3,)),
                dma((n - 1,)), dma((n - 1,)),
                dma((n - 1,)), dma((n - 1,)),
                dma((PARTS, chips - 1)), dma((PARTS, chips - 1)),
                dma((2, n_chunks)), dma((2, n_chunks)),
                dma((chips - 1, n_chunks)), dma((chips - 1, n_chunks)),
            ],
            compiler_params=pltpu.CompilerParams(
                collective_id=0, has_side_effects=True, vmem_limit_bytes=60 * 1024 * 1024
            ),
        )(
            freq, seg_ids.reshape(1, toks), positions.reshape(1, toks), prefix_seg.reshape(1, pre),
            gain_q, gain_kv,
            hidden, prefix_lat.T, w_dq, w_uq, w_dkv.T, w_ukv, w_o,
        )

    return jax.shard_map(
        device_step,
        mesh=mesh,
        in_specs=(tok_spec, vec_spec, vec_spec, tok_spec, vec_spec, mat_spec, gain_spec, mat_spec, mat_spec, gain_spec, mat_spec, mat_spec),
        out_specs=tok_spec,
        check_vma=False,
    )
```

```python
import functools
import math

import jax
import jax.numpy as jnp
import numpy as np
from jax import lax
from jax.experimental import pallas as pl
from jax.experimental.pallas import tpu as pltpu
from jax.sharding import PartitionSpec as P

ROPE_DIM = 64
HALF = ROPE_DIM // 2
NOPE_DIM = 128
V_DIM = 128
QK_DIM = NOPE_DIM + ROPE_DIM
KV_HEAD = NOPE_DIM + V_DIM
CORES = 2
EPS = 1e-6
ROPE_BASE = 10000.0
NEG_BIG = -1e30
EXP_SCALE = QK_DIM ** -0.5 * math.log2(math.e)
LANES = 128
N_CHUNK = 512
ORDER = ((2, 1), (3, 0))
PARTS = 2
KV_LOADS = 2
DQ_LOADS = 4
LATE_PAIRS = 3
UNROLL_KV = 8
SCORE_BUFS = 4

F32 = jnp.float32
BF16 = jnp.bfloat16


def dot(a, b):
    return jnp.dot(a, b, preferred_element_type=F32)


def dot_nt(a, b):
    return lax.dot_general(a, b, (((1,), (1,)), ((), ())), preferred_element_type=F32)


def dot_tn(a, b):
    return lax.dot_general(a, b, (((0,), (0,)), ((), ())), preferred_element_type=F32)


def rms_norm(values, gain):
    inv_rms = lax.rsqrt(jnp.mean(values * values, axis=-1, keepdims=True) + EPS)
    return values * inv_rms * gain.astype(F32).reshape(1, gain.shape[0])


def row_to_column(row):
    size = row.shape[1]
    here = lax.broadcasted_iota(jnp.int32, (size, size), 0) == lax.broadcasted_iota(jnp.int32, (size, size), 1)
    return jnp.sum(jnp.where(here, jnp.broadcast_to(row, (size, size)), 0.0), axis=1, keepdims=True)


def lane_of(shape):
    return lax.broadcasted_iota(jnp.int32, shape, len(shape) - 1)


def turn(x, amount):
    return pltpu.roll(x, amount, 1)


def unrolled(count, step, body):
    if count == step:
        for j in range(step):
            body(j)
        return

    def run(i, carry):
        for j in range(step):
            body(i * step + j)
        return carry

    lax.fori_loop(0, count // step, run, 0)


class Phases:
    def __init__(self):
        self.now = None

    def __call__(self, name):
        if self.now is not None:
            self.now.__exit__(None, None, None)
        self.now = None
        if name:
            self.now = jax.named_scope(name)
            self.now.__enter__()


def kernel(
    n,
    freq_hbm, seg_hbm, pos_hbm, pseg_hbm, gain_q_hbm, gain_kv_hbm,
    hid_hbm, pre_hbm, wdq_hbm, wuq_hbm, wdkv_hbm, wukv_hbm, wo_hbm,
    out_ref,
    freq_ref, seg_ref, pos_ref, pseg_ref, gain_q_ref, gain_kv_ref,
    hid_v, wdq_v, wdkv_v, wuq_v, wukv_v, wo_v,
    lat_t, lat, new_lat, pseg_mate, qlat_all, meta_all, cos_all, sin_all, mask_a, tail_t,
    keys_t, values, queries, probs, tops_all, sums_all,
    scores, stats, stats_rx, acc, scales, split, bias, y_part, y_mine, y_out, y_rx, z, z_rx,
    load_sem, small_sem, dq_sem, ukv_sem, mate_send, mate_recv, gat_send, gat_recv, met_send, met_recv,
    st_send, st_recv, pair_send, pair_recv, red_send, red_recv,
):
    phase = Phases()
    me = lax.axis_index("sp")
    core = lax.rem(me, CORES)
    chip = lax.div(me, CORES)
    chips = n // CORES
    mate = chip * CORES + (CORES - 1 - core)
    toks = hid_v.shape[0]
    pre = pre_hbm.shape[1]
    kv_lat = wukv_v.shape[0]
    heads = keys_t.shape[0]
    old = CORES * pre
    new = CORES * toks
    wide = lat_t.shape[1]
    all_toks = n * toks

    phase("loads")

    def load(src, dst, sem):
        copy = pltpu.make_async_copy(src, dst, sem)
        copy.start()
        return copy

    barrier = pltpu.get_barrier_semaphore()
    for j in range(1, n):
        pl.semaphore_signal(barrier, inc=1, device_id={"sp": lax.rem(me + j, n)}, device_id_type=pl.DeviceIdType.MESH)
    smalls = [
        load(src, dst, small_sem.at[i])
        for i, (src, dst) in enumerate([
            (freq_hbm, freq_ref), (seg_hbm, seg_ref), (pos_hbm, pos_ref),
            (gain_q_hbm, gain_q_ref), (gain_kv_hbm, gain_kv_ref), (pseg_hbm, pseg_ref),
        ])
    ]
    load_hid = load(hid_hbm, hid_v, load_sem.at[0])
    depth = wdq_v.shape[0] // DQ_LOADS
    load_dq = [
        load(wdq_hbm.at[pl.ds(i * depth, depth)], wdq_v.at[pl.ds(i * depth, depth)], dq_sem.at[i])
        for i in range(DQ_LOADS)
    ]
    load_pre = load(pre_hbm, lat_t.at[:, pl.ds(0, pre)], load_sem.at[3])
    kv_cols = heads * KV_HEAD
    part = kv_cols // KV_LOADS
    load_ukv = [
        load(
            wukv_hbm.at[:, pl.ds(pl.multiple_of(core * kv_cols + i * part, LANES), part)],
            wukv_v.at[:, pl.ds(i * part, part)],
            ukv_sem.at[i],
        )
        for i in range(KV_LOADS)
    ]
    load_dkv = load(wdkv_hbm, wdkv_v, load_sem.at[2])

    phase("wait_small")
    for copy in smalls:
        copy.wait()
    phase("meta")
    pos_col = row_to_column(pos_ref[...].astype(F32))
    seg_col = row_to_column(seg_ref[...].astype(F32))
    angles = pos_col * freq_ref[...]
    lane = lane_of((toks, LANES))
    cos_t = jnp.cos(angles)
    sin_t = jnp.sin(angles)
    my_rows = pl.ds(pl.multiple_of(me * toks, toks), toks)
    meta_all[my_rows, :] = jnp.where(
        lane < HALF, cos_t, jnp.where(lane < 2 * HALF, sin_t, jnp.where(lane == 2 * HALF, seg_col, pos_col))
    )

    def send(src, dst, send_sem, recv_sem, target):
        copy = pltpu.make_async_remote_copy(
            src_ref=src, dst_ref=dst, send_sem=send_sem, recv_sem=recv_sem,
            device_id={"sp": target}, device_id_type=pl.DeviceIdType.MESH,
        )
        copy.start()
        return copy

    phase("wait_dq")
    load_hid.wait()
    for copy in load_dq:
        copy.wait()
    phase("barrier")
    pl.semaphore_wait(barrier, n - 1)
    send_pre = send(pre_hbm, lat_t.at[:, pl.ds(pre, pre)], mate_send.at[0], mate_recv.at[0], mate)
    send_pseg = send(pseg_ref, pseg_mate, mate_send.at[1], mate_recv.at[1], mate)
    send_meta = [
        send(meta_all.at[my_rows], meta_all.at[my_rows], met_send.at[j - 1], met_recv.at[j - 1], lax.rem(me + j, n))
        for j in range(1, n)
    ]
    phase("qlat")
    qlat_all[my_rows, :] = rms_norm(dot(hid_v[...], wdq_v[...]), gain_q_ref[...]).astype(BF16)

    send_q = [
        send(qlat_all.at[my_rows], qlat_all.at[my_rows], gat_send.at[j - 1], gat_recv.at[j - 1], lax.rem(me + j, n))
        for j in range(1, n)
    ]
    phase("wait_pre")
    load_dkv.wait()
    load_pre.wait()
    for copy in load_ukv:
        copy.wait()
    phase("keys_own")
    down = dot_nt(hid_v[...], wdkv_v[...])
    c_kv = rms_norm(down[:, :kv_lat], gain_kv_ref[...])
    low, high = down[:, kv_lat:kv_lat + HALF], down[:, kv_lat + HALF:]
    cos_m, sin_m = cos_t[:, :HALF], sin_t[:, :HALF]
    k_new = jnp.concatenate([low * cos_m - high * sin_m, high * cos_m + low * sin_m], axis=1)
    new_lat[pl.ds(0, toks), :] = jnp.concatenate([c_kv, k_new], axis=1).astype(BF16)
    send_new = send(new_lat.at[pl.ds(0, toks)], new_lat.at[pl.ds(toks, toks)], mate_send.at[2], mate_recv.at[2], mate)

    load_uq = load(
        wuq_hbm.at[:, pl.ds(pl.multiple_of(core * heads * QK_DIM, LANES), heads * QK_DIM)], wuq_v, load_sem.at[4]
    )
    load_o = load(
        wo_hbm.at[pl.ds(pl.multiple_of(core * heads * V_DIM, LANES), heads * V_DIM)], wo_v, load_sem.at[5]
    )

    def pair_weights(pair, offset):
        first = pl.multiple_of(pair * (2 * KV_HEAD) + offset, LANES)
        second = pl.multiple_of(pair * (2 * KV_HEAD) + KV_HEAD + offset, LANES)
        return jnp.concatenate([wukv_v[:, pl.ds(first, LANES)], wukv_v[:, pl.ds(second, LANES)]], axis=1)

    def raise_keys(start, size):
        def step(pair):
            up = dot_tn(pair_weights(pair, 0), lat_t[:kv_lat, pl.ds(start, size)]).astype(BF16)
            keys_t[2 * pair, :, pl.ds(start, size)] = up[:NOPE_DIM]
            keys_t[2 * pair + 1, :, pl.ds(start, size)] = up[NOPE_DIM:]
        return step

    def raise_values(start, size):
        def step(pair):
            values[pair, pl.ds(start, size), :] = dot(lat[pl.ds(start, size), :], pair_weights(pair, NOPE_DIM)).astype(BF16)
        return step

    def put_tail(start, size, seg_row):
        hot = seg_row == lax.broadcasted_iota(jnp.int32, (ROPE_DIM, size), 0)
        hot = jnp.where(hot, 1.0, 0.0).astype(BF16)
        rope = lat_t[kv_lat:, pl.ds(start, size)]
        tail_t[0, :, pl.ds(start, size)] = jnp.concatenate([rope, hot], axis=0)
        tail_t[1, :, pl.ds(start, size)] = jnp.concatenate([hot, rope], axis=0)

    lat[pl.ds(0, pre), :] = jnp.transpose(lat_t[:kv_lat, pl.ds(0, pre)])
    put_tail(0, pre, pseg_ref[...])
    values[:, pl.ds(old + new, wide - old - new), :] = jnp.zeros((heads // 2, wide - old - new, 2 * V_DIM), BF16)
    unrolled(heads // 2, UNROLL_KV, raise_keys(0, pre))
    unrolled(heads // 2, UNROLL_KV, raise_values(0, pre))

    phase("wait_meta")
    for copy in send_meta:
        copy.wait_recv()
    phase("wait_mate")
    send_pre.wait_recv()
    send_pseg.wait_recv()
    send_new.wait_recv()
    phase("keys_mate")
    every = meta_all[...]
    lanes = lane_of((all_toks, LANES))
    q_seg = every[:, 2 * HALF:2 * HALF + 1]
    q_pos = every[:, 2 * HALF + 1:2 * HALF + 2]
    cos_q = jnp.where(lanes < HALF, every, 0.0)
    cos_q = cos_q + turn(cos_q, HALF)
    cos_all[...] = cos_q + turn(cos_q, 2 * HALF)
    sin_q = jnp.where((lanes >= HALF) & (lanes < 2 * HALF), every, 0.0)
    sin_q = sin_q - turn(sin_q, LANES - HALF)
    sin_all[...] = sin_q + turn(sin_q, 2 * HALF)
    q_mask = jnp.where(q_seg == jnp.where(lanes < ROPE_DIM, lanes, lanes - ROPE_DIM).astype(F32), 0.0, NEG_BIG)
    mask_a[...] = q_mask
    mate_rows = pl.ds(pl.multiple_of(mate * toks, toks), toks)
    new_meta = jnp.concatenate(
        [meta_all[my_rows, :], meta_all[mate_rows, :], jnp.zeros((LANES - new, LANES), F32)], axis=0
    )
    meta_rows = jnp.transpose(new_meta)
    k_seg, k_pos = meta_rows[2 * HALF:2 * HALF + 1], meta_rows[2 * HALF + 1:2 * HALF + 2]
    seen = (q_seg == k_seg) & (k_pos <= q_pos) & (lane_of((all_toks, LANES)) < new)
    bias[...] = jnp.where(seen, 0.0, NEG_BIG)

    lat[pl.ds(pre, pre), :] = jnp.transpose(lat_t[:kv_lat, pl.ds(pre, pre)])
    lat[pl.ds(old, new), :] = new_lat[:, :kv_lat]
    new_wide = jnp.concatenate([new_lat[...].astype(F32), jnp.zeros((LANES - new, kv_lat + ROPE_DIM), F32)], axis=0)
    lat_t[:, pl.ds(old, LANES)] = jnp.transpose(new_wide).astype(BF16)
    put_tail(pre, pre, pseg_mate[...])
    put_tail(old, LANES, jnp.full((1, LANES), -1, jnp.int32))
    unrolled(heads // 2, UNROLL_KV, raise_keys(pre, wide - pre))

    phase("wait_uq")
    load_uq.wait()
    for copy in send_q:
        copy.wait_recv()
    phase("queries")
    low_half = lane_of((all_toks, LANES)) < ROPE_DIM
    first_half = lax.rem(lane_of((all_toks, LANES)), ROPE_DIM) < HALF

    def raise_queries(pair):
        cols = pl.ds(pl.multiple_of(pair * (2 * QK_DIM), LANES), 2 * QK_DIM)
        q = dot(qlat_all[...], wuq_v[:, cols])
        nope_a, mid, end = q[:, :LANES], q[:, LANES:2 * LANES], q[:, 2 * LANES:]
        nope_b = turn(jnp.where(low_half, end, mid), ROPE_DIM)
        u = jnp.where(low_half, mid, end)
        swapped = jnp.where(first_half, turn(u, LANES - HALF), turn(u, HALF))
        r = u * cos_all[...] + swapped * sin_all[...]
        queries[2 * pair] = jnp.concatenate([nope_a, jnp.where(low_half, r, mask_a[...])], axis=1).astype(BF16)
        queries[2 * pair + 1] = jnp.concatenate([nope_b, jnp.where(low_half, mask_a[...], r)], axis=1).astype(BF16)

    unrolled(heads // 2, UNROLL_KV, raise_queries)

    phase("score")

    def score(head, j):
        s = dot(queries[head], jnp.concatenate([keys_t[head], tail_t[j % 2]], axis=0))
        scores[j, :, :old] = s[:, :old]
        scores[j, :, old:] = s[:, old:] + bias[...]
        step = 16
        tops = [jnp.max(scores[j, r:r + step, :], axis=1, keepdims=True) for r in range(0, all_toks, step)]
        for i, top in enumerate(tops):
            rows = pl.ds(i * step, step)
            p = jnp.exp2((scores[j, rows, :] - top) * EXP_SCALE)
            probs[head, rows, :] = p.astype(BF16)
            tops_all[head, rows, :] = jnp.broadcast_to(top, (step, LANES))
            sums_all[head, rows, :] = jnp.broadcast_to(jnp.sum(p, axis=1, keepdims=True), (step, LANES))

    raise_mate = raise_values(pre, pre + new)
    some = heads // PARTS

    def peer(j):
        return lax.rem(chip + j, chips)

    send_stats = []
    for part in range(PARTS):
        packed = jnp.zeros((all_toks, LANES), F32)
        for head in range(part * some, (part + 1) * some):
            score(head, head % SCORE_BUFS)
            if head % 2 == 0 and head // 2 < heads // 2 - LATE_PAIRS:
                raise_mate(head // 2)
        for i in range(some):
            packed = jnp.where(lanes == i, tops_all[part * some + i], packed)
            packed = jnp.where(lanes == some + i, sums_all[part * some + i], packed)
        stats[part] = jnp.transpose(packed)[:2 * some]
        send_stats.append([
            send(stats.at[part], stats_rx.at[part, j - 1], st_send.at[part, j - 1], st_recv.at[part, j - 1], peer(j) * CORES + core)
            for j in range(1, chips)
        ])
    phase("attend")
    for pair in range(heads // 2 - LATE_PAIRS, heads // 2):
        raise_mate(pair)
    for head in range(heads):
        cols = pl.ds((head % 2) * V_DIM, V_DIM)
        acc[:, pl.ds(head * V_DIM, V_DIM)] = dot(probs[head], values[head // 2, :, cols])

    width = wo_v.shape[1]
    spans = [(at, min(N_CHUNK, width - at)) for at in range(0, width, N_CHUNK)]
    pair_copies, red_copies = {}, {}
    both = CORES * toks
    half = len(ORDER[0]) * both

    def put_scale(part):
        tops = [stats[part, :some, :]] + [stats_rx[part, j, :some, :] for j in range(chips - 1)]
        sums = [stats[part, some:, :]] + [stats_rx[part, j, some:, :] for j in range(chips - 1)]
        top = functools.reduce(jnp.maximum, tops)
        shares = [jnp.exp2((t - top) * EXP_SCALE) for t in tops]
        total = functools.reduce(jnp.add, [s * w for s, w in zip(sums, shares)])
        scales[part, :, :some] = jnp.transpose(shares[0] / total)

    def put_split(part, g):
        for b, j in enumerate(ORDER[g]):
            from_rows = pl.ds(pl.multiple_of(peer(j) * both, both), both)
            factor = scales[part, from_rows, :]
            for i in range(some):
                cols = pl.ds((part * some + i) * V_DIM, V_DIM)
                o = acc[from_rows, cols] * factor[:, i:i + 1]
                o_hi = o.astype(BF16)
                split[g, pl.ds(b * both, both), cols] = o_hi
                split[g, pl.ds(half + b * both, both), cols] = (o - o_hi.astype(F32)).astype(BF16)

    def project(part, g, i):
        at, size = spans[i]
        deep = pl.ds(part * some * V_DIM, some * V_DIM)
        y = dot(split[g, :, deep], wo_v[deep, pl.ds(at, size)])
        return y[:half] + y[half:]

    def finish(g, i):
        at, size = spans[i]
        cols = pl.ds(at, size)
        y = project(PARTS - 1, g, i)
        if PARTS > 1:
            y = y + y_part[g, :, cols]
        y = y.reshape(len(ORDER[g]), CORES, toks, size)
        first, second = y[:, 0].reshape(half // CORES, size), y[:, 1].reshape(half // CORES, size)
        y_mine[g, :, cols] = jnp.where(core == 0, first, second)
        y_out[g, :, cols] = jnp.where(core == 0, second, first)
        pair_copies[g, i] = send(
            y_out.at[g, :, cols], y_rx.at[g, :, cols], pair_send.at[g, i], pair_recv.at[g, i], mate
        )

    def reduce_chunk(g, i):
        at, size = spans[i]
        cols = pl.ds(at, size)
        pair_copies[g, i].wait_recv()
        z[g, :, cols] = y_mine[g, :, cols] + y_rx[g, :, cols]
        for b, j in enumerate(ORDER[g]):
            if j:
                red_copies[j, i] = send(
                    z.at[g, pl.ds(b * toks, toks), cols], z_rx.at[j - 1, :, cols],
                    red_send.at[j - 1, i], red_recv.at[j - 1, i], peer(j) * CORES + core,
                )

    phase("wait_o")
    load_o.wait()
    steps = [(g, i) for g in range(len(ORDER)) for i in range(len(spans))]
    for part in range(PARTS):
        phase(f"wait_stats{part}")
        for copy in send_stats[part]:
            copy.wait_recv()
        phase(f"outproj{part}")
        put_scale(part)
        for g in range(len(ORDER)):
            put_split(part, g)
            for i, (at, size) in enumerate(spans):
                if part < PARTS - 1:
                    y_part[g, :, pl.ds(at, size)] = project(part, g, i)
                else:
                    finish(g, i)
    phase("pairs")
    for step in steps:
        reduce_chunk(*step)
    for j in (1, 3, 2):
        phase(f"wait_red{j}")
        for i in range(len(spans)):
            red_copies[j, i].wait_recv()
    phase("reduce")
    for i, (at, size) in enumerate(spans):
        cols = pl.ds(at, size)
        y = z[1, pl.ds(toks, toks), cols]
        for j in range(1, chips):
            y = y + z_rx[j - 1, :, cols]
        out_ref[:, cols] = y.astype(BF16)

    phase("drain")
    for copy in [send_pre, send_pseg, send_new] + send_meta + send_q + sum(send_stats, []) + list(pair_copies.values()) + list(red_copies.values()):
        copy.wait_send()
    phase("")


def solution(mesh):
    n = mesh.shape["sp"]
    chips = n // CORES
    tok_spec = P(("dp", "sp"), None)
    vec_spec = P(("dp", "sp"))
    mat_spec = P(None, None)
    gain_spec = P(None)

    def device_step(hidden, seg_ids, positions, prefix_lat, prefix_seg, w_dq, gain_q, w_uq, w_dkv, gain_kv, w_ukv, w_o):
        toks, width = hidden.shape
        pre, lat_dim = prefix_lat.shape
        q_lat = w_dq.shape[1]
        kv_lat = w_ukv.shape[0]
        heads = w_o.shape[0] // V_DIM // CORES
        rows = CORES * (pre + toks)
        wide = CORES * pre + LANES
        all_toks = n * toks
        n_chunks = -(-width // N_CHUNK)
        inv_freq = (ROPE_BASE ** (-np.arange(HALF, dtype=np.float64) / HALF)).astype(np.float32)
        freq = jnp.asarray(np.concatenate([inv_freq] * (LANES // HALF)).reshape(1, LANES))
        vmem = pl.BlockSpec(memory_space=pltpu.VMEM)
        hbm = pl.BlockSpec(memory_space=pltpu.HBM)
        dma = pltpu.SemaphoreType.DMA
        table = pltpu.VMEM((all_toks, LANES), F32)
        part = pltpu.VMEM((2, all_toks // 4, width), F32)
        return pl.pallas_call(
            functools.partial(kernel, n),
            out_shape=pltpu.VMEM((toks, width), BF16),
            in_specs=[hbm] * 13,
            scratch_shapes=[
                pltpu.VMEM((1, LANES), F32),
                pltpu.VMEM((1, toks), jnp.int32),
                pltpu.VMEM((1, toks), jnp.int32),
                pltpu.VMEM((1, pre), jnp.int32),
                pltpu.VMEM((q_lat,), BF16),
                pltpu.VMEM((kv_lat,), BF16),
                pltpu.VMEM((toks, width), BF16),
                pltpu.VMEM((width, q_lat), BF16),
                pltpu.VMEM((lat_dim, width), BF16),
                pltpu.VMEM((q_lat, heads * QK_DIM), BF16),
                pltpu.VMEM((kv_lat, heads * KV_HEAD), BF16),
                pltpu.VMEM((heads * V_DIM, width), BF16),
                pltpu.VMEM((lat_dim, wide), BF16),
                pltpu.VMEM((rows, kv_lat), BF16),
                pltpu.VMEM((CORES * toks, lat_dim), BF16),
                pltpu.VMEM((1, pre), jnp.int32),
                pltpu.VMEM((all_toks, q_lat), BF16),
                table, table, table, table,
                pltpu.VMEM((2, LANES, wide), BF16),
                pltpu.VMEM((heads, NOPE_DIM, wide), BF16),
                pltpu.VMEM((heads // 2, wide, 2 * V_DIM), BF16),
                pltpu.VMEM((heads, all_toks, 2 * LANES), BF16),
                pltpu.VMEM((heads, all_toks, wide), BF16),
                pltpu.VMEM((heads, all_toks, LANES), F32),
                pltpu.VMEM((heads, all_toks, LANES), F32),
                pltpu.VMEM((SCORE_BUFS, all_toks, wide), F32),
                pltpu.VMEM((PARTS, 2 * heads // PARTS, all_toks), F32),
                pltpu.VMEM((PARTS, chips - 1, 2 * heads // PARTS, all_toks), F32),
                pltpu.VMEM((all_toks, heads * V_DIM), F32),
                pltpu.VMEM((PARTS, all_toks, LANES), F32),
                pltpu.VMEM((2, all_toks, heads * V_DIM), BF16),
                table,
                pltpu.VMEM((2, all_toks // 2, width), F32),
                part, part, part, part,
                pltpu.VMEM((chips - 1, toks, width), F32),
                dma((6,)),
                dma((6,)),
                dma((DQ_LOADS,)),
                dma((KV_LOADS,)),
                dma((3,)), dma((3,)),
                dma((n - 1,)), dma((n - 1,)),
                dma((n - 1,)), dma((n - 1,)),
                dma((PARTS, chips - 1)), dma((PARTS, chips - 1)),
                dma((2, n_chunks)), dma((2, n_chunks)),
                dma((chips - 1, n_chunks)), dma((chips - 1, n_chunks)),
            ],
            compiler_params=pltpu.CompilerParams(
                collective_id=0, has_side_effects=True, vmem_limit_bytes=60 * 1024 * 1024
            ),
        )(
            freq, seg_ids.reshape(1, toks), positions.reshape(1, toks), prefix_seg.reshape(1, pre),
            gain_q, gain_kv,
            hidden, prefix_lat.T, w_dq, w_uq, w_dkv.T, w_ukv, w_o,
        )

    return jax.shard_map(
        device_step,
        mesh=mesh,
        in_specs=(tok_spec, vec_spec, vec_spec, tok_spec, vec_spec, mat_spec, gain_spec, mat_spec, mat_spec, gain_spec, mat_spec, mat_spec),
        out_specs=tok_spec,
        check_vma=False,
    )
```

```python
import functools
import math

import jax
import jax.numpy as jnp
import numpy as np
from jax import lax
from jax.experimental import pallas as pl
from jax.experimental.pallas import tpu as pltpu
from jax.sharding import PartitionSpec as P

ROPE_DIM = 64
HALF = ROPE_DIM // 2
NOPE_DIM = 128
V_DIM = 128
QK_DIM = NOPE_DIM + ROPE_DIM
KV_HEAD = NOPE_DIM + V_DIM
CORES = 2
EPS = 1e-6
ROPE_BASE = 10000.0
NEG_BIG = -1e30
EXP_SCALE = QK_DIM ** -0.5 * math.log2(math.e)
LANES = 128
N_CHUNK = 512
ORDER = ((2, 1), (3, 0))
PARTS = 2
KV_LOADS = 2
DQ_LOADS = 4
LATE_PAIRS = 3
UNROLL_KV = 8
SCORE_BUFS = 4

F32 = jnp.float32
BF16 = jnp.bfloat16


def dot(a, b):
    return jnp.dot(a, b, preferred_element_type=F32)


def dot_nt(a, b):
    return lax.dot_general(a, b, (((1,), (1,)), ((), ())), preferred_element_type=F32)


def dot_tn(a, b):
    return lax.dot_general(a, b, (((0,), (0,)), ((), ())), preferred_element_type=F32)


def rms_norm(values, gain):
    inv_rms = lax.rsqrt(jnp.mean(values * values, axis=-1, keepdims=True) + EPS)
    return values * inv_rms * gain.astype(F32).reshape(1, gain.shape[0])


def row_to_column(row):
    size = row.shape[1]
    here = lax.broadcasted_iota(jnp.int32, (size, size), 0) == lax.broadcasted_iota(jnp.int32, (size, size), 1)
    return jnp.sum(jnp.where(here, jnp.broadcast_to(row, (size, size)), 0.0), axis=1, keepdims=True)


def lane_of(shape):
    return lax.broadcasted_iota(jnp.int32, shape, len(shape) - 1)


def turn(x, amount):
    return pltpu.roll(x, amount, 1)


def unrolled(count, step, body):
    if count == step:
        for j in range(step):
            body(j)
        return

    def run(i, carry):
        for j in range(step):
            body(i * step + j)
        return carry

    lax.fori_loop(0, count // step, run, 0)


class Phases:
    def __init__(self):
        self.now = None

    def __call__(self, name):
        if self.now is not None:
            self.now.__exit__(None, None, None)
        self.now = None
        if name:
            self.now = jax.named_scope(name)
            self.now.__enter__()


def kernel(
    n,
    freq_hbm, seg_hbm, pos_hbm, pseg_hbm, gain_q_hbm, gain_kv_hbm,
    hid_hbm, pre_hbm, wdq_hbm, wuq_hbm, wdkv_hbm, wukv_hbm, wo_hbm,
    out_ref,
    freq_ref, seg_ref, pos_ref, pseg_ref, gain_q_ref, gain_kv_ref,
    hid_v, wdq_v, wdkv_v, wuq_v, wukv_v, wo_v,
    lat_t, lat, new_lat, pseg_mate, qlat_all, meta_all, cos_all, sin_all, mask_a, tail_t,
    keys_t, values, queries, probs, tops_all, sums_all,
    scores, stats, stats_rx, acc, scales, split, bias, y_part, y_mine, y_out, y_rx, z, z_rx,
    load_sem, small_sem, dq_sem, ukv_sem, mate_send, mate_recv, gat_send, gat_recv, met_send, met_recv,
    st_send, st_recv, pair_send, pair_recv, red_send, red_recv,
):
    phase = Phases()
    me = lax.axis_index("sp")
    core = lax.rem(me, CORES)
    chip = lax.div(me, CORES)
    chips = n // CORES
    mate = chip * CORES + (CORES - 1 - core)
    toks = hid_v.shape[0]
    pre = pre_hbm.shape[1]
    kv_lat = wukv_v.shape[0]
    heads = keys_t.shape[0]
    old = CORES * pre
    new = CORES * toks
    wide = lat_t.shape[1]
    all_toks = n * toks

    phase("loads")

    def load(src, dst, sem):
        copy = pltpu.make_async_copy(src, dst, sem)
        copy.start()
        return copy

    barrier = pltpu.get_barrier_semaphore()
    for j in range(1, n):
        pl.semaphore_signal(barrier, inc=1, device_id={"sp": lax.rem(me + j, n)}, device_id_type=pl.DeviceIdType.MESH)
    smalls = [
        load(src, dst, small_sem.at[i])
        for i, (src, dst) in enumerate([
            (freq_hbm, freq_ref), (seg_hbm, seg_ref), (pos_hbm, pos_ref),
            (gain_q_hbm, gain_q_ref), (gain_kv_hbm, gain_kv_ref), (pseg_hbm, pseg_ref),
        ])
    ]
    load_hid = load(hid_hbm, hid_v, load_sem.at[0])
    depth = wdq_v.shape[0] // DQ_LOADS
    load_dq = [
        load(wdq_hbm.at[pl.ds(i * depth, depth)], wdq_v.at[pl.ds(i * depth, depth)], dq_sem.at[i])
        for i in range(DQ_LOADS)
    ]
    kv_cols = heads * KV_HEAD
    part = kv_cols // KV_LOADS

    def load_up(i):
        return load(
            wukv_hbm.at[:, pl.ds(pl.multiple_of(core * kv_cols + i * part, LANES), part)],
            wukv_v.at[:, pl.ds(i * part, part)],
            ukv_sem.at[i],
        )

    phase("wait_small")
    for copy in smalls:
        copy.wait()
    load_pre = load(pre_hbm, lat_t.at[:, pl.ds(0, pre)], load_sem.at[3])
    load_ukv = [load_up(0)]
    phase("meta")
    pos_col = row_to_column(pos_ref[...].astype(F32))
    seg_col = row_to_column(seg_ref[...].astype(F32))
    angles = pos_col * freq_ref[...]
    lane = lane_of((toks, LANES))
    cos_t = jnp.cos(angles)
    sin_t = jnp.sin(angles)
    my_rows = pl.ds(pl.multiple_of(me * toks, toks), toks)
    meta_all[my_rows, :] = jnp.where(
        lane < HALF, cos_t, jnp.where(lane < 2 * HALF, sin_t, jnp.where(lane == 2 * HALF, seg_col, pos_col))
    )

    def send(src, dst, send_sem, recv_sem, target):
        copy = pltpu.make_async_remote_copy(
            src_ref=src, dst_ref=dst, send_sem=send_sem, recv_sem=recv_sem,
            device_id={"sp": target}, device_id_type=pl.DeviceIdType.MESH,
        )
        copy.start()
        return copy

    phase("wait_dq")
    load_hid.wait()
    for copy in load_dq:
        copy.wait()
    load_ukv += [load_up(i) for i in range(1, KV_LOADS)]
    load_dkv = load(wdkv_hbm, wdkv_v, load_sem.at[2])
    phase("barrier")
    pl.semaphore_wait(barrier, n - 1)
    send_pre = send(pre_hbm, lat_t.at[:, pl.ds(pre, pre)], mate_send.at[0], mate_recv.at[0], mate)
    send_pseg = send(pseg_ref, pseg_mate, mate_send.at[1], mate_recv.at[1], mate)
    send_meta = [
        send(meta_all.at[my_rows], meta_all.at[my_rows], met_send.at[j - 1], met_recv.at[j - 1], lax.rem(me + j, n))
        for j in range(1, n)
    ]
    phase("qlat")
    qlat_all[my_rows, :] = rms_norm(dot(hid_v[...], wdq_v[...]), gain_q_ref[...]).astype(BF16)

    send_q = [
        send(qlat_all.at[my_rows], qlat_all.at[my_rows], gat_send.at[j - 1], gat_recv.at[j - 1], lax.rem(me + j, n))
        for j in range(1, n)
    ]
    def pair_weights(pair, offset):
        first = pl.multiple_of(pair * (2 * KV_HEAD) + offset, LANES)
        second = pl.multiple_of(pair * (2 * KV_HEAD) + KV_HEAD + offset, LANES)
        return jnp.concatenate([wukv_v[:, pl.ds(first, LANES)], wukv_v[:, pl.ds(second, LANES)]], axis=1)

    def raise_keys(start, size):
        def step(pair):
            up = dot_tn(pair_weights(pair, 0), lat_t[:kv_lat, pl.ds(start, size)]).astype(BF16)
            keys_t[2 * pair, :, pl.ds(start, size)] = up[:NOPE_DIM]
            keys_t[2 * pair + 1, :, pl.ds(start, size)] = up[NOPE_DIM:]
        return step

    def raise_values(start, size):
        def step(pair):
            values[pair, pl.ds(start, size), :] = dot(lat[pl.ds(start, size), :], pair_weights(pair, NOPE_DIM)).astype(BF16)
        return step

    def put_tail(start, size, seg_row):
        hot = seg_row == lax.broadcasted_iota(jnp.int32, (ROPE_DIM, size), 0)
        hot = jnp.where(hot, 1.0, 0.0).astype(BF16)
        rope = lat_t[kv_lat:, pl.ds(start, size)]
        tail_t[0, :, pl.ds(start, size)] = jnp.concatenate([rope, hot], axis=0)
        tail_t[1, :, pl.ds(start, size)] = jnp.concatenate([hot, rope], axis=0)
    per = heads // 2 // KV_LOADS
    for i in range(KV_LOADS):
        phase(f"wait_own{i}")
        load_ukv[i].wait()
        if i == 0:
            load_pre.wait()
        else:
            load_dkv.wait()
        phase(f"own{i}")
        if i == 0:
            lat[pl.ds(0, pre), :] = jnp.transpose(lat_t[:kv_lat, pl.ds(0, pre)])
            put_tail(0, pre, pseg_ref[...])
            values[:, pl.ds(old + new, wide - old - new), :] = jnp.zeros((heads // 2, wide - old - new, 2 * V_DIM), BF16)
        else:
            down = dot_nt(hid_v[...], wdkv_v[...])
            c_kv = rms_norm(down[:, :kv_lat], gain_kv_ref[...])
            low, high = down[:, kv_lat:kv_lat + HALF], down[:, kv_lat + HALF:]
            cos_m, sin_m = cos_t[:, :HALF], sin_t[:, :HALF]
            k_new = jnp.concatenate([low * cos_m - high * sin_m, high * cos_m + low * sin_m], axis=1)
            new_lat[pl.ds(0, toks), :] = jnp.concatenate([c_kv, k_new], axis=1).astype(BF16)
            send_new = send(new_lat.at[pl.ds(0, toks)], new_lat.at[pl.ds(toks, toks)], mate_send.at[2], mate_recv.at[2], mate)

            load_uq = load(
                wuq_hbm.at[:, pl.ds(pl.multiple_of(core * heads * QK_DIM, LANES), heads * QK_DIM)], wuq_v, load_sem.at[4]
            )
            load_o = load(
                wo_hbm.at[pl.ds(pl.multiple_of(core * heads * V_DIM, LANES), heads * V_DIM)], wo_v, load_sem.at[5]
            )

        for pair in range(i * per, (i + 1) * per):
            raise_keys(0, pre)(pair)
            raise_values(0, pre)(pair)

    phase("wait_meta")
    for copy in send_meta:
        copy.wait_recv()
    phase("wait_mate")
    send_pre.wait_recv()
    send_pseg.wait_recv()
    send_new.wait_recv()
    phase("keys_mate")
    every = meta_all[...]
    lanes = lane_of((all_toks, LANES))
    q_seg = every[:, 2 * HALF:2 * HALF + 1]
    q_pos = every[:, 2 * HALF + 1:2 * HALF + 2]
    cos_q = jnp.where(lanes < HALF, every, 0.0)
    cos_q = cos_q + turn(cos_q, HALF)
    cos_all[...] = cos_q + turn(cos_q, 2 * HALF)
    sin_q = jnp.where((lanes >= HALF) & (lanes < 2 * HALF), every, 0.0)
    sin_q = sin_q - turn(sin_q, LANES - HALF)
    sin_all[...] = sin_q + turn(sin_q, 2 * HALF)
    q_mask = jnp.where(q_seg == jnp.where(lanes < ROPE_DIM, lanes, lanes - ROPE_DIM).astype(F32), 0.0, NEG_BIG)
    mask_a[...] = q_mask
    mate_rows = pl.ds(pl.multiple_of(mate * toks, toks), toks)
    new_meta = jnp.concatenate(
        [meta_all[my_rows, :], meta_all[mate_rows, :], jnp.zeros((LANES - new, LANES), F32)], axis=0
    )
    meta_rows = jnp.transpose(new_meta)
    k_seg, k_pos = meta_rows[2 * HALF:2 * HALF + 1], meta_rows[2 * HALF + 1:2 * HALF + 2]
    seen = (q_seg == k_seg) & (k_pos <= q_pos) & (lane_of((all_toks, LANES)) < new)
    bias[...] = jnp.where(seen, 0.0, NEG_BIG)

    lat[pl.ds(pre, pre), :] = jnp.transpose(lat_t[:kv_lat, pl.ds(pre, pre)])
    lat[pl.ds(old, new), :] = new_lat[:, :kv_lat]
    new_wide = jnp.concatenate([new_lat[...].astype(F32), jnp.zeros((LANES - new, kv_lat + ROPE_DIM), F32)], axis=0)
    lat_t[:, pl.ds(old, LANES)] = jnp.transpose(new_wide).astype(BF16)
    put_tail(pre, pre, pseg_mate[...])
    put_tail(old, LANES, jnp.full((1, LANES), -1, jnp.int32))
    unrolled(heads // 2, UNROLL_KV, raise_keys(pre, wide - pre))

    phase("wait_uq")
    load_uq.wait()
    for copy in send_q:
        copy.wait_recv()
    phase("queries")
    low_half = lane_of((all_toks, LANES)) < ROPE_DIM
    first_half = lax.rem(lane_of((all_toks, LANES)), ROPE_DIM) < HALF

    def raise_queries(pair):
        cols = pl.ds(pl.multiple_of(pair * (2 * QK_DIM), LANES), 2 * QK_DIM)
        q = dot(qlat_all[...], wuq_v[:, cols])
        nope_a, mid, end = q[:, :LANES], q[:, LANES:2 * LANES], q[:, 2 * LANES:]
        nope_b = turn(jnp.where(low_half, end, mid), ROPE_DIM)
        u = jnp.where(low_half, mid, end)
        swapped = jnp.where(first_half, turn(u, LANES - HALF), turn(u, HALF))
        r = u * cos_all[...] + swapped * sin_all[...]
        queries[2 * pair] = jnp.concatenate([nope_a, jnp.where(low_half, r, mask_a[...])], axis=1).astype(BF16)
        queries[2 * pair + 1] = jnp.concatenate([nope_b, jnp.where(low_half, mask_a[...], r)], axis=1).astype(BF16)

    unrolled(heads // 2, UNROLL_KV, raise_queries)

    phase("score")

    def score(head, j):
        s = dot(queries[head], jnp.concatenate([keys_t[head], tail_t[j % 2]], axis=0))
        scores[j, :, :old] = s[:, :old]
        scores[j, :, old:] = s[:, old:] + bias[...]
        step = 16
        tops = [jnp.max(scores[j, r:r + step, :], axis=1, keepdims=True) for r in range(0, all_toks, step)]
        for i, top in enumerate(tops):
            rows = pl.ds(i * step, step)
            p = jnp.exp2((scores[j, rows, :] - top) * EXP_SCALE)
            probs[head, rows, :] = p.astype(BF16)
            tops_all[head, rows, :] = jnp.broadcast_to(top, (step, LANES))
            sums_all[head, rows, :] = jnp.broadcast_to(jnp.sum(p, axis=1, keepdims=True), (step, LANES))

    raise_mate = raise_values(pre, pre + new)
    some = heads // PARTS

    def peer(j):
        return lax.rem(chip + j, chips)

    send_stats = []
    for part in range(PARTS):
        packed = jnp.zeros((all_toks, LANES), F32)
        for head in range(part * some, (part + 1) * some):
            score(head, head % SCORE_BUFS)
            if head % 2 == 0 and head // 2 < heads // 2 - LATE_PAIRS:
                raise_mate(head // 2)
        for i in range(some):
            packed = jnp.where(lanes == i, tops_all[part * some + i], packed)
            packed = jnp.where(lanes == some + i, sums_all[part * some + i], packed)
        stats[part] = jnp.transpose(packed)[:2 * some]
        send_stats.append([
            send(stats.at[part], stats_rx.at[part, j - 1], st_send.at[part, j - 1], st_recv.at[part, j - 1], peer(j) * CORES + core)
            for j in range(1, chips)
        ])
    phase("attend")
    for pair in range(heads // 2 - LATE_PAIRS, heads // 2):
        raise_mate(pair)
    for head in range(heads):
        cols = pl.ds((head % 2) * V_DIM, V_DIM)
        acc[:, pl.ds(head * V_DIM, V_DIM)] = dot(probs[head], values[head // 2, :, cols])

    width = wo_v.shape[1]
    spans = [(at, min(N_CHUNK, width - at)) for at in range(0, width, N_CHUNK)]
    pair_copies, red_copies = {}, {}
    both = CORES * toks
    half = len(ORDER[0]) * both

    def put_scale(part):
        tops = [stats[part, :some, :]] + [stats_rx[part, j, :some, :] for j in range(chips - 1)]
        sums = [stats[part, some:, :]] + [stats_rx[part, j, some:, :] for j in range(chips - 1)]
        top = functools.reduce(jnp.maximum, tops)
        shares = [jnp.exp2((t - top) * EXP_SCALE) for t in tops]
        total = functools.reduce(jnp.add, [s * w for s, w in zip(sums, shares)])
        scales[part, :, :some] = jnp.transpose(shares[0] / total)

    def put_split(part, g):
        for b, j in enumerate(ORDER[g]):
            from_rows = pl.ds(pl.multiple_of(peer(j) * both, both), both)
            factor = scales[part, from_rows, :]
            for i in range(some):
                cols = pl.ds((part * some + i) * V_DIM, V_DIM)
                o = acc[from_rows, cols] * factor[:, i:i + 1]
                o_hi = o.astype(BF16)
                split[g, pl.ds(b * both, both), cols] = o_hi
                split[g, pl.ds(half + b * both, both), cols] = (o - o_hi.astype(F32)).astype(BF16)

    def project(part, g, i):
        at, size = spans[i]
        deep = pl.ds(part * some * V_DIM, some * V_DIM)
        y = dot(split[g, :, deep], wo_v[deep, pl.ds(at, size)])
        return y[:half] + y[half:]

    def finish(g, i):
        at, size = spans[i]
        cols = pl.ds(at, size)
        y = project(PARTS - 1, g, i)
        if PARTS > 1:
            y = y + y_part[g, :, cols]
        y = y.reshape(len(ORDER[g]), CORES, toks, size)
        first, second = y[:, 0].reshape(half // CORES, size), y[:, 1].reshape(half // CORES, size)
        y_mine[g, :, cols] = jnp.where(core == 0, first, second)
        y_out[g, :, cols] = jnp.where(core == 0, second, first)
        pair_copies[g, i] = send(
            y_out.at[g, :, cols], y_rx.at[g, :, cols], pair_send.at[g, i], pair_recv.at[g, i], mate
        )

    def reduce_chunk(g, i):
        at, size = spans[i]
        cols = pl.ds(at, size)
        pair_copies[g, i].wait_recv()
        z[g, :, cols] = y_mine[g, :, cols] + y_rx[g, :, cols]
        for b, j in enumerate(ORDER[g]):
            if j:
                red_copies[j, i] = send(
                    z.at[g, pl.ds(b * toks, toks), cols], z_rx.at[j - 1, :, cols],
                    red_send.at[j - 1, i], red_recv.at[j - 1, i], peer(j) * CORES + core,
                )

    phase("wait_o")
    load_o.wait()
    steps = [(g, i) for g in range(len(ORDER)) for i in range(len(spans))]
    for part in range(PARTS):
        phase(f"wait_stats{part}")
        for copy in send_stats[part]:
            copy.wait_recv()
        phase(f"outproj{part}")
        put_scale(part)
        for g in range(len(ORDER)):
            put_split(part, g)
            for i, (at, size) in enumerate(spans):
                if part < PARTS - 1:
                    y_part[g, :, pl.ds(at, size)] = project(part, g, i)
                else:
                    finish(g, i)
    phase("pairs")
    for step in steps:
        reduce_chunk(*step)
    for j in (1, 3, 2):
        phase(f"wait_red{j}")
        for i in range(len(spans)):
            red_copies[j, i].wait_recv()
    phase("reduce")
    for i, (at, size) in enumerate(spans):
        cols = pl.ds(at, size)
        y = z[1, pl.ds(toks, toks), cols]
        for j in range(1, chips):
            y = y + z_rx[j - 1, :, cols]
        out_ref[:, cols] = y.astype(BF16)

    phase("drain")
    for copy in [send_pre, send_pseg, send_new] + send_meta + send_q + sum(send_stats, []) + list(pair_copies.values()) + list(red_copies.values()):
        copy.wait_send()
    phase("")


def solution(mesh):
    n = mesh.shape["sp"]
    chips = n // CORES
    tok_spec = P(("dp", "sp"), None)
    vec_spec = P(("dp", "sp"))
    mat_spec = P(None, None)
    gain_spec = P(None)

    def device_step(hidden, seg_ids, positions, prefix_lat, prefix_seg, w_dq, gain_q, w_uq, w_dkv, gain_kv, w_ukv, w_o):
        toks, width = hidden.shape
        pre, lat_dim = prefix_lat.shape
        q_lat = w_dq.shape[1]
        kv_lat = w_ukv.shape[0]
        heads = w_o.shape[0] // V_DIM // CORES
        rows = CORES * (pre + toks)
        wide = CORES * pre + LANES
        all_toks = n * toks
        n_chunks = -(-width // N_CHUNK)
        inv_freq = (ROPE_BASE ** (-np.arange(HALF, dtype=np.float64) / HALF)).astype(np.float32)
        freq = jnp.asarray(np.concatenate([inv_freq] * (LANES // HALF)).reshape(1, LANES))
        vmem = pl.BlockSpec(memory_space=pltpu.VMEM)
        hbm = pl.BlockSpec(memory_space=pltpu.HBM)
        dma = pltpu.SemaphoreType.DMA
        table = pltpu.VMEM((all_toks, LANES), F32)
        part = pltpu.VMEM((2, all_toks // 4, width), F32)
        return pl.pallas_call(
            functools.partial(kernel, n),
            out_shape=pltpu.VMEM((toks, width), BF16),
            in_specs=[hbm] * 13,
            scratch_shapes=[
                pltpu.VMEM((1, LANES), F32),
                pltpu.VMEM((1, toks), jnp.int32),
                pltpu.VMEM((1, toks), jnp.int32),
                pltpu.VMEM((1, pre), jnp.int32),
                pltpu.VMEM((q_lat,), BF16),
                pltpu.VMEM((kv_lat,), BF16),
                pltpu.VMEM((toks, width), BF16),
                pltpu.VMEM((width, q_lat), BF16),
                pltpu.VMEM((lat_dim, width), BF16),
                pltpu.VMEM((q_lat, heads * QK_DIM), BF16),
                pltpu.VMEM((kv_lat, heads * KV_HEAD), BF16),
                pltpu.VMEM((heads * V_DIM, width), BF16),
                pltpu.VMEM((lat_dim, wide), BF16),
                pltpu.VMEM((rows, kv_lat), BF16),
                pltpu.VMEM((CORES * toks, lat_dim), BF16),
                pltpu.VMEM((1, pre), jnp.int32),
                pltpu.VMEM((all_toks, q_lat), BF16),
                table, table, table, table,
                pltpu.VMEM((2, LANES, wide), BF16),
                pltpu.VMEM((heads, NOPE_DIM, wide), BF16),
                pltpu.VMEM((heads // 2, wide, 2 * V_DIM), BF16),
                pltpu.VMEM((heads, all_toks, 2 * LANES), BF16),
                pltpu.VMEM((heads, all_toks, wide), BF16),
                pltpu.VMEM((heads, all_toks, LANES), F32),
                pltpu.VMEM((heads, all_toks, LANES), F32),
                pltpu.VMEM((SCORE_BUFS, all_toks, wide), F32),
                pltpu.VMEM((PARTS, 2 * heads // PARTS, all_toks), F32),
                pltpu.VMEM((PARTS, chips - 1, 2 * heads // PARTS, all_toks), F32),
                pltpu.VMEM((all_toks, heads * V_DIM), F32),
                pltpu.VMEM((PARTS, all_toks, LANES), F32),
                pltpu.VMEM((2, all_toks, heads * V_DIM), BF16),
                table,
                pltpu.VMEM((2, all_toks // 2, width), F32),
                part, part, part, part,
                pltpu.VMEM((chips - 1, toks, width), F32),
                dma((6,)),
                dma((6,)),
                dma((DQ_LOADS,)),
                dma((KV_LOADS,)),
                dma((3,)), dma((3,)),
                dma((n - 1,)), dma((n - 1,)),
                dma((n - 1,)), dma((n - 1,)),
                dma((PARTS, chips - 1)), dma((PARTS, chips - 1)),
                dma((2, n_chunks)), dma((2, n_chunks)),
                dma((chips - 1, n_chunks)), dma((chips - 1, n_chunks)),
            ],
            compiler_params=pltpu.CompilerParams(
                collective_id=0, has_side_effects=True, vmem_limit_bytes=60 * 1024 * 1024
            ),
        )(
            freq, seg_ids.reshape(1, toks), positions.reshape(1, toks), prefix_seg.reshape(1, pre),
            gain_q, gain_kv,
            hidden, prefix_lat.T, w_dq, w_uq, w_dkv.T, w_ukv, w_o,
        )

    return jax.shard_map(
        device_step,
        mesh=mesh,
        in_specs=(tok_spec, vec_spec, vec_spec, tok_spec, vec_spec, mat_spec, gain_spec, mat_spec, mat_spec, gain_spec, mat_spec, mat_spec),
        out_specs=tok_spec,
        check_vma=False,
    )
```

```python
import functools
import math

import jax
import jax.numpy as jnp
import numpy as np
from jax import lax
from jax.experimental import pallas as pl
from jax.experimental.pallas import tpu as pltpu
from jax.sharding import PartitionSpec as P

ROPE_DIM = 64
HALF = ROPE_DIM // 2
NOPE_DIM = 128
V_DIM = 128
QK_DIM = NOPE_DIM + ROPE_DIM
KV_HEAD = NOPE_DIM + V_DIM
CORES = 2
EPS = 1e-6
ROPE_BASE = 10000.0
NEG_BIG = -1e30
EXP_SCALE = QK_DIM ** -0.5 * math.log2(math.e)
LANES = 128
ORDER = ((2, 1), (3, 0))
PARTS = 2
SWAP = 4
KV_LOADS = 2
DQ_LOADS = 4
LATE_PAIRS = 3
UNROLL_KV = 8
SCORE_BUFS = 4

F32 = jnp.float32
BF16 = jnp.bfloat16


def dot(a, b):
    return jnp.dot(a, b, preferred_element_type=F32)


def dot_nt(a, b):
    return lax.dot_general(a, b, (((1,), (1,)), ((), ())), preferred_element_type=F32)


def dot_tn(a, b):
    return lax.dot_general(a, b, (((0,), (0,)), ((), ())), preferred_element_type=F32)


def rms_norm(values, gain):
    inv_rms = lax.rsqrt(jnp.mean(values * values, axis=-1, keepdims=True) + EPS)
    return values * inv_rms * gain.astype(F32).reshape(1, gain.shape[0])


def row_to_column(row):
    size = row.shape[1]
    here = lax.broadcasted_iota(jnp.int32, (size, size), 0) == lax.broadcasted_iota(jnp.int32, (size, size), 1)
    return jnp.sum(jnp.where(here, jnp.broadcast_to(row, (size, size)), 0.0), axis=1, keepdims=True)


def lane_of(shape):
    return lax.broadcasted_iota(jnp.int32, shape, len(shape) - 1)


def turn(x, amount):
    return pltpu.roll(x, amount, 1)


def unrolled(count, step, body):
    if count == step:
        for j in range(step):
            body(j)
        return

    def run(i, carry):
        for j in range(step):
            body(i * step + j)
        return carry

    lax.fori_loop(0, count // step, run, 0)


class Phases:
    def __init__(self):
        self.now = None

    def __call__(self, name):
        if self.now is not None:
            self.now.__exit__(None, None, None)
        self.now = None
        if name:
            self.now = jax.named_scope(name)
            self.now.__enter__()


def kernel(
    n,
    freq_hbm, seg_hbm, pos_hbm, pseg_hbm, gain_q_hbm, gain_kv_hbm,
    hid_hbm, pre_hbm, wdq_hbm, wuq_hbm, wdkv_hbm, wukv_hbm, wo_hbm,
    out_ref,
    freq_ref, seg_ref, pos_ref, pseg_ref, gain_q_ref, gain_kv_ref,
    hid_v, wdq_v, wdkv_v, wuq_v, wukv_v, wo_v,
    lat_t, lat, new_lat, pseg_mate, qlat_all, meta_all, cos_all, sin_all, mask_a, tail_t,
    keys_t, values, queries, probs, tops_all, sums_all,
    scores, stats, stats_rx, acc, scales, split, bias, z, z_rx,
    load_sem, small_sem, dq_sem, wo_sem, ukv_sem, mate_send, mate_recv, gat_send, gat_recv, met_send, met_recv,
    st_send, st_recv, acc_send, acc_recv, red_send, red_recv,
):
    phase = Phases()
    me = lax.axis_index("sp")
    core = lax.rem(me, CORES)
    chip = lax.div(me, CORES)
    chips = n // CORES
    mate = chip * CORES + (CORES - 1 - core)
    toks = hid_v.shape[0]
    pre = pre_hbm.shape[1]
    kv_lat = wukv_v.shape[0]
    heads = keys_t.shape[0]
    old = CORES * pre
    new = CORES * toks
    wide = lat_t.shape[1]
    all_toks = n * toks
    some = heads // PARTS
    deep = some * V_DIM
    half_width = wo_v.shape[1]

    phase("loads")

    def load(src, dst, sem):
        copy = pltpu.make_async_copy(src, dst, sem)
        copy.start()
        return copy

    barrier = pltpu.get_barrier_semaphore()
    for j in range(1, n):
        pl.semaphore_signal(barrier, inc=1, device_id={"sp": lax.rem(me + j, n)}, device_id_type=pl.DeviceIdType.MESH)
    smalls = [
        load(src, dst, small_sem.at[i])
        for i, (src, dst) in enumerate([
            (freq_hbm, freq_ref), (seg_hbm, seg_ref), (pos_hbm, pos_ref),
            (gain_q_hbm, gain_q_ref), (gain_kv_hbm, gain_kv_ref), (pseg_hbm, pseg_ref),
        ])
    ]
    load_hid = load(hid_hbm, hid_v, load_sem.at[0])
    depth = wdq_v.shape[0] // DQ_LOADS
    load_dq = [
        load(wdq_hbm.at[pl.ds(i * depth, depth)], wdq_v.at[pl.ds(i * depth, depth)], dq_sem.at[i])
        for i in range(DQ_LOADS)
    ]
    kv_cols = heads * KV_HEAD
    part = kv_cols // KV_LOADS

    def load_up(i):
        return load(
            wukv_hbm.at[:, pl.ds(pl.multiple_of(core * kv_cols + i * part, LANES), part)],
            wukv_v.at[:, pl.ds(i * part, part)],
            ukv_sem.at[i],
        )

    load_pre = load(pre_hbm, lat_t.at[:, pl.ds(0, pre)], load_sem.at[3])
    load_ukv = [load_up(0)]

    phase("wait_small")
    for copy in smalls:
        copy.wait()
    phase("meta")
    pos_col = row_to_column(pos_ref[...].astype(F32))
    seg_col = row_to_column(seg_ref[...].astype(F32))
    angles = pos_col * freq_ref[...]
    lane = lane_of((toks, LANES))
    cos_t = jnp.cos(angles)
    sin_t = jnp.sin(angles)
    my_rows = pl.ds(pl.multiple_of(me * toks, toks), toks)
    meta_all[my_rows, :] = jnp.where(
        lane < HALF, cos_t, jnp.where(lane < 2 * HALF, sin_t, jnp.where(lane == 2 * HALF, seg_col, pos_col))
    )

    def send(src, dst, send_sem, recv_sem, target):
        copy = pltpu.make_async_remote_copy(
            src_ref=src, dst_ref=dst, send_sem=send_sem, recv_sem=recv_sem,
            device_id={"sp": target}, device_id_type=pl.DeviceIdType.MESH,
        )
        copy.start()
        return copy

    phase("wait_dq")
    load_hid.wait()
    for copy in load_dq:
        copy.wait()
    load_ukv += [load_up(i) for i in range(1, KV_LOADS)]
    load_dkv = load(wdkv_hbm, wdkv_v, load_sem.at[2])
    phase("barrier")
    pl.semaphore_wait(barrier, n - 1)
    send_pre = send(pre_hbm, lat_t.at[:, pl.ds(pre, pre)], mate_send.at[0], mate_recv.at[0], mate)
    send_pseg = send(pseg_ref, pseg_mate, mate_send.at[1], mate_recv.at[1], mate)
    send_meta = [
        send(meta_all.at[my_rows], meta_all.at[my_rows], met_send.at[j - 1], met_recv.at[j - 1], lax.rem(me + j, n))
        for j in range(1, n)
    ]
    phase("qlat")
    qlat_all[my_rows, :] = rms_norm(dot(hid_v[...], wdq_v[...]), gain_q_ref[...]).astype(BF16)

    send_q = [
        send(qlat_all.at[my_rows], qlat_all.at[my_rows], gat_send.at[j - 1], gat_recv.at[j - 1], lax.rem(me + j, n))
        for j in range(1, n)
    ]
    def pair_weights(pair, offset):
        first = pl.multiple_of(pair * (2 * KV_HEAD) + offset, LANES)
        second = pl.multiple_of(pair * (2 * KV_HEAD) + KV_HEAD + offset, LANES)
        return jnp.concatenate([wukv_v[:, pl.ds(first, LANES)], wukv_v[:, pl.ds(second, LANES)]], axis=1)

    def raise_keys(start, size):
        def step(pair):
            up = dot_tn(pair_weights(pair, 0), lat_t[:kv_lat, pl.ds(start, size)]).astype(BF16)
            keys_t[2 * pair, :, pl.ds(start, size)] = up[:NOPE_DIM]
            keys_t[2 * pair + 1, :, pl.ds(start, size)] = up[NOPE_DIM:]
        return step

    def raise_values(start, size):
        def step(pair):
            values[pair, pl.ds(start, size), :] = dot(lat[pl.ds(start, size), :], pair_weights(pair, NOPE_DIM)).astype(BF16)
        return step

    def put_tail(start, size, seg_row):
        hot = seg_row == lax.broadcasted_iota(jnp.int32, (ROPE_DIM, size), 0)
        hot = jnp.where(hot, 1.0, 0.0).astype(BF16)
        rope = lat_t[kv_lat:, pl.ds(start, size)]
        tail_t[0, :, pl.ds(start, size)] = jnp.concatenate([rope, hot], axis=0)
        tail_t[1, :, pl.ds(start, size)] = jnp.concatenate([hot, rope], axis=0)
    per = heads // 2 // KV_LOADS
    for i in range(KV_LOADS):
        phase(f"wait_own{i}")
        load_ukv[i].wait()
        if i == 0:
            load_pre.wait()
        else:
            load_dkv.wait()
        phase(f"own{i}")
        if i == 0:
            lat[pl.ds(0, pre), :] = jnp.transpose(lat_t[:kv_lat, pl.ds(0, pre)])
            put_tail(0, pre, pseg_ref[...])
            values[:, pl.ds(old + new, wide - old - new), :] = jnp.zeros((heads // 2, wide - old - new, 2 * V_DIM), BF16)
        else:
            down = dot_nt(hid_v[...], wdkv_v[...])
            c_kv = rms_norm(down[:, :kv_lat], gain_kv_ref[...])
            low, high = down[:, kv_lat:kv_lat + HALF], down[:, kv_lat + HALF:]
            cos_m, sin_m = cos_t[:, :HALF], sin_t[:, :HALF]
            k_new = jnp.concatenate([low * cos_m - high * sin_m, high * cos_m + low * sin_m], axis=1)
            new_lat[pl.ds(0, toks), :] = jnp.concatenate([c_kv, k_new], axis=1).astype(BF16)
            send_new = send(new_lat.at[pl.ds(0, toks)], new_lat.at[pl.ds(toks, toks)], mate_send.at[2], mate_recv.at[2], mate)

            load_uq = load(
                wuq_hbm.at[:, pl.ds(pl.multiple_of(core * heads * QK_DIM, LANES), heads * QK_DIM)], wuq_v, load_sem.at[4]
            )
            load_o = [
                load(
                    wo_hbm.at[
                        pl.ds(pl.multiple_of(lax.rem(core + side, CORES) * (heads * V_DIM) + part * deep, LANES), deep),
                        pl.ds(pl.multiple_of(core * half_width, LANES), half_width),
                    ],
                    wo_v.at[pl.ds((part * CORES + side) * deep, deep)],
                    wo_sem.at[part, side],
                )
                for part in range(PARTS) for side in range(CORES)
            ]

        for pair in range(i * per, (i + 1) * per):
            raise_keys(0, pre)(pair)
            raise_values(0, pre)(pair)

    phase("wait_meta")
    for copy in send_meta:
        copy.wait_recv()
    phase("wait_mate")
    send_pre.wait_recv()
    send_pseg.wait_recv()
    send_new.wait_recv()
    phase("keys_mate")
    every = meta_all[...]
    lanes = lane_of((all_toks, LANES))
    q_seg = every[:, 2 * HALF:2 * HALF + 1]
    q_pos = every[:, 2 * HALF + 1:2 * HALF + 2]
    cos_q = jnp.where(lanes < HALF, every, 0.0)
    cos_q = cos_q + turn(cos_q, HALF)
    cos_all[...] = cos_q + turn(cos_q, 2 * HALF)
    sin_q = jnp.where((lanes >= HALF) & (lanes < 2 * HALF), every, 0.0)
    sin_q = sin_q - turn(sin_q, LANES - HALF)
    sin_all[...] = sin_q + turn(sin_q, 2 * HALF)
    q_mask = jnp.where(q_seg == jnp.where(lanes < ROPE_DIM, lanes, lanes - ROPE_DIM).astype(F32), 0.0, NEG_BIG)
    mask_a[...] = q_mask
    mate_rows = pl.ds(pl.multiple_of(mate * toks, toks), toks)
    new_meta = jnp.concatenate(
        [meta_all[my_rows, :], meta_all[mate_rows, :], jnp.zeros((LANES - new, LANES), F32)], axis=0
    )
    meta_rows = jnp.transpose(new_meta)
    k_seg, k_pos = meta_rows[2 * HALF:2 * HALF + 1], meta_rows[2 * HALF + 1:2 * HALF + 2]
    seen = (q_seg == k_seg) & (k_pos <= q_pos) & (lane_of((all_toks, LANES)) < new)
    bias[...] = jnp.where(seen, 0.0, NEG_BIG)

    lat[pl.ds(pre, pre), :] = jnp.transpose(lat_t[:kv_lat, pl.ds(pre, pre)])
    lat[pl.ds(old, new), :] = new_lat[:, :kv_lat]
    new_wide = jnp.concatenate([new_lat[...].astype(F32), jnp.zeros((LANES - new, kv_lat + ROPE_DIM), F32)], axis=0)
    lat_t[:, pl.ds(old, LANES)] = jnp.transpose(new_wide).astype(BF16)
    put_tail(pre, pre, pseg_mate[...])
    put_tail(old, LANES, jnp.full((1, LANES), -1, jnp.int32))
    unrolled(heads // 2, UNROLL_KV, raise_keys(pre, wide - pre))

    phase("wait_uq")
    load_uq.wait()
    for copy in send_q:
        copy.wait_recv()
    phase("queries")
    low_half = lane_of((all_toks, LANES)) < ROPE_DIM
    first_half = lax.rem(lane_of((all_toks, LANES)), ROPE_DIM) < HALF

    def raise_queries(pair):
        cols = pl.ds(pl.multiple_of(pair * (2 * QK_DIM), LANES), 2 * QK_DIM)
        q = dot(qlat_all[...], wuq_v[:, cols])
        nope_a, mid, end = q[:, :LANES], q[:, LANES:2 * LANES], q[:, 2 * LANES:]
        nope_b = turn(jnp.where(low_half, end, mid), ROPE_DIM)
        u = jnp.where(low_half, mid, end)
        swapped = jnp.where(first_half, turn(u, LANES - HALF), turn(u, HALF))
        r = u * cos_all[...] + swapped * sin_all[...]
        queries[2 * pair] = jnp.concatenate([nope_a, jnp.where(low_half, r, mask_a[...])], axis=1).astype(BF16)
        queries[2 * pair + 1] = jnp.concatenate([nope_b, jnp.where(low_half, mask_a[...], r)], axis=1).astype(BF16)

    unrolled(heads // 2, UNROLL_KV, raise_queries)

    phase("score")

    def score(head, j):
        s = dot(queries[head], jnp.concatenate([keys_t[head], tail_t[j % 2]], axis=0))
        scores[j, :, :old] = s[:, :old]
        scores[j, :, old:] = s[:, old:] + bias[...]
        step = 16
        tops = [jnp.max(scores[j, r:r + step, :], axis=1, keepdims=True) for r in range(0, all_toks, step)]
        for i, top in enumerate(tops):
            rows = pl.ds(i * step, step)
            p = jnp.exp2((scores[j, rows, :] - top) * EXP_SCALE)
            probs[head, rows, :] = p.astype(BF16)
            tops_all[head, rows, :] = jnp.broadcast_to(top, (step, LANES))
            sums_all[head, rows, :] = jnp.broadcast_to(jnp.sum(p, axis=1, keepdims=True), (step, LANES))

    raise_mate = raise_values(pre, pre + new)

    def peer(j):
        return lax.rem(chip + j, chips)

    send_stats = []
    for part in range(PARTS):
        packed = jnp.zeros((all_toks, LANES), F32)
        for head in range(part * some, (part + 1) * some):
            score(head, head % SCORE_BUFS)
            if head % 2 == 0 and head // 2 < heads // 2 - LATE_PAIRS:
                raise_mate(head // 2)
        for i in range(some):
            packed = jnp.where(lanes == i, tops_all[part * some + i], packed)
            packed = jnp.where(lanes == some + i, sums_all[part * some + i], packed)
        stats[part] = jnp.transpose(packed)[:2 * some]
        send_stats.append([
            send(stats.at[part], stats_rx.at[part, j - 1], st_send.at[part, j - 1], st_recv.at[part, j - 1], lax.rem(me + j, n))
            for j in range(1, n)
        ])
    phase("attend")
    for pair in range(heads // 2 - LATE_PAIRS, heads // 2):
        raise_mate(pair)
    send_acc = []
    for head in range(heads):
        cols = pl.ds((head % 2) * V_DIM, V_DIM)
        acc[0, head] = dot(probs[head], values[head // 2, :, cols])
        if (head + 1) % SWAP == 0:
            group = pl.ds(head + 1 - SWAP, SWAP)
            i = head // SWAP
            send_acc.append(send(acc.at[0, group], acc.at[1, group], acc_send.at[i], acc_recv.at[i], mate))

    red_copies = {}
    both = CORES * toks
    half = len(ORDER[0]) * both

    def put_scale(part):
        for side in range(CORES):
            got = [stats_rx[part, j - 1] for j in range(1 + (1 - side), n, CORES)]
            mine = stats[part] if side == 0 else jnp.where(core == 0, got[-1], got[0])
            every = got + [mine] if side == 0 else got
            top = functools.reduce(jnp.maximum, [g[:some] for g in every])
            total = functools.reduce(jnp.add, [g[some:] * jnp.exp2((g[:some] - top) * EXP_SCALE) for g in every])
            share = jnp.exp2((mine[:some] - top) * EXP_SCALE)
            scales[part, side, :, :some] = jnp.transpose(share / total)

    def put_split(part, g):
        for b, j in enumerate(ORDER[g]):
            from_rows = pl.ds(pl.multiple_of(peer(j) * both, both), both)
            for side in range(CORES):
                factor = scales[part, side, from_rows, :]
                for i in range(some):
                    cols = pl.ds(((part * CORES + side) * some + i) * V_DIM, V_DIM)
                    o = acc[side, part * some + i, from_rows, :] * factor[:, i:i + 1]
                    o_hi = o.astype(BF16)
                    split[g, pl.ds(b * both, both), cols] = o_hi
                    split[g, pl.ds(half + b * both, both), cols] = (o - o_hi.astype(F32)).astype(BF16)

    def project(part, g):
        ks = pl.ds(part * CORES * deep, CORES * deep)
        y = dot(split[g, :, ks], wo_v[ks, :])
        return y[:half] + y[half:]

    def deliver(g):
        for b, j in enumerate(ORDER[g]):
            for r in range(CORES):
                if j or r:
                    to = lax.rem(core + r, CORES)
                    rows = pl.ds(pl.multiple_of(b * both + to * toks, toks), toks)
                    red_copies[j, r] = send(
                        z.at[g, rows], z_rx.at[j, r], red_send.at[j, r], red_recv.at[j, r], peer(j) * CORES + to
                    )

    phase("wait_o")
    for copy in load_o:
        copy.wait()
    for part in range(PARTS):
        phase(f"wait_acc{part}")
        for copy in send_acc[part * some // SWAP:(part + 1) * some // SWAP]:
            copy.wait_recv()
        phase(f"wait_stats{part}")
        for copy in send_stats[part]:
            copy.wait_recv()
        phase(f"outproj{part}")
        put_scale(part)
        for g in range(len(ORDER)):
            put_split(part, g)
            if part == 0:
                z[g] = project(part, g)
            else:
                z[g] = z[g] + project(part, g)
            if part == PARTS - 1:
                deliver(g)
    for j in (0, 1, 3, 2):
        phase(f"wait_red{j}")
        for r in range(CORES):
            if j or r:
                red_copies[j, r].wait_recv()
    phase("reduce")
    own = pl.ds(pl.multiple_of(both + core * toks, toks), toks)
    for r in range(CORES):
        y = z[1, own, :] if r == 0 else z_rx[0, 1]
        for j in range(1, chips):
            y = y + z_rx[j, r]
        cols = pl.ds(pl.multiple_of(lax.rem(core + r, CORES) * half_width, LANES), half_width)
        out_ref[:, cols] = y.astype(BF16)

    phase("drain")
    for copy in [send_pre, send_pseg, send_new] + send_meta + send_q + sum(send_stats, []) + send_acc + list(red_copies.values()):
        copy.wait_send()
    phase("")


def solution(mesh):
    n = mesh.shape["sp"]
    chips = n // CORES
    tok_spec = P(("dp", "sp"), None)
    vec_spec = P(("dp", "sp"))
    mat_spec = P(None, None)
    gain_spec = P(None)

    def device_step(hidden, seg_ids, positions, prefix_lat, prefix_seg, w_dq, gain_q, w_uq, w_dkv, gain_kv, w_ukv, w_o):
        toks, width = hidden.shape
        pre, lat_dim = prefix_lat.shape
        q_lat = w_dq.shape[1]
        kv_lat = w_ukv.shape[0]
        heads = w_o.shape[0] // V_DIM // CORES
        rows = CORES * (pre + toks)
        wide = CORES * pre + LANES
        all_toks = n * toks
        inv_freq = (ROPE_BASE ** (-np.arange(HALF, dtype=np.float64) / HALF)).astype(np.float32)
        freq = jnp.asarray(np.concatenate([inv_freq] * (LANES // HALF)).reshape(1, LANES))
        vmem = pl.BlockSpec(memory_space=pltpu.VMEM)
        hbm = pl.BlockSpec(memory_space=pltpu.HBM)
        dma = pltpu.SemaphoreType.DMA
        table = pltpu.VMEM((all_toks, LANES), F32)
        return pl.pallas_call(
            functools.partial(kernel, n),
            out_shape=pltpu.VMEM((toks, width), BF16),
            in_specs=[hbm] * 13,
            scratch_shapes=[
                pltpu.VMEM((1, LANES), F32),
                pltpu.VMEM((1, toks), jnp.int32),
                pltpu.VMEM((1, toks), jnp.int32),
                pltpu.VMEM((1, pre), jnp.int32),
                pltpu.VMEM((q_lat,), BF16),
                pltpu.VMEM((kv_lat,), BF16),
                pltpu.VMEM((toks, width), BF16),
                pltpu.VMEM((width, q_lat), BF16),
                pltpu.VMEM((lat_dim, width), BF16),
                pltpu.VMEM((q_lat, heads * QK_DIM), BF16),
                pltpu.VMEM((kv_lat, heads * KV_HEAD), BF16),
                pltpu.VMEM((CORES * heads * V_DIM, width // CORES), BF16),
                pltpu.VMEM((lat_dim, wide), BF16),
                pltpu.VMEM((rows, kv_lat), BF16),
                pltpu.VMEM((CORES * toks, lat_dim), BF16),
                pltpu.VMEM((1, pre), jnp.int32),
                pltpu.VMEM((all_toks, q_lat), BF16),
                table, table, table, table,
                pltpu.VMEM((2, LANES, wide), BF16),
                pltpu.VMEM((heads, NOPE_DIM, wide), BF16),
                pltpu.VMEM((heads // 2, wide, 2 * V_DIM), BF16),
                pltpu.VMEM((heads, all_toks, 2 * LANES), BF16),
                pltpu.VMEM((heads, all_toks, wide), BF16),
                pltpu.VMEM((heads, all_toks, LANES), F32),
                pltpu.VMEM((heads, all_toks, LANES), F32),
                pltpu.VMEM((SCORE_BUFS, all_toks, wide), F32),
                pltpu.VMEM((PARTS, 2 * heads // PARTS, all_toks), F32),
                pltpu.VMEM((PARTS, n - 1, 2 * heads // PARTS, all_toks), F32),
                pltpu.VMEM((CORES, heads, all_toks, V_DIM), F32),
                pltpu.VMEM((PARTS, CORES, all_toks, LANES), F32),
                pltpu.VMEM((2, all_toks, CORES * heads * V_DIM), BF16),
                table,
                pltpu.VMEM((2, all_toks // 2, width // CORES), F32),
                pltpu.VMEM((chips, CORES, toks, width // CORES), F32),
                dma((6,)),
                dma((6,)),
                dma((DQ_LOADS,)),
                dma((PARTS, CORES)),
                dma((KV_LOADS,)),
                dma((3,)), dma((3,)),
                dma((n - 1,)), dma((n - 1,)),
                dma((n - 1,)), dma((n - 1,)),
                dma((PARTS, n - 1)), dma((PARTS, n - 1)),
                dma((heads // SWAP,)), dma((heads // SWAP,)),
                dma((chips, CORES)), dma((chips, CORES)),
            ],
            compiler_params=pltpu.CompilerParams(
                collective_id=0, has_side_effects=True, vmem_limit_bytes=60 * 1024 * 1024
            ),
        )(
            freq, seg_ids.reshape(1, toks), positions.reshape(1, toks), prefix_seg.reshape(1, pre),
            gain_q, gain_kv,
            hidden, prefix_lat.T, w_dq, w_uq, w_dkv.T, w_ukv, w_o,
        )

    return jax.shard_map(
        device_step,
        mesh=mesh,
        in_specs=(tok_spec, vec_spec, vec_spec, tok_spec, vec_spec, mat_spec, gain_spec, mat_spec, mat_spec, gain_spec, mat_spec, mat_spec),
        out_specs=tok_spec,
        check_vma=False,
    )
```

```python
import functools
import math

import jax
import jax.numpy as jnp
import numpy as np
from jax import lax
from jax.experimental import pallas as pl
from jax.experimental.pallas import tpu as pltpu
from jax.sharding import PartitionSpec as P

ROPE_DIM = 64
HALF = ROPE_DIM // 2
NOPE_DIM = 128
V_DIM = 128
QK_DIM = NOPE_DIM + ROPE_DIM
KV_HEAD = NOPE_DIM + V_DIM
CORES = 2
EPS = 1e-6
ROPE_BASE = 10000.0
NEG_BIG = -1e30
EXP_SCALE = QK_DIM ** -0.5 * math.log2(math.e)
LANES = 128
ORDER = ((2, 1), (3, 0))
PARTS = 2
VALUE_PAIRS = (4, 2, 2)
KV_LOADS = 2
DQ_LOADS = 4
UNROLL_KV = 8
SCORE_BUFS = 8

F32 = jnp.float32
BF16 = jnp.bfloat16


def dot(a, b):
    return jnp.dot(a, b, preferred_element_type=F32)


def dot_nt(a, b):
    return lax.dot_general(a, b, (((1,), (1,)), ((), ())), preferred_element_type=F32)


def dot_tn(a, b):
    return lax.dot_general(a, b, (((0,), (0,)), ((), ())), preferred_element_type=F32)


def rms_norm(values, gain):
    inv_rms = lax.rsqrt(jnp.mean(values * values, axis=-1, keepdims=True) + EPS)
    return values * inv_rms * gain.astype(F32).reshape(1, gain.shape[0])


def row_to_column(row):
    size = row.shape[1]
    here = lax.broadcasted_iota(jnp.int32, (size, size), 0) == lax.broadcasted_iota(jnp.int32, (size, size), 1)
    return jnp.sum(jnp.where(here, jnp.broadcast_to(row, (size, size)), 0.0), axis=1, keepdims=True)


def lane_of(shape):
    return lax.broadcasted_iota(jnp.int32, shape, len(shape) - 1)


def turn(x, amount):
    return pltpu.roll(x, amount, 1)


def unrolled(count, step, body):
    if count == step:
        for j in range(step):
            body(j)
        return

    def run(i, carry):
        for j in range(step):
            body(i * step + j)
        return carry

    lax.fori_loop(0, count // step, run, 0)


class Phases:
    def __init__(self):
        self.now = None

    def __call__(self, name):
        if self.now is not None:
            self.now.__exit__(None, None, None)
        self.now = None
        if name:
            self.now = jax.named_scope(name)
            self.now.__enter__()


def kernel(
    n,
    freq_hbm, seg_hbm, pos_hbm, pseg_hbm, gain_q_hbm, gain_kv_hbm,
    hid_hbm, pre_hbm, wdq_hbm, wuq_hbm, wdkv_hbm, wukv_hbm, wo_hbm,
    out_ref,
    freq_ref, seg_ref, pos_ref, pseg_ref, gain_q_ref, gain_kv_ref,
    hid_v, wdq_v, wdkv_v, wuq_v, wukv_v, wo_v,
    lat_t, lat, new_lat, pseg_mate, qlat_all, meta_all, cos_all, sin_all, mask_a, tail_t,
    keys_t, values, queries, probs, tops_all, sums_all,
    scores, stats, stats_rx, acc, scales, split, bias, z, z_rx,
    load_sem, small_sem, dq_sem, wo_sem, ukv_sem, mate_send, mate_recv, gat_send, gat_recv, met_send, met_recv,
    st_send, st_recv, acc_send, acc_recv, red_send, red_recv,
):
    phase = Phases()
    me = lax.axis_index("sp")
    core = lax.rem(me, CORES)
    chip = lax.div(me, CORES)
    chips = n // CORES
    mate = chip * CORES + (CORES - 1 - core)
    toks = hid_v.shape[0]
    pre = pre_hbm.shape[1]
    kv_lat = wukv_v.shape[0]
    heads = keys_t.shape[0]
    old = CORES * pre
    new = CORES * toks
    wide = lat_t.shape[1]
    all_toks = n * toks
    some = heads // PARTS
    deep = some * V_DIM
    half_width = wo_v.shape[1]

    phase("loads")

    def load(src, dst, sem):
        copy = pltpu.make_async_copy(src, dst, sem)
        copy.start()
        return copy

    barrier = pltpu.get_barrier_semaphore()
    for j in range(1, n):
        pl.semaphore_signal(barrier, inc=1, device_id={"sp": lax.rem(me + j, n)}, device_id_type=pl.DeviceIdType.MESH)
    smalls = [
        load(src, dst, small_sem.at[i])
        for i, (src, dst) in enumerate([
            (freq_hbm, freq_ref), (seg_hbm, seg_ref), (pos_hbm, pos_ref),
            (gain_q_hbm, gain_q_ref), (gain_kv_hbm, gain_kv_ref), (pseg_hbm, pseg_ref),
        ])
    ]
    load_hid = load(hid_hbm, hid_v, load_sem.at[0])
    depth = wdq_v.shape[0] // DQ_LOADS
    load_dq = [
        load(wdq_hbm.at[pl.ds(i * depth, depth)], wdq_v.at[pl.ds(i * depth, depth)], dq_sem.at[i])
        for i in range(DQ_LOADS)
    ]
    kv_cols = heads * KV_HEAD
    part = kv_cols // KV_LOADS

    def load_up(i):
        return load(
            wukv_hbm.at[:, pl.ds(pl.multiple_of(core * kv_cols + i * part, LANES), part)],
            wukv_v.at[:, pl.ds(i * part, part)],
            ukv_sem.at[i],
        )

    load_pre = load(pre_hbm, lat_t.at[:, pl.ds(0, pre)], load_sem.at[3])
    load_ukv = [load_up(0)]

    phase("wait_small")
    for copy in smalls:
        copy.wait()
    phase("meta")
    pos_col = row_to_column(pos_ref[...].astype(F32))
    seg_col = row_to_column(seg_ref[...].astype(F32))
    angles = pos_col * freq_ref[...]
    lane = lane_of((toks, LANES))
    cos_t = jnp.cos(angles)
    sin_t = jnp.sin(angles)
    my_rows = pl.ds(pl.multiple_of(me * toks, toks), toks)
    meta_all[my_rows, :] = jnp.where(
        lane < HALF, cos_t, jnp.where(lane < 2 * HALF, sin_t, jnp.where(lane == 2 * HALF, seg_col, pos_col))
    )

    def send(src, dst, send_sem, recv_sem, target):
        copy = pltpu.make_async_remote_copy(
            src_ref=src, dst_ref=dst, send_sem=send_sem, recv_sem=recv_sem,
            device_id={"sp": target}, device_id_type=pl.DeviceIdType.MESH,
        )
        copy.start()
        return copy

    phase("wait_dq")
    load_hid.wait()
    for copy in load_dq:
        copy.wait()
    load_ukv += [load_up(i) for i in range(1, KV_LOADS)]
    load_dkv = load(wdkv_hbm, wdkv_v, load_sem.at[2])
    phase("barrier")
    pl.semaphore_wait(barrier, n - 1)
    send_pre = send(pre_hbm, lat_t.at[:, pl.ds(pre, pre)], mate_send.at[0], mate_recv.at[0], mate)
    send_pseg = send(pseg_ref, pseg_mate, mate_send.at[1], mate_recv.at[1], mate)
    send_meta = [
        send(meta_all.at[my_rows], meta_all.at[my_rows], met_send.at[j - 1], met_recv.at[j - 1], lax.rem(me + j, n))
        for j in range(1, n)
    ]
    phase("qlat")
    qlat_all[my_rows, :] = rms_norm(dot(hid_v[...], wdq_v[...]), gain_q_ref[...]).astype(BF16)

    send_q = [
        send(qlat_all.at[my_rows], qlat_all.at[my_rows], gat_send.at[j - 1], gat_recv.at[j - 1], lax.rem(me + j, n))
        for j in range(1, n)
    ]
    def pair_weights(pair, offset):
        first = pl.multiple_of(pair * (2 * KV_HEAD) + offset, LANES)
        second = pl.multiple_of(pair * (2 * KV_HEAD) + KV_HEAD + offset, LANES)
        return jnp.concatenate([wukv_v[:, pl.ds(first, LANES)], wukv_v[:, pl.ds(second, LANES)]], axis=1)

    def raise_keys(start, size):
        def step(pair):
            up = dot_tn(pair_weights(pair, 0), lat_t[:kv_lat, pl.ds(start, size)]).astype(BF16)
            keys_t[2 * pair, :, pl.ds(start, size)] = up[:NOPE_DIM]
            keys_t[2 * pair + 1, :, pl.ds(start, size)] = up[NOPE_DIM:]
        return step

    def raise_values(start, size):
        def step(pair):
            values[pair, pl.ds(start, size), :] = dot(lat[pl.ds(start, size), :], pair_weights(pair, NOPE_DIM)).astype(BF16)
        return step

    def put_tail(start, size, seg_row):
        hot = seg_row == lax.broadcasted_iota(jnp.int32, (ROPE_DIM, size), 0)
        hot = jnp.where(hot, 1.0, 0.0).astype(BF16)
        rope = lat_t[kv_lat:, pl.ds(start, size)]
        tail_t[0, :, pl.ds(start, size)] = jnp.concatenate([rope, hot], axis=0)
        tail_t[1, :, pl.ds(start, size)] = jnp.concatenate([hot, rope], axis=0)
    per = heads // 2 // KV_LOADS
    for i in range(KV_LOADS):
        phase(f"wait_own{i}")
        load_ukv[i].wait()
        if i == 0:
            load_pre.wait()
        else:
            load_dkv.wait()
        phase(f"own{i}")
        if i == 0:
            lat[pl.ds(0, pre), :] = jnp.transpose(lat_t[:kv_lat, pl.ds(0, pre)])
            put_tail(0, pre, pseg_ref[...])
            values[:, pl.ds(old + new, wide - old - new), :] = jnp.zeros((heads // 2, wide - old - new, 2 * V_DIM), BF16)
        else:
            load_uq = load(
                wuq_hbm.at[:, pl.ds(pl.multiple_of(core * heads * QK_DIM, LANES), heads * QK_DIM)], wuq_v, load_sem.at[4]
            )
            load_o = [
                load(
                    wo_hbm.at[
                        pl.ds(pl.multiple_of(lax.rem(core + side, CORES) * (heads * V_DIM) + part * deep, LANES), deep),
                        pl.ds(pl.multiple_of(core * half_width, LANES), half_width),
                    ],
                    wo_v.at[pl.ds((part * CORES + side) * deep, deep)],
                    wo_sem.at[part, side],
                )
                for part in range(PARTS) for side in range(CORES)
            ]
            down = dot_nt(hid_v[...], wdkv_v[...])
            c_kv = rms_norm(down[:, :kv_lat], gain_kv_ref[...])
            low, high = down[:, kv_lat:kv_lat + HALF], down[:, kv_lat + HALF:]
            cos_m, sin_m = cos_t[:, :HALF], sin_t[:, :HALF]
            k_new = jnp.concatenate([low * cos_m - high * sin_m, high * cos_m + low * sin_m], axis=1)
            new_lat[pl.ds(0, toks), :] = jnp.concatenate([c_kv, k_new], axis=1).astype(BF16)
        for pair in range(i * per, (i + 1) * per):
            raise_keys(0, pre)(pair)
            raise_values(0, pre)(pair)
    send_new = send(new_lat.at[pl.ds(0, toks)], new_lat.at[pl.ds(toks, toks)], mate_send.at[2], mate_recv.at[2], mate)

    phase("wait_meta")
    for copy in send_meta:
        copy.wait_recv()
    phase("wait_mate")
    send_pre.wait_recv()
    send_pseg.wait_recv()
    phase("keys_mate")
    every = meta_all[...]
    lanes = lane_of((all_toks, LANES))
    q_seg = every[:, 2 * HALF:2 * HALF + 1]
    q_pos = every[:, 2 * HALF + 1:2 * HALF + 2]
    cos_q = jnp.where(lanes < HALF, every, 0.0)
    cos_q = cos_q + turn(cos_q, HALF)
    cos_all[...] = cos_q + turn(cos_q, 2 * HALF)
    sin_q = jnp.where((lanes >= HALF) & (lanes < 2 * HALF), every, 0.0)
    sin_q = sin_q - turn(sin_q, LANES - HALF)
    sin_all[...] = sin_q + turn(sin_q, 2 * HALF)
    q_mask = jnp.where(q_seg == jnp.where(lanes < ROPE_DIM, lanes, lanes - ROPE_DIM).astype(F32), 0.0, NEG_BIG)
    mask_a[...] = q_mask
    mate_rows = pl.ds(pl.multiple_of(mate * toks, toks), toks)
    new_meta = jnp.concatenate(
        [meta_all[my_rows, :], meta_all[mate_rows, :], jnp.zeros((LANES - new, LANES), F32)], axis=0
    )
    meta_rows = jnp.transpose(new_meta)
    k_seg, k_pos = meta_rows[2 * HALF:2 * HALF + 1], meta_rows[2 * HALF + 1:2 * HALF + 2]
    seen = (q_seg == k_seg) & (k_pos <= q_pos) & (lane_of((all_toks, LANES)) < new)
    bias[...] = jnp.where(seen, 0.0, NEG_BIG)

    lat[pl.ds(pre, pre), :] = jnp.transpose(lat_t[:kv_lat, pl.ds(pre, pre)])
    put_tail(pre, pre, pseg_mate[...])
    unrolled(heads // 2, UNROLL_KV, raise_keys(pre, pre))

    phase("wait_uq")
    load_uq.wait()
    for copy in send_q:
        copy.wait_recv()
    send_new.wait_recv()
    phase("queries")
    lat[pl.ds(old, new), :] = new_lat[:, :kv_lat]
    new_rope = jnp.concatenate([new_lat[:, kv_lat:].astype(F32), jnp.zeros((new, LANES - ROPE_DIM), F32)], axis=1)
    new_rope = jnp.concatenate([new_rope, jnp.zeros((LANES - new, LANES), F32)], axis=0)
    new_rope = jnp.transpose(new_rope).astype(BF16)
    tail_t[0, :, pl.ds(old, LANES)] = new_rope
    tail_t[1, :ROPE_DIM, pl.ds(old, LANES)] = new_rope[ROPE_DIM:]
    tail_t[1, ROPE_DIM:, pl.ds(old, LANES)] = new_rope[:ROPE_DIM]
    low_half = lane_of((all_toks, LANES)) < ROPE_DIM
    first_half = lax.rem(lane_of((all_toks, LANES)), ROPE_DIM) < HALF

    def raise_queries(pair):
        cols = pl.ds(pl.multiple_of(pair * (2 * QK_DIM), LANES), 2 * QK_DIM)
        q = dot(qlat_all[...], wuq_v[:, cols])
        nope_a, mid, end = q[:, :LANES], q[:, LANES:2 * LANES], q[:, 2 * LANES:]
        nope_b = turn(jnp.where(low_half, end, mid), ROPE_DIM)
        u = jnp.where(low_half, mid, end)
        swapped = jnp.where(first_half, turn(u, LANES - HALF), turn(u, HALF))
        r = u * cos_all[...] + swapped * sin_all[...]
        queries[2 * pair] = jnp.concatenate([nope_a, jnp.where(low_half, r, mask_a[...])], axis=1).astype(BF16)
        queries[2 * pair + 1] = jnp.concatenate([nope_b, jnp.where(low_half, mask_a[...], r)], axis=1).astype(BF16)

    def raise_new_keys(pair):
        up = dot(new_lat[:, :kv_lat], pair_weights(pair, 0))
        up = jnp.transpose(jnp.concatenate([up, jnp.zeros((LANES - new, 2 * NOPE_DIM), F32)], axis=0)).astype(BF16)
        keys_t[2 * pair, :, pl.ds(old, LANES)] = up[:NOPE_DIM]
        keys_t[2 * pair + 1, :, pl.ds(old, LANES)] = up[NOPE_DIM:]

    for pair in range(heads // 2):
        raise_queries(pair)
        raise_new_keys(pair)

    phase("score")

    def score(head, j):
        s = dot(queries[head], jnp.concatenate([keys_t[head], tail_t[j % 2]], axis=0))
        scores[j, :, :old] = s[:, :old]
        scores[j, :, old:] = s[:, old:] + bias[...]
        step = 16
        tops = [jnp.max(scores[j, r:r + step, :], axis=1, keepdims=True) for r in range(0, all_toks, step)]
        for i, top in enumerate(tops):
            rows = pl.ds(i * step, step)
            p = jnp.exp2((scores[j, rows, :] - top) * EXP_SCALE)
            probs[head, rows, :] = p.astype(BF16)
            tops_all[head, rows, :] = jnp.broadcast_to(top, (step, LANES))
            sums_all[head, rows, :] = jnp.broadcast_to(jnp.sum(p, axis=1, keepdims=True), (step, LANES))

    raise_mate = raise_values(pre, pre + new)

    def peer(j):
        return lax.rem(chip + j, chips)

    send_stats = []
    for part in range(PARTS):
        packed = jnp.zeros((all_toks, LANES), F32)
        for head in range(part * some, (part + 1) * some):
            score(head, head % SCORE_BUFS)
        for pair in range(sum(VALUE_PAIRS[:part]), sum(VALUE_PAIRS[:part + 1])):
            raise_mate(pair)
        for i in range(some):
            packed = jnp.where(lanes == i, tops_all[part * some + i], packed)
            packed = jnp.where(lanes == some + i, sums_all[part * some + i], packed)
        stats[part] = jnp.transpose(packed)[:2 * some]
        send_stats.append([
            send(stats.at[part], stats_rx.at[part, j - 1], st_send.at[part, j - 1], st_recv.at[part, j - 1], lax.rem(me + j, n))
            for j in range(1, n)
        ])
    red_copies = {}
    both = CORES * toks
    half = len(ORDER[0]) * both

    def put_scale(part):
        for side in range(CORES):
            got = [stats_rx[part, j - 1] for j in range(1 + (1 - side), n, CORES)]
            mine = stats[part] if side == 0 else jnp.where(core == 0, got[-1], got[0])
            every = got + [mine] if side == 0 else got
            top = functools.reduce(jnp.maximum, [g[:some] for g in every])
            total = functools.reduce(jnp.add, [g[some:] * jnp.exp2((g[:some] - top) * EXP_SCALE) for g in every])
            share = jnp.exp2((mine[:some] - top) * EXP_SCALE)
            scales[part, side, :, :some] = jnp.transpose(share / total)

    def put_split(part, g, sides):
        for b, j in enumerate(ORDER[g]):
            from_rows = pl.ds(pl.multiple_of(peer(j) * both, both), both)
            for side in sides:
                factor = scales[part, side, from_rows, :]
                for i in range(some):
                    cols = pl.ds(((part * CORES + side) * some + i) * V_DIM, V_DIM)
                    o = acc[side, part * some + i, from_rows, :] * factor[:, i:i + 1]
                    o_hi = o.astype(BF16)
                    split[g, pl.ds(b * both, both), cols] = o_hi
                    split[g, pl.ds(half + b * both, both), cols] = (o - o_hi.astype(F32)).astype(BF16)

    def project(part, g):
        ks = pl.ds(part * CORES * deep, CORES * deep)
        y = dot(split[g, :, ks], wo_v[ks, :])
        return y[:half] + y[half:]

    def deliver(g):
        for b, j in enumerate(ORDER[g]):
            for r in range(CORES):
                if j or r:
                    to = lax.rem(core + r, CORES)
                    rows = pl.ds(pl.multiple_of(b * both + to * toks, toks), toks)
                    red_copies[j, r] = send(
                        z.at[g, rows], z_rx.at[j, r], red_send.at[j, r], red_recv.at[j, r], peer(j) * CORES + to
                    )

    def attend(part):
        for head in range(part * some, (part + 1) * some):
            cols = pl.ds((head % 2) * V_DIM, V_DIM)
            acc[0, head] = dot(probs[head], values[head // 2, :, cols])

    def swap(part):
        group = pl.ds(part * some, some)
        return send(acc.at[0, group], acc.at[1, group], acc_send.at[part], acc_recv.at[part], mate)

    phase("attend0")
    for pair in range(sum(VALUE_PAIRS[:PARTS]), heads // 2):
        raise_mate(pair)
    attend(0)
    send_acc = [swap(0)]
    phase("wait_stats0")
    for copy in load_o:
        copy.wait()
    for copy in send_stats[0]:
        copy.wait_recv()
    phase("attend1")
    put_scale(0)
    attend(1)
    for g in range(len(ORDER)):
        put_split(0, g, (0,))
    send_acc.append(swap(1))
    phase("wait_acc0")
    send_acc[0].wait_recv()
    phase("outproj0")
    for g in range(len(ORDER)):
        put_split(0, g, (1,))
    z[0] = project(0, 0)
    phase("wait_acc1")
    send_acc[1].wait_recv()
    phase("wait_stats1")
    for copy in send_stats[1]:
        copy.wait_recv()
    phase("outproj1")
    put_scale(1)
    z[1] = project(0, 1)
    for g in range(len(ORDER)):
        put_split(1, g, range(CORES))
        z[g] = z[g] + project(1, g)
        deliver(g)
    for j in (0, 1, 3, 2):
        phase(f"wait_red{j}")
        for r in range(CORES):
            if j or r:
                red_copies[j, r].wait_recv()
    phase("reduce")
    own = pl.ds(pl.multiple_of(both + core * toks, toks), toks)
    for r in range(CORES):
        y = z[1, own, :] if r == 0 else z_rx[0, 1]
        for j in range(1, chips):
            y = y + z_rx[j, r]
        cols = pl.ds(pl.multiple_of(lax.rem(core + r, CORES) * half_width, LANES), half_width)
        out_ref[:, cols] = y.astype(BF16)

    phase("drain")
    for copy in [send_pre, send_pseg, send_new] + send_meta + send_q + sum(send_stats, []) + send_acc + list(red_copies.values()):
        copy.wait_send()
    phase("")


def solution(mesh):
    n = mesh.shape["sp"]
    chips = n // CORES
    tok_spec = P(("dp", "sp"), None)
    vec_spec = P(("dp", "sp"))
    mat_spec = P(None, None)
    gain_spec = P(None)

    def device_step(hidden, seg_ids, positions, prefix_lat, prefix_seg, w_dq, gain_q, w_uq, w_dkv, gain_kv, w_ukv, w_o):
        toks, width = hidden.shape
        pre, lat_dim = prefix_lat.shape
        q_lat = w_dq.shape[1]
        kv_lat = w_ukv.shape[0]
        heads = w_o.shape[0] // V_DIM // CORES
        rows = CORES * (pre + toks)
        wide = CORES * pre + LANES
        all_toks = n * toks
        inv_freq = (ROPE_BASE ** (-np.arange(HALF, dtype=np.float64) / HALF)).astype(np.float32)
        freq = jnp.asarray(np.concatenate([inv_freq] * (LANES // HALF)).reshape(1, LANES))
        vmem = pl.BlockSpec(memory_space=pltpu.VMEM)
        hbm = pl.BlockSpec(memory_space=pltpu.HBM)
        dma = pltpu.SemaphoreType.DMA
        table = pltpu.VMEM((all_toks, LANES), F32)
        return pl.pallas_call(
            functools.partial(kernel, n),
            out_shape=pltpu.VMEM((toks, width), BF16),
            in_specs=[hbm] * 13,
            scratch_shapes=[
                pltpu.VMEM((1, LANES), F32),
                pltpu.VMEM((1, toks), jnp.int32),
                pltpu.VMEM((1, toks), jnp.int32),
                pltpu.VMEM((1, pre), jnp.int32),
                pltpu.VMEM((q_lat,), BF16),
                pltpu.VMEM((kv_lat,), BF16),
                pltpu.VMEM((toks, width), BF16),
                pltpu.VMEM((width, q_lat), BF16),
                pltpu.VMEM((lat_dim, width), BF16),
                pltpu.VMEM((q_lat, heads * QK_DIM), BF16),
                pltpu.VMEM((kv_lat, heads * KV_HEAD), BF16),
                pltpu.VMEM((CORES * heads * V_DIM, width // CORES), BF16),
                pltpu.VMEM((lat_dim, wide), BF16),
                pltpu.VMEM((rows, kv_lat), BF16),
                pltpu.VMEM((CORES * toks, lat_dim), BF16),
                pltpu.VMEM((1, pre), jnp.int32),
                pltpu.VMEM((all_toks, q_lat), BF16),
                table, table, table, table,
                pltpu.VMEM((2, LANES, wide), BF16),
                pltpu.VMEM((heads, NOPE_DIM, wide), BF16),
                pltpu.VMEM((heads // 2, wide, 2 * V_DIM), BF16),
                pltpu.VMEM((heads, all_toks, 2 * LANES), BF16),
                pltpu.VMEM((heads, all_toks, wide), BF16),
                pltpu.VMEM((heads, all_toks, LANES), F32),
                pltpu.VMEM((heads, all_toks, LANES), F32),
                pltpu.VMEM((SCORE_BUFS, all_toks, wide), F32),
                pltpu.VMEM((PARTS, 2 * heads // PARTS, all_toks), F32),
                pltpu.VMEM((PARTS, n - 1, 2 * heads // PARTS, all_toks), F32),
                pltpu.VMEM((CORES, heads, all_toks, V_DIM), F32),
                pltpu.VMEM((PARTS, CORES, all_toks, LANES), F32),
                pltpu.VMEM((2, all_toks, CORES * heads * V_DIM), BF16),
                table,
                pltpu.VMEM((2, all_toks // 2, width // CORES), F32),
                pltpu.VMEM((chips, CORES, toks, width // CORES), F32),
                dma((6,)),
                dma((6,)),
                dma((DQ_LOADS,)),
                dma((PARTS, CORES)),
                dma((KV_LOADS,)),
                dma((3,)), dma((3,)),
                dma((n - 1,)), dma((n - 1,)),
                dma((n - 1,)), dma((n - 1,)),
                dma((PARTS, n - 1)), dma((PARTS, n - 1)),
                dma((PARTS,)), dma((PARTS,)),
                dma((chips, CORES)), dma((chips, CORES)),
            ],
            compiler_params=pltpu.CompilerParams(
                collective_id=0, has_side_effects=True, vmem_limit_bytes=60 * 1024 * 1024
            ),
        )(
            freq, seg_ids.reshape(1, toks), positions.reshape(1, toks), prefix_seg.reshape(1, pre),
            gain_q, gain_kv,
            hidden, prefix_lat.T, w_dq, w_uq, w_dkv.T, w_ukv, w_o,
        )

    return jax.shard_map(
        device_step,
        mesh=mesh,
        in_specs=(tok_spec, vec_spec, vec_spec, tok_spec, vec_spec, mat_spec, gain_spec, mat_spec, mat_spec, gain_spec, mat_spec, mat_spec),
        out_specs=tok_spec,
        check_vma=False,
    )
```

```python
import functools
import math

import jax
import jax.numpy as jnp
import numpy as np
from jax import lax
from jax.experimental import pallas as pl
from jax.experimental.pallas import tpu as pltpu
from jax.sharding import PartitionSpec as P

ROPE_DIM = 64
HALF = ROPE_DIM // 2
NOPE_DIM = 128
V_DIM = 128
QK_DIM = NOPE_DIM + ROPE_DIM
KV_HEAD = NOPE_DIM + V_DIM
CORES = 2
EPS = 1e-6
ROPE_BASE = 10000.0
NEG_BIG = -1e30
EXP_SCALE = QK_DIM ** -0.5 * math.log2(math.e)
LANES = 128
ORDER = ((2, 1), (3, 0))
PARTS = 2
KV_LOADS = 2
DQ_LOADS = 4
UNROLL_KV = 8
SCORE_BUFS = 8

F32 = jnp.float32
BF16 = jnp.bfloat16


def dot(a, b):
    return jnp.dot(a, b, preferred_element_type=F32)


def dot_nt(a, b):
    return lax.dot_general(a, b, (((1,), (1,)), ((), ())), preferred_element_type=F32)


def dot_tn(a, b):
    return lax.dot_general(a, b, (((0,), (0,)), ((), ())), preferred_element_type=F32)


def rms_norm(values, gain):
    inv_rms = lax.rsqrt(jnp.mean(values * values, axis=-1, keepdims=True) + EPS)
    return values * inv_rms * gain.astype(F32).reshape(1, gain.shape[0])


def row_to_column(row):
    size = row.shape[1]
    here = lax.broadcasted_iota(jnp.int32, (size, size), 0) == lax.broadcasted_iota(jnp.int32, (size, size), 1)
    return jnp.sum(jnp.where(here, jnp.broadcast_to(row, (size, size)), 0.0), axis=1, keepdims=True)


def lane_of(shape):
    return lax.broadcasted_iota(jnp.int32, shape, len(shape) - 1)


def turn(x, amount):
    return pltpu.roll(x, amount, 1)


def unrolled(count, step, body):
    if count == step:
        for j in range(step):
            body(j)
        return

    def run(i, carry):
        for j in range(step):
            body(i * step + j)
        return carry

    lax.fori_loop(0, count // step, run, 0)


class Phases:
    def __init__(self):
        self.now = None

    def __call__(self, name):
        if self.now is not None:
            self.now.__exit__(None, None, None)
        self.now = None
        if name:
            self.now = jax.named_scope(name)
            self.now.__enter__()


def kernel(
    n,
    freq_hbm, seg_hbm, pos_hbm, pseg_hbm, gain_q_hbm, gain_kv_hbm,
    hid_hbm, pre_hbm, wdq_hbm, wuq_hbm, wdkv_hbm, wukv_hbm, wo_hbm,
    out_ref,
    freq_ref, seg_ref, pos_ref, pseg_ref, gain_q_ref, gain_kv_ref,
    hid_v, wdq_v, wdkv_v, wuq_v, wukv_v, wo_v,
    lat_t, lat, new_lat, pseg_mate, qlat_all, meta_all, cos_all, sin_all, mask_a, tail_t,
    keys_t, values, queries, probs, tops_all, sums_all,
    scores, stats, stats_rx, acc, scales, split, bias, z, z_rx,
    load_sem, small_sem, dq_sem, wo_sem, ukv_sem, mate_send, mate_recv, gat_send, gat_recv, met_send, met_recv,
    st_send, st_recv, acc_send, acc_recv, red_send, red_recv,
):
    phase = Phases()
    me = lax.axis_index("sp")
    core = lax.rem(me, CORES)
    chip = lax.div(me, CORES)
    chips = n // CORES
    mate = chip * CORES + (CORES - 1 - core)
    toks = hid_v.shape[0]
    pre = pre_hbm.shape[1]
    kv_lat = wukv_v.shape[0]
    heads = keys_t.shape[0]
    old = CORES * pre
    new = CORES * toks
    wide = lat_t.shape[1]
    all_toks = n * toks
    some = heads // PARTS
    deep = some * V_DIM
    half_width = wo_v.shape[1]

    phase("loads")

    def load(src, dst, sem):
        copy = pltpu.make_async_copy(src, dst, sem)
        copy.start()
        return copy

    barrier = pltpu.get_barrier_semaphore()
    for j in range(1, n):
        pl.semaphore_signal(barrier, inc=1, device_id={"sp": lax.rem(me + j, n)}, device_id_type=pl.DeviceIdType.MESH)
    smalls = [
        load(src, dst, small_sem.at[i])
        for i, (src, dst) in enumerate([
            (freq_hbm, freq_ref), (seg_hbm, seg_ref), (pos_hbm, pos_ref),
            (gain_q_hbm, gain_q_ref), (gain_kv_hbm, gain_kv_ref), (pseg_hbm, pseg_ref),
        ])
    ]
    load_hid = load(hid_hbm, hid_v, load_sem.at[0])
    depth = wdq_v.shape[0] // DQ_LOADS
    load_dq = [
        load(wdq_hbm.at[pl.ds(i * depth, depth)], wdq_v.at[pl.ds(i * depth, depth)], dq_sem.at[i])
        for i in range(DQ_LOADS)
    ]
    kv_cols = heads * KV_HEAD
    part = kv_cols // KV_LOADS

    def load_up(i):
        return load(
            wukv_hbm.at[:, pl.ds(pl.multiple_of(core * kv_cols + i * part, LANES), part)],
            wukv_v.at[:, pl.ds(i * part, part)],
            ukv_sem.at[i],
        )

    load_pre = load(pre_hbm, lat_t.at[:, pl.ds(0, pre)], load_sem.at[3])
    load_ukv = [load_up(0)]

    phase("wait_small")
    for copy in smalls:
        copy.wait()
    phase("meta")
    pos_col = row_to_column(pos_ref[...].astype(F32))
    seg_col = row_to_column(seg_ref[...].astype(F32))
    angles = pos_col * freq_ref[...]
    lane = lane_of((toks, LANES))
    cos_t = jnp.cos(angles)
    sin_t = jnp.sin(angles)
    my_rows = pl.ds(pl.multiple_of(me * toks, toks), toks)
    meta_all[my_rows, :] = jnp.where(
        lane < HALF, cos_t, jnp.where(lane < 2 * HALF, sin_t, jnp.where(lane == 2 * HALF, seg_col, pos_col))
    )

    def send(src, dst, send_sem, recv_sem, target):
        copy = pltpu.make_async_remote_copy(
            src_ref=src, dst_ref=dst, send_sem=send_sem, recv_sem=recv_sem,
            device_id={"sp": target}, device_id_type=pl.DeviceIdType.MESH,
        )
        copy.start()
        return copy

    phase("wait_dq")
    load_hid.wait()
    for copy in load_dq:
        copy.wait()
    load_ukv += [load_up(i) for i in range(1, KV_LOADS)]
    load_dkv = load(wdkv_hbm, wdkv_v, load_sem.at[2])
    phase("barrier")
    pl.semaphore_wait(barrier, n - 1)
    send_pre = send(pre_hbm, lat_t.at[:, pl.ds(pre, pre)], mate_send.at[0], mate_recv.at[0], mate)
    send_pseg = send(pseg_ref, pseg_mate, mate_send.at[1], mate_recv.at[1], mate)
    send_meta = [
        send(meta_all.at[my_rows], meta_all.at[my_rows], met_send.at[j - 1], met_recv.at[j - 1], lax.rem(me + j, n))
        for j in range(1, n)
    ]
    phase("qlat")
    qlat_all[my_rows, :] = rms_norm(dot(hid_v[...], wdq_v[...]), gain_q_ref[...]).astype(BF16)

    send_q = [
        send(qlat_all.at[my_rows], qlat_all.at[my_rows], gat_send.at[j - 1], gat_recv.at[j - 1], lax.rem(me + j, n))
        for j in range(1, n)
    ]
    def pair_weights(pair, offset):
        first = pl.multiple_of(pair * (2 * KV_HEAD) + offset, LANES)
        second = pl.multiple_of(pair * (2 * KV_HEAD) + KV_HEAD + offset, LANES)
        return jnp.concatenate([wukv_v[:, pl.ds(first, LANES)], wukv_v[:, pl.ds(second, LANES)]], axis=1)

    def raise_keys(start, size):
        def step(pair):
            up = dot_tn(pair_weights(pair, 0), lat_t[:kv_lat, pl.ds(start, size)]).astype(BF16)
            keys_t[2 * pair, :, pl.ds(start, size)] = up[:NOPE_DIM]
            keys_t[2 * pair + 1, :, pl.ds(start, size)] = up[NOPE_DIM:]
        return step

    def raise_values(start, size):
        def step(pair):
            values[pair, pl.ds(start, size), :] = dot(lat[pl.ds(start, size), :], pair_weights(pair, NOPE_DIM)).astype(BF16)
        return step

    def put_tail(start, size, seg_row):
        hot = seg_row == lax.broadcasted_iota(jnp.int32, (ROPE_DIM, size), 0)
        hot = jnp.where(hot, 1.0, 0.0).astype(BF16)
        rope = lat_t[kv_lat:, pl.ds(start, size)]
        tail_t[0, :, pl.ds(start, size)] = jnp.concatenate([rope, hot], axis=0)
        tail_t[1, :, pl.ds(start, size)] = jnp.concatenate([hot, rope], axis=0)
    per = heads // 2 // KV_LOADS
    for i in range(KV_LOADS):
        phase(f"wait_own{i}")
        load_ukv[i].wait()
        if i == 0:
            load_pre.wait()
        else:
            load_dkv.wait()
        phase(f"own{i}")
        if i == 0:
            lat[pl.ds(0, pre), :] = jnp.transpose(lat_t[:kv_lat, pl.ds(0, pre)])
            put_tail(0, pre, pseg_ref[...])
            values[:, pl.ds(old + new, wide - old - new), :] = jnp.zeros((heads // 2, wide - old - new, 2 * V_DIM), BF16)
        else:
            load_uq = load(
                wuq_hbm.at[:, pl.ds(pl.multiple_of(core * heads * QK_DIM, LANES), heads * QK_DIM)], wuq_v, load_sem.at[4]
            )
            load_o = [
                load(
                    wo_hbm.at[
                        pl.ds(pl.multiple_of(lax.rem(core + side, CORES) * (heads * V_DIM) + part * deep, LANES), deep),
                        pl.ds(pl.multiple_of(core * half_width, LANES), half_width),
                    ],
                    wo_v.at[pl.ds((part * CORES + side) * deep, deep)],
                    wo_sem.at[part, side],
                )
                for part in range(PARTS) for side in range(CORES)
            ]
            down = dot_nt(hid_v[...], wdkv_v[...])
            c_kv = rms_norm(down[:, :kv_lat], gain_kv_ref[...])
            low, high = down[:, kv_lat:kv_lat + HALF], down[:, kv_lat + HALF:]
            cos_m, sin_m = cos_t[:, :HALF], sin_t[:, :HALF]
            k_new = jnp.concatenate([low * cos_m - high * sin_m, high * cos_m + low * sin_m], axis=1)
            new_lat[pl.ds(0, toks), :] = jnp.concatenate([c_kv, k_new], axis=1).astype(BF16)
        for pair in range(i * per, (i + 1) * per):
            raise_keys(0, pre)(pair)
            raise_values(0, pre)(pair)
    send_new = send(new_lat.at[pl.ds(0, toks)], new_lat.at[pl.ds(toks, toks)], mate_send.at[2], mate_recv.at[2], mate)

    phase("wait_meta")
    for copy in send_meta:
        copy.wait_recv()
    phase("wait_mate")
    send_pre.wait_recv()
    send_pseg.wait_recv()
    phase("keys_mate")
    every = meta_all[...]
    lanes = lane_of((all_toks, LANES))
    q_seg = every[:, 2 * HALF:2 * HALF + 1]
    q_pos = every[:, 2 * HALF + 1:2 * HALF + 2]
    cos_q = jnp.where(lanes < HALF, every, 0.0)
    cos_q = cos_q + turn(cos_q, HALF)
    cos_all[...] = cos_q + turn(cos_q, 2 * HALF)
    sin_q = jnp.where((lanes >= HALF) & (lanes < 2 * HALF), every, 0.0)
    sin_q = sin_q - turn(sin_q, LANES - HALF)
    sin_all[...] = sin_q + turn(sin_q, 2 * HALF)
    q_mask = jnp.where(q_seg == jnp.where(lanes < ROPE_DIM, lanes, lanes - ROPE_DIM).astype(F32), 0.0, NEG_BIG)
    mask_a[...] = q_mask
    mate_rows = pl.ds(pl.multiple_of(mate * toks, toks), toks)
    new_meta = jnp.concatenate(
        [meta_all[my_rows, :], meta_all[mate_rows, :], jnp.zeros((LANES - new, LANES), F32)], axis=0
    )
    meta_rows = jnp.transpose(new_meta)
    k_seg, k_pos = meta_rows[2 * HALF:2 * HALF + 1], meta_rows[2 * HALF + 1:2 * HALF + 2]
    seen = (q_seg == k_seg) & (k_pos <= q_pos) & (lane_of((all_toks, LANES)) < new)
    bias[...] = jnp.where(seen, 0.0, NEG_BIG)

    lat[pl.ds(pre, pre), :] = jnp.transpose(lat_t[:kv_lat, pl.ds(pre, pre)])
    put_tail(pre, pre, pseg_mate[...])
    unrolled(heads // 2, UNROLL_KV, raise_keys(pre, pre))

    phase("wait_uq")
    load_uq.wait()
    for copy in send_q:
        copy.wait_recv()
    send_new.wait_recv()
    phase("queries")
    lat[pl.ds(old, new), :] = new_lat[:, :kv_lat]
    new_rope = jnp.concatenate([new_lat[:, kv_lat:].astype(F32), jnp.zeros((new, LANES - ROPE_DIM), F32)], axis=1)
    new_rope = jnp.concatenate([new_rope, jnp.zeros((LANES - new, LANES), F32)], axis=0)
    new_rope = jnp.transpose(new_rope).astype(BF16)
    tail_t[0, :, pl.ds(old, LANES)] = new_rope
    tail_t[1, :ROPE_DIM, pl.ds(old, LANES)] = new_rope[ROPE_DIM:]
    tail_t[1, ROPE_DIM:, pl.ds(old, LANES)] = new_rope[:ROPE_DIM]
    low_half = lane_of((all_toks, LANES)) < ROPE_DIM
    first_half = lax.rem(lane_of((all_toks, LANES)), ROPE_DIM) < HALF

    def raise_queries(pair):
        cols = pl.ds(pl.multiple_of(pair * (2 * QK_DIM), LANES), 2 * QK_DIM)
        q = dot(qlat_all[...], wuq_v[:, cols])
        nope_a, mid, end = q[:, :LANES], q[:, LANES:2 * LANES], q[:, 2 * LANES:]
        nope_b = turn(jnp.where(low_half, end, mid), ROPE_DIM)
        u = jnp.where(low_half, mid, end)
        swapped = jnp.where(first_half, turn(u, LANES - HALF), turn(u, HALF))
        r = u * cos_all[...] + swapped * sin_all[...]
        queries[2 * pair] = jnp.concatenate([nope_a, jnp.where(low_half, r, mask_a[...])], axis=1).astype(BF16)
        queries[2 * pair + 1] = jnp.concatenate([nope_b, jnp.where(low_half, mask_a[...], r)], axis=1).astype(BF16)

    def raise_new_keys(pair):
        up = dot(new_lat[:, :kv_lat], pair_weights(pair, 0))
        up = jnp.transpose(jnp.concatenate([up, jnp.zeros((LANES - new, 2 * NOPE_DIM), F32)], axis=0)).astype(BF16)
        keys_t[2 * pair, :, pl.ds(old, LANES)] = up[:NOPE_DIM]
        keys_t[2 * pair + 1, :, pl.ds(old, LANES)] = up[NOPE_DIM:]

    for pair in range(heads // 2):
        raise_queries(pair)
        raise_new_keys(pair)

    phase("score")

    def score(head, j):
        s = dot(queries[head], jnp.concatenate([keys_t[head], tail_t[j % 2]], axis=0))
        scores[j, :, :old] = s[:, :old]
        scores[j, :, old:] = s[:, old:] + bias[...]
        step = 16
        tops = [jnp.max(scores[j, r:r + step, :], axis=1, keepdims=True) for r in range(0, all_toks, step)]
        for i, top in enumerate(tops):
            rows = pl.ds(i * step, step)
            p = jnp.exp2((scores[j, rows, :] - top) * EXP_SCALE)
            probs[head, rows, :] = p.astype(BF16)
            tops_all[head, rows, :] = jnp.broadcast_to(top, (step, LANES))
            sums_all[head, rows, :] = jnp.broadcast_to(jnp.sum(p, axis=1, keepdims=True), (step, LANES))

    raise_mate = raise_values(pre, pre + new)

    def peer(j):
        return lax.rem(chip + j, chips)

    def attend(head):
        cols = pl.ds((head % 2) * V_DIM, V_DIM)
        acc[0, head] = dot(probs[head], values[head // 2, :, cols])

    def swap(part):
        group = pl.ds(part * some, some)
        return send(acc.at[0, group], acc.at[1, group], acc_send.at[part], acc_recv.at[part], mate)

    send_stats = []
    for part in range(PARTS):
        packed = jnp.zeros((all_toks, LANES), F32)
        for head in range(part * some, (part + 1) * some):
            score(head, head % SCORE_BUFS)
            if head % 2:
                raise_mate(head // 2)
            if part:
                attend(head - some)
        for i in range(some):
            packed = jnp.where(lanes == i, tops_all[part * some + i], packed)
            packed = jnp.where(lanes == some + i, sums_all[part * some + i], packed)
        stats[part] = jnp.transpose(packed)[:2 * some]
        send_stats.append([
            send(stats.at[part], stats_rx.at[part, j - 1], st_send.at[part, j - 1], st_recv.at[part, j - 1], lax.rem(me + j, n))
            for j in range(1, n)
        ])
    send_acc = [swap(0)]
    red_copies = {}
    both = CORES * toks
    half = len(ORDER[0]) * both

    def put_scale(part):
        for side in range(CORES):
            got = [stats_rx[part, j - 1] for j in range(1 + (1 - side), n, CORES)]
            mine = stats[part] if side == 0 else jnp.where(core == 0, got[-1], got[0])
            every = got + [mine] if side == 0 else got
            top = functools.reduce(jnp.maximum, [g[:some] for g in every])
            total = functools.reduce(jnp.add, [g[some:] * jnp.exp2((g[:some] - top) * EXP_SCALE) for g in every])
            share = jnp.exp2((mine[:some] - top) * EXP_SCALE)
            scales[part, side, :, :some] = jnp.transpose(share / total)

    def put_split(part, g, sides):
        for b, j in enumerate(ORDER[g]):
            from_rows = pl.ds(pl.multiple_of(peer(j) * both, both), both)
            for side in sides:
                factor = scales[part, side, from_rows, :]
                for i in range(some):
                    cols = pl.ds(((part * CORES + side) * some + i) * V_DIM, V_DIM)
                    o = acc[side, part * some + i, from_rows, :] * factor[:, i:i + 1]
                    o_hi = o.astype(BF16)
                    split[g, pl.ds(b * both, both), cols] = o_hi
                    split[g, pl.ds(half + b * both, both), cols] = (o - o_hi.astype(F32)).astype(BF16)

    def project(part, g):
        ks = pl.ds(part * CORES * deep, CORES * deep)
        y = dot(split[g, :, ks], wo_v[ks, :])
        return y[:half] + y[half:]

    def deliver(g):
        for b, j in enumerate(ORDER[g]):
            for r in range(CORES):
                if j or r:
                    to = lax.rem(core + r, CORES)
                    rows = pl.ds(pl.multiple_of(b * both + to * toks, toks), toks)
                    red_copies[j, r] = send(
                        z.at[g, rows], z_rx.at[j, r], red_send.at[j, r], red_recv.at[j, r], peer(j) * CORES + to
                    )

    phase("wait_stats0")
    for copy in load_o:
        copy.wait()
    for copy in send_stats[0]:
        copy.wait_recv()
    phase("attend1")
    put_scale(0)
    for head in range(some, heads):
        attend(head)
    for g in range(len(ORDER)):
        put_split(0, g, (0,))
    send_acc.append(swap(1))
    phase("wait_acc0")
    send_acc[0].wait_recv()
    phase("outproj0")
    for g in range(len(ORDER)):
        put_split(0, g, (1,))
    z[0] = project(0, 0)
    phase("wait_acc1")
    send_acc[1].wait_recv()
    phase("wait_stats1")
    for copy in send_stats[1]:
        copy.wait_recv()
    phase("outproj1")
    put_scale(1)
    z[1] = project(0, 1)
    for g in range(len(ORDER)):
        put_split(1, g, range(CORES))
        z[g] = z[g] + project(1, g)
        deliver(g)
    for j in (0, 1, 3, 2):
        phase(f"wait_red{j}")
        for r in range(CORES):
            if j or r:
                red_copies[j, r].wait_recv()
    phase("reduce")
    own = pl.ds(pl.multiple_of(both + core * toks, toks), toks)
    for r in range(CORES):
        y = z[1, own, :] if r == 0 else z_rx[0, 1]
        for j in range(1, chips):
            y = y + z_rx[j, r]
        cols = pl.ds(pl.multiple_of(lax.rem(core + r, CORES) * half_width, LANES), half_width)
        out_ref[:, cols] = y.astype(BF16)

    phase("drain")
    for copy in [send_pre, send_pseg, send_new] + send_meta + send_q + sum(send_stats, []) + send_acc + list(red_copies.values()):
        copy.wait_send()
    phase("")


def solution(mesh):
    n = mesh.shape["sp"]
    chips = n // CORES
    tok_spec = P(("dp", "sp"), None)
    vec_spec = P(("dp", "sp"))
    mat_spec = P(None, None)
    gain_spec = P(None)

    def device_step(hidden, seg_ids, positions, prefix_lat, prefix_seg, w_dq, gain_q, w_uq, w_dkv, gain_kv, w_ukv, w_o):
        toks, width = hidden.shape
        pre, lat_dim = prefix_lat.shape
        q_lat = w_dq.shape[1]
        kv_lat = w_ukv.shape[0]
        heads = w_o.shape[0] // V_DIM // CORES
        rows = CORES * (pre + toks)
        wide = CORES * pre + LANES
        all_toks = n * toks
        inv_freq = (ROPE_BASE ** (-np.arange(HALF, dtype=np.float64) / HALF)).astype(np.float32)
        freq = jnp.asarray(np.concatenate([inv_freq] * (LANES // HALF)).reshape(1, LANES))
        vmem = pl.BlockSpec(memory_space=pltpu.VMEM)
        hbm = pl.BlockSpec(memory_space=pltpu.HBM)
        dma = pltpu.SemaphoreType.DMA
        table = pltpu.VMEM((all_toks, LANES), F32)
        return pl.pallas_call(
            functools.partial(kernel, n),
            out_shape=pltpu.VMEM((toks, width), BF16),
            in_specs=[hbm] * 13,
            scratch_shapes=[
                pltpu.VMEM((1, LANES), F32),
                pltpu.VMEM((1, toks), jnp.int32),
                pltpu.VMEM((1, toks), jnp.int32),
                pltpu.VMEM((1, pre), jnp.int32),
                pltpu.VMEM((q_lat,), BF16),
                pltpu.VMEM((kv_lat,), BF16),
                pltpu.VMEM((toks, width), BF16),
                pltpu.VMEM((width, q_lat), BF16),
                pltpu.VMEM((lat_dim, width), BF16),
                pltpu.VMEM((q_lat, heads * QK_DIM), BF16),
                pltpu.VMEM((kv_lat, heads * KV_HEAD), BF16),
                pltpu.VMEM((CORES * heads * V_DIM, width // CORES), BF16),
                pltpu.VMEM((lat_dim, wide), BF16),
                pltpu.VMEM((rows, kv_lat), BF16),
                pltpu.VMEM((CORES * toks, lat_dim), BF16),
                pltpu.VMEM((1, pre), jnp.int32),
                pltpu.VMEM((all_toks, q_lat), BF16),
                table, table, table, table,
                pltpu.VMEM((2, LANES, wide), BF16),
                pltpu.VMEM((heads, NOPE_DIM, wide), BF16),
                pltpu.VMEM((heads // 2, wide, 2 * V_DIM), BF16),
                pltpu.VMEM((heads, all_toks, 2 * LANES), BF16),
                pltpu.VMEM((heads, all_toks, wide), BF16),
                pltpu.VMEM((heads, all_toks, LANES), F32),
                pltpu.VMEM((heads, all_toks, LANES), F32),
                pltpu.VMEM((SCORE_BUFS, all_toks, wide), F32),
                pltpu.VMEM((PARTS, 2 * heads // PARTS, all_toks), F32),
                pltpu.VMEM((PARTS, n - 1, 2 * heads // PARTS, all_toks), F32),
                pltpu.VMEM((CORES, heads, all_toks, V_DIM), F32),
                pltpu.VMEM((PARTS, CORES, all_toks, LANES), F32),
                pltpu.VMEM((2, all_toks, CORES * heads * V_DIM), BF16),
                table,
                pltpu.VMEM((2, all_toks // 2, width // CORES), F32),
                pltpu.VMEM((chips, CORES, toks, width // CORES), F32),
                dma((6,)),
                dma((6,)),
                dma((DQ_LOADS,)),
                dma((PARTS, CORES)),
                dma((KV_LOADS,)),
                dma((3,)), dma((3,)),
                dma((n - 1,)), dma((n - 1,)),
                dma((n - 1,)), dma((n - 1,)),
                dma((PARTS, n - 1)), dma((PARTS, n - 1)),
                dma((PARTS,)), dma((PARTS,)),
                dma((chips, CORES)), dma((chips, CORES)),
            ],
            compiler_params=pltpu.CompilerParams(
                collective_id=0, has_side_effects=True, vmem_limit_bytes=60 * 1024 * 1024
            ),
        )(
            freq, seg_ids.reshape(1, toks), positions.reshape(1, toks), prefix_seg.reshape(1, pre),
            gain_q, gain_kv,
            hidden, prefix_lat.T, w_dq, w_uq, w_dkv.T, w_ukv, w_o,
        )

    return jax.shard_map(
        device_step,
        mesh=mesh,
        in_specs=(tok_spec, vec_spec, vec_spec, tok_spec, vec_spec, mat_spec, gain_spec, mat_spec, mat_spec, gain_spec, mat_spec, mat_spec),
        out_specs=tok_spec,
        check_vma=False,
    )
```

```python
import functools
import math

import jax
import jax.numpy as jnp
import numpy as np
from jax import lax
from jax.experimental import pallas as pl
from jax.experimental.pallas import tpu as pltpu
from jax.sharding import PartitionSpec as P

ROPE_DIM = 64
HALF = ROPE_DIM // 2
NOPE_DIM = 128
V_DIM = 128
QK_DIM = NOPE_DIM + ROPE_DIM
KV_HEAD = NOPE_DIM + V_DIM
CORES = 2
EPS = 1e-6
ROPE_BASE = 10000.0
NEG_BIG = -1e30
EXP_SCALE = QK_DIM ** -0.5 * math.log2(math.e)
LANES = 128
ORDER = ((2, 1), (3, 0))
PARTS = 2
SWAPS = 2
VALUE_PAIRS = (4, 2, 2)
KV_LOADS = 2
DQ_LOADS = 4
UNROLL_KV = 8
SCORE_BUFS = 8

F32 = jnp.float32
BF16 = jnp.bfloat16


def dot(a, b):
    return jnp.dot(a, b, preferred_element_type=F32)


def dot_nt(a, b):
    return lax.dot_general(a, b, (((1,), (1,)), ((), ())), preferred_element_type=F32)


def dot_tn(a, b):
    return lax.dot_general(a, b, (((0,), (0,)), ((), ())), preferred_element_type=F32)


def rms_norm(values, gain):
    inv_rms = lax.rsqrt(jnp.mean(values * values, axis=-1, keepdims=True) + EPS)
    return values * inv_rms * gain.astype(F32).reshape(1, gain.shape[0])


def row_to_column(row):
    size = row.shape[1]
    here = lax.broadcasted_iota(jnp.int32, (size, size), 0) == lax.broadcasted_iota(jnp.int32, (size, size), 1)
    return jnp.sum(jnp.where(here, jnp.broadcast_to(row, (size, size)), 0.0), axis=1, keepdims=True)


def lane_of(shape):
    return lax.broadcasted_iota(jnp.int32, shape, len(shape) - 1)


def turn(x, amount):
    return pltpu.roll(x, amount, 1)


def unrolled(count, step, body):
    if count == step:
        for j in range(step):
            body(j)
        return

    def run(i, carry):
        for j in range(step):
            body(i * step + j)
        return carry

    lax.fori_loop(0, count // step, run, 0)


class Phases:
    def __init__(self):
        self.now = None

    def __call__(self, name):
        if self.now is not None:
            self.now.__exit__(None, None, None)
        self.now = None
        if name:
            self.now = jax.named_scope(name)
            self.now.__enter__()


def kernel(
    n,
    freq_hbm, seg_hbm, pos_hbm, pseg_hbm, gain_q_hbm, gain_kv_hbm,
    hid_hbm, pre_hbm, wdq_hbm, wuq_hbm, wdkv_hbm, wukv_hbm, wo_hbm,
    out_ref,
    freq_ref, seg_ref, pos_ref, pseg_ref, gain_q_ref, gain_kv_ref,
    hid_v, wdq_v, wdkv_v, wuq_v, wukv_v, wo_v,
    lat_t, lat, new_lat, pseg_mate, qlat_all, meta_all, cos_all, sin_all, mask_a, tail_t,
    keys_t, values, queries, probs, tops_all, sums_all,
    scores, stats, stats_rx, acc, scales, split, bias, z, z_rx,
    load_sem, small_sem, dq_sem, wo_sem, ukv_sem, mate_send, mate_recv, gat_send, gat_recv, met_send, met_recv,
    st_send, st_recv, acc_send, acc_recv, red_send, red_recv,
):
    phase = Phases()
    me = lax.axis_index("sp")
    core = lax.rem(me, CORES)
    chip = lax.div(me, CORES)
    chips = n // CORES
    mate = chip * CORES + (CORES - 1 - core)
    toks = hid_v.shape[0]
    pre = pre_hbm.shape[1]
    kv_lat = wukv_v.shape[0]
    heads = keys_t.shape[0]
    old = CORES * pre
    new = CORES * toks
    wide = lat_t.shape[1]
    all_toks = n * toks
    some = heads // PARTS
    deep = some * V_DIM
    half_width = wo_v.shape[1]

    phase("loads")

    def load(src, dst, sem):
        copy = pltpu.make_async_copy(src, dst, sem)
        copy.start()
        return copy

    barrier = pltpu.get_barrier_semaphore()
    for j in range(1, n):
        pl.semaphore_signal(barrier, inc=1, device_id={"sp": lax.rem(me + j, n)}, device_id_type=pl.DeviceIdType.MESH)
    smalls = [
        load(src, dst, small_sem.at[i])
        for i, (src, dst) in enumerate([
            (freq_hbm, freq_ref), (seg_hbm, seg_ref), (pos_hbm, pos_ref),
            (gain_q_hbm, gain_q_ref), (gain_kv_hbm, gain_kv_ref), (pseg_hbm, pseg_ref),
        ])
    ]
    load_hid = load(hid_hbm, hid_v, load_sem.at[0])
    depth = wdq_v.shape[0] // DQ_LOADS
    load_dq = [
        load(wdq_hbm.at[pl.ds(i * depth, depth)], wdq_v.at[pl.ds(i * depth, depth)], dq_sem.at[i])
        for i in range(DQ_LOADS)
    ]
    kv_cols = heads * KV_HEAD
    part = kv_cols // KV_LOADS

    def load_up(i):
        return load(
            wukv_hbm.at[:, pl.ds(pl.multiple_of(core * kv_cols + i * part, LANES), part)],
            wukv_v.at[:, pl.ds(i * part, part)],
            ukv_sem.at[i],
        )

    load_pre = load(pre_hbm, lat_t.at[:, pl.ds(0, pre)], load_sem.at[3])
    load_ukv = [load_up(0)]

    phase("wait_small")
    for copy in smalls:
        copy.wait()
    phase("meta")
    pos_col = row_to_column(pos_ref[...].astype(F32))
    seg_col = row_to_column(seg_ref[...].astype(F32))
    angles = pos_col * freq_ref[...]
    lane = lane_of((toks, LANES))
    cos_t = jnp.cos(angles)
    sin_t = jnp.sin(angles)
    my_rows = pl.ds(pl.multiple_of(me * toks, toks), toks)
    meta_all[my_rows, :] = jnp.where(
        lane < HALF, cos_t, jnp.where(lane < 2 * HALF, sin_t, jnp.where(lane == 2 * HALF, seg_col, pos_col))
    )

    def send(src, dst, send_sem, recv_sem, target):
        copy = pltpu.make_async_remote_copy(
            src_ref=src, dst_ref=dst, send_sem=send_sem, recv_sem=recv_sem,
            device_id={"sp": target}, device_id_type=pl.DeviceIdType.MESH,
        )
        copy.start()
        return copy

    phase("wait_dq")
    load_hid.wait()
    for copy in load_dq:
        copy.wait()
    load_ukv += [load_up(i) for i in range(1, KV_LOADS)]
    load_dkv = load(wdkv_hbm, wdkv_v, load_sem.at[2])
    phase("barrier")
    pl.semaphore_wait(barrier, n - 1)
    send_pre = send(pre_hbm, lat_t.at[:, pl.ds(pre, pre)], mate_send.at[0], mate_recv.at[0], mate)
    send_pseg = send(pseg_ref, pseg_mate, mate_send.at[1], mate_recv.at[1], mate)
    send_meta = [
        send(meta_all.at[my_rows], meta_all.at[my_rows], met_send.at[j - 1], met_recv.at[j - 1], lax.rem(me + j, n))
        for j in range(1, n)
    ]
    phase("qlat")
    qlat_all[my_rows, :] = rms_norm(dot(hid_v[...], wdq_v[...]), gain_q_ref[...]).astype(BF16)

    send_q = [
        send(qlat_all.at[my_rows], qlat_all.at[my_rows], gat_send.at[j - 1], gat_recv.at[j - 1], lax.rem(me + j, n))
        for j in range(1, n)
    ]
    def pair_weights(pair, offset):
        first = pl.multiple_of(pair * (2 * KV_HEAD) + offset, LANES)
        second = pl.multiple_of(pair * (2 * KV_HEAD) + KV_HEAD + offset, LANES)
        return jnp.concatenate([wukv_v[:, pl.ds(first, LANES)], wukv_v[:, pl.ds(second, LANES)]], axis=1)

    def raise_keys(start, size):
        def step(pair):
            up = dot_tn(pair_weights(pair, 0), lat_t[:kv_lat, pl.ds(start, size)]).astype(BF16)
            keys_t[2 * pair, :, pl.ds(start, size)] = up[:NOPE_DIM]
            keys_t[2 * pair + 1, :, pl.ds(start, size)] = up[NOPE_DIM:]
        return step

    def raise_values(start, size):
        def step(pair):
            values[pair, pl.ds(start, size), :] = dot(lat[pl.ds(start, size), :], pair_weights(pair, NOPE_DIM)).astype(BF16)
        return step

    def put_tail(start, size, seg_row):
        hot = seg_row == lax.broadcasted_iota(jnp.int32, (ROPE_DIM, size), 0)
        hot = jnp.where(hot, 1.0, 0.0).astype(BF16)
        rope = lat_t[kv_lat:, pl.ds(start, size)]
        tail_t[0, :, pl.ds(start, size)] = jnp.concatenate([rope, hot], axis=0)
        tail_t[1, :, pl.ds(start, size)] = jnp.concatenate([hot, rope], axis=0)
    per = heads // 2 // KV_LOADS
    for i in range(KV_LOADS):
        phase(f"wait_own{i}")
        load_ukv[i].wait()
        if i == 0:
            load_pre.wait()
        else:
            load_dkv.wait()
        phase(f"own{i}")
        if i == 0:
            lat[pl.ds(0, pre), :] = jnp.transpose(lat_t[:kv_lat, pl.ds(0, pre)])
            put_tail(0, pre, pseg_ref[...])
            values[:, pl.ds(old + new, wide - old - new), :] = jnp.zeros((heads // 2, wide - old - new, 2 * V_DIM), BF16)
        else:
            load_uq = load(
                wuq_hbm.at[:, pl.ds(pl.multiple_of(core * heads * QK_DIM, LANES), heads * QK_DIM)], wuq_v, load_sem.at[4]
            )
            load_o = [
                load(
                    wo_hbm.at[
                        pl.ds(pl.multiple_of(lax.rem(core + side, CORES) * (heads * V_DIM) + part * deep, LANES), deep),
                        pl.ds(pl.multiple_of(core * half_width, LANES), half_width),
                    ],
                    wo_v.at[pl.ds((part * CORES + side) * deep, deep)],
                    wo_sem.at[part, side],
                )
                for part in range(PARTS) for side in range(CORES)
            ]
            down = dot_nt(hid_v[...], wdkv_v[...])
            c_kv = rms_norm(down[:, :kv_lat], gain_kv_ref[...])
            low, high = down[:, kv_lat:kv_lat + HALF], down[:, kv_lat + HALF:]
            cos_m, sin_m = cos_t[:, :HALF], sin_t[:, :HALF]
            k_new = jnp.concatenate([low * cos_m - high * sin_m, high * cos_m + low * sin_m], axis=1)
            new_lat[pl.ds(0, toks), :] = jnp.concatenate([c_kv, k_new], axis=1).astype(BF16)
        for pair in range(i * per, (i + 1) * per):
            raise_keys(0, pre)(pair)
            raise_values(0, pre)(pair)
    send_new = send(new_lat.at[pl.ds(0, toks)], new_lat.at[pl.ds(toks, toks)], mate_send.at[2], mate_recv.at[2], mate)

    phase("wait_meta")
    for copy in send_meta:
        copy.wait_recv()
    phase("wait_mate")
    send_pre.wait_recv()
    send_pseg.wait_recv()
    phase("keys_mate")
    every = meta_all[...]
    lanes = lane_of((all_toks, LANES))
    q_seg = every[:, 2 * HALF:2 * HALF + 1]
    q_pos = every[:, 2 * HALF + 1:2 * HALF + 2]
    cos_q = jnp.where(lanes < HALF, every, 0.0)
    cos_q = cos_q + turn(cos_q, HALF)
    cos_all[...] = cos_q + turn(cos_q, 2 * HALF)
    sin_q = jnp.where((lanes >= HALF) & (lanes < 2 * HALF), every, 0.0)
    sin_q = sin_q - turn(sin_q, LANES - HALF)
    sin_all[...] = sin_q + turn(sin_q, 2 * HALF)
    q_mask = jnp.where(q_seg == jnp.where(lanes < ROPE_DIM, lanes, lanes - ROPE_DIM).astype(F32), 0.0, NEG_BIG)
    mask_a[...] = q_mask
    mate_rows = pl.ds(pl.multiple_of(mate * toks, toks), toks)
    new_meta = jnp.concatenate(
        [meta_all[my_rows, :], meta_all[mate_rows, :], jnp.zeros((LANES - new, LANES), F32)], axis=0
    )
    meta_rows = jnp.transpose(new_meta)
    k_seg, k_pos = meta_rows[2 * HALF:2 * HALF + 1], meta_rows[2 * HALF + 1:2 * HALF + 2]
    seen = (q_seg == k_seg) & (k_pos <= q_pos) & (lane_of((all_toks, LANES)) < new)
    bias[...] = jnp.where(seen, 0.0, NEG_BIG)

    lat[pl.ds(pre, pre), :] = jnp.transpose(lat_t[:kv_lat, pl.ds(pre, pre)])
    put_tail(pre, pre, pseg_mate[...])
    unrolled(heads // 2, UNROLL_KV, raise_keys(pre, pre))

    phase("wait_uq")
    load_uq.wait()
    for copy in send_q:
        copy.wait_recv()
    send_new.wait_recv()
    phase("queries")
    lat[pl.ds(old, new), :] = new_lat[:, :kv_lat]
    new_rope = jnp.concatenate([new_lat[:, kv_lat:].astype(F32), jnp.zeros((new, LANES - ROPE_DIM), F32)], axis=1)
    new_rope = jnp.concatenate([new_rope, jnp.zeros((LANES - new, LANES), F32)], axis=0)
    new_rope = jnp.transpose(new_rope).astype(BF16)
    tail_t[0, :, pl.ds(old, LANES)] = new_rope
    tail_t[1, :ROPE_DIM, pl.ds(old, LANES)] = new_rope[ROPE_DIM:]
    tail_t[1, ROPE_DIM:, pl.ds(old, LANES)] = new_rope[:ROPE_DIM]
    low_half = lane_of((all_toks, LANES)) < ROPE_DIM
    first_half = lax.rem(lane_of((all_toks, LANES)), ROPE_DIM) < HALF

    def raise_queries(pair):
        cols = pl.ds(pl.multiple_of(pair * (2 * QK_DIM), LANES), 2 * QK_DIM)
        q = dot(qlat_all[...], wuq_v[:, cols])
        nope_a, mid, end = q[:, :LANES], q[:, LANES:2 * LANES], q[:, 2 * LANES:]
        nope_b = turn(jnp.where(low_half, end, mid), ROPE_DIM)
        u = jnp.where(low_half, mid, end)
        swapped = jnp.where(first_half, turn(u, LANES - HALF), turn(u, HALF))
        r = u * cos_all[...] + swapped * sin_all[...]
        queries[2 * pair] = jnp.concatenate([nope_a, jnp.where(low_half, r, mask_a[...])], axis=1).astype(BF16)
        queries[2 * pair + 1] = jnp.concatenate([nope_b, jnp.where(low_half, mask_a[...], r)], axis=1).astype(BF16)

    def raise_new_keys(pair):
        up = dot(new_lat[:, :kv_lat], pair_weights(pair, 0))
        up = jnp.transpose(jnp.concatenate([up, jnp.zeros((LANES - new, 2 * NOPE_DIM), F32)], axis=0)).astype(BF16)
        keys_t[2 * pair, :, pl.ds(old, LANES)] = up[:NOPE_DIM]
        keys_t[2 * pair + 1, :, pl.ds(old, LANES)] = up[NOPE_DIM:]

    for pair in range(heads // 2):
        raise_queries(pair)
        raise_new_keys(pair)

    phase("score")

    def score(head, j):
        s = dot(queries[head], jnp.concatenate([keys_t[head], tail_t[j % 2]], axis=0))
        scores[j, :, :old] = s[:, :old]
        scores[j, :, old:] = s[:, old:] + bias[...]
        step = 16
        tops = [jnp.max(scores[j, r:r + step, :], axis=1, keepdims=True) for r in range(0, all_toks, step)]
        for i, top in enumerate(tops):
            rows = pl.ds(i * step, step)
            p = jnp.exp2((scores[j, rows, :] - top) * EXP_SCALE)
            probs[head, rows, :] = p.astype(BF16)
            tops_all[head, rows, :] = jnp.broadcast_to(top, (step, LANES))
            sums_all[head, rows, :] = jnp.broadcast_to(jnp.sum(p, axis=1, keepdims=True), (step, LANES))

    raise_mate = raise_values(pre, pre + new)

    def peer(j):
        return lax.rem(chip + j, chips)

    send_stats = []
    for part in range(PARTS):
        packed = jnp.zeros((all_toks, LANES), F32)
        for head in range(part * some, (part + 1) * some):
            score(head, head % SCORE_BUFS)
        for pair in range(sum(VALUE_PAIRS[:part]), sum(VALUE_PAIRS[:part + 1])):
            raise_mate(pair)
        for i in range(some):
            packed = jnp.where(lanes == i, tops_all[part * some + i], packed)
            packed = jnp.where(lanes == some + i, sums_all[part * some + i], packed)
        stats[part] = jnp.transpose(packed)[:2 * some]
        send_stats.append([
            send(stats.at[part], stats_rx.at[part, j - 1], st_send.at[part, j - 1], st_recv.at[part, j - 1], lax.rem(me + j, n))
            for j in range(1, n)
        ])
    red_copies = {}
    both = CORES * toks
    half = len(ORDER[0]) * both

    def put_scale(part):
        for side in range(CORES):
            got = [stats_rx[part, j - 1] for j in range(1 + (1 - side), n, CORES)]
            mine = stats[part] if side == 0 else jnp.where(core == 0, got[-1], got[0])
            every = got + [mine] if side == 0 else got
            top = functools.reduce(jnp.maximum, [g[:some] for g in every])
            total = functools.reduce(jnp.add, [g[some:] * jnp.exp2((g[:some] - top) * EXP_SCALE) for g in every])
            share = jnp.exp2((mine[:some] - top) * EXP_SCALE)
            scales[part, side, :, :some] = jnp.transpose(share / total)

    def put_split(part, g, sides):
        for b, j in enumerate(ORDER[g]):
            from_rows = pl.ds(pl.multiple_of(peer(j) * both, both), both)
            for side in sides:
                factor = scales[part, side, from_rows, :]
                for i in range(some):
                    cols = pl.ds(((part * CORES + side) * some + i) * V_DIM, V_DIM)
                    o = acc[side, part * some + i, from_rows, :] * factor[:, i:i + 1]
                    o_hi = o.astype(BF16)
                    split[g, pl.ds(b * both, both), cols] = o_hi
                    split[g, pl.ds(half + b * both, both), cols] = (o - o_hi.astype(F32)).astype(BF16)

    def project(part, g):
        ks = pl.ds(part * CORES * deep, CORES * deep)
        y = dot(split[g, :, ks], wo_v[ks, :])
        return y[:half] + y[half:]

    def deliver(g):
        for b, j in enumerate(ORDER[g]):
            for r in range(CORES):
                if j or r:
                    to = lax.rem(core + r, CORES)
                    rows = pl.ds(pl.multiple_of(b * both + to * toks, toks), toks)
                    red_copies[j, r] = send(
                        z.at[g, rows], z_rx.at[j, r], red_send.at[j, r], red_recv.at[j, r], peer(j) * CORES + to
                    )

    def swap(i):
        group = pl.ds(i * (heads // SWAPS), heads // SWAPS)
        return send(acc.at[0, group], acc.at[1, group], acc_send.at[i], acc_recv.at[i], mate)

    phase("attend")
    for pair in range(sum(VALUE_PAIRS[:PARTS]), heads // 2):
        raise_mate(pair)
    send_acc = []
    for head in range(heads):
        cols = pl.ds((head % 2) * V_DIM, V_DIM)
        acc[0, head] = dot(probs[head], values[head // 2, :, cols])
        if (head + 1) % (heads // SWAPS) == 0:
            send_acc.append(swap(head * SWAPS // heads))
    phase("wait_stats0")
    for copy in load_o:
        copy.wait()
    for copy in send_stats[0]:
        copy.wait_recv()
    phase("wait_acc0")
    for copy in send_acc[:SWAPS // PARTS]:
        copy.wait_recv()
    phase("outproj0")
    put_scale(0)
    for g in range(len(ORDER)):
        put_split(0, g, range(CORES))
        z[g] = project(0, g)
    phase("wait_stats1")
    for copy in send_stats[1]:
        copy.wait_recv()
    phase("wait_acc1")
    for copy in send_acc[SWAPS // PARTS:]:
        copy.wait_recv()
    phase("outproj1")
    put_scale(1)
    for g in range(len(ORDER)):
        put_split(1, g, range(CORES))
        z[g] = z[g] + project(1, g)
        deliver(g)
    for j in (0, 1, 3, 2):
        phase(f"wait_red{j}")
        for r in range(CORES):
            if j or r:
                red_copies[j, r].wait_recv()
    phase("reduce")
    own = pl.ds(pl.multiple_of(both + core * toks, toks), toks)
    for r in range(CORES):
        y = z[1, own, :] if r == 0 else z_rx[0, 1]
        for j in range(1, chips):
            y = y + z_rx[j, r]
        cols = pl.ds(pl.multiple_of(lax.rem(core + r, CORES) * half_width, LANES), half_width)
        out_ref[:, cols] = y.astype(BF16)

    phase("drain")
    for copy in [send_pre, send_pseg, send_new] + send_meta + send_q + sum(send_stats, []) + send_acc + list(red_copies.values()):
        copy.wait_send()
    phase("")


def solution(mesh):
    n = mesh.shape["sp"]
    chips = n // CORES
    tok_spec = P(("dp", "sp"), None)
    vec_spec = P(("dp", "sp"))
    mat_spec = P(None, None)
    gain_spec = P(None)

    def device_step(hidden, seg_ids, positions, prefix_lat, prefix_seg, w_dq, gain_q, w_uq, w_dkv, gain_kv, w_ukv, w_o):
        toks, width = hidden.shape
        pre, lat_dim = prefix_lat.shape
        q_lat = w_dq.shape[1]
        kv_lat = w_ukv.shape[0]
        heads = w_o.shape[0] // V_DIM // CORES
        rows = CORES * (pre + toks)
        wide = CORES * pre + LANES
        all_toks = n * toks
        inv_freq = (ROPE_BASE ** (-np.arange(HALF, dtype=np.float64) / HALF)).astype(np.float32)
        freq = jnp.asarray(np.concatenate([inv_freq] * (LANES // HALF)).reshape(1, LANES))
        vmem = pl.BlockSpec(memory_space=pltpu.VMEM)
        hbm = pl.BlockSpec(memory_space=pltpu.HBM)
        dma = pltpu.SemaphoreType.DMA
        table = pltpu.VMEM((all_toks, LANES), F32)
        return pl.pallas_call(
            functools.partial(kernel, n),
            out_shape=pltpu.VMEM((toks, width), BF16),
            in_specs=[hbm] * 13,
            scratch_shapes=[
                pltpu.VMEM((1, LANES), F32),
                pltpu.VMEM((1, toks), jnp.int32),
                pltpu.VMEM((1, toks), jnp.int32),
                pltpu.VMEM((1, pre), jnp.int32),
                pltpu.VMEM((q_lat,), BF16),
                pltpu.VMEM((kv_lat,), BF16),
                pltpu.VMEM((toks, width), BF16),
                pltpu.VMEM((width, q_lat), BF16),
                pltpu.VMEM((lat_dim, width), BF16),
                pltpu.VMEM((q_lat, heads * QK_DIM), BF16),
                pltpu.VMEM((kv_lat, heads * KV_HEAD), BF16),
                pltpu.VMEM((CORES * heads * V_DIM, width // CORES), BF16),
                pltpu.VMEM((lat_dim, wide), BF16),
                pltpu.VMEM((rows, kv_lat), BF16),
                pltpu.VMEM((CORES * toks, lat_dim), BF16),
                pltpu.VMEM((1, pre), jnp.int32),
                pltpu.VMEM((all_toks, q_lat), BF16),
                table, table, table, table,
                pltpu.VMEM((2, LANES, wide), BF16),
                pltpu.VMEM((heads, NOPE_DIM, wide), BF16),
                pltpu.VMEM((heads // 2, wide, 2 * V_DIM), BF16),
                pltpu.VMEM((heads, all_toks, 2 * LANES), BF16),
                pltpu.VMEM((heads, all_toks, wide), BF16),
                pltpu.VMEM((heads, all_toks, LANES), F32),
                pltpu.VMEM((heads, all_toks, LANES), F32),
                pltpu.VMEM((SCORE_BUFS, all_toks, wide), F32),
                pltpu.VMEM((PARTS, 2 * heads // PARTS, all_toks), F32),
                pltpu.VMEM((PARTS, n - 1, 2 * heads // PARTS, all_toks), F32),
                pltpu.VMEM((CORES, heads, all_toks, V_DIM), F32),
                pltpu.VMEM((PARTS, CORES, all_toks, LANES), F32),
                pltpu.VMEM((2, all_toks, CORES * heads * V_DIM), BF16),
                table,
                pltpu.VMEM((2, all_toks // 2, width // CORES), F32),
                pltpu.VMEM((chips, CORES, toks, width // CORES), F32),
                dma((6,)),
                dma((6,)),
                dma((DQ_LOADS,)),
                dma((PARTS, CORES)),
                dma((KV_LOADS,)),
                dma((3,)), dma((3,)),
                dma((n - 1,)), dma((n - 1,)),
                dma((n - 1,)), dma((n - 1,)),
                dma((PARTS, n - 1)), dma((PARTS, n - 1)),
                dma((SWAPS,)), dma((SWAPS,)),
                dma((chips, CORES)), dma((chips, CORES)),
            ],
            compiler_params=pltpu.CompilerParams(
                collective_id=0, has_side_effects=True, vmem_limit_bytes=60 * 1024 * 1024
            ),
        )(
            freq, seg_ids.reshape(1, toks), positions.reshape(1, toks), prefix_seg.reshape(1, pre),
            gain_q, gain_kv,
            hidden, prefix_lat.T, w_dq, w_uq, w_dkv.T, w_ukv, w_o,
        )

    return jax.shard_map(
        device_step,
        mesh=mesh,
        in_specs=(tok_spec, vec_spec, vec_spec, tok_spec, vec_spec, mat_spec, gain_spec, mat_spec, mat_spec, gain_spec, mat_spec, mat_spec),
        out_specs=tok_spec,
        check_vma=False,
    )
```

```python
import functools
import math

import jax
import jax.numpy as jnp
import numpy as np
from jax import lax
from jax.experimental import pallas as pl
from jax.experimental.pallas import tpu as pltpu
from jax.sharding import PartitionSpec as P

ROPE_DIM = 64
HALF = ROPE_DIM // 2
NOPE_DIM = 128
V_DIM = 128
QK_DIM = NOPE_DIM + ROPE_DIM
KV_HEAD = NOPE_DIM + V_DIM
CORES = 2
EPS = 1e-6
ROPE_BASE = 10000.0
NEG_BIG = -1e30
EXP_SCALE = QK_DIM ** -0.5 * math.log2(math.e)
LANES = 128
ORDER = ((2, 1), (3, 0))
PARTS = 2
SWAPS = 2
VALUE_PAIRS = (4, 2, 2)
KV_LOADS = 2
DQ_LOADS = 4
UNROLL_KV = 8
SCORE_BUFS = 8

F32 = jnp.float32
BF16 = jnp.bfloat16


def dot(a, b):
    return jnp.dot(a, b, preferred_element_type=F32)


def dot_nt(a, b):
    return lax.dot_general(a, b, (((1,), (1,)), ((), ())), preferred_element_type=F32)


def dot_tn(a, b):
    return lax.dot_general(a, b, (((0,), (0,)), ((), ())), preferred_element_type=F32)


def rms_norm(values, gain):
    inv_rms = lax.rsqrt(jnp.mean(values * values, axis=-1, keepdims=True) + EPS)
    return values * inv_rms * gain.astype(F32).reshape(1, gain.shape[0])


def row_to_column(row):
    size = row.shape[1]
    here = lax.broadcasted_iota(jnp.int32, (size, size), 0) == lax.broadcasted_iota(jnp.int32, (size, size), 1)
    return jnp.sum(jnp.where(here, jnp.broadcast_to(row, (size, size)), 0.0), axis=1, keepdims=True)


def lane_of(shape):
    return lax.broadcasted_iota(jnp.int32, shape, len(shape) - 1)


def turn(x, amount):
    return pltpu.roll(x, amount, 1)


def unrolled(count, step, body):
    if count == step:
        for j in range(step):
            body(j)
        return

    def run(i, carry):
        for j in range(step):
            body(i * step + j)
        return carry

    lax.fori_loop(0, count // step, run, 0)


class Phases:
    def __init__(self):
        self.now = None

    def __call__(self, name):
        if self.now is not None:
            self.now.__exit__(None, None, None)
        self.now = None
        if name:
            self.now = jax.named_scope(name)
            self.now.__enter__()


def kernel(
    n,
    freq_hbm, seg_hbm, pos_hbm, pseg_hbm, gain_q_hbm, gain_kv_hbm,
    hid_hbm, pre_hbm, wdq_hbm, wuq_hbm, wdkv_hbm, wukv_hbm, wo_hbm,
    out_ref,
    freq_ref, seg_ref, pos_ref, pseg_ref, gain_q_ref, gain_kv_ref,
    hid_v, wdq_v, wdkv_v, wuq_v, wukv_v, wo_v,
    lat_t, lat, new_lat, pseg_mate, qlat_all, meta_all, cos_all, sin_all, mask_a, tail_t,
    keys_t, values, queries, probs, tops_all, sums_all,
    scores, stats, stats_rx, acc, scales, split, bias, z, z_rx,
    load_sem, small_sem, dq_sem, wo_sem, ukv_sem, mate_send, mate_recv, gat_send, gat_recv, met_send, met_recv,
    st_send, st_recv, acc_send, acc_recv, red_send, red_recv,
):
    phase = Phases()
    me = lax.axis_index("sp")
    core = lax.rem(me, CORES)
    chip = lax.div(me, CORES)
    chips = n // CORES
    mate = chip * CORES + (CORES - 1 - core)
    toks = hid_v.shape[0]
    pre = pre_hbm.shape[1]
    kv_lat = wukv_v.shape[0]
    heads = keys_t.shape[0]
    old = CORES * pre
    new = CORES * toks
    wide = lat_t.shape[1]
    all_toks = n * toks
    some = heads // PARTS
    deep = some * V_DIM
    half_width = wo_v.shape[1]

    phase("loads")

    def load(src, dst, sem):
        copy = pltpu.make_async_copy(src, dst, sem)
        copy.start()
        return copy

    barrier = pltpu.get_barrier_semaphore()
    for j in range(1, n):
        pl.semaphore_signal(barrier, inc=1, device_id={"sp": lax.rem(me + j, n)}, device_id_type=pl.DeviceIdType.MESH)
    smalls = [
        load(src, dst, small_sem.at[i])
        for i, (src, dst) in enumerate([
            (freq_hbm, freq_ref), (seg_hbm, seg_ref), (pos_hbm, pos_ref),
            (gain_q_hbm, gain_q_ref), (gain_kv_hbm, gain_kv_ref), (pseg_hbm, pseg_ref),
        ])
    ]
    load_hid = load(hid_hbm, hid_v, load_sem.at[0])
    depth = wdq_v.shape[0] // DQ_LOADS
    load_dq = [
        load(wdq_hbm.at[pl.ds(i * depth, depth)], wdq_v.at[pl.ds(i * depth, depth)], dq_sem.at[i])
        for i in range(DQ_LOADS)
    ]
    kv_cols = heads * KV_HEAD
    part = kv_cols // KV_LOADS

    def load_up(i):
        return load(
            wukv_hbm.at[:, pl.ds(pl.multiple_of(core * kv_cols + i * part, LANES), part)],
            wukv_v.at[:, pl.ds(i * part, part)],
            ukv_sem.at[i],
        )

    load_pre = load(pre_hbm, lat_t.at[:, pl.ds(0, pre)], load_sem.at[3])
    load_ukv = [load_up(0)]

    phase("wait_small")
    for copy in smalls:
        copy.wait()
    phase("meta")
    pos_col = row_to_column(pos_ref[...].astype(F32))
    seg_col = row_to_column(seg_ref[...].astype(F32))
    angles = pos_col * freq_ref[...]
    lane = lane_of((toks, LANES))
    cos_t = jnp.cos(angles)
    sin_t = jnp.sin(angles)
    my_rows = pl.ds(pl.multiple_of(me * toks, toks), toks)
    meta_all[my_rows, :] = jnp.where(
        lane < HALF, cos_t, jnp.where(lane < 2 * HALF, sin_t, jnp.where(lane == 2 * HALF, seg_col, pos_col))
    )

    def send(src, dst, send_sem, recv_sem, target):
        copy = pltpu.make_async_remote_copy(
            src_ref=src, dst_ref=dst, send_sem=send_sem, recv_sem=recv_sem,
            device_id={"sp": target}, device_id_type=pl.DeviceIdType.MESH,
        )
        copy.start()
        return copy

    phase("wait_dq")
    load_hid.wait()
    for copy in load_dq:
        copy.wait()
    load_ukv += [load_up(i) for i in range(1, KV_LOADS)]
    load_dkv = load(wdkv_hbm, wdkv_v, load_sem.at[2])
    phase("barrier")
    pl.semaphore_wait(barrier, n - 1)
    send_pre = send(pre_hbm, lat_t.at[:, pl.ds(pre, pre)], mate_send.at[0], mate_recv.at[0], mate)
    send_pseg = send(pseg_ref, pseg_mate, mate_send.at[1], mate_recv.at[1], mate)
    send_meta = [
        send(meta_all.at[my_rows], meta_all.at[my_rows], met_send.at[j - 1], met_recv.at[j - 1], lax.rem(me + j, n))
        for j in range(1, n)
    ]
    phase("qlat")
    qlat_all[my_rows, :] = rms_norm(dot(hid_v[...], wdq_v[...]), gain_q_ref[...]).astype(BF16)

    send_q = [
        send(qlat_all.at[my_rows], qlat_all.at[my_rows], gat_send.at[j - 1], gat_recv.at[j - 1], lax.rem(me + j, n))
        for j in range(1, n)
    ]
    def pair_weights(pair, offset):
        first = pl.multiple_of(pair * (2 * KV_HEAD) + offset, LANES)
        second = pl.multiple_of(pair * (2 * KV_HEAD) + KV_HEAD + offset, LANES)
        return jnp.concatenate([wukv_v[:, pl.ds(first, LANES)], wukv_v[:, pl.ds(second, LANES)]], axis=1)

    def raise_keys(start, size):
        def step(pair):
            up = dot_tn(pair_weights(pair, 0), lat_t[:kv_lat, pl.ds(start, size)]).astype(BF16)
            keys_t[2 * pair, :, pl.ds(start, size)] = up[:NOPE_DIM]
            keys_t[2 * pair + 1, :, pl.ds(start, size)] = up[NOPE_DIM:]
        return step

    def raise_values(start, size):
        def step(pair):
            values[pair, pl.ds(start, size), :] = dot(lat[pl.ds(start, size), :], pair_weights(pair, NOPE_DIM)).astype(BF16)
        return step

    def put_tail(start, size, seg_row):
        hot = seg_row == lax.broadcasted_iota(jnp.int32, (ROPE_DIM, size), 0)
        hot = jnp.where(hot, 1.0, 0.0).astype(BF16)
        rope = lat_t[kv_lat:, pl.ds(start, size)]
        tail_t[0, :, pl.ds(start, size)] = jnp.concatenate([rope, hot], axis=0)
        tail_t[1, :, pl.ds(start, size)] = jnp.concatenate([hot, rope], axis=0)
    per = heads // 2 // KV_LOADS
    for i in range(KV_LOADS):
        phase(f"wait_own{i}")
        load_ukv[i].wait()
        if i == 0:
            load_pre.wait()
        else:
            load_dkv.wait()
        phase(f"own{i}")
        if i:
            load_uq = load(
                wuq_hbm.at[:, pl.ds(pl.multiple_of(core * heads * QK_DIM, LANES), heads * QK_DIM)], wuq_v, load_sem.at[4]
            )
            load_o = [
                load(
                    wo_hbm.at[
                        pl.ds(pl.multiple_of(lax.rem(core + side, CORES) * (heads * V_DIM) + part * deep, LANES), deep),
                        pl.ds(pl.multiple_of(core * half_width, LANES), half_width),
                    ],
                    wo_v.at[pl.ds((part * CORES + side) * deep, deep)],
                    wo_sem.at[part, side],
                )
                for part in range(PARTS) for side in range(CORES)
            ]
            down = dot_nt(hid_v[...], wdkv_v[...])
            c_kv = rms_norm(down[:, :kv_lat], gain_kv_ref[...])
            low, high = down[:, kv_lat:kv_lat + HALF], down[:, kv_lat + HALF:]
            cos_m, sin_m = cos_t[:, :HALF], sin_t[:, :HALF]
            k_new = jnp.concatenate([low * cos_m - high * sin_m, high * cos_m + low * sin_m], axis=1)
            new_lat[pl.ds(0, toks), :] = jnp.concatenate([c_kv, k_new], axis=1).astype(BF16)
        for pair in range(i * per, (i + 1) * per):
            raise_keys(0, pre)(pair)
        if i == 0:
            lat[pl.ds(0, pre), :] = jnp.transpose(lat_t[:kv_lat, pl.ds(0, pre)])
            put_tail(0, pre, pseg_ref[...])
            values[:, pl.ds(old + new, wide - old - new), :] = jnp.zeros((heads // 2, wide - old - new, 2 * V_DIM), BF16)
        for pair in range(i * per, (i + 1) * per):
            raise_values(0, pre)(pair)
    send_new = send(new_lat.at[pl.ds(0, toks)], new_lat.at[pl.ds(toks, toks)], mate_send.at[2], mate_recv.at[2], mate)

    phase("wait_meta")
    for copy in send_meta:
        copy.wait_recv()
    phase("wait_mate")
    send_pre.wait_recv()
    send_pseg.wait_recv()
    phase("keys_mate")
    unrolled(heads // 2, UNROLL_KV, raise_keys(pre, pre))
    lat[pl.ds(pre, pre), :] = jnp.transpose(lat_t[:kv_lat, pl.ds(pre, pre)])
    every = meta_all[...]
    lanes = lane_of((all_toks, LANES))
    q_seg = every[:, 2 * HALF:2 * HALF + 1]
    q_pos = every[:, 2 * HALF + 1:2 * HALF + 2]
    cos_q = jnp.where(lanes < HALF, every, 0.0)
    cos_q = cos_q + turn(cos_q, HALF)
    cos_all[...] = cos_q + turn(cos_q, 2 * HALF)
    sin_q = jnp.where((lanes >= HALF) & (lanes < 2 * HALF), every, 0.0)
    sin_q = sin_q - turn(sin_q, LANES - HALF)
    sin_all[...] = sin_q + turn(sin_q, 2 * HALF)
    q_mask = jnp.where(q_seg == jnp.where(lanes < ROPE_DIM, lanes, lanes - ROPE_DIM).astype(F32), 0.0, NEG_BIG)
    mask_a[...] = q_mask
    mate_rows = pl.ds(pl.multiple_of(mate * toks, toks), toks)
    new_meta = jnp.concatenate(
        [meta_all[my_rows, :], meta_all[mate_rows, :], jnp.zeros((LANES - new, LANES), F32)], axis=0
    )
    meta_rows = jnp.transpose(new_meta)
    k_seg, k_pos = meta_rows[2 * HALF:2 * HALF + 1], meta_rows[2 * HALF + 1:2 * HALF + 2]
    seen = (q_seg == k_seg) & (k_pos <= q_pos) & (lane_of((all_toks, LANES)) < new)
    bias[...] = jnp.where(seen, 0.0, NEG_BIG)

    put_tail(pre, pre, pseg_mate[...])

    phase("wait_uq")
    load_uq.wait()
    for copy in send_q:
        copy.wait_recv()
    send_new.wait_recv()
    phase("queries")
    lat[pl.ds(old, new), :] = new_lat[:, :kv_lat]
    new_rope = jnp.concatenate([new_lat[:, kv_lat:].astype(F32), jnp.zeros((new, LANES - ROPE_DIM), F32)], axis=1)
    new_rope = jnp.concatenate([new_rope, jnp.zeros((LANES - new, LANES), F32)], axis=0)
    new_rope = jnp.transpose(new_rope).astype(BF16)
    tail_t[0, :, pl.ds(old, LANES)] = new_rope
    tail_t[1, :ROPE_DIM, pl.ds(old, LANES)] = new_rope[ROPE_DIM:]
    tail_t[1, ROPE_DIM:, pl.ds(old, LANES)] = new_rope[:ROPE_DIM]
    low_half = lane_of((all_toks, LANES)) < ROPE_DIM
    first_half = lax.rem(lane_of((all_toks, LANES)), ROPE_DIM) < HALF

    def raise_queries(pair):
        cols = pl.ds(pl.multiple_of(pair * (2 * QK_DIM), LANES), 2 * QK_DIM)
        q = dot(qlat_all[...], wuq_v[:, cols])
        nope_a, mid, end = q[:, :LANES], q[:, LANES:2 * LANES], q[:, 2 * LANES:]
        nope_b = turn(jnp.where(low_half, end, mid), ROPE_DIM)
        u = jnp.where(low_half, mid, end)
        swapped = jnp.where(first_half, turn(u, LANES - HALF), turn(u, HALF))
        r = u * cos_all[...] + swapped * sin_all[...]
        queries[2 * pair] = jnp.concatenate([nope_a, jnp.where(low_half, r, mask_a[...])], axis=1).astype(BF16)
        queries[2 * pair + 1] = jnp.concatenate([nope_b, jnp.where(low_half, mask_a[...], r)], axis=1).astype(BF16)

    def raise_new_keys(pair):
        up = dot(new_lat[:, :kv_lat], pair_weights(pair, 0))
        up = jnp.transpose(jnp.concatenate([up, jnp.zeros((LANES - new, 2 * NOPE_DIM), F32)], axis=0)).astype(BF16)
        keys_t[2 * pair, :, pl.ds(old, LANES)] = up[:NOPE_DIM]
        keys_t[2 * pair + 1, :, pl.ds(old, LANES)] = up[NOPE_DIM:]

    for pair in range(heads // 2):
        raise_queries(pair)
        raise_new_keys(pair)

    phase("score")

    def score(head, j):
        s = dot(queries[head], jnp.concatenate([keys_t[head], tail_t[j % 2]], axis=0))
        scores[j, :, :old] = s[:, :old]
        scores[j, :, old:] = s[:, old:] + bias[...]
        step = 16
        tops = [jnp.max(scores[j, r:r + step, :], axis=1, keepdims=True) for r in range(0, all_toks, step)]
        for i, top in enumerate(tops):
            rows = pl.ds(i * step, step)
            p = jnp.exp2((scores[j, rows, :] - top) * EXP_SCALE)
            probs[head, rows, :] = p.astype(BF16)
            tops_all[head, rows, :] = jnp.broadcast_to(top, (step, LANES))
            sums_all[head, rows, :] = jnp.broadcast_to(jnp.sum(p, axis=1, keepdims=True), (step, LANES))

    raise_mate = raise_values(pre, pre + new)

    def peer(j):
        return lax.rem(chip + j, chips)

    send_stats = []
    for part in range(PARTS):
        packed = jnp.zeros((all_toks, LANES), F32)
        for head in range(part * some, (part + 1) * some):
            score(head, head % SCORE_BUFS)
        for pair in range(sum(VALUE_PAIRS[:part]), sum(VALUE_PAIRS[:part + 1])):
            raise_mate(pair)
        for i in range(some):
            packed = jnp.where(lanes == i, tops_all[part * some + i], packed)
            packed = jnp.where(lanes == some + i, sums_all[part * some + i], packed)
        stats[part] = jnp.transpose(packed)[:2 * some]
        send_stats.append([
            send(stats.at[part], stats_rx.at[part, j - 1], st_send.at[part, j - 1], st_recv.at[part, j - 1], lax.rem(me + j, n))
            for j in range(1, n)
        ])
    red_copies = {}
    both = CORES * toks
    half = len(ORDER[0]) * both

    def put_scale(part):
        for side in range(CORES):
            got = [stats_rx[part, j - 1] for j in range(1 + (1 - side), n, CORES)]
            mine = stats[part] if side == 0 else jnp.where(core == 0, got[-1], got[0])
            every = got + [mine] if side == 0 else got
            top = functools.reduce(jnp.maximum, [g[:some] for g in every])
            total = functools.reduce(jnp.add, [g[some:] * jnp.exp2((g[:some] - top) * EXP_SCALE) for g in every])
            share = jnp.exp2((mine[:some] - top) * EXP_SCALE)
            scales[part, side, :, :some] = jnp.transpose(share / total)

    def put_split(part, g, sides):
        for b, j in enumerate(ORDER[g]):
            from_rows = pl.ds(pl.multiple_of(peer(j) * both, both), both)
            for side in sides:
                factor = scales[part, side, from_rows, :]
                for i in range(some):
                    cols = pl.ds(((part * CORES + side) * some + i) * V_DIM, V_DIM)
                    o = acc[side, part * some + i, from_rows, :] * factor[:, i:i + 1]
                    o_hi = o.astype(BF16)
                    split[g, pl.ds(b * both, both), cols] = o_hi
                    split[g, pl.ds(half + b * both, both), cols] = (o - o_hi.astype(F32)).astype(BF16)

    def project(part, g, side=None):
        first = part * CORES * deep
        ks = pl.ds(first, CORES * deep) if side is None else pl.ds(first + side * deep, deep)
        y = dot(split[g, :, ks], wo_v[ks, :])
        return y[:half] + y[half:]

    def deliver(g):
        for b, j in enumerate(ORDER[g]):
            for r in range(CORES):
                if j or r:
                    to = lax.rem(core + r, CORES)
                    rows = pl.ds(pl.multiple_of(b * both + to * toks, toks), toks)
                    red_copies[j, r] = send(
                        z.at[g, rows], z_rx.at[j, r], red_send.at[j, r], red_recv.at[j, r], peer(j) * CORES + to
                    )

    def swap(i):
        group = pl.ds(i * (heads // SWAPS), heads // SWAPS)
        return send(acc.at[0, group], acc.at[1, group], acc_send.at[i], acc_recv.at[i], mate)

    phase("attend")
    for pair in range(sum(VALUE_PAIRS[:PARTS]), heads // 2):
        raise_mate(pair)
    send_acc = []
    for head in range(heads):
        cols = pl.ds((head % 2) * V_DIM, V_DIM)
        acc[0, head] = dot(probs[head], values[head // 2, :, cols])
        if (head + 1) % (heads // SWAPS) == 0:
            send_acc.append(swap(head * SWAPS // heads))
    phase("wait_stats0")
    for copy in load_o:
        copy.wait()
    for copy in send_stats[0]:
        copy.wait_recv()
    phase("outproj0")
    put_scale(0)
    for g in range(len(ORDER)):
        put_split(0, g, (0,))
        z[g] = project(0, g, 0)
    phase("wait_acc0")
    for copy in send_acc[:SWAPS // PARTS]:
        copy.wait_recv()
    phase("outproj0m")
    for g in range(len(ORDER)):
        put_split(0, g, (1,))
        z[g] = z[g] + project(0, g, 1)
    phase("wait_stats1")
    for copy in send_stats[1]:
        copy.wait_recv()
    phase("wait_acc1")
    for copy in send_acc[SWAPS // PARTS:]:
        copy.wait_recv()
    phase("outproj1")
    put_scale(1)
    for g in range(len(ORDER)):
        put_split(1, g, range(CORES))
        z[g] = z[g] + project(1, g)
        deliver(g)
    for j in (0, 1, 3, 2):
        phase(f"wait_red{j}")
        for r in range(CORES):
            if j or r:
                red_copies[j, r].wait_recv()
    phase("reduce")
    own = pl.ds(pl.multiple_of(both + core * toks, toks), toks)
    for r in range(CORES):
        y = z[1, own, :] if r == 0 else z_rx[0, 1]
        for j in range(1, chips):
            y = y + z_rx[j, r]
        cols = pl.ds(pl.multiple_of(lax.rem(core + r, CORES) * half_width, LANES), half_width)
        out_ref[:, cols] = y.astype(BF16)

    phase("drain")
    for copy in [send_pre, send_pseg, send_new] + send_meta + send_q + sum(send_stats, []) + send_acc + list(red_copies.values()):
        copy.wait_send()
    phase("")


def solution(mesh):
    n = mesh.shape["sp"]
    chips = n // CORES
    tok_spec = P(("dp", "sp"), None)
    vec_spec = P(("dp", "sp"))
    mat_spec = P(None, None)
    gain_spec = P(None)

    def device_step(hidden, seg_ids, positions, prefix_lat, prefix_seg, w_dq, gain_q, w_uq, w_dkv, gain_kv, w_ukv, w_o):
        toks, width = hidden.shape
        pre, lat_dim = prefix_lat.shape
        q_lat = w_dq.shape[1]
        kv_lat = w_ukv.shape[0]
        heads = w_o.shape[0] // V_DIM // CORES
        rows = CORES * (pre + toks)
        wide = CORES * pre + LANES
        all_toks = n * toks
        inv_freq = (ROPE_BASE ** (-np.arange(HALF, dtype=np.float64) / HALF)).astype(np.float32)
        freq = jnp.asarray(np.concatenate([inv_freq] * (LANES // HALF)).reshape(1, LANES))
        vmem = pl.BlockSpec(memory_space=pltpu.VMEM)
        hbm = pl.BlockSpec(memory_space=pltpu.HBM)
        dma = pltpu.SemaphoreType.DMA
        table = pltpu.VMEM((all_toks, LANES), F32)
        return pl.pallas_call(
            functools.partial(kernel, n),
            out_shape=pltpu.VMEM((toks, width), BF16),
            in_specs=[hbm] * 13,
            scratch_shapes=[
                pltpu.VMEM((1, LANES), F32),
                pltpu.VMEM((1, toks), jnp.int32),
                pltpu.VMEM((1, toks), jnp.int32),
                pltpu.VMEM((1, pre), jnp.int32),
                pltpu.VMEM((q_lat,), BF16),
                pltpu.VMEM((kv_lat,), BF16),
                pltpu.VMEM((toks, width), BF16),
                pltpu.VMEM((width, q_lat), BF16),
                pltpu.VMEM((lat_dim, width), BF16),
                pltpu.VMEM((q_lat, heads * QK_DIM), BF16),
                pltpu.VMEM((kv_lat, heads * KV_HEAD), BF16),
                pltpu.VMEM((CORES * heads * V_DIM, width // CORES), BF16),
                pltpu.VMEM((lat_dim, wide), BF16),
                pltpu.VMEM((rows, kv_lat), BF16),
                pltpu.VMEM((CORES * toks, lat_dim), BF16),
                pltpu.VMEM((1, pre), jnp.int32),
                pltpu.VMEM((all_toks, q_lat), BF16),
                table, table, table, table,
                pltpu.VMEM((2, LANES, wide), BF16),
                pltpu.VMEM((heads, NOPE_DIM, wide), BF16),
                pltpu.VMEM((heads // 2, wide, 2 * V_DIM), BF16),
                pltpu.VMEM((heads, all_toks, 2 * LANES), BF16),
                pltpu.VMEM((heads, all_toks, wide), BF16),
                pltpu.VMEM((heads, all_toks, LANES), F32),
                pltpu.VMEM((heads, all_toks, LANES), F32),
                pltpu.VMEM((SCORE_BUFS, all_toks, wide), F32),
                pltpu.VMEM((PARTS, 2 * heads // PARTS, all_toks), F32),
                pltpu.VMEM((PARTS, n - 1, 2 * heads // PARTS, all_toks), F32),
                pltpu.VMEM((CORES, heads, all_toks, V_DIM), F32),
                pltpu.VMEM((PARTS, CORES, all_toks, LANES), F32),
                pltpu.VMEM((2, all_toks, CORES * heads * V_DIM), BF16),
                table,
                pltpu.VMEM((2, all_toks // 2, width // CORES), F32),
                pltpu.VMEM((chips, CORES, toks, width // CORES), F32),
                dma((6,)),
                dma((6,)),
                dma((DQ_LOADS,)),
                dma((PARTS, CORES)),
                dma((KV_LOADS,)),
                dma((3,)), dma((3,)),
                dma((n - 1,)), dma((n - 1,)),
                dma((n - 1,)), dma((n - 1,)),
                dma((PARTS, n - 1)), dma((PARTS, n - 1)),
                dma((SWAPS,)), dma((SWAPS,)),
                dma((chips, CORES)), dma((chips, CORES)),
            ],
            compiler_params=pltpu.CompilerParams(
                collective_id=0, has_side_effects=True, vmem_limit_bytes=60 * 1024 * 1024
            ),
        )(
            freq, seg_ids.reshape(1, toks), positions.reshape(1, toks), prefix_seg.reshape(1, pre),
            gain_q, gain_kv,
            hidden, prefix_lat.T, w_dq, w_uq, w_dkv.T, w_ukv, w_o,
        )

    return jax.shard_map(
        device_step,
        mesh=mesh,
        in_specs=(tok_spec, vec_spec, vec_spec, tok_spec, vec_spec, mat_spec, gain_spec, mat_spec, mat_spec, gain_spec, mat_spec, mat_spec),
        out_specs=tok_spec,
        check_vma=False,
    )
```

```python
import functools
import math

import jax
import jax.numpy as jnp
import numpy as np
from jax import lax
from jax.experimental import pallas as pl
from jax.experimental.pallas import tpu as pltpu
from jax.sharding import PartitionSpec as P

ROPE_DIM = 64
HALF = ROPE_DIM // 2
NOPE_DIM = 128
V_DIM = 128
QK_DIM = NOPE_DIM + ROPE_DIM
KV_HEAD = NOPE_DIM + V_DIM
CORES = 2
EPS = 1e-6
ROPE_BASE = 10000.0
NEG_BIG = -1e30
EXP_SCALE = QK_DIM ** -0.5 * math.log2(math.e)
LANES = 128
ORDER = ((2, 1), (3, 0))
PARTS = 2
SWAPS = 2
VALUES_AFTER = {7: (0, 1, 2, 3), 15: (4, 5)}
AHEAD = 0
KV_LOADS = 2
DQ_LOADS = 4
UNROLL_KV = 8
SCORE_BUFS = 8

F32 = jnp.float32
BF16 = jnp.bfloat16


def dot(a, b):
    return jnp.dot(a, b, preferred_element_type=F32)


def dot_nt(a, b):
    return lax.dot_general(a, b, (((1,), (1,)), ((), ())), preferred_element_type=F32)


def dot_tn(a, b):
    return lax.dot_general(a, b, (((0,), (0,)), ((), ())), preferred_element_type=F32)


def rms_norm(values, gain):
    inv_rms = lax.rsqrt(jnp.mean(values * values, axis=-1, keepdims=True) + EPS)
    return values * inv_rms * gain.astype(F32).reshape(1, gain.shape[0])


def row_to_column(row):
    size = row.shape[1]
    here = lax.broadcasted_iota(jnp.int32, (size, size), 0) == lax.broadcasted_iota(jnp.int32, (size, size), 1)
    return jnp.sum(jnp.where(here, jnp.broadcast_to(row, (size, size)), 0.0), axis=1, keepdims=True)


def lane_of(shape):
    return lax.broadcasted_iota(jnp.int32, shape, len(shape) - 1)


def turn(x, amount):
    return pltpu.roll(x, amount, 1)


def unrolled(count, step, body):
    if count == step:
        for j in range(step):
            body(j)
        return

    def run(i, carry):
        for j in range(step):
            body(i * step + j)
        return carry

    lax.fori_loop(0, count // step, run, 0)


class Phases:
    def __init__(self):
        self.now = None

    def __call__(self, name):
        if self.now is not None:
            self.now.__exit__(None, None, None)
        self.now = None
        if name:
            self.now = jax.named_scope(name)
            self.now.__enter__()


def kernel(
    n,
    freq_hbm, seg_hbm, pos_hbm, pseg_hbm, gain_q_hbm, gain_kv_hbm,
    hid_hbm, pre_hbm, wdq_hbm, wuq_hbm, wdkv_hbm, wukv_hbm, wo_hbm,
    out_ref,
    freq_ref, seg_ref, pos_ref, pseg_ref, gain_q_ref, gain_kv_ref,
    hid_v, wdq_v, wdkv_v, wuq_v, wukv_v, wo_v,
    lat_t, lat, new_lat, pseg_mate, qlat_all, meta_all, cos_all, sin_all, mask_a, tail_t,
    keys_t, values, queries, probs, tops_all, sums_all,
    scores, stats, stats_rx, acc, scales, split, bias, z, z_rx,
    load_sem, small_sem, dq_sem, wo_sem, ukv_sem, mate_send, mate_recv, gat_send, gat_recv, met_send, met_recv,
    st_send, st_recv, acc_send, acc_recv, red_send, red_recv,
):
    phase = Phases()
    me = lax.axis_index("sp")
    core = lax.rem(me, CORES)
    chip = lax.div(me, CORES)
    chips = n // CORES
    mate = chip * CORES + (CORES - 1 - core)
    toks = hid_v.shape[0]
    pre = pre_hbm.shape[1]
    kv_lat = wukv_v.shape[0]
    heads = keys_t.shape[0]
    old = CORES * pre
    new = CORES * toks
    wide = lat_t.shape[1]
    all_toks = n * toks
    some = heads // PARTS
    deep = some * V_DIM
    half_width = wo_v.shape[1]

    phase("loads")

    def load(src, dst, sem):
        copy = pltpu.make_async_copy(src, dst, sem)
        copy.start()
        return copy

    barrier = pltpu.get_barrier_semaphore()
    for j in range(1, n):
        pl.semaphore_signal(barrier, inc=1, device_id={"sp": lax.rem(me + j, n)}, device_id_type=pl.DeviceIdType.MESH)
    smalls = [
        load(src, dst, small_sem.at[i])
        for i, (src, dst) in enumerate([
            (freq_hbm, freq_ref), (seg_hbm, seg_ref), (pos_hbm, pos_ref),
            (gain_q_hbm, gain_q_ref), (gain_kv_hbm, gain_kv_ref), (pseg_hbm, pseg_ref),
        ])
    ]
    load_hid = load(hid_hbm, hid_v, load_sem.at[0])
    depth = wdq_v.shape[0] // DQ_LOADS
    load_dq = [
        load(wdq_hbm.at[pl.ds(i * depth, depth)], wdq_v.at[pl.ds(i * depth, depth)], dq_sem.at[i])
        for i in range(DQ_LOADS)
    ]
    kv_cols = heads * KV_HEAD
    part = kv_cols // KV_LOADS

    def load_up(i):
        return load(
            wukv_hbm.at[:, pl.ds(pl.multiple_of(core * kv_cols + i * part, LANES), part)],
            wukv_v.at[:, pl.ds(i * part, part)],
            ukv_sem.at[i],
        )

    load_pre = load(pre_hbm, lat_t.at[:, pl.ds(0, pre)], load_sem.at[3])
    load_ukv = [load_up(0)]

    phase("wait_small")
    for copy in smalls:
        copy.wait()
    phase("meta")
    pos_col = row_to_column(pos_ref[...].astype(F32))
    seg_col = row_to_column(seg_ref[...].astype(F32))
    angles = pos_col * freq_ref[...]
    lane = lane_of((toks, LANES))
    cos_t = jnp.cos(angles)
    sin_t = jnp.sin(angles)
    my_rows = pl.ds(pl.multiple_of(me * toks, toks), toks)
    meta_all[my_rows, :] = jnp.where(
        lane < HALF, cos_t, jnp.where(lane < 2 * HALF, sin_t, jnp.where(lane == 2 * HALF, seg_col, pos_col))
    )

    def send(src, dst, send_sem, recv_sem, target):
        copy = pltpu.make_async_remote_copy(
            src_ref=src, dst_ref=dst, send_sem=send_sem, recv_sem=recv_sem,
            device_id={"sp": target}, device_id_type=pl.DeviceIdType.MESH,
        )
        copy.start()
        return copy

    phase("wait_dq")
    load_hid.wait()
    for copy in load_dq:
        copy.wait()
    load_ukv += [load_up(i) for i in range(1, KV_LOADS)]
    load_dkv = load(wdkv_hbm, wdkv_v, load_sem.at[2])
    phase("barrier")
    pl.semaphore_wait(barrier, n - 1)
    send_pre = send(pre_hbm, lat_t.at[:, pl.ds(pre, pre)], mate_send.at[0], mate_recv.at[0], mate)
    send_pseg = send(pseg_ref, pseg_mate, mate_send.at[1], mate_recv.at[1], mate)
    send_meta = [
        send(meta_all.at[my_rows], meta_all.at[my_rows], met_send.at[j - 1], met_recv.at[j - 1], lax.rem(me + j, n))
        for j in range(1, n)
    ]
    phase("qlat")
    qlat_all[my_rows, :] = rms_norm(dot(hid_v[...], wdq_v[...]), gain_q_ref[...]).astype(BF16)

    send_q = [
        send(qlat_all.at[my_rows], qlat_all.at[my_rows], gat_send.at[j - 1], gat_recv.at[j - 1], lax.rem(me + j, n))
        for j in range(1, n)
    ]
    def pair_weights(pair, offset):
        first = pl.multiple_of(pair * (2 * KV_HEAD) + offset, LANES)
        second = pl.multiple_of(pair * (2 * KV_HEAD) + KV_HEAD + offset, LANES)
        return jnp.concatenate([wukv_v[:, pl.ds(first, LANES)], wukv_v[:, pl.ds(second, LANES)]], axis=1)

    def raise_keys(start, size):
        def step(pair):
            up = dot_tn(pair_weights(pair, 0), lat_t[:kv_lat, pl.ds(start, size)]).astype(BF16)
            keys_t[2 * pair, :, pl.ds(start, size)] = up[:NOPE_DIM]
            keys_t[2 * pair + 1, :, pl.ds(start, size)] = up[NOPE_DIM:]
        return step

    def raise_values(start, size):
        def step(pair):
            values[pair, pl.ds(start, size), :] = dot(lat[pl.ds(start, size), :], pair_weights(pair, NOPE_DIM)).astype(BF16)
        return step

    def put_tail(start, size, seg_row):
        hot = seg_row == lax.broadcasted_iota(jnp.int32, (ROPE_DIM, size), 0)
        hot = jnp.where(hot, 1.0, 0.0).astype(BF16)
        rope = lat_t[kv_lat:, pl.ds(start, size)]
        tail_t[0, :, pl.ds(start, size)] = jnp.concatenate([rope, hot], axis=0)
        tail_t[1, :, pl.ds(start, size)] = jnp.concatenate([hot, rope], axis=0)
    per = heads // 2 // KV_LOADS
    for i in range(KV_LOADS):
        phase(f"wait_own{i}")
        load_ukv[i].wait()
        if i == 0:
            load_pre.wait()
        else:
            load_dkv.wait()
        phase(f"own{i}")
        if i:
            load_uq = load(
                wuq_hbm.at[:, pl.ds(pl.multiple_of(core * heads * QK_DIM, LANES), heads * QK_DIM)], wuq_v, load_sem.at[4]
            )
            load_o = [
                load(
                    wo_hbm.at[
                        pl.ds(pl.multiple_of(lax.rem(core + side, CORES) * (heads * V_DIM) + part * deep, LANES), deep),
                        pl.ds(pl.multiple_of(core * half_width, LANES), half_width),
                    ],
                    wo_v.at[pl.ds((part * CORES + side) * deep, deep)],
                    wo_sem.at[part, side],
                )
                for part in range(PARTS) for side in range(CORES)
            ]
            down = dot_nt(hid_v[...], wdkv_v[...])
            c_kv = rms_norm(down[:, :kv_lat], gain_kv_ref[...])
            low, high = down[:, kv_lat:kv_lat + HALF], down[:, kv_lat + HALF:]
            cos_m, sin_m = cos_t[:, :HALF], sin_t[:, :HALF]
            k_new = jnp.concatenate([low * cos_m - high * sin_m, high * cos_m + low * sin_m], axis=1)
            new_lat[pl.ds(0, toks), :] = jnp.concatenate([c_kv, k_new], axis=1).astype(BF16)
        for pair in range(i * per, (i + 1) * per):
            raise_keys(0, pre)(pair)
        if i == 0:
            lat[pl.ds(0, pre), :] = jnp.transpose(lat_t[:kv_lat, pl.ds(0, pre)])
            put_tail(0, pre, pseg_ref[...])
            values[:, pl.ds(old + new, wide - old - new), :] = jnp.zeros((heads // 2, wide - old - new, 2 * V_DIM), BF16)
        for pair in range(i * per, (i + 1) * per):
            raise_values(0, pre)(pair)
    send_new = send(new_lat.at[pl.ds(0, toks)], new_lat.at[pl.ds(toks, toks)], mate_send.at[2], mate_recv.at[2], mate)

    phase("wait_meta")
    for copy in send_meta:
        copy.wait_recv()
    phase("wait_mate")
    send_pre.wait_recv()
    send_pseg.wait_recv()
    phase("keys_mate")
    unrolled(heads // 2, UNROLL_KV, raise_keys(pre, pre))
    lat[pl.ds(pre, pre), :] = jnp.transpose(lat_t[:kv_lat, pl.ds(pre, pre)])
    every = meta_all[...]
    lanes = lane_of((all_toks, LANES))
    q_seg = every[:, 2 * HALF:2 * HALF + 1]
    q_pos = every[:, 2 * HALF + 1:2 * HALF + 2]
    cos_q = jnp.where(lanes < HALF, every, 0.0)
    cos_q = cos_q + turn(cos_q, HALF)
    cos_all[...] = cos_q + turn(cos_q, 2 * HALF)
    sin_q = jnp.where((lanes >= HALF) & (lanes < 2 * HALF), every, 0.0)
    sin_q = sin_q - turn(sin_q, LANES - HALF)
    sin_all[...] = sin_q + turn(sin_q, 2 * HALF)
    q_mask = jnp.where(q_seg == jnp.where(lanes < ROPE_DIM, lanes, lanes - ROPE_DIM).astype(F32), 0.0, NEG_BIG)
    mask_a[...] = q_mask
    mate_rows = pl.ds(pl.multiple_of(mate * toks, toks), toks)
    new_meta = jnp.concatenate(
        [meta_all[my_rows, :], meta_all[mate_rows, :], jnp.zeros((LANES - new, LANES), F32)], axis=0
    )
    meta_rows = jnp.transpose(new_meta)
    k_seg, k_pos = meta_rows[2 * HALF:2 * HALF + 1], meta_rows[2 * HALF + 1:2 * HALF + 2]
    seen = (q_seg == k_seg) & (k_pos <= q_pos) & (lane_of((all_toks, LANES)) < new)
    bias[...] = jnp.where(seen, 0.0, NEG_BIG)

    put_tail(pre, pre, pseg_mate[...])

    phase("wait_uq")
    load_uq.wait()
    for copy in send_q:
        copy.wait_recv()
    send_new.wait_recv()
    phase("queries")
    lat[pl.ds(old, new), :] = new_lat[:, :kv_lat]
    new_rope = jnp.concatenate([new_lat[:, kv_lat:].astype(F32), jnp.zeros((new, LANES - ROPE_DIM), F32)], axis=1)
    new_rope = jnp.concatenate([new_rope, jnp.zeros((LANES - new, LANES), F32)], axis=0)
    new_rope = jnp.transpose(new_rope).astype(BF16)
    tail_t[0, :, pl.ds(old, LANES)] = new_rope
    tail_t[1, :ROPE_DIM, pl.ds(old, LANES)] = new_rope[ROPE_DIM:]
    tail_t[1, ROPE_DIM:, pl.ds(old, LANES)] = new_rope[:ROPE_DIM]
    low_half = lane_of((all_toks, LANES)) < ROPE_DIM
    first_half = lax.rem(lane_of((all_toks, LANES)), ROPE_DIM) < HALF

    def raise_queries(pair):
        cols = pl.ds(pl.multiple_of(pair * (2 * QK_DIM), LANES), 2 * QK_DIM)
        q = dot(qlat_all[...], wuq_v[:, cols])
        nope_a, mid, end = q[:, :LANES], q[:, LANES:2 * LANES], q[:, 2 * LANES:]
        nope_b = turn(jnp.where(low_half, end, mid), ROPE_DIM)
        u = jnp.where(low_half, mid, end)
        swapped = jnp.where(first_half, turn(u, LANES - HALF), turn(u, HALF))
        r = u * cos_all[...] + swapped * sin_all[...]
        queries[2 * pair] = jnp.concatenate([nope_a, jnp.where(low_half, r, mask_a[...])], axis=1).astype(BF16)
        queries[2 * pair + 1] = jnp.concatenate([nope_b, jnp.where(low_half, mask_a[...], r)], axis=1).astype(BF16)

    def raise_new_keys(pair):
        up = dot(new_lat[:, :kv_lat], pair_weights(pair, 0))
        up = jnp.transpose(jnp.concatenate([up, jnp.zeros((LANES - new, 2 * NOPE_DIM), F32)], axis=0)).astype(BF16)
        keys_t[2 * pair, :, pl.ds(old, LANES)] = up[:NOPE_DIM]
        keys_t[2 * pair + 1, :, pl.ds(old, LANES)] = up[NOPE_DIM:]

    def score(head):
        j = head % SCORE_BUFS
        s = dot(queries[head], jnp.concatenate([keys_t[head], tail_t[head % 2]], axis=0))
        scores[j, :, :old] = s[:, :old]
        scores[j, :, old:] = s[:, old:] + bias[...]

    def soften(head):
        j = head % SCORE_BUFS
        step = 16
        tops = [jnp.max(scores[j, r:r + step, :], axis=1, keepdims=True) for r in range(0, all_toks, step)]
        for i, top in enumerate(tops):
            rows = pl.ds(i * step, step)
            p = jnp.exp2((scores[j, rows, :] - top) * EXP_SCALE)
            probs[head, rows, :] = p.astype(BF16)
            tops_all[head, rows, :] = jnp.broadcast_to(top, (step, LANES))
            sums_all[head, rows, :] = jnp.broadcast_to(jnp.sum(p, axis=1, keepdims=True), (step, LANES))

    raise_mate = raise_values(pre, pre + new)

    def peer(j):
        return lax.rem(chip + j, chips)

    send_stats = []
    late = list(range(heads // 2))

    def make_ready(head):
        if head % 2 == 0:
            raise_queries(head // 2)
            raise_new_keys(head // 2)

    for head in range(heads):
        make_ready(head)
    for head in range(AHEAD):
        score(head)
    for head in range(heads):
        if head + AHEAD < heads:
            score(head + AHEAD)
        soften(head)
        for pair in VALUES_AFTER.get(head, ()):
            raise_mate(pair)
            late.remove(pair)
        if (head + 1) % some == 0:
            part = head // some
            packed = jnp.zeros((all_toks, LANES), F32)
            for i in range(some):
                packed = jnp.where(lanes == i, tops_all[part * some + i], packed)
                packed = jnp.where(lanes == some + i, sums_all[part * some + i], packed)
            stats[part] = jnp.transpose(packed)[:2 * some]
            send_stats.append([
                send(
                    stats.at[part], stats_rx.at[part, j - 1], st_send.at[part, j - 1], st_recv.at[part, j - 1],
                    lax.rem(me + j, n),
                )
                for j in range(1, n)
            ])

    red_copies = {}
    both = CORES * toks
    half = len(ORDER[0]) * both

    def put_scale(part):
        for side in range(CORES):
            got = [stats_rx[part, j - 1] for j in range(1 + (1 - side), n, CORES)]
            mine = stats[part] if side == 0 else jnp.where(core == 0, got[-1], got[0])
            every = got + [mine] if side == 0 else got
            top = functools.reduce(jnp.maximum, [g[:some] for g in every])
            total = functools.reduce(jnp.add, [g[some:] * jnp.exp2((g[:some] - top) * EXP_SCALE) for g in every])
            share = jnp.exp2((mine[:some] - top) * EXP_SCALE)
            scales[part, side, :, :some] = jnp.transpose(share / total)

    def put_split(part, g, sides):
        for b, j in enumerate(ORDER[g]):
            from_rows = pl.ds(pl.multiple_of(peer(j) * both, both), both)
            for side in sides:
                factor = scales[part, side, from_rows, :]
                for i in range(some):
                    cols = pl.ds(((part * CORES + side) * some + i) * V_DIM, V_DIM)
                    o = acc[side, part * some + i, from_rows, :] * factor[:, i:i + 1]
                    o_hi = o.astype(BF16)
                    split[g, pl.ds(b * both, both), cols] = o_hi
                    split[g, pl.ds(half + b * both, both), cols] = (o - o_hi.astype(F32)).astype(BF16)

    def project(part, g, side=None):
        first = part * CORES * deep
        ks = pl.ds(first, CORES * deep) if side is None else pl.ds(first + side * deep, deep)
        y = dot(split[g, :, ks], wo_v[ks, :])
        return y[:half] + y[half:]

    def deliver(g):
        for b, j in enumerate(ORDER[g]):
            for r in range(CORES):
                if j or r:
                    to = lax.rem(core + r, CORES)
                    rows = pl.ds(pl.multiple_of(b * both + to * toks, toks), toks)
                    red_copies[j, r] = send(
                        z.at[g, rows], z_rx.at[j, r], red_send.at[j, r], red_recv.at[j, r], peer(j) * CORES + to
                    )

    def swap(i):
        group = pl.ds(i * (heads // SWAPS), heads // SWAPS)
        return send(acc.at[0, group], acc.at[1, group], acc_send.at[i], acc_recv.at[i], mate)

    phase("attend")
    for pair in late:
        raise_mate(pair)
    send_acc = []
    for head in range(heads):
        cols = pl.ds((head % 2) * V_DIM, V_DIM)
        acc[0, head] = dot(probs[head], values[head // 2, :, cols])
        if (head + 1) % (heads // SWAPS) == 0:
            send_acc.append(swap(head * SWAPS // heads))
    phase("wait_stats0")
    for copy in load_o:
        copy.wait()
    for copy in send_stats[0]:
        copy.wait_recv()
    phase("outproj0")
    put_scale(0)
    for g in range(len(ORDER)):
        put_split(0, g, (0,))
        z[g] = project(0, g, 0)
    phase("wait_acc0")
    for copy in send_acc[:SWAPS // PARTS]:
        copy.wait_recv()
    phase("outproj0m")
    for g in range(len(ORDER)):
        put_split(0, g, (1,))
        z[g] = z[g] + project(0, g, 1)
    phase("wait_stats1")
    for copy in send_stats[1]:
        copy.wait_recv()
    phase("wait_acc1")
    for copy in send_acc[SWAPS // PARTS:]:
        copy.wait_recv()
    phase("outproj1")
    put_scale(1)
    for g in range(len(ORDER)):
        put_split(1, g, range(CORES))
    for g in range(len(ORDER)):
        z[g] = z[g] + project(1, g)
        deliver(g)
    for j in (0, 1, 3, 2):
        phase(f"wait_red{j}")
        for r in range(CORES):
            if j or r:
                red_copies[j, r].wait_recv()
    phase("reduce")
    own = pl.ds(pl.multiple_of(both + core * toks, toks), toks)
    for r in range(CORES):
        y = z[1, own, :] if r == 0 else z_rx[0, 1]
        for j in range(1, chips):
            y = y + z_rx[j, r]
        cols = pl.ds(pl.multiple_of(lax.rem(core + r, CORES) * half_width, LANES), half_width)
        out_ref[:, cols] = y.astype(BF16)

    phase("drain")
    for copy in [send_pre, send_pseg, send_new] + send_meta + send_q + sum(send_stats, []) + send_acc + list(red_copies.values()):
        copy.wait_send()
    phase("")


def solution(mesh):
    n = mesh.shape["sp"]
    chips = n // CORES
    tok_spec = P(("dp", "sp"), None)
    vec_spec = P(("dp", "sp"))
    mat_spec = P(None, None)
    gain_spec = P(None)

    def device_step(hidden, seg_ids, positions, prefix_lat, prefix_seg, w_dq, gain_q, w_uq, w_dkv, gain_kv, w_ukv, w_o):
        toks, width = hidden.shape
        pre, lat_dim = prefix_lat.shape
        q_lat = w_dq.shape[1]
        kv_lat = w_ukv.shape[0]
        heads = w_o.shape[0] // V_DIM // CORES
        rows = CORES * (pre + toks)
        wide = CORES * pre + LANES
        all_toks = n * toks
        inv_freq = (ROPE_BASE ** (-np.arange(HALF, dtype=np.float64) / HALF)).astype(np.float32)
        freq = jnp.asarray(np.concatenate([inv_freq] * (LANES // HALF)).reshape(1, LANES))
        vmem = pl.BlockSpec(memory_space=pltpu.VMEM)
        hbm = pl.BlockSpec(memory_space=pltpu.HBM)
        dma = pltpu.SemaphoreType.DMA
        table = pltpu.VMEM((all_toks, LANES), F32)
        return pl.pallas_call(
            functools.partial(kernel, n),
            out_shape=pltpu.VMEM((toks, width), BF16),
            in_specs=[hbm] * 13,
            scratch_shapes=[
                pltpu.VMEM((1, LANES), F32),
                pltpu.VMEM((1, toks), jnp.int32),
                pltpu.VMEM((1, toks), jnp.int32),
                pltpu.VMEM((1, pre), jnp.int32),
                pltpu.VMEM((q_lat,), BF16),
                pltpu.VMEM((kv_lat,), BF16),
                pltpu.VMEM((toks, width), BF16),
                pltpu.VMEM((width, q_lat), BF16),
                pltpu.VMEM((lat_dim, width), BF16),
                pltpu.VMEM((q_lat, heads * QK_DIM), BF16),
                pltpu.VMEM((kv_lat, heads * KV_HEAD), BF16),
                pltpu.VMEM((CORES * heads * V_DIM, width // CORES), BF16),
                pltpu.VMEM((lat_dim, wide), BF16),
                pltpu.VMEM((rows, kv_lat), BF16),
                pltpu.VMEM((CORES * toks, lat_dim), BF16),
                pltpu.VMEM((1, pre), jnp.int32),
                pltpu.VMEM((all_toks, q_lat), BF16),
                table, table, table, table,
                pltpu.VMEM((2, LANES, wide), BF16),
                pltpu.VMEM((heads, NOPE_DIM, wide), BF16),
                pltpu.VMEM((heads // 2, wide, 2 * V_DIM), BF16),
                pltpu.VMEM((heads, all_toks, 2 * LANES), BF16),
                pltpu.VMEM((heads, all_toks, wide), BF16),
                pltpu.VMEM((heads, all_toks, LANES), F32),
                pltpu.VMEM((heads, all_toks, LANES), F32),
                pltpu.VMEM((SCORE_BUFS, all_toks, wide), F32),
                pltpu.VMEM((PARTS, 2 * heads // PARTS, all_toks), F32),
                pltpu.VMEM((PARTS, n - 1, 2 * heads // PARTS, all_toks), F32),
                pltpu.VMEM((CORES, heads, all_toks, V_DIM), F32),
                pltpu.VMEM((PARTS, CORES, all_toks, LANES), F32),
                pltpu.VMEM((2, all_toks, CORES * heads * V_DIM), BF16),
                table,
                pltpu.VMEM((2, all_toks // 2, width // CORES), F32),
                pltpu.VMEM((chips, CORES, toks, width // CORES), F32),
                dma((6,)),
                dma((6,)),
                dma((DQ_LOADS,)),
                dma((PARTS, CORES)),
                dma((KV_LOADS,)),
                dma((3,)), dma((3,)),
                dma((n - 1,)), dma((n - 1,)),
                dma((n - 1,)), dma((n - 1,)),
                dma((PARTS, n - 1)), dma((PARTS, n - 1)),
                dma((SWAPS,)), dma((SWAPS,)),
                dma((chips, CORES)), dma((chips, CORES)),
            ],
            compiler_params=pltpu.CompilerParams(
                collective_id=0, has_side_effects=True, vmem_limit_bytes=60 * 1024 * 1024
            ),
        )(
            freq, seg_ids.reshape(1, toks), positions.reshape(1, toks), prefix_seg.reshape(1, pre),
            gain_q, gain_kv,
            hidden, prefix_lat.T, w_dq, w_uq, w_dkv.T, w_ukv, w_o,
        )

    return jax.shard_map(
        device_step,
        mesh=mesh,
        in_specs=(tok_spec, vec_spec, vec_spec, tok_spec, vec_spec, mat_spec, gain_spec, mat_spec, mat_spec, gain_spec, mat_spec, mat_spec),
        out_specs=tok_spec,
        check_vma=False,
    )
```

```python
import functools
import math

import jax
import jax.numpy as jnp
import numpy as np
from jax import lax
from jax.experimental import pallas as pl
from jax.experimental.pallas import tpu as pltpu
from jax.sharding import PartitionSpec as P

ROPE_DIM = 64
HALF = ROPE_DIM // 2
NOPE_DIM = 128
V_DIM = 128
QK_DIM = NOPE_DIM + ROPE_DIM
KV_HEAD = NOPE_DIM + V_DIM
CORES = 2
EPS = 1e-6
ROPE_BASE = 10000.0
NEG_BIG = -1e30
EXP_SCALE = QK_DIM ** -0.5 * math.log2(math.e)
LANES = 128
ORDER = ((2, 1), (3, 0))
PARTS = 2
SWAPS = 2
VALUES_AFTER = {7: (0, 1, 2, 3), 15: (4, 5)}
AHEAD = 0
KV_LOADS = 2
UP_LOADS = 4
DQ_LOADS = 4
UNROLL_KV = 8
SCORE_BUFS = 8

F32 = jnp.float32
BF16 = jnp.bfloat16


def dot(a, b):
    return jnp.dot(a, b, preferred_element_type=F32)


def dot_nt(a, b):
    return lax.dot_general(a, b, (((1,), (1,)), ((), ())), preferred_element_type=F32)


def dot_tn(a, b):
    return lax.dot_general(a, b, (((0,), (0,)), ((), ())), preferred_element_type=F32)


def rms_norm(values, gain):
    inv_rms = lax.rsqrt(jnp.mean(values * values, axis=-1, keepdims=True) + EPS)
    return values * inv_rms * gain.astype(F32).reshape(1, gain.shape[0])


def row_to_column(row):
    size = row.shape[1]
    here = lax.broadcasted_iota(jnp.int32, (size, size), 0) == lax.broadcasted_iota(jnp.int32, (size, size), 1)
    return jnp.sum(jnp.where(here, jnp.broadcast_to(row, (size, size)), 0.0), axis=1, keepdims=True)


def lane_of(shape):
    return lax.broadcasted_iota(jnp.int32, shape, len(shape) - 1)


def turn(x, amount):
    return pltpu.roll(x, amount, 1)


def unrolled(count, step, body):
    if count == step:
        for j in range(step):
            body(j)
        return

    def run(i, carry):
        for j in range(step):
            body(i * step + j)
        return carry

    lax.fori_loop(0, count // step, run, 0)


class Phases:
    def __init__(self):
        self.now = None

    def __call__(self, name):
        if self.now is not None:
            self.now.__exit__(None, None, None)
        self.now = None
        if name:
            self.now = jax.named_scope(name)
            self.now.__enter__()


def kernel(
    n,
    freq_hbm, seg_hbm, pos_hbm, pseg_hbm, gain_q_hbm, gain_kv_hbm,
    hid_hbm, pre_hbm, wdq_hbm, wuq_hbm, wdkv_hbm, wukv_hbm, wo_hbm,
    out_ref,
    freq_ref, seg_ref, pos_ref, pseg_ref, gain_q_ref, gain_kv_ref,
    hid_v, wdq_v, wdkv_v, wuq_v, wukv_v, wo_v,
    lat_t, lat, new_lat, pseg_mate, qlat_all, meta_all, cos_all, sin_all, mask_a, tail_t,
    keys_t, values, queries, probs, tops_all, sums_all,
    scores, stats, stats_rx, acc, scales, split, bias, z, z_rx,
    load_sem, small_sem, dq_sem, wo_sem, ukv_sem, mate_send, mate_recv, gat_send, gat_recv, met_send, met_recv,
    st_send, st_recv, acc_send, acc_recv, red_send, red_recv,
):
    phase = Phases()
    me = lax.axis_index("sp")
    core = lax.rem(me, CORES)
    chip = lax.div(me, CORES)
    chips = n // CORES
    mate = chip * CORES + (CORES - 1 - core)
    toks = hid_v.shape[0]
    pre = pre_hbm.shape[1]
    kv_lat = wukv_v.shape[0]
    heads = keys_t.shape[0]
    old = CORES * pre
    new = CORES * toks
    wide = lat_t.shape[1]
    all_toks = n * toks
    some = heads // PARTS
    deep = some * V_DIM
    half_width = wo_v.shape[1]

    phase("loads")

    def load(src, dst, sem):
        copy = pltpu.make_async_copy(src, dst, sem)
        copy.start()
        return copy

    barrier = pltpu.get_barrier_semaphore()
    for j in range(1, n):
        pl.semaphore_signal(barrier, inc=1, device_id={"sp": lax.rem(me + j, n)}, device_id_type=pl.DeviceIdType.MESH)
    smalls = [
        load(src, dst, small_sem.at[i])
        for i, (src, dst) in enumerate([
            (freq_hbm, freq_ref), (seg_hbm, seg_ref), (pos_hbm, pos_ref),
            (gain_q_hbm, gain_q_ref), (gain_kv_hbm, gain_kv_ref), (pseg_hbm, pseg_ref),
        ])
    ]
    load_hid = load(hid_hbm, hid_v, load_sem.at[0])
    depth = wdq_v.shape[0] // DQ_LOADS
    load_dq = [
        load(wdq_hbm.at[pl.ds(i * depth, depth)], wdq_v.at[pl.ds(i * depth, depth)], dq_sem.at[i])
        for i in range(DQ_LOADS)
    ]
    kv_cols = heads * KV_HEAD
    part = kv_cols // KV_LOADS

    def load_up(i):
        deep_kv = kv_lat // UP_LOADS
        return [
            load(
                wukv_hbm.at[pl.ds(d * deep_kv, deep_kv), pl.ds(pl.multiple_of(core * kv_cols + i * part, LANES), part)],
                wukv_v.at[pl.ds(d * deep_kv, deep_kv), pl.ds(i * part, part)],
                ukv_sem.at[i, d],
            )
            for d in range(UP_LOADS)
        ]

    load_pre = load(pre_hbm, lat_t.at[:, pl.ds(0, pre)], load_sem.at[3])
    load_ukv = [load_up(0)]

    phase("wait_small")
    for copy in smalls:
        copy.wait()
    phase("meta")
    pos_col = row_to_column(pos_ref[...].astype(F32))
    seg_col = row_to_column(seg_ref[...].astype(F32))
    angles = pos_col * freq_ref[...]
    lane = lane_of((toks, LANES))
    cos_t = jnp.cos(angles)
    sin_t = jnp.sin(angles)
    my_rows = pl.ds(pl.multiple_of(me * toks, toks), toks)
    meta_all[my_rows, :] = jnp.where(
        lane < HALF, cos_t, jnp.where(lane < 2 * HALF, sin_t, jnp.where(lane == 2 * HALF, seg_col, pos_col))
    )

    def send(src, dst, send_sem, recv_sem, target):
        copy = pltpu.make_async_remote_copy(
            src_ref=src, dst_ref=dst, send_sem=send_sem, recv_sem=recv_sem,
            device_id={"sp": target}, device_id_type=pl.DeviceIdType.MESH,
        )
        copy.start()
        return copy

    phase("wait_dq")
    load_hid.wait()
    for copy in load_dq:
        copy.wait()
    load_ukv += [load_up(i) for i in range(1, KV_LOADS)]
    load_dkv = load(wdkv_hbm, wdkv_v, load_sem.at[2])
    phase("barrier")
    pl.semaphore_wait(barrier, n - 1)
    send_pre = send(pre_hbm, lat_t.at[:, pl.ds(pre, pre)], mate_send.at[0], mate_recv.at[0], mate)
    send_pseg = send(pseg_ref, pseg_mate, mate_send.at[1], mate_recv.at[1], mate)
    phase("qlat")
    qlat_all[my_rows, :] = rms_norm(dot(hid_v[...], wdq_v[...]), gain_q_ref[...]).astype(BF16)

    send_q = [
        send(qlat_all.at[my_rows], qlat_all.at[my_rows], gat_send.at[j - 1], gat_recv.at[j - 1], lax.rem(me + j, n))
        for j in range(1, n)
    ]
    send_meta = [
        send(meta_all.at[my_rows], meta_all.at[my_rows], met_send.at[j - 1], met_recv.at[j - 1], lax.rem(me + j, n))
        for j in range(1, n)
    ]
    def pair_weights(pair, offset):
        first = pl.multiple_of(pair * (2 * KV_HEAD) + offset, LANES)
        second = pl.multiple_of(pair * (2 * KV_HEAD) + KV_HEAD + offset, LANES)
        return jnp.concatenate([wukv_v[:, pl.ds(first, LANES)], wukv_v[:, pl.ds(second, LANES)]], axis=1)

    def raise_keys(start, size):
        def step(pair):
            up = dot_tn(pair_weights(pair, 0), lat_t[:kv_lat, pl.ds(start, size)]).astype(BF16)
            keys_t[2 * pair, :, pl.ds(start, size)] = up[:NOPE_DIM]
            keys_t[2 * pair + 1, :, pl.ds(start, size)] = up[NOPE_DIM:]
        return step

    def raise_values(start, size):
        def step(pair):
            values[pair, pl.ds(start, size), :] = dot(lat[pl.ds(start, size), :], pair_weights(pair, NOPE_DIM)).astype(BF16)
        return step

    def put_tail(start, size, seg_row):
        hot = seg_row == lax.broadcasted_iota(jnp.int32, (ROPE_DIM, size), 0)
        hot = jnp.where(hot, 1.0, 0.0).astype(BF16)
        rope = lat_t[kv_lat:, pl.ds(start, size)]
        tail_t[0, :, pl.ds(start, size)] = jnp.concatenate([rope, hot], axis=0)
        tail_t[1, :, pl.ds(start, size)] = jnp.concatenate([hot, rope], axis=0)
    per = heads // 2 // KV_LOADS
    for i in range(KV_LOADS):
        phase(f"wait_own{i}")
        for copy in load_ukv[i]:
            copy.wait()
        if i == 0:
            load_pre.wait()
        else:
            load_dkv.wait()
        phase(f"own{i}")
        if i:
            load_uq = load(
                wuq_hbm.at[:, pl.ds(pl.multiple_of(core * heads * QK_DIM, LANES), heads * QK_DIM)], wuq_v, load_sem.at[4]
            )
            load_o = [
                load(
                    wo_hbm.at[
                        pl.ds(pl.multiple_of(lax.rem(core + side, CORES) * (heads * V_DIM) + part * deep, LANES), deep),
                        pl.ds(pl.multiple_of(core * half_width, LANES), half_width),
                    ],
                    wo_v.at[pl.ds((part * CORES + side) * deep, deep)],
                    wo_sem.at[part, side],
                )
                for part in range(PARTS) for side in range(CORES)
            ]
            down = dot_nt(hid_v[...], wdkv_v[...])
            c_kv = rms_norm(down[:, :kv_lat], gain_kv_ref[...])
            low, high = down[:, kv_lat:kv_lat + HALF], down[:, kv_lat + HALF:]
            cos_m, sin_m = cos_t[:, :HALF], sin_t[:, :HALF]
            k_new = jnp.concatenate([low * cos_m - high * sin_m, high * cos_m + low * sin_m], axis=1)
            new_lat[pl.ds(0, toks), :] = jnp.concatenate([c_kv, k_new], axis=1).astype(BF16)
        for pair in range(i * per, (i + 1) * per):
            raise_keys(0, pre)(pair)
        if i == 0:
            lat[pl.ds(0, pre), :] = jnp.transpose(lat_t[:kv_lat, pl.ds(0, pre)])
            put_tail(0, pre, pseg_ref[...])
            values[:, pl.ds(old + new, wide - old - new), :] = jnp.zeros((heads // 2, wide - old - new, 2 * V_DIM), BF16)
        for pair in range(i * per, (i + 1) * per):
            raise_values(0, pre)(pair)
    send_new = send(new_lat.at[pl.ds(0, toks)], new_lat.at[pl.ds(toks, toks)], mate_send.at[2], mate_recv.at[2], mate)

    phase("wait_mate")
    send_pre.wait_recv()
    send_pseg.wait_recv()
    phase("keys_mate")
    unrolled(heads // 2, UNROLL_KV, raise_keys(pre, pre))
    lat[pl.ds(pre, pre), :] = jnp.transpose(lat_t[:kv_lat, pl.ds(pre, pre)])
    put_tail(pre, pre, pseg_mate[...])

    phase("wait_uq")
    load_uq.wait()
    for copy in send_q:
        copy.wait_recv()
    send_new.wait_recv()
    for copy in send_meta:
        copy.wait_recv()
    phase("queries")
    every = meta_all[...]
    lanes = lane_of((all_toks, LANES))
    q_seg = every[:, 2 * HALF:2 * HALF + 1]
    q_pos = every[:, 2 * HALF + 1:2 * HALF + 2]
    cos_q = jnp.where(lanes < HALF, every, 0.0)
    cos_q = cos_q + turn(cos_q, HALF)
    cos_all[...] = cos_q + turn(cos_q, 2 * HALF)
    sin_q = jnp.where((lanes >= HALF) & (lanes < 2 * HALF), every, 0.0)
    sin_q = sin_q - turn(sin_q, LANES - HALF)
    sin_all[...] = sin_q + turn(sin_q, 2 * HALF)
    q_mask = jnp.where(q_seg == jnp.where(lanes < ROPE_DIM, lanes, lanes - ROPE_DIM).astype(F32), 0.0, NEG_BIG)
    mask_a[...] = q_mask
    mate_rows = pl.ds(pl.multiple_of(mate * toks, toks), toks)
    new_meta = jnp.concatenate(
        [meta_all[my_rows, :], meta_all[mate_rows, :], jnp.zeros((LANES - new, LANES), F32)], axis=0
    )
    meta_rows = jnp.transpose(new_meta)
    k_seg, k_pos = meta_rows[2 * HALF:2 * HALF + 1], meta_rows[2 * HALF + 1:2 * HALF + 2]
    seen = (q_seg == k_seg) & (k_pos <= q_pos) & (lane_of((all_toks, LANES)) < new)
    bias[...] = jnp.where(seen, 0.0, NEG_BIG)

    lat[pl.ds(old, new), :] = new_lat[:, :kv_lat]
    new_rope = jnp.concatenate([new_lat[:, kv_lat:].astype(F32), jnp.zeros((new, LANES - ROPE_DIM), F32)], axis=1)
    new_rope = jnp.concatenate([new_rope, jnp.zeros((LANES - new, LANES), F32)], axis=0)
    new_rope = jnp.transpose(new_rope).astype(BF16)
    tail_t[0, :, pl.ds(old, LANES)] = new_rope
    tail_t[1, :ROPE_DIM, pl.ds(old, LANES)] = new_rope[ROPE_DIM:]
    tail_t[1, ROPE_DIM:, pl.ds(old, LANES)] = new_rope[:ROPE_DIM]
    low_half = lane_of((all_toks, LANES)) < ROPE_DIM
    first_half = lax.rem(lane_of((all_toks, LANES)), ROPE_DIM) < HALF

    def raise_queries(pair):
        cols = pl.ds(pl.multiple_of(pair * (2 * QK_DIM), LANES), 2 * QK_DIM)
        q = dot(qlat_all[...], wuq_v[:, cols])
        nope_a, mid, end = q[:, :LANES], q[:, LANES:2 * LANES], q[:, 2 * LANES:]
        nope_b = turn(jnp.where(low_half, end, mid), ROPE_DIM)
        u = jnp.where(low_half, mid, end)
        swapped = jnp.where(first_half, turn(u, LANES - HALF), turn(u, HALF))
        r = u * cos_all[...] + swapped * sin_all[...]
        queries[2 * pair] = jnp.concatenate([nope_a, jnp.where(low_half, r, mask_a[...])], axis=1).astype(BF16)
        queries[2 * pair + 1] = jnp.concatenate([nope_b, jnp.where(low_half, mask_a[...], r)], axis=1).astype(BF16)

    def raise_new_keys(pair):
        up = dot(new_lat[:, :kv_lat], pair_weights(pair, 0))
        up = jnp.transpose(jnp.concatenate([up, jnp.zeros((LANES - new, 2 * NOPE_DIM), F32)], axis=0)).astype(BF16)
        keys_t[2 * pair, :, pl.ds(old, LANES)] = up[:NOPE_DIM]
        keys_t[2 * pair + 1, :, pl.ds(old, LANES)] = up[NOPE_DIM:]

    def score(head):
        j = head % SCORE_BUFS
        s = dot(queries[head], jnp.concatenate([keys_t[head], tail_t[head % 2]], axis=0))
        scores[j, :, :old] = s[:, :old]
        scores[j, :, old:] = s[:, old:] + bias[...]

    def soften(head):
        j = head % SCORE_BUFS
        step = 16
        tops = [jnp.max(scores[j, r:r + step, :], axis=1, keepdims=True) for r in range(0, all_toks, step)]
        for i, top in enumerate(tops):
            rows = pl.ds(i * step, step)
            p = jnp.exp2((scores[j, rows, :] - top) * EXP_SCALE)
            probs[head, rows, :] = p.astype(BF16)
            tops_all[head, rows, :] = jnp.broadcast_to(top, (step, LANES))
            sums_all[head, rows, :] = jnp.broadcast_to(jnp.sum(p, axis=1, keepdims=True), (step, LANES))

    raise_mate = raise_values(pre, pre + new)

    def peer(j):
        return lax.rem(chip + j, chips)

    send_stats = []
    late = list(range(heads // 2))

    def make_ready(head):
        if head % 2 == 0:
            raise_queries(head // 2)
            raise_new_keys(head // 2)

    for head in range(heads):
        make_ready(head)
    for head in range(AHEAD):
        score(head)
    for head in range(heads):
        if head + AHEAD < heads:
            score(head + AHEAD)
        soften(head)
        for pair in VALUES_AFTER.get(head, ()):
            raise_mate(pair)
            late.remove(pair)
        if (head + 1) % some == 0:
            part = head // some
            packed = jnp.zeros((all_toks, LANES), F32)
            for i in range(some):
                packed = jnp.where(lanes == i, tops_all[part * some + i], packed)
                packed = jnp.where(lanes == some + i, sums_all[part * some + i], packed)
            stats[part] = jnp.transpose(packed)[:2 * some]
            send_stats.append([
                send(
                    stats.at[part], stats_rx.at[part, j - 1], st_send.at[part, j - 1], st_recv.at[part, j - 1],
                    lax.rem(me + j, n),
                )
                for j in range(1, n)
            ])

    red_copies = {}
    both = CORES * toks
    half = len(ORDER[0]) * both

    def put_scale(part):
        for side in range(CORES):
            got = [stats_rx[part, j - 1] for j in range(1 + (1 - side), n, CORES)]
            mine = stats[part] if side == 0 else jnp.where(core == 0, got[-1], got[0])
            every = got + [mine] if side == 0 else got
            top = functools.reduce(jnp.maximum, [g[:some] for g in every])
            total = functools.reduce(jnp.add, [g[some:] * jnp.exp2((g[:some] - top) * EXP_SCALE) for g in every])
            share = jnp.exp2((mine[:some] - top) * EXP_SCALE)
            scales[part, side, :, :some] = jnp.transpose(share / total)

    def put_split(part, g, sides):
        for b, j in enumerate(ORDER[g]):
            from_rows = pl.ds(pl.multiple_of(peer(j) * both, both), both)
            for side in sides:
                factor = scales[part, side, from_rows, :]
                for i in range(some):
                    cols = pl.ds(((part * CORES + side) * some + i) * V_DIM, V_DIM)
                    o = acc[side, part * some + i, from_rows, :] * factor[:, i:i + 1]
                    o_hi = o.astype(BF16)
                    split[g, pl.ds(b * both, both), cols] = o_hi
                    split[g, pl.ds(half + b * both, both), cols] = (o - o_hi.astype(F32)).astype(BF16)

    def project(part, g, side=None):
        first = part * CORES * deep
        ks = pl.ds(first, CORES * deep) if side is None else pl.ds(first + side * deep, deep)
        y = dot(split[g, :, ks], wo_v[ks, :])
        return y[:half] + y[half:]

    def deliver(g):
        for b, j in enumerate(ORDER[g]):
            for r in range(CORES):
                if j or r:
                    to = lax.rem(core + r, CORES)
                    rows = pl.ds(pl.multiple_of(b * both + to * toks, toks), toks)
                    red_copies[j, r] = send(
                        z.at[g, rows], z_rx.at[j, r], red_send.at[j, r], red_recv.at[j, r], peer(j) * CORES + to
                    )

    def swap(i):
        group = pl.ds(i * (heads // SWAPS), heads // SWAPS)
        return send(acc.at[0, group], acc.at[1, group], acc_send.at[i], acc_recv.at[i], mate)

    phase("attend")
    for pair in late:
        raise_mate(pair)
    send_acc = []
    for head in range(heads):
        cols = pl.ds((head % 2) * V_DIM, V_DIM)
        acc[0, head] = dot(probs[head], values[head // 2, :, cols])
        if (head + 1) % (heads // SWAPS) == 0:
            send_acc.append(swap(head * SWAPS // heads))
    phase("wait_stats0")
    for copy in load_o:
        copy.wait()
    for copy in send_stats[0]:
        copy.wait_recv()
    phase("outproj0")
    put_scale(0)
    for g in range(len(ORDER)):
        put_split(0, g, (0,))
        z[g] = project(0, g, 0)
    phase("wait_acc0")
    for copy in send_acc[:SWAPS // PARTS]:
        copy.wait_recv()
    phase("outproj0m")
    for g in range(len(ORDER)):
        put_split(0, g, (1,))
        z[g] = z[g] + project(0, g, 1)
    phase("wait_stats1")
    for copy in send_stats[1]:
        copy.wait_recv()
    phase("wait_acc1")
    for copy in send_acc[SWAPS // PARTS:]:
        copy.wait_recv()
    phase("outproj1")
    put_scale(1)
    for g in range(len(ORDER)):
        put_split(1, g, range(CORES))
    for g in range(len(ORDER)):
        z[g] = z[g] + project(1, g)
        deliver(g)
    for j in (0, 1, 3, 2):
        phase(f"wait_red{j}")
        for r in range(CORES):
            if j or r:
                red_copies[j, r].wait_recv()
    phase("reduce")
    own = pl.ds(pl.multiple_of(both + core * toks, toks), toks)
    for r in range(CORES):
        y = z[1, own, :] if r == 0 else z_rx[0, 1]
        for j in range(1, chips):
            y = y + z_rx[j, r]
        cols = pl.ds(pl.multiple_of(lax.rem(core + r, CORES) * half_width, LANES), half_width)
        out_ref[:, cols] = y.astype(BF16)

    phase("drain")
    for copy in [send_pre, send_pseg, send_new] + send_meta + send_q + sum(send_stats, []) + send_acc + list(red_copies.values()):
        copy.wait_send()
    phase("")


def solution(mesh):
    n = mesh.shape["sp"]
    chips = n // CORES
    tok_spec = P(("dp", "sp"), None)
    vec_spec = P(("dp", "sp"))
    mat_spec = P(None, None)
    gain_spec = P(None)

    def device_step(hidden, seg_ids, positions, prefix_lat, prefix_seg, w_dq, gain_q, w_uq, w_dkv, gain_kv, w_ukv, w_o):
        toks, width = hidden.shape
        pre, lat_dim = prefix_lat.shape
        q_lat = w_dq.shape[1]
        kv_lat = w_ukv.shape[0]
        heads = w_o.shape[0] // V_DIM // CORES
        rows = CORES * (pre + toks)
        wide = CORES * pre + LANES
        all_toks = n * toks
        inv_freq = (ROPE_BASE ** (-np.arange(HALF, dtype=np.float64) / HALF)).astype(np.float32)
        freq = jnp.asarray(np.concatenate([inv_freq] * (LANES // HALF)).reshape(1, LANES))
        vmem = pl.BlockSpec(memory_space=pltpu.VMEM)
        hbm = pl.BlockSpec(memory_space=pltpu.HBM)
        dma = pltpu.SemaphoreType.DMA
        table = pltpu.VMEM((all_toks, LANES), F32)
        return pl.pallas_call(
            functools.partial(kernel, n),
            out_shape=pltpu.VMEM((toks, width), BF16),
            in_specs=[hbm] * 13,
            scratch_shapes=[
                pltpu.VMEM((1, LANES), F32),
                pltpu.VMEM((1, toks), jnp.int32),
                pltpu.VMEM((1, toks), jnp.int32),
                pltpu.VMEM((1, pre), jnp.int32),
                pltpu.VMEM((q_lat,), BF16),
                pltpu.VMEM((kv_lat,), BF16),
                pltpu.VMEM((toks, width), BF16),
                pltpu.VMEM((width, q_lat), BF16),
                pltpu.VMEM((lat_dim, width), BF16),
                pltpu.VMEM((q_lat, heads * QK_DIM), BF16),
                pltpu.VMEM((kv_lat, heads * KV_HEAD), BF16),
                pltpu.VMEM((CORES * heads * V_DIM, width // CORES), BF16),
                pltpu.VMEM((lat_dim, wide), BF16),
                pltpu.VMEM((rows, kv_lat), BF16),
                pltpu.VMEM((CORES * toks, lat_dim), BF16),
                pltpu.VMEM((1, pre), jnp.int32),
                pltpu.VMEM((all_toks, q_lat), BF16),
                table, table, table, table,
                pltpu.VMEM((2, LANES, wide), BF16),
                pltpu.VMEM((heads, NOPE_DIM, wide), BF16),
                pltpu.VMEM((heads // 2, wide, 2 * V_DIM), BF16),
                pltpu.VMEM((heads, all_toks, 2 * LANES), BF16),
                pltpu.VMEM((heads, all_toks, wide), BF16),
                pltpu.VMEM((heads, all_toks, LANES), F32),
                pltpu.VMEM((heads, all_toks, LANES), F32),
                pltpu.VMEM((SCORE_BUFS, all_toks, wide), F32),
                pltpu.VMEM((PARTS, 2 * heads // PARTS, all_toks), F32),
                pltpu.VMEM((PARTS, n - 1, 2 * heads // PARTS, all_toks), F32),
                pltpu.VMEM((CORES, heads, all_toks, V_DIM), F32),
                pltpu.VMEM((PARTS, CORES, all_toks, LANES), F32),
                pltpu.VMEM((2, all_toks, CORES * heads * V_DIM), BF16),
                table,
                pltpu.VMEM((2, all_toks // 2, width // CORES), F32),
                pltpu.VMEM((chips, CORES, toks, width // CORES), F32),
                dma((6,)),
                dma((6,)),
                dma((DQ_LOADS,)),
                dma((PARTS, CORES)),
                dma((KV_LOADS, UP_LOADS)),
                dma((3,)), dma((3,)),
                dma((n - 1,)), dma((n - 1,)),
                dma((n - 1,)), dma((n - 1,)),
                dma((PARTS, n - 1)), dma((PARTS, n - 1)),
                dma((SWAPS,)), dma((SWAPS,)),
                dma((chips, CORES)), dma((chips, CORES)),
            ],
            compiler_params=pltpu.CompilerParams(
                collective_id=0, has_side_effects=True, vmem_limit_bytes=60 * 1024 * 1024
            ),
        )(
            freq, seg_ids.reshape(1, toks), positions.reshape(1, toks), prefix_seg.reshape(1, pre),
            gain_q, gain_kv,
            hidden, prefix_lat.T, w_dq, w_uq, w_dkv.T, w_ukv, w_o,
        )

    return jax.shard_map(
        device_step,
        mesh=mesh,
        in_specs=(tok_spec, vec_spec, vec_spec, tok_spec, vec_spec, mat_spec, gain_spec, mat_spec, mat_spec, gain_spec, mat_spec, mat_spec),
        out_specs=tok_spec,
        check_vma=False,
    )
```

```python
import functools
import math

import jax
import jax.numpy as jnp
import numpy as np
from jax import lax
from jax.experimental import pallas as pl
from jax.experimental.pallas import tpu as pltpu
from jax.sharding import PartitionSpec as P

ROPE_DIM = 64
HALF = ROPE_DIM // 2
NOPE_DIM = 128
V_DIM = 128
QK_DIM = NOPE_DIM + ROPE_DIM
KV_HEAD = NOPE_DIM + V_DIM
CORES = 2
EPS = 1e-6
ROPE_BASE = 10000.0
NEG_BIG = -1e30
EXP_SCALE = QK_DIM ** -0.5 * math.log2(math.e)
LANES = 128
ORDER = ((2, 1), (3, 0))
PARTS = 2
SWAPS = 2
VALUES_AFTER = {7: (0, 1, 2, 3), 15: (4, 5)}
AHEAD = 0
KV_LOADS = 2
DQ_LOADS = 4
UNROLL_KV = 8
SCORE_BUFS = 8

F32 = jnp.float32
BF16 = jnp.bfloat16


def dot(a, b):
    return jnp.dot(a, b, preferred_element_type=F32)


def dot_nt(a, b):
    return lax.dot_general(a, b, (((1,), (1,)), ((), ())), preferred_element_type=F32)


def dot_tn(a, b):
    return lax.dot_general(a, b, (((0,), (0,)), ((), ())), preferred_element_type=F32)


def rms_norm(values, gain):
    inv_rms = lax.rsqrt(jnp.mean(values * values, axis=-1, keepdims=True) + EPS)
    return values * inv_rms * gain.astype(F32).reshape(1, gain.shape[0])


def row_to_column(row):
    size = row.shape[1]
    here = lax.broadcasted_iota(jnp.int32, (size, size), 0) == lax.broadcasted_iota(jnp.int32, (size, size), 1)
    return jnp.sum(jnp.where(here, jnp.broadcast_to(row, (size, size)), 0.0), axis=1, keepdims=True)


def lane_of(shape):
    return lax.broadcasted_iota(jnp.int32, shape, len(shape) - 1)


def turn(x, amount):
    return pltpu.roll(x, amount, 1)


def unrolled(count, step, body):
    if count == step:
        for j in range(step):
            body(j)
        return

    def run(i, carry):
        for j in range(step):
            body(i * step + j)
        return carry

    lax.fori_loop(0, count // step, run, 0)


class Phases:
    def __init__(self):
        self.now = None

    def __call__(self, name):
        if self.now is not None:
            self.now.__exit__(None, None, None)
        self.now = None
        if name:
            self.now = jax.named_scope(name)
            self.now.__enter__()


def kernel(
    n,
    freq_hbm, seg_hbm, pos_hbm, pseg_hbm, gain_q_hbm, gain_kv_hbm,
    hid_hbm, pre_hbm, wdq_hbm, wuq_hbm, wdkv_hbm, wukv_hbm, wo_hbm,
    out_ref,
    freq_ref, seg_ref, pos_ref, pseg_ref, gain_q_ref, gain_kv_ref,
    hid_v, wdq_v, wdkv_v, wuq_v, wukv_v, wo_v,
    lat_t, lat, new_lat, pseg_mate, qlat_all, meta_all, cos_all, sin_all, mask_a, tail_t,
    keys_t, values, queries, probs, tops_all, sums_all,
    scores, stats, stats_rx, acc, scales, split, bias, z, z_rx,
    load_sem, small_sem, dq_sem, wo_sem, ukv_sem, mate_send, mate_recv, gat_send, gat_recv, met_send, met_recv,
    st_send, st_recv, acc_send, acc_recv, red_send, red_recv,
):
    phase = Phases()
    me = lax.axis_index("sp")
    core = lax.rem(me, CORES)
    chip = lax.div(me, CORES)
    chips = n // CORES
    mate = chip * CORES + (CORES - 1 - core)
    toks = hid_v.shape[0]
    pre = pre_hbm.shape[1]
    kv_lat = wukv_v.shape[0]
    heads = keys_t.shape[0]
    old = CORES * pre
    new = CORES * toks
    wide = lat_t.shape[1]
    all_toks = n * toks
    some = heads // PARTS
    deep = some * V_DIM
    half_width = wo_v.shape[1]

    phase("loads")

    def load(src, dst, sem):
        copy = pltpu.make_async_copy(src, dst, sem)
        copy.start()
        return copy

    barrier = pltpu.get_barrier_semaphore()
    for j in range(1, n):
        pl.semaphore_signal(barrier, inc=1, device_id={"sp": lax.rem(me + j, n)}, device_id_type=pl.DeviceIdType.MESH)
    smalls = [
        load(src, dst, small_sem.at[i])
        for i, (src, dst) in enumerate([
            (freq_hbm, freq_ref), (seg_hbm, seg_ref), (pos_hbm, pos_ref),
            (gain_q_hbm, gain_q_ref), (gain_kv_hbm, gain_kv_ref), (pseg_hbm, pseg_ref),
        ])
    ]
    load_hid = load(hid_hbm, hid_v, load_sem.at[0])
    depth = wdq_v.shape[0] // DQ_LOADS
    load_dq = [
        load(wdq_hbm.at[pl.ds(i * depth, depth)], wdq_v.at[pl.ds(i * depth, depth)], dq_sem.at[i])
        for i in range(DQ_LOADS)
    ]
    kv_cols = heads * KV_HEAD
    part = kv_cols // KV_LOADS

    def load_up(i):
        return load(
            wukv_hbm.at[:, pl.ds(pl.multiple_of(core * kv_cols + i * part, LANES), part)],
            wukv_v.at[:, pl.ds(i * part, part)],
            ukv_sem.at[i],
        )

    load_pre = load(pre_hbm, lat_t.at[:, pl.ds(0, pre)], load_sem.at[3])
    load_ukv = [load_up(0)]

    phase("wait_small")
    for copy in smalls:
        copy.wait()
    phase("meta")
    pos_col = row_to_column(pos_ref[...].astype(F32))
    seg_col = row_to_column(seg_ref[...].astype(F32))
    angles = pos_col * freq_ref[...]
    lane = lane_of((toks, LANES))
    cos_t = jnp.cos(angles)
    sin_t = jnp.sin(angles)
    my_rows = pl.ds(pl.multiple_of(me * toks, toks), toks)
    meta_all[my_rows, :] = jnp.where(
        lane < HALF, cos_t, jnp.where(lane < 2 * HALF, sin_t, jnp.where(lane == 2 * HALF, seg_col, pos_col))
    )

    def send(src, dst, send_sem, recv_sem, target):
        copy = pltpu.make_async_remote_copy(
            src_ref=src, dst_ref=dst, send_sem=send_sem, recv_sem=recv_sem,
            device_id={"sp": target}, device_id_type=pl.DeviceIdType.MESH,
        )
        copy.start()
        return copy

    phase("wait_dq")
    load_hid.wait()
    for copy in load_dq:
        copy.wait()
    load_ukv += [load_up(i) for i in range(1, KV_LOADS)]
    load_dkv = load(wdkv_hbm, wdkv_v, load_sem.at[2])
    phase("qlat")
    qlat_all[my_rows, :] = rms_norm(dot(hid_v[...], wdq_v[...]), gain_q_ref[...]).astype(BF16)

    phase("barrier")
    pl.semaphore_wait(barrier, n - 1)
    send_pre = send(pre_hbm, lat_t.at[:, pl.ds(pre, pre)], mate_send.at[0], mate_recv.at[0], mate)
    send_pseg = send(pseg_ref, pseg_mate, mate_send.at[1], mate_recv.at[1], mate)
    send_meta = [
        send(meta_all.at[my_rows], meta_all.at[my_rows], met_send.at[j - 1], met_recv.at[j - 1], lax.rem(me + j, n))
        for j in range(1, n)
    ]
    send_q = [
        send(qlat_all.at[my_rows], qlat_all.at[my_rows], gat_send.at[j - 1], gat_recv.at[j - 1], lax.rem(me + j, n))
        for j in range(1, n)
    ]
    def pair_weights(pair, offset):
        first = pl.multiple_of(pair * (2 * KV_HEAD) + offset, LANES)
        second = pl.multiple_of(pair * (2 * KV_HEAD) + KV_HEAD + offset, LANES)
        return jnp.concatenate([wukv_v[:, pl.ds(first, LANES)], wukv_v[:, pl.ds(second, LANES)]], axis=1)

    def raise_keys(start, size):
        def step(pair):
            up = dot_tn(pair_weights(pair, 0), lat_t[:kv_lat, pl.ds(start, size)]).astype(BF16)
            keys_t[2 * pair, :, pl.ds(start, size)] = up[:NOPE_DIM]
            keys_t[2 * pair + 1, :, pl.ds(start, size)] = up[NOPE_DIM:]
        return step

    def raise_values(start, size):
        def step(pair):
            values[pair, pl.ds(start, size), :] = dot(lat[pl.ds(start, size), :], pair_weights(pair, NOPE_DIM)).astype(BF16)
        return step

    def put_tail(start, size, seg_row):
        hot = seg_row == lax.broadcasted_iota(jnp.int32, (ROPE_DIM, size), 0)
        hot = jnp.where(hot, 1.0, 0.0).astype(BF16)
        rope = lat_t[kv_lat:, pl.ds(start, size)]
        tail_t[0, :, pl.ds(start, size)] = jnp.concatenate([rope, hot], axis=0)
        tail_t[1, :, pl.ds(start, size)] = jnp.concatenate([hot, rope], axis=0)
    per = heads // 2 // KV_LOADS
    for i in range(KV_LOADS):
        phase(f"wait_own{i}")
        load_ukv[i].wait()
        if i == 0:
            load_pre.wait()
        else:
            load_dkv.wait()
        phase(f"own{i}")
        if i:
            load_uq = load(
                wuq_hbm.at[:, pl.ds(pl.multiple_of(core * heads * QK_DIM, LANES), heads * QK_DIM)], wuq_v, load_sem.at[4]
            )
            load_o = [
                load(
                    wo_hbm.at[
                        pl.ds(pl.multiple_of(lax.rem(core + side, CORES) * (heads * V_DIM) + part * deep, LANES), deep),
                        pl.ds(pl.multiple_of(core * half_width, LANES), half_width),
                    ],
                    wo_v.at[pl.ds((part * CORES + side) * deep, deep)],
                    wo_sem.at[part, side],
                )
                for part in range(PARTS) for side in range(CORES)
            ]
            down = dot_nt(hid_v[...], wdkv_v[...])
            c_kv = rms_norm(down[:, :kv_lat], gain_kv_ref[...])
            low, high = down[:, kv_lat:kv_lat + HALF], down[:, kv_lat + HALF:]
            cos_m, sin_m = cos_t[:, :HALF], sin_t[:, :HALF]
            k_new = jnp.concatenate([low * cos_m - high * sin_m, high * cos_m + low * sin_m], axis=1)
            new_lat[pl.ds(0, toks), :] = jnp.concatenate([c_kv, k_new], axis=1).astype(BF16)
        for pair in range(i * per, (i + 1) * per):
            raise_keys(0, pre)(pair)
        if i == 0:
            lat[pl.ds(0, pre), :] = jnp.transpose(lat_t[:kv_lat, pl.ds(0, pre)])
            put_tail(0, pre, pseg_ref[...])
            values[:, pl.ds(old + new, wide - old - new), :] = jnp.zeros((heads // 2, wide - old - new, 2 * V_DIM), BF16)
        for pair in range(i * per, (i + 1) * per):
            raise_values(0, pre)(pair)
    send_new = send(new_lat.at[pl.ds(0, toks)], new_lat.at[pl.ds(toks, toks)], mate_send.at[2], mate_recv.at[2], mate)

    phase("wait_meta")
    for copy in send_meta:
        copy.wait_recv()
    phase("wait_mate")
    send_pre.wait_recv()
    send_pseg.wait_recv()
    phase("keys_mate")
    unrolled(heads // 2, UNROLL_KV, raise_keys(pre, pre))
    lat[pl.ds(pre, pre), :] = jnp.transpose(lat_t[:kv_lat, pl.ds(pre, pre)])
    every = meta_all[...]
    lanes = lane_of((all_toks, LANES))
    q_seg = every[:, 2 * HALF:2 * HALF + 1]
    q_pos = every[:, 2 * HALF + 1:2 * HALF + 2]
    cos_q = jnp.where(lanes < HALF, every, 0.0)
    cos_q = cos_q + turn(cos_q, HALF)
    cos_all[...] = cos_q + turn(cos_q, 2 * HALF)
    sin_q = jnp.where((lanes >= HALF) & (lanes < 2 * HALF), every, 0.0)
    sin_q = sin_q - turn(sin_q, LANES - HALF)
    sin_all[...] = sin_q + turn(sin_q, 2 * HALF)
    q_mask = jnp.where(q_seg == jnp.where(lanes < ROPE_DIM, lanes, lanes - ROPE_DIM).astype(F32), 0.0, NEG_BIG)
    mask_a[...] = q_mask
    mate_rows = pl.ds(pl.multiple_of(mate * toks, toks), toks)
    new_meta = jnp.concatenate(
        [meta_all[my_rows, :], meta_all[mate_rows, :], jnp.zeros((LANES - new, LANES), F32)], axis=0
    )
    meta_rows = jnp.transpose(new_meta)
    k_seg, k_pos = meta_rows[2 * HALF:2 * HALF + 1], meta_rows[2 * HALF + 1:2 * HALF + 2]
    seen = (q_seg == k_seg) & (k_pos <= q_pos) & (lane_of((all_toks, LANES)) < new)
    bias[...] = jnp.where(seen, 0.0, NEG_BIG)

    put_tail(pre, pre, pseg_mate[...])

    phase("wait_uq")
    load_uq.wait()
    for copy in send_q:
        copy.wait_recv()
    send_new.wait_recv()
    phase("queries")
    lat[pl.ds(old, new), :] = new_lat[:, :kv_lat]
    new_rope = jnp.concatenate([new_lat[:, kv_lat:].astype(F32), jnp.zeros((new, LANES - ROPE_DIM), F32)], axis=1)
    new_rope = jnp.concatenate([new_rope, jnp.zeros((LANES - new, LANES), F32)], axis=0)
    new_rope = jnp.transpose(new_rope).astype(BF16)
    tail_t[0, :, pl.ds(old, LANES)] = new_rope
    tail_t[1, :ROPE_DIM, pl.ds(old, LANES)] = new_rope[ROPE_DIM:]
    tail_t[1, ROPE_DIM:, pl.ds(old, LANES)] = new_rope[:ROPE_DIM]
    low_half = lane_of((all_toks, LANES)) < ROPE_DIM
    first_half = lax.rem(lane_of((all_toks, LANES)), ROPE_DIM) < HALF

    def raise_queries(pair):
        cols = pl.ds(pl.multiple_of(pair * (2 * QK_DIM), LANES), 2 * QK_DIM)
        q = dot(qlat_all[...], wuq_v[:, cols])
        nope_a, mid, end = q[:, :LANES], q[:, LANES:2 * LANES], q[:, 2 * LANES:]
        nope_b = turn(jnp.where(low_half, end, mid), ROPE_DIM)
        u = jnp.where(low_half, mid, end)
        swapped = jnp.where(first_half, turn(u, LANES - HALF), turn(u, HALF))
        r = u * cos_all[...] + swapped * sin_all[...]
        queries[2 * pair] = jnp.concatenate([nope_a, jnp.where(low_half, r, mask_a[...])], axis=1).astype(BF16)
        queries[2 * pair + 1] = jnp.concatenate([nope_b, jnp.where(low_half, mask_a[...], r)], axis=1).astype(BF16)

    def raise_new_keys(pair):
        up = dot(new_lat[:, :kv_lat], pair_weights(pair, 0))
        up = jnp.transpose(jnp.concatenate([up, jnp.zeros((LANES - new, 2 * NOPE_DIM), F32)], axis=0)).astype(BF16)
        keys_t[2 * pair, :, pl.ds(old, LANES)] = up[:NOPE_DIM]
        keys_t[2 * pair + 1, :, pl.ds(old, LANES)] = up[NOPE_DIM:]

    def score(head):
        j = head % SCORE_BUFS
        s = dot(queries[head], jnp.concatenate([keys_t[head], tail_t[head % 2]], axis=0))
        scores[j, :, :old] = s[:, :old]
        scores[j, :, old:] = s[:, old:] + bias[...]

    def soften(head):
        j = head % SCORE_BUFS
        step = 16
        tops = [jnp.max(scores[j, r:r + step, :], axis=1, keepdims=True) for r in range(0, all_toks, step)]
        for i, top in enumerate(tops):
            rows = pl.ds(i * step, step)
            p = jnp.exp2((scores[j, rows, :] - top) * EXP_SCALE)
            probs[head, rows, :] = p.astype(BF16)
            tops_all[head, rows, :] = jnp.broadcast_to(top, (step, LANES))
            sums_all[head, rows, :] = jnp.broadcast_to(jnp.sum(p, axis=1, keepdims=True), (step, LANES))

    raise_mate = raise_values(pre, pre + new)

    def peer(j):
        return lax.rem(chip + j, chips)

    send_stats = []
    late = list(range(heads // 2))

    def make_ready(head):
        if head % 2 == 0:
            raise_queries(head // 2)
            raise_new_keys(head // 2)

    for head in range(heads):
        make_ready(head)
    for head in range(AHEAD):
        score(head)
    for head in range(heads):
        if head + AHEAD < heads:
            score(head + AHEAD)
        soften(head)
        for pair in VALUES_AFTER.get(head, ()):
            raise_mate(pair)
            late.remove(pair)
        if (head + 1) % some == 0:
            part = head // some
            packed = jnp.zeros((all_toks, LANES), F32)
            for i in range(some):
                packed = jnp.where(lanes == i, tops_all[part * some + i], packed)
                packed = jnp.where(lanes == some + i, sums_all[part * some + i], packed)
            stats[part] = jnp.transpose(packed)[:2 * some]
            send_stats.append([
                send(
                    stats.at[part], stats_rx.at[part, j - 1], st_send.at[part, j - 1], st_recv.at[part, j - 1],
                    lax.rem(me + j, n),
                )
                for j in range(1, n)
            ])

    red_copies = {}
    both = CORES * toks
    half = len(ORDER[0]) * both

    def put_scale(part):
        for side in range(CORES):
            got = [stats_rx[part, j - 1] for j in range(1 + (1 - side), n, CORES)]
            mine = stats[part] if side == 0 else jnp.where(core == 0, got[-1], got[0])
            every = got + [mine] if side == 0 else got
            top = functools.reduce(jnp.maximum, [g[:some] for g in every])
            total = functools.reduce(jnp.add, [g[some:] * jnp.exp2((g[:some] - top) * EXP_SCALE) for g in every])
            share = jnp.exp2((mine[:some] - top) * EXP_SCALE)
            scales[part, side, :, :some] = jnp.transpose(share / total)

    def put_split(part, g, sides):
        for b, j in enumerate(ORDER[g]):
            from_rows = pl.ds(pl.multiple_of(peer(j) * both, both), both)
            for side in sides:
                factor = scales[part, side, from_rows, :]
                for i in range(some):
                    cols = pl.ds(((part * CORES + side) * some + i) * V_DIM, V_DIM)
                    o = acc[side, part * some + i, from_rows, :] * factor[:, i:i + 1]
                    o_hi = o.astype(BF16)
                    split[g, pl.ds(b * both, both), cols] = o_hi
                    split[g, pl.ds(half + b * both, both), cols] = (o - o_hi.astype(F32)).astype(BF16)

    def project(part, g, side=None):
        first = part * CORES * deep
        ks = pl.ds(first, CORES * deep) if side is None else pl.ds(first + side * deep, deep)
        y = dot(split[g, :, ks], wo_v[ks, :])
        return y[:half] + y[half:]

    def deliver(g):
        for b, j in enumerate(ORDER[g]):
            for r in range(CORES):
                if j or r:
                    to = lax.rem(core + r, CORES)
                    rows = pl.ds(pl.multiple_of(b * both + to * toks, toks), toks)
                    red_copies[j, r] = send(
                        z.at[g, rows], z_rx.at[j, r], red_send.at[j, r], red_recv.at[j, r], peer(j) * CORES + to
                    )

    def swap(i):
        group = pl.ds(i * (heads // SWAPS), heads // SWAPS)
        return send(acc.at[0, group], acc.at[1, group], acc_send.at[i], acc_recv.at[i], mate)

    phase("attend")
    for pair in late:
        raise_mate(pair)
    send_acc = []
    for head in range(heads):
        cols = pl.ds((head % 2) * V_DIM, V_DIM)
        acc[0, head] = dot(probs[head], values[head // 2, :, cols])
        if (head + 1) % (heads // SWAPS) == 0:
            send_acc.append(swap(head * SWAPS // heads))
    phase("wait_stats0")
    for copy in load_o:
        copy.wait()
    for copy in send_stats[0]:
        copy.wait_recv()
    phase("outproj0")
    put_scale(0)
    for g in range(len(ORDER)):
        put_split(0, g, (0,))
        z[g] = project(0, g, 0)
    phase("wait_acc0")
    for copy in send_acc[:SWAPS // PARTS]:
        copy.wait_recv()
    phase("outproj0m")
    for g in range(len(ORDER)):
        put_split(0, g, (1,))
        z[g] = z[g] + project(0, g, 1)
    phase("wait_stats1")
    for copy in send_stats[1]:
        copy.wait_recv()
    phase("wait_acc1")
    for copy in send_acc[SWAPS // PARTS:]:
        copy.wait_recv()
    phase("outproj1")
    put_scale(1)
    for g in range(len(ORDER)):
        put_split(1, g, range(CORES))
    for g in range(len(ORDER)):
        z[g] = z[g] + project(1, g)
        deliver(g)
    for j in (0, 1, 3, 2):
        phase(f"wait_red{j}")
        for r in range(CORES):
            if j or r:
                red_copies[j, r].wait_recv()
    phase("reduce")
    own = pl.ds(pl.multiple_of(both + core * toks, toks), toks)
    for r in range(CORES):
        y = z[1, own, :] if r == 0 else z_rx[0, 1]
        for j in range(1, chips):
            y = y + z_rx[j, r]
        cols = pl.ds(pl.multiple_of(lax.rem(core + r, CORES) * half_width, LANES), half_width)
        out_ref[:, cols] = y.astype(BF16)

    phase("drain")
    for copy in [send_pre, send_pseg, send_new] + send_meta + send_q + sum(send_stats, []) + send_acc + list(red_copies.values()):
        copy.wait_send()
    phase("")


def solution(mesh):
    n = mesh.shape["sp"]
    chips = n // CORES
    tok_spec = P(("dp", "sp"), None)
    vec_spec = P(("dp", "sp"))
    mat_spec = P(None, None)
    gain_spec = P(None)

    def device_step(hidden, seg_ids, positions, prefix_lat, prefix_seg, w_dq, gain_q, w_uq, w_dkv, gain_kv, w_ukv, w_o):
        toks, width = hidden.shape
        pre, lat_dim = prefix_lat.shape
        q_lat = w_dq.shape[1]
        kv_lat = w_ukv.shape[0]
        heads = w_o.shape[0] // V_DIM // CORES
        rows = CORES * (pre + toks)
        wide = CORES * pre + LANES
        all_toks = n * toks
        inv_freq = (ROPE_BASE ** (-np.arange(HALF, dtype=np.float64) / HALF)).astype(np.float32)
        freq = jnp.asarray(np.concatenate([inv_freq] * (LANES // HALF)).reshape(1, LANES))
        vmem = pl.BlockSpec(memory_space=pltpu.VMEM)
        hbm = pl.BlockSpec(memory_space=pltpu.HBM)
        dma = pltpu.SemaphoreType.DMA
        table = pltpu.VMEM((all_toks, LANES), F32)
        return pl.pallas_call(
            functools.partial(kernel, n),
            out_shape=pltpu.VMEM((toks, width), BF16),
            in_specs=[hbm] * 13,
            scratch_shapes=[
                pltpu.VMEM((1, LANES), F32),
                pltpu.VMEM((1, toks), jnp.int32),
                pltpu.VMEM((1, toks), jnp.int32),
                pltpu.VMEM((1, pre), jnp.int32),
                pltpu.VMEM((q_lat,), BF16),
                pltpu.VMEM((kv_lat,), BF16),
                pltpu.VMEM((toks, width), BF16),
                pltpu.VMEM((width, q_lat), BF16),
                pltpu.VMEM((lat_dim, width), BF16),
                pltpu.VMEM((q_lat, heads * QK_DIM), BF16),
                pltpu.VMEM((kv_lat, heads * KV_HEAD), BF16),
                pltpu.VMEM((CORES * heads * V_DIM, width // CORES), BF16),
                pltpu.VMEM((lat_dim, wide), BF16),
                pltpu.VMEM((rows, kv_lat), BF16),
                pltpu.VMEM((CORES * toks, lat_dim), BF16),
                pltpu.VMEM((1, pre), jnp.int32),
                pltpu.VMEM((all_toks, q_lat), BF16),
                table, table, table, table,
                pltpu.VMEM((2, LANES, wide), BF16),
                pltpu.VMEM((heads, NOPE_DIM, wide), BF16),
                pltpu.VMEM((heads // 2, wide, 2 * V_DIM), BF16),
                pltpu.VMEM((heads, all_toks, 2 * LANES), BF16),
                pltpu.VMEM((heads, all_toks, wide), BF16),
                pltpu.VMEM((heads, all_toks, LANES), F32),
                pltpu.VMEM((heads, all_toks, LANES), F32),
                pltpu.VMEM((SCORE_BUFS, all_toks, wide), F32),
                pltpu.VMEM((PARTS, 2 * heads // PARTS, all_toks), F32),
                pltpu.VMEM((PARTS, n - 1, 2 * heads // PARTS, all_toks), F32),
                pltpu.VMEM((CORES, heads, all_toks, V_DIM), F32),
                pltpu.VMEM((PARTS, CORES, all_toks, LANES), F32),
                pltpu.VMEM((2, all_toks, CORES * heads * V_DIM), BF16),
                table,
                pltpu.VMEM((2, all_toks // 2, width // CORES), F32),
                pltpu.VMEM((chips, CORES, toks, width // CORES), F32),
                dma((6,)),
                dma((6,)),
                dma((DQ_LOADS,)),
                dma((PARTS, CORES)),
                dma((KV_LOADS,)),
                dma((3,)), dma((3,)),
                dma((n - 1,)), dma((n - 1,)),
                dma((n - 1,)), dma((n - 1,)),
                dma((PARTS, n - 1)), dma((PARTS, n - 1)),
                dma((SWAPS,)), dma((SWAPS,)),
                dma((chips, CORES)), dma((chips, CORES)),
            ],
            compiler_params=pltpu.CompilerParams(
                collective_id=0, has_side_effects=True, vmem_limit_bytes=60 * 1024 * 1024
            ),
        )(
            freq, seg_ids.reshape(1, toks), positions.reshape(1, toks), prefix_seg.reshape(1, pre),
            gain_q, gain_kv,
            hidden, prefix_lat.T, w_dq, w_uq, w_dkv.T, w_ukv, w_o,
        )

    return jax.shard_map(
        device_step,
        mesh=mesh,
        in_specs=(tok_spec, vec_spec, vec_spec, tok_spec, vec_spec, mat_spec, gain_spec, mat_spec, mat_spec, gain_spec, mat_spec, mat_spec),
        out_specs=tok_spec,
        check_vma=False,
    )
```

```python
import functools
import math

import jax
import jax.numpy as jnp
import numpy as np
from jax import lax
from jax.experimental import pallas as pl
from jax.experimental.pallas import tpu as pltpu
from jax.sharding import PartitionSpec as P

ROPE_DIM = 64
HALF = ROPE_DIM // 2
NOPE_DIM = 128
V_DIM = 128
QK_DIM = NOPE_DIM + ROPE_DIM
KV_HEAD = NOPE_DIM + V_DIM
CORES = 2
EPS = 1e-6
ROPE_BASE = 10000.0
NEG_BIG = -1e30
EXP_SCALE = QK_DIM ** -0.5 * math.log2(math.e)
LANES = 128
ORDER = ((2, 1), (3, 0))
PARTS = 2
SWAPS = 2
VALUES_AFTER = {7: (0, 1, 2, 3), 15: (4, 5)}
AHEAD = 0
KV_LOADS = 2
DQ_LOADS = 4
UNROLL_KV = 8
SCORE_BUFS = 8

F32 = jnp.float32
BF16 = jnp.bfloat16


def dot(a, b):
    return jnp.dot(a, b, preferred_element_type=F32)


def dot_nt(a, b):
    return lax.dot_general(a, b, (((1,), (1,)), ((), ())), preferred_element_type=F32)


def dot_tn(a, b):
    return lax.dot_general(a, b, (((0,), (0,)), ((), ())), preferred_element_type=F32)


def rms_norm(values, gain):
    inv_rms = lax.rsqrt(jnp.mean(values * values, axis=-1, keepdims=True) + EPS)
    return values * inv_rms * gain.astype(F32).reshape(1, gain.shape[0])


def row_to_column(row):
    size = row.shape[1]
    here = lax.broadcasted_iota(jnp.int32, (size, size), 0) == lax.broadcasted_iota(jnp.int32, (size, size), 1)
    return jnp.sum(jnp.where(here, jnp.broadcast_to(row, (size, size)), 0.0), axis=1, keepdims=True)


def lane_of(shape):
    return lax.broadcasted_iota(jnp.int32, shape, len(shape) - 1)


def turn(x, amount):
    return pltpu.roll(x, amount, 1)


def unrolled(count, step, body):
    if count == step:
        for j in range(step):
            body(j)
        return

    def run(i, carry):
        for j in range(step):
            body(i * step + j)
        return carry

    lax.fori_loop(0, count // step, run, 0)


class Phases:
    def __init__(self):
        self.now = None

    def __call__(self, name):
        if self.now is not None:
            self.now.__exit__(None, None, None)
        self.now = None
        if name:
            self.now = jax.named_scope(name)
            self.now.__enter__()


def kernel(
    n,
    freq_hbm, seg_hbm, pos_hbm, pseg_hbm, gain_q_hbm, gain_kv_hbm,
    hid_hbm, pre_hbm, wdq_hbm, wuq_hbm, wdkv_hbm, wukv_hbm, wo_hbm,
    out_ref,
    freq_ref, seg_ref, pos_ref, pseg_ref, gain_q_ref, gain_kv_ref,
    hid_v, wdq_v, wdkv_v, wuq_v, wukv_v, wo_v,
    lat_t, lat, new_lat, pseg_mate, qlat_all, meta_all, cos_all, sin_all, mask_a, tail_t,
    keys_t, values, queries, probs, tops_all, sums_all,
    scores, stats, stats_rx, acc, scales, split, bias, z, z_rx,
    load_sem, small_sem, dq_sem, wo_sem, ukv_sem, mate_send, mate_recv, gat_send, gat_recv, met_send, met_recv,
    st_send, st_recv, acc_send, acc_recv, red_send, red_recv,
):
    phase = Phases()
    me = lax.axis_index("sp")
    core = lax.rem(me, CORES)
    chip = lax.div(me, CORES)
    chips = n // CORES
    mate = chip * CORES + (CORES - 1 - core)
    toks = hid_v.shape[0]
    pre = pre_hbm.shape[1]
    kv_lat = wukv_v.shape[0]
    heads = keys_t.shape[0]
    old = CORES * pre
    new = CORES * toks
    wide = lat_t.shape[1]
    all_toks = n * toks
    some = heads // PARTS
    deep = some * V_DIM
    half_width = wo_v.shape[1]

    phase("loads")

    def load(src, dst, sem):
        copy = pltpu.make_async_copy(src, dst, sem)
        copy.start()
        return copy

    far_first = sorted(range(1, n), key=lambda j: -min(j, n - j))
    barrier = pltpu.get_barrier_semaphore()
    for j in far_first:
        pl.semaphore_signal(barrier, inc=1, device_id={"sp": lax.rem(me + j, n)}, device_id_type=pl.DeviceIdType.MESH)
    smalls = [
        load(src, dst, small_sem.at[i])
        for i, (src, dst) in enumerate([
            (freq_hbm, freq_ref), (seg_hbm, seg_ref), (pos_hbm, pos_ref),
            (gain_q_hbm, gain_q_ref), (gain_kv_hbm, gain_kv_ref), (pseg_hbm, pseg_ref),
        ])
    ]
    load_hid = load(hid_hbm, hid_v, load_sem.at[0])
    depth = wdq_v.shape[0] // DQ_LOADS
    load_dq = [
        load(wdq_hbm.at[pl.ds(i * depth, depth)], wdq_v.at[pl.ds(i * depth, depth)], dq_sem.at[i])
        for i in range(DQ_LOADS)
    ]
    kv_cols = heads * KV_HEAD
    part = kv_cols // KV_LOADS

    def load_up(i):
        return load(
            wukv_hbm.at[:, pl.ds(pl.multiple_of(core * kv_cols + i * part, LANES), part)],
            wukv_v.at[:, pl.ds(i * part, part)],
            ukv_sem.at[i],
        )

    load_pre = load(pre_hbm, lat_t.at[:, pl.ds(0, pre)], load_sem.at[3])
    load_ukv = [load_up(0)]

    phase("wait_small")
    for copy in smalls:
        copy.wait()
    phase("meta")
    pos_col = row_to_column(pos_ref[...].astype(F32))
    seg_col = row_to_column(seg_ref[...].astype(F32))
    angles = pos_col * freq_ref[...]
    lane = lane_of((toks, LANES))
    cos_t = jnp.cos(angles)
    sin_t = jnp.sin(angles)
    my_rows = pl.ds(pl.multiple_of(me * toks, toks), toks)
    meta_all[my_rows, :] = jnp.where(
        lane < HALF, cos_t, jnp.where(lane < 2 * HALF, sin_t, jnp.where(lane == 2 * HALF, seg_col, pos_col))
    )

    def send(src, dst, send_sem, recv_sem, target):
        copy = pltpu.make_async_remote_copy(
            src_ref=src, dst_ref=dst, send_sem=send_sem, recv_sem=recv_sem,
            device_id={"sp": target}, device_id_type=pl.DeviceIdType.MESH,
        )
        copy.start()
        return copy

    phase("wait_dq")
    load_hid.wait()
    for copy in load_dq:
        copy.wait()
    load_ukv += [load_up(i) for i in range(1, KV_LOADS)]
    load_dkv = load(wdkv_hbm, wdkv_v, load_sem.at[2])
    phase("qlat")
    qlat_all[my_rows, :] = rms_norm(dot(hid_v[...], wdq_v[...]), gain_q_ref[...]).astype(BF16)

    phase("barrier")
    pl.semaphore_wait(barrier, n - 1)
    send_pre = send(pre_hbm, lat_t.at[:, pl.ds(pre, pre)], mate_send.at[0], mate_recv.at[0], mate)
    send_pseg = send(pseg_ref, pseg_mate, mate_send.at[1], mate_recv.at[1], mate)
    send_meta = [
        send(meta_all.at[my_rows], meta_all.at[my_rows], met_send.at[j - 1], met_recv.at[j - 1], lax.rem(me + j, n))
        for j in far_first
    ]
    send_q = [
        send(qlat_all.at[my_rows], qlat_all.at[my_rows], gat_send.at[j - 1], gat_recv.at[j - 1], lax.rem(me + j, n))
        for j in far_first
    ]
    def pair_weights(pair, offset):
        first = pl.multiple_of(pair * (2 * KV_HEAD) + offset, LANES)
        second = pl.multiple_of(pair * (2 * KV_HEAD) + KV_HEAD + offset, LANES)
        return jnp.concatenate([wukv_v[:, pl.ds(first, LANES)], wukv_v[:, pl.ds(second, LANES)]], axis=1)

    def raise_keys(start, size):
        def step(pair):
            up = dot_tn(pair_weights(pair, 0), lat_t[:kv_lat, pl.ds(start, size)]).astype(BF16)
            keys_t[2 * pair, :, pl.ds(start, size)] = up[:NOPE_DIM]
            keys_t[2 * pair + 1, :, pl.ds(start, size)] = up[NOPE_DIM:]
        return step

    def raise_values(start, size):
        def step(pair):
            values[pair, pl.ds(start, size), :] = dot(lat[pl.ds(start, size), :], pair_weights(pair, NOPE_DIM)).astype(BF16)
        return step

    def put_tail(start, size, seg_row):
        hot = seg_row == lax.broadcasted_iota(jnp.int32, (ROPE_DIM, size), 0)
        hot = jnp.where(hot, 1.0, 0.0).astype(BF16)
        rope = lat_t[kv_lat:, pl.ds(start, size)]
        tail_t[0, :, pl.ds(start, size)] = jnp.concatenate([rope, hot], axis=0)
        tail_t[1, :, pl.ds(start, size)] = jnp.concatenate([hot, rope], axis=0)
    per = heads // 2 // KV_LOADS
    for i in range(KV_LOADS):
        phase(f"wait_own{i}")
        load_ukv[i].wait()
        if i == 0:
            load_pre.wait()
        else:
            load_dkv.wait()
        phase(f"own{i}")
        if i:
            load_uq = load(
                wuq_hbm.at[:, pl.ds(pl.multiple_of(core * heads * QK_DIM, LANES), heads * QK_DIM)], wuq_v, load_sem.at[4]
            )
            load_o = [
                load(
                    wo_hbm.at[
                        pl.ds(pl.multiple_of(lax.rem(core + side, CORES) * (heads * V_DIM) + part * deep, LANES), deep),
                        pl.ds(pl.multiple_of(core * half_width, LANES), half_width),
                    ],
                    wo_v.at[pl.ds((part * CORES + side) * deep, deep)],
                    wo_sem.at[part, side],
                )
                for part in range(PARTS) for side in range(CORES)
            ]
            down = dot_nt(hid_v[...], wdkv_v[...])
            c_kv = rms_norm(down[:, :kv_lat], gain_kv_ref[...])
            low, high = down[:, kv_lat:kv_lat + HALF], down[:, kv_lat + HALF:]
            cos_m, sin_m = cos_t[:, :HALF], sin_t[:, :HALF]
            k_new = jnp.concatenate([low * cos_m - high * sin_m, high * cos_m + low * sin_m], axis=1)
            new_lat[pl.ds(0, toks), :] = jnp.concatenate([c_kv, k_new], axis=1).astype(BF16)
        for pair in range(i * per, (i + 1) * per):
            raise_keys(0, pre)(pair)
        if i == 0:
            lat[pl.ds(0, pre), :] = jnp.transpose(lat_t[:kv_lat, pl.ds(0, pre)])
            put_tail(0, pre, pseg_ref[...])
            values[:, pl.ds(old + new, wide - old - new), :] = jnp.zeros((heads // 2, wide - old - new, 2 * V_DIM), BF16)
        for pair in range(i * per, (i + 1) * per):
            raise_values(0, pre)(pair)
    send_new = send(new_lat.at[pl.ds(0, toks)], new_lat.at[pl.ds(toks, toks)], mate_send.at[2], mate_recv.at[2], mate)

    phase("wait_meta")
    for copy in send_meta:
        copy.wait_recv()
    phase("wait_mate")
    send_pre.wait_recv()
    send_pseg.wait_recv()
    phase("keys_mate")
    unrolled(heads // 2, UNROLL_KV, raise_keys(pre, pre))
    lat[pl.ds(pre, pre), :] = jnp.transpose(lat_t[:kv_lat, pl.ds(pre, pre)])
    every = meta_all[...]
    lanes = lane_of((all_toks, LANES))
    q_seg = every[:, 2 * HALF:2 * HALF + 1]
    q_pos = every[:, 2 * HALF + 1:2 * HALF + 2]
    cos_q = jnp.where(lanes < HALF, every, 0.0)
    cos_q = cos_q + turn(cos_q, HALF)
    cos_all[...] = cos_q + turn(cos_q, 2 * HALF)
    sin_q = jnp.where((lanes >= HALF) & (lanes < 2 * HALF), every, 0.0)
    sin_q = sin_q - turn(sin_q, LANES - HALF)
    sin_all[...] = sin_q + turn(sin_q, 2 * HALF)
    q_mask = jnp.where(q_seg == jnp.where(lanes < ROPE_DIM, lanes, lanes - ROPE_DIM).astype(F32), 0.0, NEG_BIG)
    mask_a[...] = q_mask
    mate_rows = pl.ds(pl.multiple_of(mate * toks, toks), toks)
    new_meta = jnp.concatenate(
        [meta_all[my_rows, :], meta_all[mate_rows, :], jnp.zeros((LANES - new, LANES), F32)], axis=0
    )
    meta_rows = jnp.transpose(new_meta)
    k_seg, k_pos = meta_rows[2 * HALF:2 * HALF + 1], meta_rows[2 * HALF + 1:2 * HALF + 2]
    seen = (q_seg == k_seg) & (k_pos <= q_pos) & (lane_of((all_toks, LANES)) < new)
    bias[...] = jnp.where(seen, 0.0, NEG_BIG)

    put_tail(pre, pre, pseg_mate[...])

    phase("wait_uq")
    load_uq.wait()
    for copy in send_q:
        copy.wait_recv()
    send_new.wait_recv()
    phase("queries")
    lat[pl.ds(old, new), :] = new_lat[:, :kv_lat]
    new_rope = jnp.concatenate([new_lat[:, kv_lat:].astype(F32), jnp.zeros((new, LANES - ROPE_DIM), F32)], axis=1)
    new_rope = jnp.concatenate([new_rope, jnp.zeros((LANES - new, LANES), F32)], axis=0)
    new_rope = jnp.transpose(new_rope).astype(BF16)
    tail_t[0, :, pl.ds(old, LANES)] = new_rope
    tail_t[1, :ROPE_DIM, pl.ds(old, LANES)] = new_rope[ROPE_DIM:]
    tail_t[1, ROPE_DIM:, pl.ds(old, LANES)] = new_rope[:ROPE_DIM]
    low_half = lane_of((all_toks, LANES)) < ROPE_DIM
    first_half = lax.rem(lane_of((all_toks, LANES)), ROPE_DIM) < HALF

    def raise_queries(pair):
        cols = pl.ds(pl.multiple_of(pair * (2 * QK_DIM), LANES), 2 * QK_DIM)
        q = dot(qlat_all[...], wuq_v[:, cols])
        nope_a, mid, end = q[:, :LANES], q[:, LANES:2 * LANES], q[:, 2 * LANES:]
        nope_b = turn(jnp.where(low_half, end, mid), ROPE_DIM)
        u = jnp.where(low_half, mid, end)
        swapped = jnp.where(first_half, turn(u, LANES - HALF), turn(u, HALF))
        r = u * cos_all[...] + swapped * sin_all[...]
        queries[2 * pair] = jnp.concatenate([nope_a, jnp.where(low_half, r, mask_a[...])], axis=1).astype(BF16)
        queries[2 * pair + 1] = jnp.concatenate([nope_b, jnp.where(low_half, mask_a[...], r)], axis=1).astype(BF16)

    def raise_new_keys(pair):
        up = dot(new_lat[:, :kv_lat], pair_weights(pair, 0))
        up = jnp.transpose(jnp.concatenate([up, jnp.zeros((LANES - new, 2 * NOPE_DIM), F32)], axis=0)).astype(BF16)
        keys_t[2 * pair, :, pl.ds(old, LANES)] = up[:NOPE_DIM]
        keys_t[2 * pair + 1, :, pl.ds(old, LANES)] = up[NOPE_DIM:]

    def score(head):
        j = head % SCORE_BUFS
        s = dot(queries[head], jnp.concatenate([keys_t[head], tail_t[head % 2]], axis=0))
        scores[j, :, :old] = s[:, :old]
        scores[j, :, old:] = s[:, old:] + bias[...]

    def soften(head):
        j = head % SCORE_BUFS
        step = 16
        tops = [jnp.max(scores[j, r:r + step, :], axis=1, keepdims=True) for r in range(0, all_toks, step)]
        for i, top in enumerate(tops):
            rows = pl.ds(i * step, step)
            p = jnp.exp2((scores[j, rows, :] - top) * EXP_SCALE)
            probs[head, rows, :] = p.astype(BF16)
            tops_all[head, rows, :] = jnp.broadcast_to(top, (step, LANES))
            sums_all[head, rows, :] = jnp.broadcast_to(jnp.sum(p, axis=1, keepdims=True), (step, LANES))

    raise_mate = raise_values(pre, pre + new)

    def peer(j):
        return lax.rem(chip + j, chips)

    send_stats = []
    late = list(range(heads // 2))

    def make_ready(head):
        if head % 2 == 0:
            raise_queries(head // 2)
            raise_new_keys(head // 2)

    for head in range(heads):
        make_ready(head)
    for head in range(AHEAD):
        score(head)
    for head in range(heads):
        if head + AHEAD < heads:
            score(head + AHEAD)
        soften(head)
        for pair in VALUES_AFTER.get(head, ()):
            raise_mate(pair)
            late.remove(pair)
        if (head + 1) % some == 0:
            part = head // some
            packed = jnp.zeros((all_toks, LANES), F32)
            for i in range(some):
                packed = jnp.where(lanes == i, tops_all[part * some + i], packed)
                packed = jnp.where(lanes == some + i, sums_all[part * some + i], packed)
            stats[part] = jnp.transpose(packed)[:2 * some]
            send_stats.append([
                send(
                    stats.at[part], stats_rx.at[part, j - 1], st_send.at[part, j - 1], st_recv.at[part, j - 1],
                    lax.rem(me + j, n),
                )
                for j in far_first
            ])

    red_copies = {}
    both = CORES * toks
    half = len(ORDER[0]) * both

    def put_scale(part):
        for side in range(CORES):
            got = [stats_rx[part, j - 1] for j in range(1 + (1 - side), n, CORES)]
            mine = stats[part] if side == 0 else jnp.where(core == 0, got[-1], got[0])
            every = got + [mine] if side == 0 else got
            top = functools.reduce(jnp.maximum, [g[:some] for g in every])
            total = functools.reduce(jnp.add, [g[some:] * jnp.exp2((g[:some] - top) * EXP_SCALE) for g in every])
            share = jnp.exp2((mine[:some] - top) * EXP_SCALE)
            scales[part, side, :, :some] = jnp.transpose(share / total)

    def put_split(part, g, sides):
        for b, j in enumerate(ORDER[g]):
            from_rows = pl.ds(pl.multiple_of(peer(j) * both, both), both)
            for side in sides:
                factor = scales[part, side, from_rows, :]
                for i in range(some):
                    cols = pl.ds(((part * CORES + side) * some + i) * V_DIM, V_DIM)
                    o = acc[side, part * some + i, from_rows, :] * factor[:, i:i + 1]
                    o_hi = o.astype(BF16)
                    split[g, pl.ds(b * both, both), cols] = o_hi
                    split[g, pl.ds(half + b * both, both), cols] = (o - o_hi.astype(F32)).astype(BF16)

    def project(part, g, side=None):
        first = part * CORES * deep
        ks = pl.ds(first, CORES * deep) if side is None else pl.ds(first + side * deep, deep)
        y = dot(split[g, :, ks], wo_v[ks, :])
        return y[:half] + y[half:]

    def deliver(g):
        for b, j in enumerate(ORDER[g]):
            for r in range(CORES):
                if j or r:
                    to = lax.rem(core + r, CORES)
                    rows = pl.ds(pl.multiple_of(b * both + to * toks, toks), toks)
                    red_copies[j, r] = send(
                        z.at[g, rows], z_rx.at[j, r], red_send.at[j, r], red_recv.at[j, r], peer(j) * CORES + to
                    )

    def swap(i):
        group = pl.ds(i * (heads // SWAPS), heads // SWAPS)
        return send(acc.at[0, group], acc.at[1, group], acc_send.at[i], acc_recv.at[i], mate)

    phase("attend")
    for pair in late:
        raise_mate(pair)
    send_acc = []
    for head in range(heads):
        cols = pl.ds((head % 2) * V_DIM, V_DIM)
        acc[0, head] = dot(probs[head], values[head // 2, :, cols])
        if (head + 1) % (heads // SWAPS) == 0:
            send_acc.append(swap(head * SWAPS // heads))
    phase("wait_stats0")
    for copy in load_o:
        copy.wait()
    for copy in send_stats[0]:
        copy.wait_recv()
    phase("outproj0")
    put_scale(0)
    for g in range(len(ORDER)):
        put_split(0, g, (0,))
        z[g] = project(0, g, 0)
    phase("wait_acc0")
    for copy in send_acc[:SWAPS // PARTS]:
        copy.wait_recv()
    phase("outproj0m")
    for g in range(len(ORDER)):
        put_split(0, g, (1,))
        z[g] = z[g] + project(0, g, 1)
    phase("wait_stats1")
    for copy in send_stats[1]:
        copy.wait_recv()
    phase("wait_acc1")
    for copy in send_acc[SWAPS // PARTS:]:
        copy.wait_recv()
    phase("outproj1")
    put_scale(1)
    for g in range(len(ORDER)):
        put_split(1, g, range(CORES))
    for g in range(len(ORDER)):
        z[g] = z[g] + project(1, g)
        deliver(g)
    for j in (0, 1, 3, 2):
        phase(f"wait_red{j}")
        for r in range(CORES):
            if j or r:
                red_copies[j, r].wait_recv()
    phase("reduce")
    own = pl.ds(pl.multiple_of(both + core * toks, toks), toks)
    for r in range(CORES):
        y = z[1, own, :] if r == 0 else z_rx[0, 1]
        for j in range(1, chips):
            y = y + z_rx[j, r]
        cols = pl.ds(pl.multiple_of(lax.rem(core + r, CORES) * half_width, LANES), half_width)
        out_ref[:, cols] = y.astype(BF16)

    phase("drain")
    for copy in [send_pre, send_pseg, send_new] + send_meta + send_q + sum(send_stats, []) + send_acc + list(red_copies.values()):
        copy.wait_send()
    phase("")


def solution(mesh):
    n = mesh.shape["sp"]
    chips = n // CORES
    tok_spec = P(("dp", "sp"), None)
    vec_spec = P(("dp", "sp"))
    mat_spec = P(None, None)
    gain_spec = P(None)

    def device_step(hidden, seg_ids, positions, prefix_lat, prefix_seg, w_dq, gain_q, w_uq, w_dkv, gain_kv, w_ukv, w_o):
        toks, width = hidden.shape
        pre, lat_dim = prefix_lat.shape
        q_lat = w_dq.shape[1]
        kv_lat = w_ukv.shape[0]
        heads = w_o.shape[0] // V_DIM // CORES
        rows = CORES * (pre + toks)
        wide = CORES * pre + LANES
        all_toks = n * toks
        inv_freq = (ROPE_BASE ** (-np.arange(HALF, dtype=np.float64) / HALF)).astype(np.float32)
        freq = jnp.asarray(np.concatenate([inv_freq] * (LANES // HALF)).reshape(1, LANES))
        vmem = pl.BlockSpec(memory_space=pltpu.VMEM)
        hbm = pl.BlockSpec(memory_space=pltpu.HBM)
        dma = pltpu.SemaphoreType.DMA
        table = pltpu.VMEM((all_toks, LANES), F32)
        return pl.pallas_call(
            functools.partial(kernel, n),
            out_shape=pltpu.VMEM((toks, width), BF16),
            in_specs=[hbm] * 13,
            scratch_shapes=[
                pltpu.VMEM((1, LANES), F32),
                pltpu.VMEM((1, toks), jnp.int32),
                pltpu.VMEM((1, toks), jnp.int32),
                pltpu.VMEM((1, pre), jnp.int32),
                pltpu.VMEM((q_lat,), BF16),
                pltpu.VMEM((kv_lat,), BF16),
                pltpu.VMEM((toks, width), BF16),
                pltpu.VMEM((width, q_lat), BF16),
                pltpu.VMEM((lat_dim, width), BF16),
                pltpu.VMEM((q_lat, heads * QK_DIM), BF16),
                pltpu.VMEM((kv_lat, heads * KV_HEAD), BF16),
                pltpu.VMEM((CORES * heads * V_DIM, width // CORES), BF16),
                pltpu.VMEM((lat_dim, wide), BF16),
                pltpu.VMEM((rows, kv_lat), BF16),
                pltpu.VMEM((CORES * toks, lat_dim), BF16),
                pltpu.VMEM((1, pre), jnp.int32),
                pltpu.VMEM((all_toks, q_lat), BF16),
                table, table, table, table,
                pltpu.VMEM((2, LANES, wide), BF16),
                pltpu.VMEM((heads, NOPE_DIM, wide), BF16),
                pltpu.VMEM((heads // 2, wide, 2 * V_DIM), BF16),
                pltpu.VMEM((heads, all_toks, 2 * LANES), BF16),
                pltpu.VMEM((heads, all_toks, wide), BF16),
                pltpu.VMEM((heads, all_toks, LANES), F32),
                pltpu.VMEM((heads, all_toks, LANES), F32),
                pltpu.VMEM((SCORE_BUFS, all_toks, wide), F32),
                pltpu.VMEM((PARTS, 2 * heads // PARTS, all_toks), F32),
                pltpu.VMEM((PARTS, n - 1, 2 * heads // PARTS, all_toks), F32),
                pltpu.VMEM((CORES, heads, all_toks, V_DIM), F32),
                pltpu.VMEM((PARTS, CORES, all_toks, LANES), F32),
                pltpu.VMEM((2, all_toks, CORES * heads * V_DIM), BF16),
                table,
                pltpu.VMEM((2, all_toks // 2, width // CORES), F32),
                pltpu.VMEM((chips, CORES, toks, width // CORES), F32),
                dma((6,)),
                dma((6,)),
                dma((DQ_LOADS,)),
                dma((PARTS, CORES)),
                dma((KV_LOADS,)),
                dma((3,)), dma((3,)),
                dma((n - 1,)), dma((n - 1,)),
                dma((n - 1,)), dma((n - 1,)),
                dma((PARTS, n - 1)), dma((PARTS, n - 1)),
                dma((SWAPS,)), dma((SWAPS,)),
                dma((chips, CORES)), dma((chips, CORES)),
            ],
            compiler_params=pltpu.CompilerParams(
                collective_id=0, has_side_effects=True, vmem_limit_bytes=60 * 1024 * 1024
            ),
        )(
            freq, seg_ids.reshape(1, toks), positions.reshape(1, toks), prefix_seg.reshape(1, pre),
            gain_q, gain_kv,
            hidden, prefix_lat.T, w_dq, w_uq, w_dkv.T, w_ukv, w_o,
        )

    return jax.shard_map(
        device_step,
        mesh=mesh,
        in_specs=(tok_spec, vec_spec, vec_spec, tok_spec, vec_spec, mat_spec, gain_spec, mat_spec, mat_spec, gain_spec, mat_spec, mat_spec),
        out_specs=tok_spec,
        check_vma=False,
    )
```

```python
import functools
import math

import jax
import jax.numpy as jnp
import numpy as np
from jax import lax
from jax.experimental import pallas as pl
from jax.experimental.pallas import tpu as pltpu
from jax.sharding import PartitionSpec as P

ROPE_DIM = 64
HALF = ROPE_DIM // 2
NOPE_DIM = 128
V_DIM = 128
QK_DIM = NOPE_DIM + ROPE_DIM
KV_HEAD = NOPE_DIM + V_DIM
CORES = 2
EPS = 1e-6
ROPE_BASE = 10000.0
NEG_BIG = -1e30
EXP_SCALE = QK_DIM ** -0.5 * math.log2(math.e)
LANES = 128
ORDER = ((2, 1), (3, 0))
PARTS = 2
SWAPS = 2
VALUES_AFTER = {7: (0, 1, 2, 3), 15: (4, 5)}
AHEAD = 0
KV_LOADS = 2
DQ_LOADS = 4
UNROLL_KV = 8
SCORE_BUFS = 8

F32 = jnp.float32
BF16 = jnp.bfloat16


def dot(a, b):
    return jnp.dot(a, b, preferred_element_type=F32)


def dot_nt(a, b):
    return lax.dot_general(a, b, (((1,), (1,)), ((), ())), preferred_element_type=F32)


def dot_tn(a, b):
    return lax.dot_general(a, b, (((0,), (0,)), ((), ())), preferred_element_type=F32)


def rms_norm(values, gain):
    inv_rms = lax.rsqrt(jnp.mean(values * values, axis=-1, keepdims=True) + EPS)
    return values * inv_rms * gain.astype(F32).reshape(1, gain.shape[0])


def row_to_column(row):
    size = row.shape[1]
    here = lax.broadcasted_iota(jnp.int32, (size, size), 0) == lax.broadcasted_iota(jnp.int32, (size, size), 1)
    return jnp.sum(jnp.where(here, jnp.broadcast_to(row, (size, size)), 0.0), axis=1, keepdims=True)


def lane_of(shape):
    return lax.broadcasted_iota(jnp.int32, shape, len(shape) - 1)


def turn(x, amount):
    return pltpu.roll(x, amount, 1)


def unrolled(count, step, body):
    if count == step:
        for j in range(step):
            body(j)
        return

    def run(i, carry):
        for j in range(step):
            body(i * step + j)
        return carry

    lax.fori_loop(0, count // step, run, 0)


class Phases:
    def __init__(self):
        self.now = None

    def __call__(self, name):
        if self.now is not None:
            self.now.__exit__(None, None, None)
        self.now = None
        if name:
            self.now = jax.named_scope(name)
            self.now.__enter__()


def kernel(
    n,
    freq_hbm, seg_hbm, pos_hbm, pseg_hbm, gain_q_hbm, gain_kv_hbm,
    hid_hbm, pre_hbm, wdq_hbm, wuq_hbm, wdkv_hbm, wukv_hbm, wo_hbm,
    out_ref,
    freq_ref, seg_ref, pos_ref, pseg_ref, gain_q_ref, gain_kv_ref,
    hid_v, wdq_v, wdkv_v, wuq_v, wukv_v, wo_v,
    lat_t, lat, new_lat, pseg_mate, qlat_all, meta_all, cos_all, sin_all, mask_a, tail_t,
    keys_t, values, queries, probs, tops_all, sums_all,
    scores, stats, stats_rx, acc, scales, split, bias, z, z_rx,
    load_sem, small_sem, dq_sem, wo_sem, ukv_sem, mate_send, mate_recv, gat_send, gat_recv, met_send, met_recv,
    st_send, st_recv, acc_send, acc_recv, red_send, red_recv,
):
    phase = Phases()
    me = lax.axis_index("sp")
    core = lax.rem(me, CORES)
    chip = lax.div(me, CORES)
    chips = n // CORES
    mate = chip * CORES + (CORES - 1 - core)
    toks = hid_v.shape[0]
    pre = pre_hbm.shape[1]
    kv_lat = wukv_v.shape[0]
    heads = keys_t.shape[0]
    old = CORES * pre
    new = CORES * toks
    wide = lat_t.shape[1]
    all_toks = n * toks
    some = heads // PARTS
    deep = some * V_DIM
    half_width = wo_v.shape[1]

    phase("loads")

    def load(src, dst, sem):
        copy = pltpu.make_async_copy(src, dst, sem)
        copy.start()
        return copy

    barrier = pltpu.get_barrier_semaphore()
    for j in range(1, n):
        pl.semaphore_signal(barrier, inc=1, device_id={"sp": lax.rem(me + j, n)}, device_id_type=pl.DeviceIdType.MESH)
    kv_cols = heads * KV_HEAD
    part = kv_cols // KV_LOADS

    def load_up(i):
        return load(
            wukv_hbm.at[:, pl.ds(pl.multiple_of(core * kv_cols + i * part, LANES), part)],
            wukv_v.at[:, pl.ds(i * part, part)],
            ukv_sem.at[i],
        )

    load_pre = load(pre_hbm, lat_t.at[:, pl.ds(0, pre)], load_sem.at[3])
    load_ukv = [load_up(0)]
    smalls = [
        load(src, dst, small_sem.at[i])
        for i, (src, dst) in enumerate([
            (freq_hbm, freq_ref), (seg_hbm, seg_ref), (pos_hbm, pos_ref),
            (gain_q_hbm, gain_q_ref), (gain_kv_hbm, gain_kv_ref), (pseg_hbm, pseg_ref),
        ])
    ]
    load_hid = load(hid_hbm, hid_v, load_sem.at[0])
    depth = wdq_v.shape[0] // DQ_LOADS
    load_dq = [
        load(wdq_hbm.at[pl.ds(i * depth, depth)], wdq_v.at[pl.ds(i * depth, depth)], dq_sem.at[i])
        for i in range(DQ_LOADS)
    ]
    phase("wait_small")
    for copy in smalls:
        copy.wait()
    phase("meta")
    pos_col = row_to_column(pos_ref[...].astype(F32))
    seg_col = row_to_column(seg_ref[...].astype(F32))
    angles = pos_col * freq_ref[...]
    lane = lane_of((toks, LANES))
    cos_t = jnp.cos(angles)
    sin_t = jnp.sin(angles)
    my_rows = pl.ds(pl.multiple_of(me * toks, toks), toks)
    meta_all[my_rows, :] = jnp.where(
        lane < HALF, cos_t, jnp.where(lane < 2 * HALF, sin_t, jnp.where(lane == 2 * HALF, seg_col, pos_col))
    )

    def send(src, dst, send_sem, recv_sem, target):
        copy = pltpu.make_async_remote_copy(
            src_ref=src, dst_ref=dst, send_sem=send_sem, recv_sem=recv_sem,
            device_id={"sp": target}, device_id_type=pl.DeviceIdType.MESH,
        )
        copy.start()
        return copy

    phase("wait_dq")
    load_hid.wait()
    for copy in load_dq:
        copy.wait()
    load_ukv += [load_up(i) for i in range(1, KV_LOADS)]
    load_dkv = load(wdkv_hbm, wdkv_v, load_sem.at[2])
    phase("barrier")
    pl.semaphore_wait(barrier, n - 1)
    send_pre = send(pre_hbm, lat_t.at[:, pl.ds(pre, pre)], mate_send.at[0], mate_recv.at[0], mate)
    send_pseg = send(pseg_ref, pseg_mate, mate_send.at[1], mate_recv.at[1], mate)
    send_meta = [
        send(meta_all.at[my_rows], meta_all.at[my_rows], met_send.at[j - 1], met_recv.at[j - 1], lax.rem(me + j, n))
        for j in range(1, n)
    ]
    phase("qlat")
    qlat_all[my_rows, :] = rms_norm(dot(hid_v[...], wdq_v[...]), gain_q_ref[...]).astype(BF16)

    send_q = [
        send(qlat_all.at[my_rows], qlat_all.at[my_rows], gat_send.at[j - 1], gat_recv.at[j - 1], lax.rem(me + j, n))
        for j in range(1, n)
    ]
    def pair_weights(pair, offset):
        first = pl.multiple_of(pair * (2 * KV_HEAD) + offset, LANES)
        second = pl.multiple_of(pair * (2 * KV_HEAD) + KV_HEAD + offset, LANES)
        return jnp.concatenate([wukv_v[:, pl.ds(first, LANES)], wukv_v[:, pl.ds(second, LANES)]], axis=1)

    def raise_keys(start, size):
        def step(pair):
            up = dot_tn(pair_weights(pair, 0), lat_t[:kv_lat, pl.ds(start, size)]).astype(BF16)
            keys_t[2 * pair, :, pl.ds(start, size)] = up[:NOPE_DIM]
            keys_t[2 * pair + 1, :, pl.ds(start, size)] = up[NOPE_DIM:]
        return step

    def raise_values(start, size):
        def step(pair):
            values[pair, pl.ds(start, size), :] = dot(lat[pl.ds(start, size), :], pair_weights(pair, NOPE_DIM)).astype(BF16)
        return step

    def put_tail(start, size, seg_row):
        hot = seg_row == lax.broadcasted_iota(jnp.int32, (ROPE_DIM, size), 0)
        hot = jnp.where(hot, 1.0, 0.0).astype(BF16)
        rope = lat_t[kv_lat:, pl.ds(start, size)]
        tail_t[0, :, pl.ds(start, size)] = jnp.concatenate([rope, hot], axis=0)
        tail_t[1, :, pl.ds(start, size)] = jnp.concatenate([hot, rope], axis=0)
    per = heads // 2 // KV_LOADS
    for i in range(KV_LOADS):
        phase(f"wait_own{i}")
        load_ukv[i].wait()
        if i == 0:
            load_pre.wait()
        else:
            load_dkv.wait()
        phase(f"own{i}")
        if i:
            load_uq = load(
                wuq_hbm.at[:, pl.ds(pl.multiple_of(core * heads * QK_DIM, LANES), heads * QK_DIM)], wuq_v, load_sem.at[4]
            )
            load_o = [
                load(
                    wo_hbm.at[
                        pl.ds(pl.multiple_of(lax.rem(core + side, CORES) * (heads * V_DIM) + part * deep, LANES), deep),
                        pl.ds(pl.multiple_of(core * half_width, LANES), half_width),
                    ],
                    wo_v.at[pl.ds((part * CORES + side) * deep, deep)],
                    wo_sem.at[part, side],
                )
                for part in range(PARTS) for side in range(CORES)
            ]
            down = dot_nt(hid_v[...], wdkv_v[...])
            c_kv = rms_norm(down[:, :kv_lat], gain_kv_ref[...])
            low, high = down[:, kv_lat:kv_lat + HALF], down[:, kv_lat + HALF:]
            cos_m, sin_m = cos_t[:, :HALF], sin_t[:, :HALF]
            k_new = jnp.concatenate([low * cos_m - high * sin_m, high * cos_m + low * sin_m], axis=1)
            new_lat[pl.ds(0, toks), :] = jnp.concatenate([c_kv, k_new], axis=1).astype(BF16)
        for pair in range(i * per, (i + 1) * per):
            raise_keys(0, pre)(pair)
        if i == 0:
            lat[pl.ds(0, pre), :] = jnp.transpose(lat_t[:kv_lat, pl.ds(0, pre)])
            put_tail(0, pre, pseg_ref[...])
            values[:, pl.ds(old + new, wide - old - new), :] = jnp.zeros((heads // 2, wide - old - new, 2 * V_DIM), BF16)
        for pair in range(i * per, (i + 1) * per):
            raise_values(0, pre)(pair)
    send_new = send(new_lat.at[pl.ds(0, toks)], new_lat.at[pl.ds(toks, toks)], mate_send.at[2], mate_recv.at[2], mate)

    phase("wait_meta")
    for copy in send_meta:
        copy.wait_recv()
    phase("wait_mate")
    send_pre.wait_recv()
    send_pseg.wait_recv()
    phase("keys_mate")
    unrolled(heads // 2, UNROLL_KV, raise_keys(pre, pre))
    lat[pl.ds(pre, pre), :] = jnp.transpose(lat_t[:kv_lat, pl.ds(pre, pre)])
    every = meta_all[...]
    lanes = lane_of((all_toks, LANES))
    q_seg = every[:, 2 * HALF:2 * HALF + 1]
    q_pos = every[:, 2 * HALF + 1:2 * HALF + 2]
    cos_q = jnp.where(lanes < HALF, every, 0.0)
    cos_q = cos_q + turn(cos_q, HALF)
    cos_all[...] = cos_q + turn(cos_q, 2 * HALF)
    sin_q = jnp.where((lanes >= HALF) & (lanes < 2 * HALF), every, 0.0)
    sin_q = sin_q - turn(sin_q, LANES - HALF)
    sin_all[...] = sin_q + turn(sin_q, 2 * HALF)
    q_mask = jnp.where(q_seg == jnp.where(lanes < ROPE_DIM, lanes, lanes - ROPE_DIM).astype(F32), 0.0, NEG_BIG)
    mask_a[...] = q_mask
    mate_rows = pl.ds(pl.multiple_of(mate * toks, toks), toks)
    new_meta = jnp.concatenate(
        [meta_all[my_rows, :], meta_all[mate_rows, :], jnp.zeros((LANES - new, LANES), F32)], axis=0
    )
    meta_rows = jnp.transpose(new_meta)
    k_seg, k_pos = meta_rows[2 * HALF:2 * HALF + 1], meta_rows[2 * HALF + 1:2 * HALF + 2]
    seen = (q_seg == k_seg) & (k_pos <= q_pos) & (lane_of((all_toks, LANES)) < new)
    bias[...] = jnp.where(seen, 0.0, NEG_BIG)

    put_tail(pre, pre, pseg_mate[...])

    phase("wait_uq")
    load_uq.wait()
    for copy in send_q:
        copy.wait_recv()
    send_new.wait_recv()
    phase("queries")
    lat[pl.ds(old, new), :] = new_lat[:, :kv_lat]
    new_rope = jnp.concatenate([new_lat[:, kv_lat:].astype(F32), jnp.zeros((new, LANES - ROPE_DIM), F32)], axis=1)
    new_rope = jnp.concatenate([new_rope, jnp.zeros((LANES - new, LANES), F32)], axis=0)
    new_rope = jnp.transpose(new_rope).astype(BF16)
    tail_t[0, :, pl.ds(old, LANES)] = new_rope
    tail_t[1, :ROPE_DIM, pl.ds(old, LANES)] = new_rope[ROPE_DIM:]
    tail_t[1, ROPE_DIM:, pl.ds(old, LANES)] = new_rope[:ROPE_DIM]
    low_half = lane_of((all_toks, LANES)) < ROPE_DIM
    first_half = lax.rem(lane_of((all_toks, LANES)), ROPE_DIM) < HALF

    def raise_queries(pair):
        cols = pl.ds(pl.multiple_of(pair * (2 * QK_DIM), LANES), 2 * QK_DIM)
        q = dot(qlat_all[...], wuq_v[:, cols])
        nope_a, mid, end = q[:, :LANES], q[:, LANES:2 * LANES], q[:, 2 * LANES:]
        nope_b = turn(jnp.where(low_half, end, mid), ROPE_DIM)
        u = jnp.where(low_half, mid, end)
        swapped = jnp.where(first_half, turn(u, LANES - HALF), turn(u, HALF))
        r = u * cos_all[...] + swapped * sin_all[...]
        queries[2 * pair] = jnp.concatenate([nope_a, jnp.where(low_half, r, mask_a[...])], axis=1).astype(BF16)
        queries[2 * pair + 1] = jnp.concatenate([nope_b, jnp.where(low_half, mask_a[...], r)], axis=1).astype(BF16)

    def raise_new_keys(pair):
        up = dot(new_lat[:, :kv_lat], pair_weights(pair, 0))
        up = jnp.transpose(jnp.concatenate([up, jnp.zeros((LANES - new, 2 * NOPE_DIM), F32)], axis=0)).astype(BF16)
        keys_t[2 * pair, :, pl.ds(old, LANES)] = up[:NOPE_DIM]
        keys_t[2 * pair + 1, :, pl.ds(old, LANES)] = up[NOPE_DIM:]

    def score(head):
        j = head % SCORE_BUFS
        s = dot(queries[head], jnp.concatenate([keys_t[head], tail_t[head % 2]], axis=0))
        scores[j, :, :old] = s[:, :old]
        scores[j, :, old:] = s[:, old:] + bias[...]

    def soften(head):
        j = head % SCORE_BUFS
        step = 16
        tops = [jnp.max(scores[j, r:r + step, :], axis=1, keepdims=True) for r in range(0, all_toks, step)]
        for i, top in enumerate(tops):
            rows = pl.ds(i * step, step)
            p = jnp.exp2((scores[j, rows, :] - top) * EXP_SCALE)
            probs[head, rows, :] = p.astype(BF16)
            tops_all[head, rows, :] = jnp.broadcast_to(top, (step, LANES))
            sums_all[head, rows, :] = jnp.broadcast_to(jnp.sum(p, axis=1, keepdims=True), (step, LANES))

    raise_mate = raise_values(pre, pre + new)

    def peer(j):
        return lax.rem(chip + j, chips)

    send_stats = []
    late = list(range(heads // 2))

    def make_ready(head):
        if head % 2 == 0:
            raise_queries(head // 2)
            raise_new_keys(head // 2)

    for head in range(heads):
        make_ready(head)
    for head in range(AHEAD):
        score(head)
    for head in range(heads):
        if head + AHEAD < heads:
            score(head + AHEAD)
        soften(head)
        for pair in VALUES_AFTER.get(head, ()):
            raise_mate(pair)
            late.remove(pair)
        if (head + 1) % some == 0:
            part = head // some
            packed = jnp.zeros((all_toks, LANES), F32)
            for i in range(some):
                packed = jnp.where(lanes == i, tops_all[part * some + i], packed)
                packed = jnp.where(lanes == some + i, sums_all[part * some + i], packed)
            stats[part] = jnp.transpose(packed)[:2 * some]
            send_stats.append([
                send(
                    stats.at[part], stats_rx.at[part, j - 1], st_send.at[part, j - 1], st_recv.at[part, j - 1],
                    lax.rem(me + j, n),
                )
                for j in range(1, n)
            ])

    red_copies = {}
    both = CORES * toks
    half = len(ORDER[0]) * both

    def put_scale(part):
        for side in range(CORES):
            got = [stats_rx[part, j - 1] for j in range(1 + (1 - side), n, CORES)]
            mine = stats[part] if side == 0 else jnp.where(core == 0, got[-1], got[0])
            every = got + [mine] if side == 0 else got
            top = functools.reduce(jnp.maximum, [g[:some] for g in every])
            total = functools.reduce(jnp.add, [g[some:] * jnp.exp2((g[:some] - top) * EXP_SCALE) for g in every])
            share = jnp.exp2((mine[:some] - top) * EXP_SCALE)
            scales[part, side, :, :some] = jnp.transpose(share / total)

    def put_split(part, g, sides):
        for b, j in enumerate(ORDER[g]):
            from_rows = pl.ds(pl.multiple_of(peer(j) * both, both), both)
            for side in sides:
                factor = scales[part, side, from_rows, :]
                for i in range(some):
                    cols = pl.ds(((part * CORES + side) * some + i) * V_DIM, V_DIM)
                    o = acc[side, part * some + i, from_rows, :] * factor[:, i:i + 1]
                    o_hi = o.astype(BF16)
                    split[g, pl.ds(b * both, both), cols] = o_hi
                    split[g, pl.ds(half + b * both, both), cols] = (o - o_hi.astype(F32)).astype(BF16)

    def project(part, g, side=None):
        first = part * CORES * deep
        ks = pl.ds(first, CORES * deep) if side is None else pl.ds(first + side * deep, deep)
        y = dot(split[g, :, ks], wo_v[ks, :])
        return y[:half] + y[half:]

    def deliver(g):
        for b, j in enumerate(ORDER[g]):
            for r in range(CORES):
                if j or r:
                    to = lax.rem(core + r, CORES)
                    rows = pl.ds(pl.multiple_of(b * both + to * toks, toks), toks)
                    red_copies[j, r] = send(
                        z.at[g, rows], z_rx.at[j, r], red_send.at[j, r], red_recv.at[j, r], peer(j) * CORES + to
                    )

    def swap(i):
        group = pl.ds(i * (heads // SWAPS), heads // SWAPS)
        return send(acc.at[0, group], acc.at[1, group], acc_send.at[i], acc_recv.at[i], mate)

    phase("attend")
    for pair in late:
        raise_mate(pair)
    send_acc = []
    for head in range(heads):
        cols = pl.ds((head % 2) * V_DIM, V_DIM)
        acc[0, head] = dot(probs[head], values[head // 2, :, cols])
        if (head + 1) % (heads // SWAPS) == 0:
            send_acc.append(swap(head * SWAPS // heads))
    phase("wait_stats0")
    for copy in load_o:
        copy.wait()
    for copy in send_stats[0]:
        copy.wait_recv()
    phase("outproj0")
    put_scale(0)
    for g in range(len(ORDER)):
        put_split(0, g, (0,))
        z[g] = project(0, g, 0)
    phase("wait_acc0")
    for copy in send_acc[:SWAPS // PARTS]:
        copy.wait_recv()
    phase("outproj0m")
    for g in range(len(ORDER)):
        put_split(0, g, (1,))
        z[g] = z[g] + project(0, g, 1)
    phase("wait_stats1")
    for copy in send_stats[1]:
        copy.wait_recv()
    phase("wait_acc1")
    for copy in send_acc[SWAPS // PARTS:]:
        copy.wait_recv()
    phase("outproj1")
    put_scale(1)
    for g in range(len(ORDER)):
        put_split(1, g, range(CORES))
    for g in range(len(ORDER)):
        z[g] = z[g] + project(1, g)
        deliver(g)
    for j in (0, 1, 3, 2):
        phase(f"wait_red{j}")
        for r in range(CORES):
            if j or r:
                red_copies[j, r].wait_recv()
    phase("reduce")
    own = pl.ds(pl.multiple_of(both + core * toks, toks), toks)
    for r in range(CORES):
        y = z[1, own, :] if r == 0 else z_rx[0, 1]
        for j in range(1, chips):
            y = y + z_rx[j, r]
        cols = pl.ds(pl.multiple_of(lax.rem(core + r, CORES) * half_width, LANES), half_width)
        out_ref[:, cols] = y.astype(BF16)

    phase("drain")
    for copy in [send_pre, send_pseg, send_new] + send_meta + send_q + sum(send_stats, []) + send_acc + list(red_copies.values()):
        copy.wait_send()
    phase("")


def solution(mesh):
    n = mesh.shape["sp"]
    chips = n // CORES
    tok_spec = P(("dp", "sp"), None)
    vec_spec = P(("dp", "sp"))
    mat_spec = P(None, None)
    gain_spec = P(None)

    def device_step(hidden, seg_ids, positions, prefix_lat, prefix_seg, w_dq, gain_q, w_uq, w_dkv, gain_kv, w_ukv, w_o):
        toks, width = hidden.shape
        pre, lat_dim = prefix_lat.shape
        q_lat = w_dq.shape[1]
        kv_lat = w_ukv.shape[0]
        heads = w_o.shape[0] // V_DIM // CORES
        rows = CORES * (pre + toks)
        wide = CORES * pre + LANES
        all_toks = n * toks
        inv_freq = (ROPE_BASE ** (-np.arange(HALF, dtype=np.float64) / HALF)).astype(np.float32)
        freq = jnp.asarray(np.concatenate([inv_freq] * (LANES // HALF)).reshape(1, LANES))
        vmem = pl.BlockSpec(memory_space=pltpu.VMEM)
        hbm = pl.BlockSpec(memory_space=pltpu.HBM)
        dma = pltpu.SemaphoreType.DMA
        table = pltpu.VMEM((all_toks, LANES), F32)
        return pl.pallas_call(
            functools.partial(kernel, n),
            out_shape=pltpu.VMEM((toks, width), BF16),
            in_specs=[hbm] * 13,
            scratch_shapes=[
                pltpu.VMEM((1, LANES), F32),
                pltpu.VMEM((1, toks), jnp.int32),
                pltpu.VMEM((1, toks), jnp.int32),
                pltpu.VMEM((1, pre), jnp.int32),
                pltpu.VMEM((q_lat,), BF16),
                pltpu.VMEM((kv_lat,), BF16),
                pltpu.VMEM((toks, width), BF16),
                pltpu.VMEM((width, q_lat), BF16),
                pltpu.VMEM((lat_dim, width), BF16),
                pltpu.VMEM((q_lat, heads * QK_DIM), BF16),
                pltpu.VMEM((kv_lat, heads * KV_HEAD), BF16),
                pltpu.VMEM((CORES * heads * V_DIM, width // CORES), BF16),
                pltpu.VMEM((lat_dim, wide), BF16),
                pltpu.VMEM((rows, kv_lat), BF16),
                pltpu.VMEM((CORES * toks, lat_dim), BF16),
                pltpu.VMEM((1, pre), jnp.int32),
                pltpu.VMEM((all_toks, q_lat), BF16),
                table, table, table, table,
                pltpu.VMEM((2, LANES, wide), BF16),
                pltpu.VMEM((heads, NOPE_DIM, wide), BF16),
                pltpu.VMEM((heads // 2, wide, 2 * V_DIM), BF16),
                pltpu.VMEM((heads, all_toks, 2 * LANES), BF16),
                pltpu.VMEM((heads, all_toks, wide), BF16),
                pltpu.VMEM((heads, all_toks, LANES), F32),
                pltpu.VMEM((heads, all_toks, LANES), F32),
                pltpu.VMEM((SCORE_BUFS, all_toks, wide), F32),
                pltpu.VMEM((PARTS, 2 * heads // PARTS, all_toks), F32),
                pltpu.VMEM((PARTS, n - 1, 2 * heads // PARTS, all_toks), F32),
                pltpu.VMEM((CORES, heads, all_toks, V_DIM), F32),
                pltpu.VMEM((PARTS, CORES, all_toks, LANES), F32),
                pltpu.VMEM((2, all_toks, CORES * heads * V_DIM), BF16),
                table,
                pltpu.VMEM((2, all_toks // 2, width // CORES), F32),
                pltpu.VMEM((chips, CORES, toks, width // CORES), F32),
                dma((6,)),
                dma((6,)),
                dma((DQ_LOADS,)),
                dma((PARTS, CORES)),
                dma((KV_LOADS,)),
                dma((3,)), dma((3,)),
                dma((n - 1,)), dma((n - 1,)),
                dma((n - 1,)), dma((n - 1,)),
                dma((PARTS, n - 1)), dma((PARTS, n - 1)),
                dma((SWAPS,)), dma((SWAPS,)),
                dma((chips, CORES)), dma((chips, CORES)),
            ],
            compiler_params=pltpu.CompilerParams(
                collective_id=0, has_side_effects=True, vmem_limit_bytes=60 * 1024 * 1024
            ),
        )(
            freq, seg_ids.reshape(1, toks), positions.reshape(1, toks), prefix_seg.reshape(1, pre),
            gain_q, gain_kv,
            hidden, prefix_lat.T, w_dq, w_uq, w_dkv.T, w_ukv, w_o,
        )

    return jax.shard_map(
        device_step,
        mesh=mesh,
        in_specs=(tok_spec, vec_spec, vec_spec, tok_spec, vec_spec, mat_spec, gain_spec, mat_spec, mat_spec, gain_spec, mat_spec, mat_spec),
        out_specs=tok_spec,
        check_vma=False,
    )
```
